32 devices in a mesh: pod: 2 (over x), data: 4 (over z), tensor: 4 (over y, core).
Axes of the slice: x: 2, y: 2, z: 4, core: 2. Of those that a mesh axis runs over, the one named last changes fastest.
Arguments:
- token_ids: int32 [4096], P(('pod', 'data')), parts along dimension 0
- embed_table: bfloat16 [32000, 2048], P('tensor')
- norm_gain: bfloat16 [2048], replicated
- w_in: bfloat16 [2048, 5632], P(None, 'tensor')
- w_out: bfloat16 [5632, 2048], P('tensor')
- d_out: bfloat16 [4096, 2048], P(('pod', 'data', 'tensor')), parts along dimension 0
Outputs:
- output 1: bfloat16 [4096, 2048], P(('pod', 'data', 'tensor')), parts along dimension 0
- output 2: float32 [64000, 2048], P(('pod', 'tensor')), parts along dimension 0
- output 3: float32 [4096, 5632], P('pod', 'tensor'), parts along dimension 0
- output 4: float32 [11264, 2048], P(('pod', 'tensor')), parts along dimension 0
There are 2 independent parts. The reference program is written for one: setup_inputs(seed, part) draws one part's arguments, and reference() takes and returns one part's arrays. A program takes and returns all parts, laid end to end along the dimension named above; an argument that names none is the same for every part.
All inputs are finite; a program needn't handle non-finite values.
Results may differ from the reference program's by a relative error of at most 0.00496674.
Values are sent between devices in bfloat16 or wider.
A program may use at most 1 GiB of HBM per device.

```python
import jax
import jax.numpy as jnp
from jax import lax

DATA_WAYS = 4
TENSOR_WAYS = 4
TOK_DEV = 128
VOCAB_SIZE = 32000
MODEL_DIM = 2048
FFN_DIM = 5632
NORM_EPS = 1e-6
TOKENS_REP = TOK_DEV * TENSOR_WAYS


def gelu_tanh(value):
    return jax.nn.gelu(value, approximate=True)


def draw_ids(id_key):
    k_base, k_shift, k_hot, k_pick, k_use = jax.random.split(id_key, 5)
    total_tok = DATA_WAYS * TOKENS_REP
    base_ids = jax.random.randint(k_base, (total_tok,), 0, VOCAB_SIZE)
    shift_by = jax.random.randint(k_shift, (total_tok,), 0, 3)
    skewed = jnp.right_shift(base_ids, shift_by)
    hot_ids = jax.random.randint(k_hot, (16,), 0, VOCAB_SIZE)
    hot_pick = jax.random.randint(k_pick, (total_tok,), 0, 16)
    use_hot = jax.random.randint(k_use, (total_tok,), 0, 4) == 0
    token_ids = jnp.where(use_hot, hot_ids[hot_pick], skewed)
    token_ids = token_ids.at[0].set(0).at[total_tok - 1].set(VOCAB_SIZE - 1)
    return token_ids.astype(jnp.int32)


def setup_inputs(seed: int = 0, part: int = 0) -> dict:
    root_key = jax.random.key(seed)
    k_table, k_gain, k_in, k_out, k_part = jax.random.split(root_key, 5)
    k_ids, k_grad = jax.random.split(jax.random.fold_in(k_part, part))
    total_tok = DATA_WAYS * TOKENS_REP
    embed_table = jax.random.normal(k_table, (VOCAB_SIZE, MODEL_DIM), jnp.float32).astype(jnp.bfloat16)
    norm_gain = (1.0 + 0.5 * jax.random.uniform(k_gain, (MODEL_DIM,), jnp.float32, -1.0, 1.0)).astype(jnp.bfloat16)
    w_in = (jax.random.normal(k_in, (MODEL_DIM, FFN_DIM), jnp.float32) * MODEL_DIM ** -0.5).astype(jnp.bfloat16)
    w_out = (jax.random.normal(k_out, (FFN_DIM, MODEL_DIM), jnp.float32) * (1.5 * FFN_DIM ** -0.5)).astype(jnp.bfloat16)
    d_out = jax.random.normal(k_grad, (total_tok, MODEL_DIM), jnp.float32).astype(jnp.bfloat16)
    return {"token_ids": draw_ids(k_ids), "embed_table": embed_table, "norm_gain": norm_gain, "w_in": w_in, "w_out": w_out, "d_out": d_out}


def reference(token_ids, embed_table, norm_gain, w_in, w_out, d_out):
    blocks = DATA_WAYS * TENSOR_WAYS
    embedded = jnp.take(embed_table, token_ids, axis=0).reshape(blocks, TOK_DEV, MODEL_DIM)
    grad_blocks = d_out.reshape(blocks, TOK_DEV, MODEL_DIM)
    gain_f32 = norm_gain.astype(jnp.float32)

    def block_step(acc_pair, step_in):
        acc_w_in, acc_w_out = acc_pair
        x_blk, dy_blk = step_in
        x_f32 = x_blk.astype(jnp.float32)
        inv_rms = lax.rsqrt(jnp.mean(x_f32 * x_f32, axis=-1, keepdims=True) + NORM_EPS)
        x_hat = x_f32 * inv_rms
        normed = (x_hat * gain_f32).astype(jnp.bfloat16)
        pre_gelu = jnp.dot(normed, w_in, preferred_element_type=jnp.float32).astype(jnp.bfloat16)
        hidden_f32, gelu_pull = jax.vjp(gelu_tanh, pre_gelu.astype(jnp.float32))
        hidden = hidden_f32.astype(jnp.bfloat16)
        mlp_out = jnp.dot(hidden, w_out, preferred_element_type=jnp.float32)
        out_blk = (x_f32 + mlp_out).astype(jnp.bfloat16)
        grad_hidden = jnp.dot(dy_blk, w_out.T, preferred_element_type=jnp.float32)
        grad_pre = gelu_pull(grad_hidden)[0].astype(jnp.bfloat16)
        acc_w_out = acc_w_out + jnp.dot(hidden.T, dy_blk, preferred_element_type=jnp.float32)
        acc_w_in = acc_w_in + jnp.dot(normed.T, grad_pre, preferred_element_type=jnp.float32)
        d_normed = jnp.dot(grad_pre, w_in.T, preferred_element_type=jnp.float32)
        d_hat = d_normed * gain_f32
        d_norm_in = inv_rms * (d_hat - x_hat * jnp.mean(d_hat * x_hat, axis=-1, keepdims=True))
        dx_blk = (dy_blk.astype(jnp.float32) + d_norm_in).astype(jnp.bfloat16)
        return (acc_w_in, acc_w_out), (out_blk, dx_blk)

    zeros_in = jnp.zeros((MODEL_DIM, FFN_DIM), jnp.float32)
    zeros_out = jnp.zeros((FFN_DIM, MODEL_DIM), jnp.float32)
    (grad_w_in, grad_w_out), (out_blocks, dx_blocks) = lax.scan(block_step, (zeros_in, zeros_out), (embedded, grad_blocks))
    grad_table = jax.ops.segment_sum(dx_blocks.reshape(-1, MODEL_DIM).astype(jnp.float32), token_ids, num_segments=VOCAB_SIZE)
    return out_blocks.reshape(-1, MODEL_DIM), grad_table, grad_w_in, grad_w_out
```

```python
import functools

import jax
import jax.numpy as jnp
from jax import lax
from jax.experimental import pallas as pl
from jax.experimental.pallas import tpu as pltpu
from jax.sharding import PartitionSpec as P

NORM_EPS = 1e-6
GELU_A = 0.7978845608028654
GELU_B = 0.044715
MESH = pl.DeviceIdType.MESH
NT = (((1,), (1,)), ((), ()))
TN = (((0,), (0,)), ((), ()))
F32, BF16 = jnp.float32, jnp.bfloat16
HOPS = (1, -1, 2, -2)

R_IDS, R_DZ, R_DY, R_DC, R_NZ, R_NC, R_XZ, R_XY, R_XC = (4 * i for i in range(9))
R_XM, R_X, R_PC, R_PY, N_R = 36, 37, 39, 41, 43
S_IDS, S_DZ, S_DY, S_DC, S_NZ, S_NC, S_XZ, S_XY, S_XC = 0, 3, 8, 12, 16, 21, 25, 30, 34
S_XM, S_X, S_PC, S_PY, N_S = 38, 39, 41, 43, 45
L_W1, L_W2, L_XM, L_DO, L_N, L_D, L_H, L_DU, L_DX, N_L = 0, 1, 2, 3, 4, 8, 12, 13, 14, 15


def tiles(total, step, body):
    full = total // step

    def one(j, carry):
        body(pl.multiple_of(j * step, step), step)
        return carry

    lax.fori_loop(0, full, one, 0)
    if total % step:
        body(full * step, total % step)


def rows_loop(total, body):
    def one(j, carry):
        body(pl.multiple_of(j * 16, 16))
        return carry

    lax.fori_loop(0, total // 16, one, 0)


def group_kernel(ids_ref, xm_hbm, w1_hbm, w2_hbm, g_ref, do_hbm,
                 out_ref, ids_o, n_o, d_o, h_o, du_o, dx_o,
                 w1, w2, n, d, xm, xr, xc, xy, dh, hs, dus, pd, pf, rd, rf, sd, sf, yd, yf, dxo, idl,
                 lsem, ssem, rsem):
    t, m = do_hbm.shape
    f = w1_hbm.shape[1]
    z = lax.axis_index("data")
    r = lax.axis_index("tensor")
    y, c = lax.div(r, 2), lax.rem(r, 2)
    partner = {"tensor": 2 * y + 1 - c}
    across = {"tensor": 2 * (1 - y) + c}
    half = lax.div(z, 2)
    inner = z + half * (3 - 2 * z)
    order = [b + half * (3 - 2 * b) for b in (1 - inner, 2, 3)]
    middle = inner == 1
    beyond = {"data": z + 2 * half - 1}

    def row(zz, cc, yy=0):
        return pl.multiple_of(zz * (4 * t) + cc * (2 * t) + yy * t, t)

    def blk(ref, zz, cc, yy):
        return ref.at[pl.ds(row(zz, cc, yy), t)]

    def duo(ref, zz, cc):
        return ref.at[pl.ds(row(zz, cc), 2 * t)]

    def remote(src, dst, s, q, dev):
        return pltpu.make_async_remote_copy(
            src_ref=src, dst_ref=dst, send_sem=ssem.at[s], recv_sem=rsem.at[q], device_id=dev, device_id_type=MESH
        )

    def local(src, dst, i):
        return pltpu.make_async_copy(src, dst, lsem.at[i])

    def arrived(ref, q):
        remote(ref, ref, 0, q, partner).wait_recv()

    def along(src, dst, s, q, act):
        for i, hop in enumerate(HOPS):
            to = z + hop

            @pl.when((to >= 0) & (to <= 3))
            def _():
                act(remote(src, dst, s + i, q + z, {"data": to}))

    def forward(src, s, q, act):
        @pl.when(middle)
        def _():
            act(remote(src, src, s + 4, q + order[2], beyond))

    def start(cp):
        cp.start()

    def sent(cp):
        cp.wait_send()

    barrier = pltpu.get_barrier_semaphore()
    pl.semaphore_signal(barrier, inc=1, device_id=partner, device_id_type=MESH)
    pl.semaphore_signal(barrier, inc=1, device_id=across, device_id_type=MESH)
    for k in range(3):
        pl.semaphore_signal(barrier, inc=1, device_id={"data": order[k]}, device_id_type=MESH)

    own_d = blk(d, z, c, y)
    local(do_hbm, own_d, L_DO).start()
    local(xm_hbm, xm, L_XM).start()
    local(w2_hbm, w2, L_W2).start()
    local(w1_hbm, w1, L_W1).start()
    pl.semaphore_wait(barrier, 5)

    local(do_hbm, own_d, L_DO).wait()
    remote(own_d, own_d, S_DY + z, R_DY + z, across).start()
    along(own_d, own_d, S_DZ, R_DZ, start)
    local(xm_hbm, xm, L_XM).wait()
    xm_out = remote(xm.at[pl.ds(row(0, 1 - c), 2 * t)], xr, S_XM, R_XM, partner)
    xm_out.start()
    for k in range(3):
        remote(ids_ref, idl.at[z], S_IDS + k, R_IDS + z, {"data": order[k]}).start()
    idl[z] = ids_ref[...]

    arrived(xr, R_XM)
    for b in range(2):
        def join(i, b=b):
            at = pl.ds(b * t + i, 16)
            xc[at, :] = xm[pl.ds(row(0, c, b) + i, 16), :] + xr[at, :]

        rows_loop(t, join)
        half_x = pl.ds(b * t, t)
        remote(xc.at[half_x], xy.at[half_x], S_X + b, R_X + b, across).start()

    def d_pair(zz, act):
        act(remote(duo(d, zz, c), duo(d, zz, c), S_DC + zz, R_DC + zz, partner))

    arrived(blk(d, z, c, 1 - y), R_DY + z)
    d_pair(z, start)
    arrived(duo(d, z, 1 - c), R_DC + z)
    local(w2_hbm, w2, L_W2).wait()

    def grad_hidden(zz):
        at = pl.ds(row(zz, 0), 4 * t)

        def body(off, w):
            dh[:, pl.ds(off, w)] = lax.dot_general(d[at, :], w2[pl.ds(off, w), :], NT, preferred_element_type=F32)

        tiles(f, 256, body)

    def hidden(zz):
        at = pl.ds(row(zz, 0), 4 * t)

        def body(off, w):
            to = pl.ds(off, w)
            u = jnp.dot(n[at, :], w1[:, to], preferred_element_type=F32).astype(BF16).astype(F32)
            uu = u * u
            th = jnp.tanh(GELU_A * (u + GELU_B * (uu * u)))
            cdf = 0.5 * (1.0 + th)
            hs[:, to] = (u * cdf).astype(BF16)
            slope = cdf + (0.5 * GELU_A) * u * (1.0 - th * th) * (1.0 + (3.0 * GELU_B) * uu)
            dus[:, to] = (dh[:, to] * slope).astype(BF16)

        tiles(f, 256, body)

    def keep(zz, act):
        at = pl.ds(row(zz, 0), 4 * t)
        act(local(hs, h_o.at[at], L_H))
        act(local(dus, du_o.at[at], L_DU))

    def keep_inputs(zz, act):
        at = pl.ds(row(zz, 0), 4 * t)
        act(local(n.at[at], n_o.at[at], L_N + zz))
        act(local(d.at[at], d_o.at[at], L_D + zz))

    def local_wait(cp):
        cp.wait()

    grad_hidden(z)

    def d_across(zz, act):
        act(remote(blk(d, zz, c, y), blk(d, zz, c, y), S_DY + zz, R_DY + zz, across))

    arrived(blk(d, order[0], c, y), R_DZ + order[0])
    d_across(order[0], start)

    gain = g_ref[...].astype(F32)
    for b in range(2):
        arrived(xy.at[pl.ds(b * t, t)], R_X + b)
        local_sent = remote(xc.at[pl.ds(b * t, t)], xy.at[pl.ds(b * t, t)], S_X + b, R_X + b, across)
        local_sent.wait_send()

        def norm(i, b=b):
            at = pl.ds(b * t + i, 16)
            x16 = xc[at, :] + xy[at, :]
            xc[at, :] = x16
            x = x16.astype(F32)
            s = lax.rsqrt(jnp.mean(x * x, axis=-1, keepdims=True) + NORM_EPS)
            n[pl.ds(row(z, c, b) + i, 16), :] = ((x * s) * gain).astype(BF16)

        rows_loop(t, norm)

    def n_pair(zz, act):
        act(remote(duo(n, zz, c), duo(n, zz, c), S_NC + zz, R_NC + zz, partner))

    n_pair(z, start)
    along(duo(n, z, c), duo(n, z, c), S_NZ, R_NZ, start)
    arrived(duo(n, z, 1 - c), R_NC + z)
    local(w1_hbm, w1, L_W1).wait()
    hidden(z)
    keep(z, start)
    keep_inputs(z, start)

    def part_dn(off, w):
        pd[:, pl.ds(off, w)] = lax.dot_general(dus[...], w1[pl.ds(off, w), :], NT, preferred_element_type=F32)

    def part_y(off, w):
        pf[:, pl.ds(off, w)] = jnp.dot(hs[...], w2[:, pl.ds(off, w)], preferred_element_type=F32)

    def part_pair(src, dst, i):
        return remote(src.at[pl.ds(row(0, 1 - c), 2 * t)], dst, S_PC + i, R_PC + i, partner)

    def part_across(src, dst, i):
        return remote(src, dst, S_PY + i, R_PY + i, across)

    def gather_part(part, got, total):
        def add(i):
            total[pl.ds(i, 16), :] = part[pl.ds(row(0, c, 1 - y) + i, 16), :] + got[pl.ds((1 - y) * t + i, 16), :]

        rows_loop(t, add)

    tiles(m, 256, part_dn)
    part_pair(pd, rd, 0).start()
    arrived(blk(d, order[2], c, y), R_DZ + order[2])
    forward(blk(d, order[2], c, y), S_DZ, R_DZ, start)
    arrived(rd, R_PC)
    gather_part(pd, rd, sd)
    part_across(sd, yd, 0).start()
    tiles(m, 256, part_y)
    part_pair(pf, rf, 1).start()
    arrived(blk(d, order[1], c, y), R_DZ + order[1])
    d_across(order[1], start)
    d_across(order[2], start)
    arrived(rf, R_PC + 1)
    gather_part(pf, rf, sf)
    part_across(sf, yf, 1).start()

    arrived(yd, R_PY)

    def grad_x(i):
        at, own = pl.ds(i, 16), pl.ds(y * t + i, 16)
        dn = pd[pl.ds(row(0, c, y) + i, 16), :] + rd[own, :] + yd[at, :]
        x = xc[own, :].astype(F32)
        s = lax.rsqrt(jnp.mean(x * x, axis=-1, keepdims=True) + NORM_EPS)
        xh = x * s
        dhat = dn * gain
        dxn = s * (dhat - xh * jnp.mean(dhat * xh, axis=-1, keepdims=True))
        dxo[at, :] = (d[pl.ds(row(z, c, y) + i, 16), :].astype(F32) + dxn).astype(BF16)

    rows_loop(t, grad_x)

    def dx_across(zz, src, act):
        act(remote(src, blk(dx_o, zz, c, y), S_XY + zz, R_XY + zz, across))

    def dx_pair(zz, act):
        act(remote(duo(dx_o, zz, c), duo(dx_o, zz, c), S_XC + zz, R_XC + zz, partner))

    dx_across(z, dxo, start)
    along(dxo, blk(dx_o, z, c, y), S_XZ, R_XZ, start)
    local(dxo, blk(dx_o, z, c, y), L_DX).start()

    def unit(k):
        zz = order[k]
        arrived(duo(n, zz, c), R_NZ + zz)
        if k == 2:
            forward(duo(n, zz, c), S_NZ, R_NZ, start)
        n_pair(zz, start)
        arrived(blk(d, zz, c, 1 - y), R_DY + zz)
        d_pair(zz, start)
        arrived(duo(d, zz, 1 - c), R_DC + zz)
        keep(z if k == 0 else order[k - 1], local_wait)
        grad_hidden(zz)
        arrived(duo(n, zz, 1 - c), R_NC + zz)
        hidden(zz)
        keep(zz, start)
        keep_inputs(zz, start)

    def dx_got(k):
        zz = order[k]
        arrived(blk(dx_o, zz, c, y), R_XZ + zz)
        if k == 2:
            forward(blk(dx_o, zz, c, y), S_XZ, R_XZ, start)
        dx_across(zz, blk(dx_o, zz, c, y), start)

    unit(0)
    unit(1)
    dx_got(0)
    unit(2)
    dx_got(1)
    dx_got(2)
    arrived(yf, R_PY + 1)

    def block_out(i):
        own = pl.ds(y * t + i, 16)
        total = pf[pl.ds(row(0, c, y) + i, 16), :] + rf[own, :] + yf[pl.ds(i, 16), :]
        out_ref[pl.ds(i, 16), :] = (xc[own, :].astype(F32) + total).astype(BF16)

    rows_loop(t, block_out)
    local(dxo, blk(dx_o, z, c, y), L_DX).wait()
    for zz in (z, *order):
        arrived(blk(dx_o, zz, c, 1 - y), R_XY + zz)
        dx_pair(zz, start)
    for k in range(3):
        arrived(idl.at[order[k]], R_IDS + order[k])
    ids_o[...] = idl[...]

    keep(order[2], local_wait)
    for zz in (z, *order):
        keep_inputs(zz, local_wait)
        arrived(duo(dx_o, zz, 1 - c), R_XC + zz)
        d_across(zz, sent)
        d_pair(zz, sent)
        n_pair(zz, sent)
        dx_pair(zz, sent)
    dx_across(z, dxo, sent)
    for k in range(3):
        dx_across(order[k], blk(dx_o, order[k], c, y), sent)
        remote(ids_ref, idl.at[z], S_IDS + k, R_IDS + z, {"data": order[k]}).wait_send()
    along(own_d, own_d, S_DZ, R_DZ, sent)
    along(duo(n, z, c), duo(n, z, c), S_NZ, R_NZ, sent)
    along(dxo, blk(dx_o, z, c, y), S_XZ, R_XZ, sent)
    forward(blk(d, order[2], c, y), S_DZ, R_DZ, sent)
    forward(duo(n, order[2], c), S_NZ, R_NZ, sent)
    forward(blk(dx_o, order[2], c, y), S_XZ, R_XZ, sent)
    xm_out.wait_send()
    part_pair(pd, rd, 0).wait_send()
    part_pair(pf, rf, 1).wait_send()
    part_across(sd, yd, 0).wait_send()
    part_across(sf, yf, 1).wait_send()


def run_group(ids, xm, w1, w2, gain, d_out):
    t, m = d_out.shape
    f = w1.shape[1]
    any_, vmem = pl.BlockSpec(memory_space=pl.ANY), pl.BlockSpec(memory_space=pltpu.VMEM)
    V = pltpu.VMEM
    sds = jax.ShapeDtypeStruct
    dots = 2 * 4 * t * m * f
    return pl.pallas_call(
        group_kernel,
        out_shape=(
            sds((t, m), BF16), sds((4, *ids.shape), jnp.int32), sds((16 * t, m), BF16), sds((16 * t, m), BF16),
            sds((16 * t, f), BF16), sds((16 * t, f), BF16), sds((16 * t, m), BF16),
        ),
        in_specs=[vmem, any_, any_, any_, vmem, any_],
        out_specs=(vmem, vmem, any_, any_, any_, any_, any_),
        scratch_shapes=[
            V((m, f), BF16), V((f, m), BF16), V((16 * t, m), BF16), V((16 * t, m), BF16),
            V((4 * t, m), BF16), V((2 * t, m), BF16), V((2 * t, m), BF16), V((2 * t, m), BF16),
            V((4 * t, f), F32), V((4 * t, f), BF16), V((4 * t, f), BF16),
            V((4 * t, m), F32), V((4 * t, m), F32), V((2 * t, m), F32), V((2 * t, m), F32),
            V((t, m), F32), V((t, m), F32), V((t, m), F32), V((t, m), F32),
            V((t, m), BF16), V((4, *ids.shape), jnp.int32),
            pltpu.SemaphoreType.DMA((N_L,)), pltpu.SemaphoreType.DMA((N_S,)), pltpu.SemaphoreType.DMA((N_R,)),
        ],
        compiler_params=pltpu.CompilerParams(collective_id=0, has_side_effects=True, vmem_limit_bytes=67043328),
        cost_estimate=pl.CostEstimate(flops=10 * dots, bytes_accessed=64 * 16 * t * m, transcendentals=16 * t * f),
        name="group_step",
    )(ids, xm, w1, w2, gain, d_out)


def table_kernel(key_ref, first_ref, dx_hbm, out_ref, dxb, dxf, sem):
    step = pl.program_id(0)
    tall = out_ref.shape[0]
    count = dxb.shape[0]

    @pl.when(step == 0)
    def _():
        cp = pltpu.make_async_copy(dx_hbm, dxb, sem)
        cp.start()
        cp.wait()

        def widen(i):
            dxf[pl.ds(i, 16), :] = dxb[pl.ds(i, 16), :].astype(F32)

        rows_loop(count, widen)

    out_ref[...] = jnp.zeros_like(out_ref)

    def add(j, carry):
        key = key_ref[j]
        to = pl.ds(lax.div(key, count) - step * tall, 1)
        out_ref[to, :] += dxf[pl.ds(lax.rem(key, count), 1), :]
        return carry

    lax.fori_loop(first_ref[step], first_ref[step + 1], add, 0)


def table_grad(ids_all, dx_all, shard_rows, tall):
    count, m = dx_all.shape
    rank0 = lax.axis_index("tensor") * shard_rows
    local_ids = ids_all.reshape(count) - rank0
    owned = (local_ids >= 0) & (local_ids < shard_rows)
    rows = jnp.where(owned, local_ids, shard_rows)
    keys = rows * count + lax.iota(jnp.int32, count)
    place = jnp.sum((keys[None, :] < keys[:, None]).astype(jnp.int32), axis=1)
    ordered = jnp.sum(jnp.where(place[:, None] == lax.iota(jnp.int32, count)[None, :], keys[:, None], 0), axis=0)
    steps = shard_rows // tall
    first = jnp.sum((rows[None, :] < (lax.iota(jnp.int32, steps + 1) * tall)[:, None]).astype(jnp.int32), axis=1)
    return pl.pallas_call(
        table_kernel,
        out_shape=jax.ShapeDtypeStruct((shard_rows, m), F32),
        grid_spec=pltpu.PrefetchScalarGridSpec(
            num_scalar_prefetch=2,
            grid=(steps,),
            in_specs=[pl.BlockSpec(memory_space=pl.ANY)],
            out_specs=pl.BlockSpec((tall, m), lambda i, *_: (i, 0)),
            scratch_shapes=[
                pltpu.VMEM((count, m), BF16), pltpu.VMEM((count, m), F32), pltpu.SemaphoreType.DMA,
            ],
        ),
        compiler_params=pltpu.CompilerParams(dimension_semantics=("arbitrary",), vmem_limit_bytes=50 << 20),
        cost_estimate=pl.CostEstimate(flops=count * m, bytes_accessed=4 * shard_rows * m, transcendentals=0),
        name="table_grad",
    )(ordered, first, dx_all)


def solution(mesh):
    tok_spec = P(("pod", "data", "tensor"), None)

    def per_device(token_ids, embed_table, norm_gain, w_in, w_out, d_out):
        shard_rows = embed_table.shape[0]
        t = d_out.shape[0]
        ids = token_ids.reshape(2, 2, t).transpose(1, 0, 2).reshape(4 * t)
        local_ids = ids - lax.axis_index("tensor") * shard_rows
        owned = (local_ids >= 0) & (local_ids < shard_rows)
        picked = jnp.take(embed_table, jnp.where(owned, local_ids, 0), axis=0)
        masked = jnp.where(owned[:, None], picked, jnp.zeros_like(picked))
        out, ids_all, n_all, d_all, h_all, du_all, dx_all = run_group(
            ids.reshape(-1, 128), masked, w_in, w_out, norm_gain.reshape(1, -1), d_out
        )
        grad_w_in = lax.dot_general(n_all, du_all, TN, preferred_element_type=F32)
        grad_w_out = lax.dot_general(h_all, d_all, TN, preferred_element_type=F32)
        tall = next(k for k in (320, 64, 8) if shard_rows % k == 0)
        grad_table = table_grad(ids_all, dx_all, shard_rows, tall)
        return out, grad_table, grad_w_in, grad_w_out

    return jax.shard_map(
        per_device,
        mesh=mesh,
        in_specs=(P(("pod", "data")), P("tensor", None), P(None), P(None, "tensor"), P("tensor", None), tok_spec),
        out_specs=(tok_spec, P(("pod", "tensor"), None), P("pod", "tensor"), P(("pod", "tensor"), None)),
        check_vma=False,
    )
```

```python
import functools

import jax
import jax.numpy as jnp
from jax import lax
from jax.experimental import pallas as pl
from jax.experimental.pallas import tpu as pltpu
from jax.sharding import PartitionSpec as P

NORM_EPS = 1e-6
GELU_A = 0.7978845608028654
GELU_B = 0.044715
MESH = pl.DeviceIdType.MESH
NT = (((1,), (1,)), ((), ()))
TN = (((0,), (0,)), ((), ()))
F32, BF16, I32 = jnp.float32, jnp.bfloat16, jnp.int32
LANES = 128
XQ = 4
PQ = 4

R_IDS, R_DZ, R_DY, R_DC, R_NZ, R_NC, R_XZ, R_XY, R_XC = 0, 4, 8, 12, 16, 24, 28, 32, 36
R_XM, R_X, R_NO, R_PC, R_PY, N_R = 40, 44, 48, 52, 60, 68
S_IDS, S_DZ, S_DY, S_DC, S_NZ, S_NC, S_XZ, S_XY, S_XC = 0, 3, 8, 12, 16, 26, 30, 35, 39
S_XM, S_X, S_NO, S_PC, S_PY, N_S = 43, 47, 51, 55, 63, 71
L_W1, L_W2, L_XM, L_DO, L_DX, L_DW, N_L = 0, 1, 5, 6, 7, 8, 10


def loop(lo, hi, body):
    def one(j, carry):
        body(j)
        return carry

    lax.fori_loop(lo, hi, one, 0)


def tiles(total, step, body):
    full = total // step
    loop(0, full, lambda j: body(pl.multiple_of(j * step, step), step))
    if total % step:
        body(full * step, total % step)


def rows_loop(total, body):
    loop(0, total // 16, lambda j: body(pl.multiple_of(j * 16, 16)))


def sort_keys(ids, keys, place, ordered, first, shard_rows, tall, rank0):
    reps, per, _ = ids.shape
    count = reps * per * LANES
    t = per * LANES // 4
    shift = t.bit_length() - 1
    lines = reps * per
    lane = lax.broadcasted_iota(I32, (per, LANES), 1)
    spot = lax.broadcasted_iota(I32, (per, LANES), 0) * LANES + lane
    block = jnp.right_shift(spot, shift)
    kept = (block & 1) * (2 * t) + jnp.right_shift(block, 1) * t + (spot & (t - 1))
    for k in range(reps):
        row = ids[k] - rank0
        row = jnp.where((row >= 0) & (row < shard_rows), row, shard_rows)
        keys[k * per : (k + 1) * per, :] = (row * count + (k * per * LANES + kept)).astype(F32)
    place[...] = jnp.zeros_like(place)
    ordered[...] = jnp.zeros_like(ordered)
    up = lax.broadcasted_iota(I32, (LANES, LANES), 0)
    over = lax.broadcasted_iota(I32, (LANES, LANES), 1)
    same = up == over
    overf = over.astype(F32)

    def column(ref, b):
        return jnp.sum(jnp.where(same, jnp.broadcast_to(ref[pl.ds(b, 1), :], (LANES, LANES)), 0.0), axis=1, keepdims=True)

    def count_below(b):
        col = column(keys, b)

        def one(a):
            at = pl.ds(a, 1)
            place[at, :] += jnp.sum(jnp.where(col < keys[at, :], 1.0, 0.0), axis=0, keepdims=True)

        loop(0, lines, one)

    loop(0, lines, count_below)

    def put(b):
        col, spot_of = column(keys, b), column(place, b)

        def one(a):
            want = overf + (a * LANES).astype(F32)
            ordered[pl.ds(a, 1), :] += jnp.sum(jnp.where(spot_of == want, col, 0.0), axis=0, keepdims=True)

        loop(0, lines, one)
        edge = overf * float(tall * count)
        first[...] += jnp.sum(jnp.where(col < edge, 1.0, 0.0), axis=0, keepdims=True)

    first[...] = jnp.zeros_like(first)
    loop(0, lines, put)


def group_kernel(shard_rows, tall, ids_ref, xm_hbm, w1_hbm, w2_hbm, g_ref, do_hbm,
                 out_ref, ord_o, first_o, dx_o, dw1_o, dw2_o,
                 w1, w2, n, d, xm, xc, xy, hs, dus, pd, pf, rd, rf, yd, yf, dxo, idl, keys, place, ordered, first,
                 lsem, ssem, rsem):
    t, m = do_hbm.shape
    f = w1_hbm.shape[1]
    tq, mq = 2 * t // XQ, m // PQ
    z = lax.axis_index("data")
    r = lax.axis_index("tensor")
    y, c = lax.div(r, 2), lax.rem(r, 2)
    partner = {"tensor": 2 * y + 1 - c}
    across = {"tensor": 2 * (1 - y) + c}
    half = lax.div(z, 2)
    inner = z + half * (3 - 2 * z)
    order = [b + half * (3 - 2 * b) for b in (1 - inner, 2, 3)]
    middle, end = inner == 1, inner == 0

    def row(zz, cc, yy=0):
        return pl.multiple_of(zz * (4 * t) + cc * (2 * t) + yy * t, t)

    def blk(ref, zz, cc, yy):
        return ref.at[pl.ds(row(zz, cc, yy), t)]

    def duo(ref, zz, cc):
        return ref.at[pl.ds(row(zz, cc), 2 * t)]

    def remote(src, dst, s, q, dev):
        return pltpu.make_async_remote_copy(
            src_ref=src, dst_ref=dst, send_sem=ssem.at[s], recv_sem=rsem.at[q], device_id=dev, device_id_type=MESH
        )

    def local(src, dst, i):
        return pltpu.make_async_copy(src, dst, lsem.at[i])

    def arrived(ref, q):
        remote(ref, ref, 0, q, partner).wait_recv()

    def start(cp):
        cp.start()

    def sent(cp):
        cp.wait_send()

    def along(src, dst, s, q, act):
        for i, hop in enumerate((1, -1)):
            to = z + hop

            @pl.when((to >= 0) & (to <= 3))
            def _():
                act(remote(src, dst, s + i, q + z, {"data": to}))

    def pass_on(k, ref, s, q, act):
        act(remote(ref, ref, s + 2 + k, q + order[k], {"data": order[1] if k == 0 else order[0]}))

    barrier = pltpu.get_barrier_semaphore()
    pl.semaphore_signal(barrier, inc=1, device_id=partner, device_id_type=MESH)
    pl.semaphore_signal(barrier, inc=1, device_id=across, device_id_type=MESH)
    for k in range(3):
        pl.semaphore_signal(barrier, inc=1, device_id={"data": order[k]}, device_id_type=MESH)

    own_d = blk(d, z, c, y)
    local(do_hbm, own_d, L_DO).start()
    local(xm_hbm, xm, L_XM).start()
    local(w2_hbm, w2, L_W2).start()
    local(w1_hbm, w1, L_W1).start()
    pl.semaphore_wait(barrier, 5)

    def piece(q):
        return pl.ds(q * tq, tq)

    local(do_hbm, own_d, L_DO).wait()
    remote(own_d, own_d, S_DY + z, R_DY + z, across).start()
    along(own_d, own_d, S_DZ, R_DZ, start)
    local(xm_hbm, xm, L_XM).wait()

    def xm_part(q):
        return remote(xm.at[pl.ds(row(0, 1 - c) + q * tq, tq)], xc.at[piece(q)], S_XM + q, R_XM + q, partner)

    def x_part(q):
        return remote(xc.at[piece(q)], xy.at[piece(q)], S_X + q, R_X + q, across)

    for q in range(XQ):
        xm_part(q).start()
    for k in range(3):
        remote(ids_ref, idl.at[z], S_IDS + k, R_IDS + z, {"data": order[k]}).start()
    idl[z] = ids_ref[...]
    for q in range(XQ):
        arrived(xc.at[piece(q)], R_XM + q)

        def join(i, q=q):
            at = pl.ds(q * tq + i, 16)
            xc[at, :] += xm[pl.ds(row(0, c) + q * tq + i, 16), :]

        rows_loop(tq, join)
        x_part(q).start()

    def d_got(k):
        arrived(blk(d, order[k], c, y), R_DZ + order[k])

    def d_on(k):
        pass_on(k, blk(d, order[k], c, y), S_DZ, R_DZ, start)

    def d_across(zz, act):
        act(remote(blk(d, zz, c, y), blk(d, zz, c, y), S_DY + zz, R_DY + zz, across))

    def d_pair(zz, act):
        act(remote(duo(d, zz, c), duo(d, zz, c), S_DC + zz, R_DC + zz, partner))

    d_got(0)

    @pl.when(middle)
    def _():
        d_on(0)
        d_got(1)
        d_on(1)

    arrived(blk(d, z, c, 1 - y), R_DY + z)
    d_pair(z, start)
    arrived(duo(d, z, 1 - c), R_DC + z)
    local(w2_hbm, w2, L_W2).wait()

    def grad_hidden(zz, dh):
        at = pl.ds(row(zz, 0), 4 * t)

        def body(off, w):
            dh[:, pl.ds(off, w)] = lax.dot_general(d[at, :], w2[pl.ds(off, w), :], NT, preferred_element_type=F32)

        tiles(f, 256, body)

    def hidden(zz, dh):
        at = pl.ds(row(zz, 0), 4 * t)

        def body(off, w):
            to = pl.ds(off, w)
            u = jnp.dot(n[at, :], w1[:, to], preferred_element_type=F32).astype(BF16).astype(F32)
            uu = u * u
            th = jnp.tanh(GELU_A * (u + GELU_B * (uu * u)))
            cdf = 0.5 * (1.0 + th)
            hs[at, to] = (u * cdf).astype(BF16)
            slope = cdf + (0.5 * GELU_A) * u * (1.0 - th * th) * (1.0 + (3.0 * GELU_B) * uu)
            dus[at, to] = (dh[:, to] * slope).astype(BF16)

        tiles(f, 256, body)

    grad_hidden(z, pf)
    d_across(order[0], start)

    gain = jnp.concatenate([g_ref[pl.ds(i, 1), :] for i in range(m // LANES)], axis=1)

    def n_own(q, act):
        at = n.at[pl.ds(row(z, c) + q * tq, tq)]
        act(remote(at, at, S_NO + q, R_NO + q, partner))

    def n_along(b, act):
        ref = blk(n, z, c, b)
        along(ref, ref, S_NZ + 5 * b, R_NZ + 4 * b, act)

    for q in range(XQ):
        arrived(xy.at[piece(q)], R_X + q)
        x_part(q).wait_send()

        def norm(i, q=q):
            at = pl.ds(q * tq + i, 16)
            x16 = xc[at, :] + xy[at, :]
            xc[at, :] = x16
            x = x16.astype(F32)
            s = lax.rsqrt(jnp.mean(x * x, axis=-1, keepdims=True) + NORM_EPS)
            n[pl.ds(row(z, c) + q * tq + i, 16), :] = ((x * s) * gain).astype(BF16)

        rows_loop(tq, norm)
        n_own(q, start)
        if q == XQ // 2 - 1:
            n_along(0, start)

            @pl.when(middle)
            def _():
                d_got(2)
                d_on(2)

        if q == XQ - 1:
            n_along(1, start)
    for q in range(XQ):
        arrived(n.at[pl.ds(row(z, 1 - c) + q * tq, tq)], R_NO + q)
    local(w1_hbm, w1, L_W1).wait()
    hidden(z, pf)

    own_rows = pl.ds(row(z, 0), 4 * t)

    def cols(q):
        return pl.ds(pl.multiple_of(q * mq, mq), mq)

    def part_pair(src, dst, i, q):
        return remote(src.at[pl.ds(row(0, 1 - c), 2 * t), cols(q)], dst.at[:, cols(q)], S_PC + PQ * i + q, R_PC + PQ * i + q, partner)

    def part_across(got, dst, i, q):
        src = got.at[pl.ds(pl.multiple_of((1 - y) * t, t), t), cols(q)]
        return remote(src, dst.at[:, cols(q)], S_PY + PQ * i + q, R_PY + PQ * i + q, across)

    def sums_out(part, got, dst, i):
        def each(q):
            arrived(got.at[:, cols(q)], R_PC + PQ * i + q)

            def add(k):
                at = pl.ds((1 - y) * t + k, 16)
                got[at, cols(q)] += part[pl.ds(row(0, c, 1 - y) + k, 16), cols(q)]

            rows_loop(t, add)
            part_across(got, dst, i, q).start()

        loop(0, PQ, each)

    def dn_part(q):
        pd[:, cols(q)] = lax.dot_general(dus[own_rows, :], w1[cols(q), :], NT, preferred_element_type=F32)
        part_pair(pd, rd, 0, q).start()

    def y_part(q):
        pf[:, cols(q)] = jnp.dot(hs[own_rows, :], w2[:, cols(q)], preferred_element_type=F32)
        part_pair(pf, rf, 1, q).start()

    loop(0, PQ, dn_part)
    sums_out(pd, rd, yd, 0)
    loop(0, PQ, y_part)

    @pl.when(end)
    def _():
        d_got(1)

    d_across(order[1], start)

    def n_got(k):
        for b in range(2):
            arrived(blk(n, order[k], c, b), R_NZ + 4 * b + order[k])

    def n_on(k):
        for b in range(2):
            pass_on(k, blk(n, order[k], c, b), S_NZ + 5 * b, R_NZ + 4 * b, start)

    def n_pair(zz, act):
        act(remote(duo(n, zz, c), duo(n, zz, c), S_NC + zz, R_NC + zz, partner))

    n_got(0)
    n_pair(order[0], start)

    @pl.when(middle)
    def _():
        n_on(0)
        n_got(1)
        n_on(1)
        n_pair(order[1], start)

    for k in range(3):
        arrived(idl.at[order[k]], R_IDS + order[k])
    sort_keys(idl, keys, place, ordered, first, shard_rows, tall, r * shard_rows)
    ord_o[...] = ordered[...].astype(I32)
    first_o[...] = first[...].astype(I32)

    for q in range(PQ):
        arrived(yd.at[:, cols(q)], R_PY + q)

    def grad_x(i):
        at, own = pl.ds(i, 16), pl.ds(y * t + i, 16)
        dn = pd[pl.ds(row(0, c, y) + i, 16), :] + rd[own, :] + yd[at, :]
        x = xc[own, :].astype(F32)
        s = lax.rsqrt(jnp.mean(x * x, axis=-1, keepdims=True) + NORM_EPS)
        xh = x * s
        dhat = dn * gain
        dxn = s * (dhat - xh * jnp.mean(dhat * xh, axis=-1, keepdims=True))
        dxo[at, :] = (d[pl.ds(row(z, c, y) + i, 16), :].astype(F32) + dxn).astype(BF16)

    rows_loop(t, grad_x)

    def dx_across(zz, src, act):
        act(remote(src, blk(dx_o, zz, c, y), S_XY + zz, R_XY + zz, across))

    def dx_pair(zz, act):
        act(remote(duo(dx_o, zz, c), duo(dx_o, zz, c), S_XC + zz, R_XC + zz, partner))

    dx_across(z, dxo, start)
    local(dxo, blk(dx_o, z, c, y), L_DX).start()

    @pl.when(end)
    def _():
        d_got(2)

    d_across(order[2], start)
    sums_out(pf, rf, yf, 1)
    for q in range(PQ):
        part_pair(pd, rd, 0, q).wait_send()

    def unit(k):
        zz = order[k]
        arrived(blk(d, zz, c, 1 - y), R_DY + zz)
        d_pair(zz, start)
        arrived(duo(d, zz, 1 - c), R_DC + zz)
        grad_hidden(zz, pd)
        arrived(duo(n, zz, 1 - c), R_NC + zz)
        hidden(zz, pd)

    def dx_got(k):
        zz = order[k]
        arrived(blk(dx_o, zz, c, y), R_XZ + zz)
        dx_across(zz, blk(dx_o, zz, c, y), start)

    def dx_on(k):
        pass_on(k, blk(dx_o, order[k], c, y), S_XZ, R_XZ, start)

    unit(0)

    @pl.when(middle)
    def _():
        n_got(2)
        n_on(2)
        n_pair(order[2], start)

    along(dxo, blk(dx_o, z, c, y), S_XZ, R_XZ, start)

    @pl.when(end)
    def _():
        n_got(1)
        n_pair(order[1], start)

    unit(1)

    @pl.when(middle)
    def _():
        for k in range(2):
            dx_got(k)
            dx_on(k)

    @pl.when(end)
    def _():
        n_got(2)
        n_pair(order[2], start)

    unit(2)

    tw = 2 * t

    def stage(i, width):
        return pd.at[pl.ds(pl.multiple_of(lax.rem(i, 2) * tw, tw), tw), pl.ds(0, width)]

    def flush(i, dst):
        return local(stage(i, dst.shape[1]), dst.at[pl.ds(pl.multiple_of(i * tw, tw), tw)], L_DW + lax.rem(i, 2))

    def weight_tile(i, lhs, rhs, dst):
        @pl.when(i >= 2)
        def _():
            flush(i - 2, dst).wait()

        at = pl.ds(pl.multiple_of(i * tw, tw), tw)
        stage(i, dst.shape[1])[...] = lax.dot_general(lhs[:, at], rhs[...], TN, preferred_element_type=F32)
        flush(i, dst).start()

    n1, n2 = m // tw, f // tw

    @pl.when(end)
    def _():
        dx_got(0)

    loop(0, n1 // 2, lambda i: weight_tile(i, n, dus, dw1_o))

    @pl.when(end)
    def _():
        dx_got(1)

    @pl.when(middle)
    def _():
        dx_got(2)
        dx_on(2)

    loop(n1 // 2, n1, lambda i: weight_tile(i, n, dus, dw1_o))
    for i in (n1 - 2, n1 - 1):
        flush(i, dw1_o).wait()

    @pl.when(end)
    def _():
        dx_got(2)

    loop(0, n2, lambda i: weight_tile(i, hs, d, dw2_o))
    for i in (n2 - 2, n2 - 1):
        flush(i, dw2_o).wait()
    if f % tw:
        rest = pd.at[pl.ds(0, f % tw)]
        rest[...] = lax.dot_general(hs[:, n2 * tw :], d[...], TN, preferred_element_type=F32)
        last = local(rest, dw2_o.at[pl.ds(n2 * tw, f % tw)], L_DW)
        last.start()
    for q in range(PQ):
        arrived(yf.at[:, cols(q)], R_PY + PQ + q)

    def block_out(i):
        own = pl.ds(y * t + i, 16)
        total = pf[pl.ds(row(0, c, y) + i, 16), :] + rf[own, :] + yf[pl.ds(i, 16), :]
        out_ref[pl.ds(i, 16), :] = (xc[own, :].astype(F32) + total).astype(BF16)

    rows_loop(t, block_out)
    local(dxo, blk(dx_o, z, c, y), L_DX).wait()
    for zz in (z, *order):
        arrived(blk(dx_o, zz, c, 1 - y), R_XY + zz)
        dx_pair(zz, start)
    if f % tw:
        last.wait()

    for zz in (z, *order):
        d_across(zz, sent)
        d_pair(zz, sent)
    for k in range(3):
        n_pair(order[k], sent)
        remote(ids_ref, idl.at[z], S_IDS + k, R_IDS + z, {"data": order[k]}).wait_send()
        dx_across(order[k], blk(dx_o, order[k], c, y), sent)
    dx_across(z, dxo, sent)
    along(own_d, own_d, S_DZ, R_DZ, sent)
    along(dxo, blk(dx_o, z, c, y), S_XZ, R_XZ, sent)
    for b in range(2):
        n_along(b, sent)

    @pl.when(middle)
    def _():
        for k in range(3):
            pass_on(k, blk(d, order[k], c, y), S_DZ, R_DZ, sent)
            pass_on(k, blk(dx_o, order[k], c, y), S_XZ, R_XZ, sent)
            for b in range(2):
                pass_on(k, blk(n, order[k], c, b), S_NZ + 5 * b, R_NZ + 4 * b, sent)

    for q in range(XQ):
        xm_part(q).wait_send()
        n_own(q, sent)
    for q in range(PQ):
        part_pair(pf, rf, 1, q).wait_send()
        part_across(rd, yd, 0, q).wait_send()
        part_across(rf, yf, 1, q).wait_send()
    for zz in (z, *order):
        arrived(duo(dx_o, zz, 1 - c), R_XC + zz)
        dx_pair(zz, sent)


def run_group(ids, xm, w1, w2, gain, d_out, shard_rows, tall):
    t, m = d_out.shape
    f = w1.shape[1]
    lines = 4 * ids.shape[0]
    any_, vmem = pl.BlockSpec(memory_space=pl.ANY), pl.BlockSpec(memory_space=pltpu.VMEM)
    V = pltpu.VMEM
    sds = jax.ShapeDtypeStruct
    dots = 2 * 4 * t * m * f
    return pl.pallas_call(
        functools.partial(group_kernel, shard_rows, tall),
        out_shape=(
            sds((t, m), BF16), sds((lines, LANES), I32), sds((1, LANES), I32), sds((16 * t, m), BF16),
            sds((m, f), F32), sds((f, m), F32),
        ),
        in_specs=[vmem, any_, any_, any_, vmem, any_],
        out_specs=(vmem, vmem, vmem, any_, any_, any_),
        scratch_shapes=[
            V((m, f), BF16), V((f, m), BF16), V((16 * t, m), BF16), V((16 * t, m), BF16),
            V((4 * t, m), BF16), V((2 * t, m), BF16), V((2 * t, m), BF16),
            V((16 * t, f), BF16), V((16 * t, f), BF16),
            V((4 * t, m), F32), V((4 * t, m), F32), V((2 * t, m), F32), V((2 * t, m), F32),
            V((t, m), F32), V((t, m), F32),
            V((t, m), BF16), V((4, *ids.shape), I32),
            V((lines, LANES), F32), V((lines, LANES), F32), V((lines, LANES), F32), V((1, LANES), F32),
            pltpu.SemaphoreType.DMA((N_L,)), pltpu.SemaphoreType.DMA((N_S,)), pltpu.SemaphoreType.DMA((N_R,)),
        ],
        compiler_params=pltpu.CompilerParams(collective_id=0, has_side_effects=True, vmem_limit_bytes=67043328),
        cost_estimate=pl.CostEstimate(flops=18 * dots, bytes_accessed=64 * 16 * t * m, transcendentals=16 * t * f),
        name="group_step",
    )(ids, xm, w1, w2, gain, d_out)


def lookup_kernel(shard_rows, ids_smem, ids_col, table, out_ref, got, sem):
    total, m = out_ref.shape
    t = total // 4
    per = 32
    chunks = total // per
    r = lax.axis_index("tensor")

    def fetch(k):
        def one(i):
            p = k * per + i
            pltpu.make_async_copy(table.at[lax.div(lax.rem(ids_smem[p], shard_rows), 8)], got.at[p], sem.at[k]).start()

        def some(j, carry):
            for u in range(8):
                one(j * 8 + u)
            return carry

        lax.fori_loop(0, per // 8, some, 0)

    loop(0, chunks, fetch)
    spot = lax.broadcasted_iota(I32, (per, 8 * per), 1)
    token = lax.broadcasted_iota(I32, (per, 8 * per), 0)

    def pick(k):
        at = pl.ds(pl.multiple_of(k * per, per), per)
        pltpu.make_async_copy(got.at[at], got.at[at], sem.at[k]).wait()
        row = ids_col[at, :] - r * shard_rows
        owned = (row >= 0) & (row < shard_rows)
        want = jnp.where(owned, (row & 7) + 8 * token, -1)
        chosen = jnp.where(want == spot, 1.0, 0.0).astype(BF16)
        rows = jnp.dot(chosen, got[at].reshape(8 * per, m), preferred_element_type=F32)
        p = k * per
        b = lax.div(p, t)
        to = lax.rem(b, 2) * (2 * t) + lax.div(b, 2) * t + lax.rem(p, t)
        out_ref[pl.ds(pl.multiple_of(to, per), per), :] = rows.astype(BF16)

    loop(0, chunks, pick)


def look_up(ids, table):
    shard_rows, m = table.shape
    total = ids.shape[0]
    return pl.pallas_call(
        functools.partial(lookup_kernel, shard_rows),
        out_shape=jax.ShapeDtypeStruct((total, m), BF16),
        grid_spec=pltpu.PrefetchScalarGridSpec(
            num_scalar_prefetch=1,
            grid=(1,),
            in_specs=[pl.BlockSpec((total, 1), lambda i, *_: (0, 0)), pl.BlockSpec(memory_space=pl.ANY)],
            out_specs=pl.BlockSpec((total, m), lambda i, *_: (0, 0)),
            scratch_shapes=[pltpu.VMEM((total, 8, m), BF16), pltpu.SemaphoreType.DMA((total // 32,))],
        ),
        compiler_params=pltpu.CompilerParams(vmem_limit_bytes=48 << 20),
        cost_estimate=pl.CostEstimate(flops=16 * total * m, bytes_accessed=20 * total * m, transcendentals=0),
        name="look_up",
    )(ids, ids.reshape(total, 1), table.reshape(shard_rows // 8, 8, m))


PHASE = 8


def table_kernel(key_ref, first_ref, dw1_ref, dw2_ref, dx_hbm, out_ref, dw1_o, dw2_o, dxb, dxf, sem):
    step = pl.program_id(0)
    tall = out_ref.shape[0]
    count = dxb.shape[0]
    each = count // PHASE

    def fetch(k):
        at = pl.ds(pl.multiple_of(k * each, each), each)
        return pltpu.make_async_copy(dx_hbm.at[at], dxb.at[at], sem.at[k])

    @pl.when(step == 0)
    def _():
        loop(0, PHASE, lambda k: fetch(k).start())

    @pl.when(step < PHASE)
    def _():
        dw1_o[...] = dw1_ref[...]
        dw2_o[...] = dw2_ref[...]
        fetch(step).wait()

        def widen(i):
            at = pl.ds(step * each + i, 16)
            dxf[at, :] = dxb[at, :].astype(F32)

        rows_loop(each, widen)

    @pl.when(step >= PHASE)
    def _():
        tile = step - PHASE
        out_ref[...] = jnp.zeros_like(out_ref)

        def add(j):
            key = key_ref[j]
            to = pl.ds(lax.div(key, count) - tile * tall, 1)
            out_ref[to, :] += dxf[pl.ds(lax.rem(key, count), 1), :]

        loop(first_ref[tile], first_ref[tile + 1], add)


def table_grad(ordered, first, dx_all, dw1, dw2, shard_rows, tall):
    count, m = dx_all.shape
    f = dw1.shape[1]

    def early(i, *_):
        return (jnp.minimum(i, PHASE - 1), 0)

    dw_specs = [pl.BlockSpec((m // PHASE, f), early), pl.BlockSpec((f // PHASE, m), early)]
    sds = jax.ShapeDtypeStruct
    return pl.pallas_call(
        table_kernel,
        out_shape=(sds((shard_rows, m), F32), sds((m, f), F32), sds((f, m), F32)),
        grid_spec=pltpu.PrefetchScalarGridSpec(
            num_scalar_prefetch=2,
            grid=(PHASE + shard_rows // tall,),
            in_specs=[*dw_specs, pl.BlockSpec(memory_space=pl.ANY)],
            out_specs=[pl.BlockSpec((tall, m), lambda i, *_: (jnp.maximum(i - PHASE, 0), 0)), *dw_specs],
            scratch_shapes=[
                pltpu.VMEM((count, m), BF16), pltpu.VMEM((count, m), F32), pltpu.SemaphoreType.DMA((PHASE,)),
            ],
        ),
        compiler_params=pltpu.CompilerParams(dimension_semantics=("arbitrary",), vmem_limit_bytes=56 << 20),
        cost_estimate=pl.CostEstimate(flops=count * m, bytes_accessed=4 * shard_rows * m + 16 * m * f, transcendentals=0),
        name="table_grad",
    )(ordered, first, dw1, dw2, dx_all)


def solution(mesh):
    tok_spec = P(("pod", "data", "tensor"), None)

    def per_device(token_ids, embed_table, norm_gain, w_in, w_out, d_out):
        shard_rows = embed_table.shape[0]
        tall = next(k for k in (320, 64, 8) if shard_rows % k == 0)
        masked = look_up(token_ids, embed_table)
        gain = norm_gain.astype(F32).reshape(-1, LANES)
        ids = token_ids.reshape(-1, LANES)
        out, ordered, first, dx_all, dw1, dw2 = run_group(ids, masked, w_in, w_out, gain, d_out, shard_rows, tall)
        grad_table, grad_w_in, grad_w_out = table_grad(
            ordered.reshape(-1), first.reshape(-1), dx_all, dw1, dw2, shard_rows, tall
        )
        return out, grad_table, grad_w_in, grad_w_out

    return jax.shard_map(
        per_device,
        mesh=mesh,
        in_specs=(P(("pod", "data")), P("tensor", None), P(None), P(None, "tensor"), P("tensor", None), tok_spec),
        out_specs=(tok_spec, P(("pod", "tensor"), None), P("pod", "tensor"), P(("pod", "tensor"), None)),
        check_vma=False,
    )
```

```python
import functools

import jax
import jax.numpy as jnp
from jax import lax
from jax.experimental import pallas as pl
from jax.experimental.pallas import tpu as pltpu
from jax.sharding import PartitionSpec as P

NORM_EPS = 1e-6
GELU_A = 0.7978845608028654
GELU_B = 0.044715
MESH = pl.DeviceIdType.MESH
NT = (((1,), (1,)), ((), ()))
TN = (((0,), (0,)), ((), ()))
F32, BF16, I32 = jnp.float32, jnp.bfloat16, jnp.int32
LANES = 128
XQ = 4
PQ = 4

R_IDS, R_DZ, R_DY, R_DC, R_NZ, R_NC, R_XZ, R_XY, R_XC = 0, 4, 8, 12, 16, 24, 28, 36, 44
R_XM, R_X, R_NO, R_PC, R_PY, N_R = 48, 52, 56, 60, 68, 72
S_IDS, S_DZ, S_DY, S_DC, S_NZ, S_NC, S_XZ, S_XY, S_XC = 0, 3, 8, 12, 16, 26, 30, 40, 48
S_XM, S_X, S_NO, S_PC, S_PY, N_S = 52, 56, 60, 64, 72, 76
L_W1, L_W2, L_XM, L_DO, L_DX, L_YS, L_YB, L_DW, N_L = 0, 1, 2, 3, 4, 5, 6, 7, 9


def loop(lo, hi, body):
    def one(j, carry):
        body(j)
        return carry

    lax.fori_loop(lo, hi, one, 0)


def tiles(total, step, body):
    full = total // step
    loop(0, full, lambda j: body(pl.multiple_of(j * step, step), step))
    if total % step:
        body(full * step, total % step)


def rows_loop(total, body):
    loop(0, total // 16, lambda j: body(pl.multiple_of(j * 16, 16)))


def sort_keys(ids, keys, place, ordered, first, shard_rows, tall, rank0):
    reps, per, _ = ids.shape
    count = reps * per * LANES
    t = per * LANES // 4
    shift = t.bit_length() - 1
    lines = reps * per
    lane = lax.broadcasted_iota(I32, (per, LANES), 1)
    spot = lax.broadcasted_iota(I32, (per, LANES), 0) * LANES + lane
    block = jnp.right_shift(spot, shift)
    kept = (block & 1) * (2 * t) + jnp.right_shift(block, 1) * t + (spot & (t - 1))
    for k in range(reps):
        row = ids[k] - rank0
        row = jnp.where((row >= 0) & (row < shard_rows), row, shard_rows)
        keys[k * per : (k + 1) * per, :] = (row * count + (k * per * LANES + kept)).astype(F32)
    place[...] = jnp.zeros_like(place)
    ordered[...] = jnp.zeros_like(ordered)
    up = lax.broadcasted_iota(I32, (LANES, LANES), 0)
    over = lax.broadcasted_iota(I32, (LANES, LANES), 1)
    same = up == over
    overf = over.astype(F32)

    def column(ref, b):
        return jnp.sum(jnp.where(same, jnp.broadcast_to(ref[pl.ds(b, 1), :], (LANES, LANES)), 0.0), axis=1, keepdims=True)

    def count_below(b):
        col = column(keys, b)

        def one(a):
            at = pl.ds(a, 1)
            place[at, :] += jnp.sum(jnp.where(col < keys[at, :], 1.0, 0.0), axis=0, keepdims=True)

        loop(0, lines, one)

    loop(0, lines, count_below)

    def put(b):
        col, spot_of = column(keys, b), column(place, b)

        def one(a):
            want = overf + (a * LANES).astype(F32)
            ordered[pl.ds(a, 1), :] += jnp.sum(jnp.where(spot_of == want, col, 0.0), axis=0, keepdims=True)

        loop(0, lines, one)
        edge = overf * float(tall * count)
        first[...] += jnp.sum(jnp.where(col < edge, 1.0, 0.0), axis=0, keepdims=True)

    first[...] = jnp.zeros_like(first)
    loop(0, lines, put)


def group_kernel(shard_rows, tall, ids_ref, xm_hbm, w1_hbm, w2_hbm, g_ref, do_hbm,
                 base_o, ysum_o, ord_o, first_o, dx_o, dw1_o, dw2_o,
                 w1, w2, n, d, xm, xc, xy, hs, dus, pd, pf, rd, rf, yd, yb, dxo, idl, keys, place, ordered, first,
                 lsem, ssem, rsem):
    t, m = do_hbm.shape
    f = w1_hbm.shape[1]
    tq, mq = 2 * t // XQ, m // PQ
    z = lax.axis_index("data")
    r = lax.axis_index("tensor")
    y, c = lax.div(r, 2), lax.rem(r, 2)
    partner = {"tensor": 2 * y + 1 - c}
    across = {"tensor": 2 * (1 - y) + c}
    half = lax.div(z, 2)
    inner = z + half * (3 - 2 * z)
    order = [b + half * (3 - 2 * b) for b in (1 - inner, 2, 3)]
    middle, end = inner == 1, inner == 0

    def row(zz, cc, yy=0):
        return pl.multiple_of(zz * (4 * t) + cc * (2 * t) + yy * t, t)

    def blk(ref, zz, cc, yy):
        return ref.at[pl.ds(row(zz, cc, yy), t)]

    def duo(ref, zz, cc):
        return ref.at[pl.ds(row(zz, cc), 2 * t)]

    def remote(src, dst, s, q, dev):
        return pltpu.make_async_remote_copy(
            src_ref=src, dst_ref=dst, send_sem=ssem.at[s], recv_sem=rsem.at[q], device_id=dev, device_id_type=MESH
        )

    def local(src, dst, i):
        return pltpu.make_async_copy(src, dst, lsem.at[i])

    def arrived(ref, q):
        remote(ref, ref, 0, q, partner).wait_recv()

    def start(cp):
        cp.start()

    def sent(cp):
        cp.wait_send()

    def along(src, dst, s, q, act):
        for i, hop in enumerate((1, -1)):
            to = z + hop

            @pl.when((to >= 0) & (to <= 3))
            def _():
                act(remote(src, dst, s + i, q + z, {"data": to}))

    def pass_on(k, ref, s, q, act):
        act(remote(ref, ref, s + 2 + k, q + order[k], {"data": order[1] if k == 0 else order[0]}))

    barrier = pltpu.get_barrier_semaphore()
    pl.semaphore_signal(barrier, inc=1, device_id=partner, device_id_type=MESH)
    pl.semaphore_signal(barrier, inc=1, device_id=across, device_id_type=MESH)
    for k in range(3):
        pl.semaphore_signal(barrier, inc=1, device_id={"data": order[k]}, device_id_type=MESH)

    own_d = blk(d, z, c, y)
    local(do_hbm, own_d, L_DO).start()
    local(xm_hbm, xm, L_XM).start()
    local(w2_hbm, w2, L_W2).start()
    local(w1_hbm, w1, L_W1).start()
    pl.semaphore_wait(barrier, 5)

    def piece(q):
        return pl.ds(q * tq, tq)

    local(do_hbm, own_d, L_DO).wait()
    along(own_d, own_d, S_DZ, R_DZ, start)
    local(xm_hbm, xm, L_XM).wait()

    def xm_part(q):
        return remote(xm.at[pl.ds(row(0, 1 - c) + q * tq, tq)], xc.at[piece(q)], S_XM + q, R_XM + q, partner)

    def x_part(q):
        return remote(xc.at[piece(q)], xy.at[piece(q)], S_X + q, R_X + q, across)

    def d_got(k):
        arrived(blk(d, order[k], c, y), R_DZ + order[k])

    def d_on(k):
        pass_on(k, blk(d, order[k], c, y), S_DZ, R_DZ, start)

    def d_across(zz, act):
        act(remote(blk(d, zz, c, y), blk(d, zz, c, y), S_DY + zz, R_DY + zz, across))

    def d_pair(zz, act):
        act(remote(duo(d, zz, c), duo(d, zz, c), S_DC + zz, R_DC + zz, partner))

    for q in range(XQ):
        xm_part(q).start()
    for k in range(3):
        remote(ids_ref, idl.at[z], S_IDS + k, R_IDS + z, {"data": order[k]}).start()
    idl[z] = ids_ref[...]
    for q in range(XQ):
        arrived(xc.at[piece(q)], R_XM + q)

        def join(i, q=q):
            at = pl.ds(q * tq + i, 16)
            xc[at, :] += xm[pl.ds(row(0, c) + q * tq + i, 16), :]

        rows_loop(tq, join)
        x_part(q).start()
    d_across(z, start)
    d_got(0)

    @pl.when(middle)
    def _():
        d_on(0)
        d_got(1)
        d_on(1)

    gain = jnp.concatenate([g_ref[pl.ds(i, 1), :] for i in range(m // LANES)], axis=1).astype(F32)

    def n_own(q, act):
        at = n.at[pl.ds(row(z, c) + q * tq, tq)]
        act(remote(at, at, S_NO + q, R_NO + q, partner))

    def n_along(b, act):
        ref = blk(n, z, c, b)
        along(ref, ref, S_NZ + 5 * b, R_NZ + 4 * b, act)

    for q in range(XQ):
        arrived(xy.at[piece(q)], R_X + q)
        x_part(q).wait_send()

        def norm(i, q=q):
            at = pl.ds(q * tq + i, 16)
            x16 = xc[at, :] + xy[at, :]
            xc[at, :] = x16
            x = x16.astype(F32)
            s = lax.rsqrt(jnp.mean(x * x, axis=-1, keepdims=True) + NORM_EPS)
            n[pl.ds(row(z, c) + q * tq + i, 16), :] = ((x * s) * gain).astype(BF16)

        rows_loop(tq, norm)
        n_own(q, start)
        if q == XQ // 2 - 1:
            n_along(0, start)

            @pl.when(middle)
            def _():
                d_got(2)
                d_on(2)

        if q == XQ - 1:
            n_along(1, start)
    d_across(order[0], start)

    def hidden(zz, slopes):
        at = pl.ds(row(zz, 0), 4 * t)

        def body(off, w):
            to = pl.ds(off, w)
            u = jnp.dot(n[at, :], w1[:, to], preferred_element_type=F32).astype(BF16).astype(F32)
            uu = u * u
            th = jnp.tanh(GELU_A * (u + GELU_B * (uu * u)))
            cdf = 0.5 * (1.0 + th)
            hs[at, to] = (u * cdf).astype(BF16)
            slopes[:, to] = cdf + (0.5 * GELU_A) * u * (1.0 - th * th) * (1.0 + (3.0 * GELU_B) * uu)

        tiles(f, 256, body)

    def grad_hidden(zz, slopes):
        at = pl.ds(row(zz, 0), 4 * t)

        def body(off, w):
            to = pl.ds(off, w)
            dh = lax.dot_general(d[at, :], w2[to, :], NT, preferred_element_type=F32)
            dus[at, to] = (dh * slopes[:, to]).astype(BF16)

        tiles(f, 256, body)

    for q in range(XQ):
        arrived(n.at[pl.ds(row(z, 1 - c) + q * tq, tq)], R_NO + q)
    local(w1_hbm, w1, L_W1).wait()
    hidden(z, pf)
    arrived(blk(d, z, c, 1 - y), R_DY + z)
    d_pair(z, start)
    arrived(duo(d, z, 1 - c), R_DC + z)
    local(w2_hbm, w2, L_W2).wait()
    grad_hidden(z, pf)

    own_rows = pl.ds(row(z, 0), 4 * t)
    far = pl.multiple_of((1 - y) * t, t)

    def cols(q):
        return pl.ds(pl.multiple_of(q * mq, mq), mq)

    def part_pair(src, dst, i, q):
        return remote(src.at[pl.ds(row(0, 1 - c), 2 * t), cols(q)], dst.at[:, cols(q)], S_PC + PQ * i + q, R_PC + PQ * i + q, partner)

    def part_across(q):
        return remote(rd.at[pl.ds(far, t), cols(q)], yd.at[:, cols(q)], S_PY + q, R_PY + q, across)

    def sum_part(part, got, i, q):
        arrived(got.at[:, cols(q)], R_PC + PQ * i + q)

        def add(k):
            got[pl.ds(far + k, 16), cols(q)] += part[pl.ds(row(0, c, 1 - y) + k, 16), cols(q)]

        rows_loop(t, add)

    def dn_part(q):
        pd[:, cols(q)] = lax.dot_general(dus[own_rows, :], w1[cols(q), :], NT, preferred_element_type=F32)
        part_pair(pd, rd, 0, q).start()

    def y_part(q):
        pf[:, cols(q)] = jnp.dot(hs[own_rows, :], w2[:, cols(q)], preferred_element_type=F32)
        part_pair(pf, rf, 1, q).start()

    def dn_out(q):
        sum_part(pd, rd, 0, q)
        part_across(q).start()

    loop(0, PQ, dn_part)
    loop(0, PQ, dn_out)
    loop(0, PQ, y_part)

    @pl.when(end)
    def _():
        d_got(1)

    d_across(order[1], start)

    def n_got(k):
        for b in range(2):
            arrived(blk(n, order[k], c, b), R_NZ + 4 * b + order[k])

    def n_on(k):
        for b in range(2):
            pass_on(k, blk(n, order[k], c, b), S_NZ + 5 * b, R_NZ + 4 * b, start)

    def n_pair(zz, act):
        act(remote(duo(n, zz, c), duo(n, zz, c), S_NC + zz, R_NC + zz, partner))

    n_got(0)
    n_pair(order[0], start)

    @pl.when(middle)
    def _():
        n_on(0)
        n_got(1)
        n_on(1)
        n_pair(order[1], start)

    for k in range(3):
        arrived(idl.at[order[k]], R_IDS + order[k])
    sort_keys(idl, keys, place, ordered, first, shard_rows, tall, r * shard_rows)
    ord_o[...] = ordered[...].astype(I32)
    first_o[...] = first[...].astype(I32)

    for q in range(PQ):
        arrived(yd.at[:, cols(q)], R_PY + q)

    def grad_x(i):
        at, own = pl.ds(i, 16), pl.ds(y * t + i, 16)
        dn = pd[pl.ds(row(0, c, y) + i, 16), :] + rd[own, :] + yd[at, :]
        x = xc[own, :].astype(F32)
        s = lax.rsqrt(jnp.mean(x * x, axis=-1, keepdims=True) + NORM_EPS)
        xh = x * s
        dhat = dn * gain
        dxn = s * (dhat - xh * jnp.mean(dhat * xh, axis=-1, keepdims=True))
        dxo[at, :] = (d[pl.ds(row(z, c, y) + i, 16), :].astype(F32) + dxn).astype(BF16)

    rows_loop(t, grad_x)
    th = t // 2

    def dx_part(zz, yy, h):
        return dx_o.at[pl.ds(pl.multiple_of(row(zz, c, yy) + h * th, th), th)]

    def dx_own(h):
        return dxo.at[pl.ds(h * th, th)]

    def dx_across(zz, src, h, act):
        act(remote(src, dx_part(zz, y, h), S_XY + 4 * h + zz, R_XY + 4 * h + zz, across))

    def dx_along(act):
        for h in range(2):
            along(dx_own(h), dx_part(z, y, h), S_XZ + 5 * h, R_XZ + 4 * h, act)

    def dx_pair(zz, act):
        act(remote(duo(dx_o, zz, c), duo(dx_o, zz, c), S_XC + zz, R_XC + zz, partner))

    def dx_got(k, on):
        zz = order[k]
        for h in range(2):
            arrived(dx_part(zz, y, h), R_XZ + 4 * h + zz)
            if on:
                pass_on(k, dx_part(zz, y, h), S_XZ + 5 * h, R_XZ + 4 * h, start)
            dx_across(zz, dx_part(zz, y, h), h, start)

    def dx_hand(zz):
        for h in range(2):
            arrived(dx_part(zz, 1 - y, h), R_XY + 4 * h + zz)
        dx_pair(zz, start)

    for h in range(2):
        dx_across(z, dx_own(h), h, start)
    local(dxo, blk(dx_o, z, c, y), L_DX).start()

    @pl.when(end)
    def _():
        d_got(2)

    d_across(order[2], start)

    loop(0, PQ, lambda q: sum_part(pf, rf, 1, q))
    y_send = local(rf.at[pl.ds(far, t)], ysum_o, L_YS)
    y_send.start()

    def base(i):
        own = pl.ds(y * t + i, 16)
        yb[pl.ds(i, 16), :] = xc[own, :].astype(F32) + (pf[pl.ds(row(0, c, y) + i, 16), :] + rf[own, :])

    rows_loop(t, base)
    y_keep = local(yb, base_o, L_YB)
    y_keep.start()
    for q in range(PQ):
        part_pair(pd, rd, 0, q).wait_send()

    def unit(k):
        zz = order[k]
        arrived(blk(d, zz, c, 1 - y), R_DY + zz)
        d_pair(zz, start)
        arrived(duo(n, zz, 1 - c), R_NC + zz)
        hidden(zz, pd)
        arrived(duo(d, zz, 1 - c), R_DC + zz)
        grad_hidden(zz, pd)

    def n_rest(k, on):
        n_got(k)
        if on:
            n_on(k)
        n_pair(order[k], start)

    pl.when(middle)(lambda: n_rest(2, True))
    unit(0)
    dx_along(start)
    pl.when(end)(lambda: n_rest(1, False))
    unit(1)

    @pl.when(middle)
    def _():
        dx_got(0, True)
        dx_got(1, True)

    pl.when(end)(lambda: n_rest(2, False))
    unit(2)

    tw = 2 * t

    def stage(i, width):
        return pd.at[pl.ds(pl.multiple_of(lax.rem(i, 2) * tw, tw), tw), pl.ds(0, width)]

    def flush(i, dst):
        return local(stage(i, dst.shape[1]), dst.at[pl.ds(pl.multiple_of(i * tw, tw), tw)], L_DW + lax.rem(i, 2))

    def weight_tile(i, lhs, rhs, dst):
        @pl.when(i >= 2)
        def _():
            flush(i - 2, dst).wait()

        at = pl.ds(pl.multiple_of(i * tw, tw), tw)
        stage(i, dst.shape[1])[...] = lax.dot_general(lhs[:, at], rhs[...], TN, preferred_element_type=F32)
        flush(i, dst).start()

    n1, n2 = m // tw, f // tw
    pl.when(end)(lambda: dx_got(0, False))
    loop(0, n1 // 2, lambda i: weight_tile(i, n, dus, dw1_o))
    pl.when(end)(lambda: dx_got(1, False))
    pl.when(middle)(lambda: dx_got(2, True))
    loop(n1 // 2, n1, lambda i: weight_tile(i, n, dus, dw1_o))
    for i in (n1 - 2, n1 - 1):
        flush(i, dw1_o).wait()
    pl.when(end)(lambda: dx_got(2, False))
    local(dxo, blk(dx_o, z, c, y), L_DX).wait()
    dx_hand(z)
    dx_hand(order[0])
    loop(0, n2 // 2 + 1, lambda i: weight_tile(i, hs, d, dw2_o))
    dx_hand(order[1])
    loop(n2 // 2 + 1, n2, lambda i: weight_tile(i, hs, d, dw2_o))
    for i in (n2 - 2, n2 - 1):
        flush(i, dw2_o).wait()
    if f % tw:
        rest = pd.at[pl.ds(0, f % tw)]
        rest[...] = lax.dot_general(hs[:, n2 * tw :], d[...], TN, preferred_element_type=F32)
        last = local(rest, dw2_o.at[pl.ds(n2 * tw, f % tw)], L_DW)
        last.start()
    dx_hand(order[2])
    if f % tw:
        last.wait()

    y_send.wait()
    y_keep.wait()
    for zz in (z, *order):
        d_across(zz, sent)
        d_pair(zz, sent)
    for k in range(3):
        n_pair(order[k], sent)
        remote(ids_ref, idl.at[z], S_IDS + k, R_IDS + z, {"data": order[k]}).wait_send()
    along(own_d, own_d, S_DZ, R_DZ, sent)
    dx_along(sent)
    for b in range(2):
        n_along(b, sent)
        dx_across(z, dx_own(b), b, sent)
        for k in range(3):
            dx_across(order[k], dx_part(order[k], y, b), b, sent)

    @pl.when(middle)
    def _():
        for k in range(3):
            pass_on(k, blk(d, order[k], c, y), S_DZ, R_DZ, sent)
            for b in range(2):
                pass_on(k, dx_part(order[k], y, b), S_XZ + 5 * b, R_XZ + 4 * b, sent)
                pass_on(k, blk(n, order[k], c, b), S_NZ + 5 * b, R_NZ + 4 * b, sent)

    for q in range(XQ):
        xm_part(q).wait_send()
        n_own(q, sent)
    for q in range(PQ):
        part_pair(pf, rf, 1, q).wait_send()
        part_across(q).wait_send()
    for zz in (z, *order):
        arrived(duo(dx_o, zz, 1 - c), R_XC + zz)
        dx_pair(zz, sent)


def run_group(ids, xm, w1, w2, gain, d_out, shard_rows, tall):
    t, m = d_out.shape
    f = w1.shape[1]
    lines = 4 * ids.shape[0]
    any_, vmem = pl.BlockSpec(memory_space=pl.ANY), pl.BlockSpec(memory_space=pltpu.VMEM)
    V = pltpu.VMEM
    sds = jax.ShapeDtypeStruct
    dots = 2 * 4 * t * m * f
    return pl.pallas_call(
        functools.partial(group_kernel, shard_rows, tall),
        out_shape=(
            sds((t, m), F32), sds((t, m), F32), sds((lines, LANES), I32), sds((1, LANES), I32), sds((16 * t, m), BF16),
            sds((m, f), F32), sds((f, m), F32),
        ),
        in_specs=[vmem, any_, any_, any_, vmem, any_],
        out_specs=(any_, any_, vmem, vmem, any_, any_, any_),
        scratch_shapes=[
            V((m, f), BF16), V((f, m), BF16), V((16 * t, m), BF16), V((16 * t, m), BF16),
            V((4 * t, m), BF16), V((2 * t, m), BF16), V((2 * t, m), BF16),
            V((16 * t, f), BF16), V((16 * t, f), BF16),
            V((4 * t, m), F32), V((4 * t, m), F32), V((2 * t, m), F32), V((2 * t, m), F32),
            V((t, m), F32), V((t, m), F32),
            V((t, m), BF16), V((4, *ids.shape), I32),
            V((lines, LANES), F32), V((lines, LANES), F32), V((lines, LANES), F32), V((1, LANES), F32),
            pltpu.SemaphoreType.DMA((N_L,)), pltpu.SemaphoreType.DMA((N_S,)), pltpu.SemaphoreType.DMA((N_R,)),
        ],
        compiler_params=pltpu.CompilerParams(collective_id=0, has_side_effects=True, vmem_limit_bytes=67043328),
        cost_estimate=pl.CostEstimate(flops=18 * dots, bytes_accessed=64 * 16 * t * m, transcendentals=16 * t * f),
        name="group_step",
    )(ids, xm, w1, w2, gain, d_out)


def lookup_kernel(shard_rows, ids_smem, ids_vmem, table, out_hbm, got, rows, sem, out_sem):
    total, m = out_hbm.shape
    t = total // 4
    per = 32
    chunks = total // per
    r = lax.axis_index("tensor")

    def fetch(k):
        def some(j, carry):
            for u in range(8):
                p = k * per + j * 8 + u
                at = lax.div(lax.rem(ids_smem[lax.div(p, LANES), lax.rem(p, LANES)], shard_rows), 8)
                pltpu.make_async_copy(table.at[at], got.at[p], sem.at[k]).start()
            return carry

        lax.fori_loop(0, per // 8, some, 0)

    loop(0, chunks, fetch)
    spot = lax.broadcasted_iota(I32, (per, 8 * per), 1)
    token = lax.broadcasted_iota(I32, (per, 8 * per), 0)
    same = lax.broadcasted_iota(I32, (LANES, LANES), 0) == lax.broadcasted_iota(I32, (LANES, LANES), 1)

    def line(b):
        ids = ids_vmem[pl.ds(b, 1), :].astype(F32)
        col = jnp.sum(jnp.where(same, jnp.broadcast_to(ids, (LANES, LANES)), 0.0), axis=1, keepdims=True).astype(I32)
        row = col - r * shard_rows
        row = jnp.where((row >= 0) & (row < shard_rows), row & 7, -8 * per)
        for j in range(LANES // per):
            k = b * (LANES // per) + j
            at = pl.ds(pl.multiple_of(k * per, per), per)
            pltpu.make_async_copy(got.at[at], got.at[at], sem.at[k]).wait()
            want = row[j * per : (j + 1) * per] + 8 * token
            chosen = jnp.where(want == spot, 1.0, 0.0).astype(BF16)
            picked = jnp.dot(chosen, got[at].reshape(8 * per, m), preferred_element_type=F32)
            p = k * per
            nat = lax.div(p, t)
            to = pl.multiple_of(lax.rem(nat, 2) * (2 * t) + lax.div(nat, 2) * t + lax.rem(p, t), per)
            rows[pl.ds(to, per), :] = picked.astype(BF16)
            pltpu.make_async_copy(rows.at[pl.ds(to, per)], out_hbm.at[pl.ds(to, per)], out_sem).start()

    loop(0, total // LANES, line)
    pltpu.make_async_copy(rows, out_hbm, out_sem).wait()


def look_up(ids, table):
    shard_rows, m = table.shape
    total = ids.size
    any_ = pl.BlockSpec(memory_space=pl.ANY)
    return pl.pallas_call(
        functools.partial(lookup_kernel, shard_rows),
        out_shape=jax.ShapeDtypeStruct((total, m), BF16),
        in_specs=[pl.BlockSpec(memory_space=pltpu.SMEM), pl.BlockSpec(memory_space=pltpu.VMEM), any_],
        out_specs=any_,
        scratch_shapes=[
            pltpu.VMEM((total, 8, m), BF16), pltpu.VMEM((total, m), BF16),
            pltpu.SemaphoreType.DMA((total // 32,)), pltpu.SemaphoreType.DMA,
        ],
        compiler_params=pltpu.CompilerParams(vmem_limit_bytes=60 << 20),
        cost_estimate=pl.CostEstimate(flops=16 * total * m, bytes_accessed=20 * total * m, transcendentals=0),
        name="look_up",
    )(ids, ids, table.reshape(shard_rows // 8, 8, m))


RING = 6


def table_kernel(tall, key_ref, first_ref, dw1_in, dw2_in, dx_in, out_hbm, dw1_o, dw2_o, dxb, dxf, w1, w2, ring, dx_sem, in_sem, w_sem, t_sem):
    count, m = dxb.shape
    f = w1.shape[1]
    shift = count.bit_length() - 1
    steps = out_hbm.shape[0] // tall
    each = count // 8

    def dx_piece(k):
        at = pl.ds(pl.multiple_of(k * each, each), each)
        return pltpu.make_async_copy(dx_in.at[at], dxb.at[at], dx_sem.at[k])

    def w_pieces(i, back):
        for src, buf, dst, n in ((dw1_in, w1, dw1_o, m // 8), (dw2_in, w2, dw2_o, f // 8)):
            at = pl.ds(pl.multiple_of(i * n, 8), n)
            if back:
                yield pltpu.make_async_copy(buf.at[at], dst.at[at], w_sem)
            else:
                yield pltpu.make_async_copy(src.at[at], buf.at[at], in_sem.at[i])

    loop(0, 8, lambda k: dx_piece(k).start())

    def w_fetch(i):
        for cp in w_pieces(i, False):
            cp.start()

    loop(0, 8, w_fetch)

    def widen_piece(k):
        dx_piece(k).wait()

        def widen(i):
            at = pl.ds(k * each + i, 16)
            dxf[at, :] = dxb[at, :].astype(F32)

        rows_loop(each, widen)

    loop(0, 8, widen_piece)

    def tile_out(i):
        slot = lax.rem(i, RING)
        return pltpu.make_async_copy(ring.at[slot], out_hbm.at[pl.ds(pl.multiple_of(i * tall, 8), tall)], t_sem.at[slot])

    def tile(i):
        slot = lax.rem(i, RING)
        here = ring.at[slot]
        pl.when(i >= RING)(lambda: tile_out(i - RING).wait())
        here[...] = jnp.zeros_like(here)

        def add(j, key):
            ahead = key_ref[jnp.minimum(j + 1, count - 1)]
            to = pl.ds(jnp.right_shift(key, shift) - i * tall, 1)
            here[to, :] += dxf[pl.ds(key & (count - 1), 1), :]
            return ahead

        low = first_ref[i]
        lax.fori_loop(low, first_ref[i + 1], add, key_ref[jnp.minimum(low, count - 1)])
        tile_out(i).start()

        @pl.when(i < 8)
        def _():
            for cp in w_pieces(i, False):
                cp.wait()
            for cp in w_pieces(i, True):
                cp.start()

    loop(0, steps, tile)
    loop(steps - RING, steps, lambda i: tile_out(i).wait())
    pltpu.make_async_copy(w1, dw1_o, w_sem).wait()
    pltpu.make_async_copy(w2, dw2_o, w_sem).wait()


def table_grad(ordered, first, dx_all, dw1, dw2, shard_rows, tall):
    count, m = dx_all.shape
    f = dw1.shape[1]
    any_ = pl.BlockSpec(memory_space=pl.ANY)
    sds = jax.ShapeDtypeStruct
    V, S = pltpu.VMEM, pltpu.SemaphoreType.DMA
    return pl.pallas_call(
        functools.partial(table_kernel, tall),
        out_shape=(sds((shard_rows, m), F32), sds((m, f), F32), sds((f, m), F32)),
        grid_spec=pltpu.PrefetchScalarGridSpec(
            num_scalar_prefetch=2,
            grid=(1,),
            in_specs=[any_, any_, any_],
            out_specs=[any_, any_, any_],
            scratch_shapes=[
                V((count, m), BF16), V((count, m), F32), V((m, f), F32), V((f, m), F32), V((RING, tall, m), F32),
                S((8,)), S((8,)), S, S((RING,)),
            ],
        ),
        compiler_params=pltpu.CompilerParams(vmem_limit_bytes=67043328),
        cost_estimate=pl.CostEstimate(flops=16 * count * m * f, bytes_accessed=4 * shard_rows * m + 16 * m * f, transcendentals=0),
        name="table_grad",
    )(ordered, first, dw1, dw2, dx_all)


def solution(mesh):
    tok_spec = P(("pod", "data", "tensor"), None)

    def per_device(token_ids, embed_table, norm_gain, w_in, w_out, d_out):
        shard_rows = embed_table.shape[0]
        tall = next(k for k in (160, 8) if shard_rows % k == 0)
        ids = token_ids.reshape(-1, LANES)
        masked = look_up(ids, embed_table)
        gain = norm_gain.reshape(-1, LANES)
        base, ysum, ordered, first, dx_all, dw1, dw2 = run_group(ids, masked, w_in, w_out, gain, d_out, shard_rows, tall)
        other = lax.ppermute(ysum, "tensor", [(0, 2), (1, 3), (2, 0), (3, 1)])
        grad_table, grad_w_in, grad_w_out = table_grad(
            ordered.reshape(-1), first.reshape(-1), dx_all, dw1, dw2, shard_rows, tall
        )
        return (base + other).astype(BF16), grad_table, grad_w_in, grad_w_out

    return jax.shard_map(
        per_device,
        mesh=mesh,
        in_specs=(P(("pod", "data")), P("tensor", None), P(None), P(None, "tensor"), P("tensor", None), tok_spec),
        out_specs=(tok_spec, P(("pod", "tensor"), None), P("pod", "tensor"), P(("pod", "tensor"), None)),
        check_vma=False,
    )
```

```python
import functools

import jax
import jax.numpy as jnp
from jax import lax
from jax.experimental import pallas as pl
from jax.experimental.pallas import tpu as pltpu
from jax.sharding import PartitionSpec as P


NORM_EPS = 1e-6
GELU_A = 0.7978845608028654
GELU_B = 0.044715
MESH = pl.DeviceIdType.MESH
NT = (((1,), (1,)), ((), ()))
TN = (((0,), (0,)), ((), ()))
F32, BF16, I32 = jnp.float32, jnp.bfloat16, jnp.int32
LANES = 128
XQ = 4
PQ = 4

R_IDS, R_DZ, R_DY, R_DC, R_NZ, R_NC, R_XZ, R_XY, R_XC = 0, 4, 8, 12, 16, 24, 28, 36, 44
R_XM, R_X, R_NO, R_PC, R_PY, N_R = 48, 52, 56, 60, 68, 72
S_IDS, S_DZ, S_DY, S_DC, S_NZ, S_NC, S_XZ, S_XY, S_XC = 0, 3, 8, 12, 16, 26, 30, 40, 48
S_XM, S_X, S_NO, S_PC, S_PY, N_S = 52, 56, 60, 64, 72, 76
L_W1, L_W2, L_XM, L_DX, L_YS, L_YB, L_DW, L_DO, N_L = 0, 1, 2, 3, 4, 5, 6, 8, 12


def loop(lo, hi, body):
    def one(j, carry):
        body(j)
        return carry

    lax.fori_loop(lo, hi, one, 0)


def tiles(total, step, body):
    full = total // step
    loop(0, full, lambda j: body(pl.multiple_of(j * step, step), step))
    if total % step:
        body(full * step, total % step)


def rows_loop(total, body):
    loop(0, total // 16, lambda j: body(pl.multiple_of(j * 16, 16)))


def sort_keys(ids, keys, place, ordered, first, shard_rows, tall, rank0):
    reps, per, _ = ids.shape
    count = reps * per * LANES
    t = per * LANES // 4
    shift = t.bit_length() - 1
    lines = reps * per
    lane = lax.broadcasted_iota(I32, (per, LANES), 1)
    spot = lax.broadcasted_iota(I32, (per, LANES), 0) * LANES + lane
    block = jnp.right_shift(spot, shift)
    kept = (block & 1) * (2 * t) + jnp.right_shift(block, 1) * t + (spot & (t - 1))
    for k in range(reps):
        row = ids[k] - rank0
        row = jnp.where((row >= 0) & (row < shard_rows), row, shard_rows)
        keys[k * per : (k + 1) * per, :] = (row * count + (k * per * LANES + kept)).astype(F32)
    place[...] = jnp.zeros_like(place)
    ordered[...] = jnp.zeros_like(ordered)
    up = lax.broadcasted_iota(I32, (LANES, LANES), 0)
    over = lax.broadcasted_iota(I32, (LANES, LANES), 1)
    same = up == over
    overf = over.astype(F32)

    def column(ref, b):
        return jnp.sum(jnp.where(same, jnp.broadcast_to(ref[pl.ds(b, 1), :], (LANES, LANES)), 0.0), axis=1, keepdims=True)

    def count_below(b):
        col = column(keys, b)

        def one(a):
            at = pl.ds(a, 1)
            place[at, :] += jnp.sum(jnp.where(col < keys[at, :], 1.0, 0.0), axis=0, keepdims=True)

        loop(0, lines, one)

    loop(0, lines, count_below)

    def put(b):
        col, spot_of = column(keys, b), column(place, b)

        def one(a):
            want = overf + (a * LANES).astype(F32)
            ordered[pl.ds(a, 1), :] += jnp.sum(jnp.where(spot_of == want, col, 0.0), axis=0, keepdims=True)

        loop(0, lines, one)
        edge = overf * float(tall * count)
        first[...] += jnp.sum(jnp.where(col < edge, 1.0, 0.0), axis=0, keepdims=True)

    first[...] = jnp.zeros_like(first)
    loop(0, lines, put)


def group_kernel(shard_rows, tall, ids_ref, xm_hbm, w1_hbm, w2_hbm, g_ref, do_hbm, do_across, do_below, do_above,
                 base_o, ysum_o, ord_o, first_o, dx_o, far_o, dw1_o, dw2_o,
                 w1, w2, n, d, xm, xc, xy, hs, dus, pd, pf, rd, rf, yd, yb, dxo, idl, keys, place, ordered, first,
                 lsem, ssem, rsem):
    t, m = do_hbm.shape
    f = w1_hbm.shape[1]
    tq, mq = 2 * t // XQ, m // PQ
    z = lax.axis_index("data")
    r = lax.axis_index("tensor")
    y, c = lax.div(r, 2), lax.rem(r, 2)
    partner = {"tensor": 2 * y + 1 - c}
    across = {"tensor": 2 * (1 - y) + c}
    half = lax.div(z, 2)
    inner = z + half * (3 - 2 * z)
    order = [b + half * (3 - 2 * b) for b in (1 - inner, 2, 3)]
    middle, end = inner == 1, inner == 0

    def row(zz, cc, yy=0):
        return pl.multiple_of(zz * (4 * t) + cc * (2 * t) + yy * t, t)

    def blk(ref, zz, cc, yy):
        return ref.at[pl.ds(row(zz, cc, yy), t)]

    def duo(ref, zz, cc):
        return ref.at[pl.ds(row(zz, cc), 2 * t)]

    def remote(src, dst, s, q, dev):
        return pltpu.make_async_remote_copy(
            src_ref=src, dst_ref=dst, send_sem=ssem.at[s], recv_sem=rsem.at[q], device_id=dev, device_id_type=MESH
        )

    def local(src, dst, i):
        return pltpu.make_async_copy(src, dst, lsem.at[i])

    def arrived(ref, q):
        remote(ref, ref, 0, q, partner).wait_recv()

    def start(cp):
        cp.start()

    def sent(cp):
        cp.wait_send()

    def along(src, dst, s, q, act):
        for i, hop in enumerate((1, -1)):
            to = z + hop

            @pl.when((to >= 0) & (to <= 3))
            def _():
                act(remote(src, dst, s + i, q + z, {"data": to}))

    def pass_on(k, ref, s, q, act):
        src, dst = ref if isinstance(ref, tuple) else (ref, ref)
        act(remote(src, dst, s + 2 + k, q + order[k], {"data": order[1] if k == 0 else order[0]}))

    barrier = pltpu.get_barrier_semaphore()
    pl.semaphore_signal(barrier, inc=1, device_id=partner, device_id_type=MESH)
    pl.semaphore_signal(barrier, inc=1, device_id=across, device_id_type=MESH)
    for k in range(3):
        pl.semaphore_signal(barrier, inc=1, device_id={"data": order[k]}, device_id_type=MESH)

    def load_d(act):
        act(local(do_hbm, blk(d, z, c, y), L_DO))
        act(local(do_across, blk(d, z, c, 1 - y), L_DO + 1))
        pl.when(z > 0)(lambda: act(local(do_below, blk(d, z - 1, c, y), L_DO + 2)))
        pl.when(z < 3)(lambda: act(local(do_above, blk(d, z + 1, c, y), L_DO + 3)))

    def local_wait(cp):
        cp.wait()

    local(xm_hbm, xm, L_XM).start()
    load_d(start)
    local(w1_hbm, w1, L_W1).start()
    local(w2_hbm, w2, L_W2).start()
    pl.semaphore_wait(barrier, 5)

    def piece(q):
        return pl.ds(q * tq, tq)

    local(xm_hbm, xm, L_XM).wait()

    def xm_part(q):
        return remote(xm.at[pl.ds(row(0, 1 - c) + q * tq, tq)], xc.at[piece(q)], S_XM + q, R_XM + q, partner)

    def x_part(q):
        return remote(xc.at[piece(q)], xy.at[piece(q)], S_X + q, R_X + q, across)

    def d_got(k):
        arrived(blk(d, order[k], c, y), R_DZ + order[k])

    def d_on(k):
        pass_on(k, blk(d, order[k], c, y), S_DZ, R_DZ, start)

    def d_across(zz, act):
        act(remote(blk(d, zz, c, y), blk(d, zz, c, y), S_DY + zz, R_DY + zz, across))

    def d_pair(zz, act):
        act(remote(duo(d, zz, c), duo(d, zz, c), S_DC + zz, R_DC + zz, partner))

    for q in range(XQ):
        xm_part(q).start()
    for k in range(3):
        remote(ids_ref, idl.at[z], S_IDS + k, R_IDS + z, {"data": order[k]}).start()
    idl[z] = ids_ref[...]
    for q in range(XQ):
        arrived(xc.at[piece(q)], R_XM + q)

        def join(i, q=q):
            at = pl.ds(q * tq + i, 16)
            xc[at, :] += xm[pl.ds(row(0, c) + q * tq + i, 16), :]

        rows_loop(tq, join)
        x_part(q).start()
        if q == 0:
            load_d(local_wait)

            @pl.when(middle)
            def _():
                d_on(0)
                d_on(1)

    d_pair(z, start)

    gain = jnp.concatenate([g_ref[pl.ds(i, 1), :] for i in range(m // LANES)], axis=1).astype(F32)

    def n_own(q, act):
        at = n.at[pl.ds(row(z, c) + q * tq, tq)]
        act(remote(at, at, S_NO + q, R_NO + q, partner))

    def n_along(b, act):
        ref = blk(n, z, c, b)
        along(ref, ref, S_NZ + 5 * b, R_NZ + 4 * b, act)

    for q in range(XQ):
        arrived(xy.at[piece(q)], R_X + q)
        x_part(q).wait_send()

        def norm(i, q=q):
            at = pl.ds(q * tq + i, 16)
            x16 = xc[at, :] + xy[at, :]
            xc[at, :] = x16
            x = x16.astype(F32)
            s = lax.rsqrt(jnp.mean(x * x, axis=-1, keepdims=True) + NORM_EPS)
            n[pl.ds(row(z, c) + q * tq + i, 16), :] = ((x * s) * gain).astype(BF16)

        rows_loop(tq, norm)
        n_own(q, start)
        if q == XQ // 2 - 1:
            n_along(0, start)

            @pl.when(middle)
            def _():
                d_got(2)
                d_on(2)

        if q == XQ - 1:
            n_along(1, start)
    d_across(order[0], start)

    def hidden(zz, slopes):
        at = pl.ds(row(zz, 0), 4 * t)

        def body(off, w):
            to = pl.ds(off, w)
            u = jnp.dot(n[at, :], w1[:, to], preferred_element_type=F32).astype(BF16).astype(F32)
            uu = u * u
            th = jnp.tanh(GELU_A * (u + GELU_B * (uu * u)))
            cdf = 0.5 * (1.0 + th)
            hs[at, to] = (u * cdf).astype(BF16)
            slopes[:, to] = cdf + (0.5 * GELU_A) * u * (1.0 - th * th) * (1.0 + (3.0 * GELU_B) * uu)

        tiles(f, 256, body)

    def grad_hidden(zz, slopes):
        at = pl.ds(row(zz, 0), 4 * t)

        def body(off, w):
            to = pl.ds(off, w)
            dh = lax.dot_general(d[at, :], w2[to, :], NT, preferred_element_type=F32)
            dus[at, to] = (dh * slopes[:, to]).astype(BF16)

        tiles(f, 256, body)

    for q in range(XQ):
        arrived(n.at[pl.ds(row(z, 1 - c) + q * tq, tq)], R_NO + q)
    local(w1_hbm, w1, L_W1).wait()
    hidden(z, pf)
    arrived(duo(d, z, 1 - c), R_DC + z)
    local(w2_hbm, w2, L_W2).wait()
    grad_hidden(z, pf)

    own_rows = pl.ds(row(z, 0), 4 * t)
    far = pl.multiple_of((1 - y) * t, t)

    def cols(q):
        return pl.ds(pl.multiple_of(q * mq, mq), mq)

    def part_pair(src, dst, i, q):
        return remote(src.at[pl.ds(row(0, 1 - c), 2 * t), cols(q)], dst.at[:, cols(q)], S_PC + PQ * i + q, R_PC + PQ * i + q, partner)

    def part_across(q):
        return remote(rd.at[pl.ds(far, t), cols(q)], yd.at[:, cols(q)], S_PY + q, R_PY + q, across)

    def sum_part(part, got, i, q):
        arrived(got.at[:, cols(q)], R_PC + PQ * i + q)

        def add(k):
            got[pl.ds(far + k, 16), cols(q)] += part[pl.ds(row(0, c, 1 - y) + k, 16), cols(q)]

        rows_loop(t, add)

    def dn_part(q):
        pd[:, cols(q)] = lax.dot_general(dus[own_rows, :], w1[cols(q), :], NT, preferred_element_type=F32)
        part_pair(pd, rd, 0, q).start()

    def y_part(q):
        pf[:, cols(q)] = jnp.dot(hs[own_rows, :], w2[:, cols(q)], preferred_element_type=F32)
        part_pair(pf, rf, 1, q).start()

    def dn_out(q):
        sum_part(pd, rd, 0, q)
        part_across(q).start()

    loop(0, PQ, dn_part)
    loop(0, PQ, dn_out)
    loop(0, PQ, y_part)

    @pl.when(end)
    def _():
        d_got(1)

    d_across(order[1], start)

    def n_got(k):
        for b in range(2):
            arrived(blk(n, order[k], c, b), R_NZ + 4 * b + order[k])

    def n_on(k):
        for b in range(2):
            pass_on(k, blk(n, order[k], c, b), S_NZ + 5 * b, R_NZ + 4 * b, start)

    def n_pair(zz, act):
        act(remote(duo(n, zz, c), duo(n, zz, c), S_NC + zz, R_NC + zz, partner))

    n_got(0)
    n_pair(order[0], start)

    @pl.when(middle)
    def _():
        n_on(0)
        n_got(1)
        n_on(1)
        n_pair(order[1], start)

    for k in range(3):
        arrived(idl.at[order[k]], R_IDS + order[k])
    sort_keys(idl, keys, place, ordered, first, shard_rows, tall, r * shard_rows)
    ord_o[...] = ordered[...].astype(I32)
    first_o[...] = first[...].astype(I32)

    for q in range(PQ):
        arrived(yd.at[:, cols(q)], R_PY + q)

    def grad_x(i):
        at, own = pl.ds(i, 16), pl.ds(y * t + i, 16)
        dn = pd[pl.ds(row(0, c, y) + i, 16), :] + rd[own, :] + yd[at, :]
        x = xc[own, :].astype(F32)
        s = lax.rsqrt(jnp.mean(x * x, axis=-1, keepdims=True) + NORM_EPS)
        xh = x * s
        dhat = dn * gain
        dxn = s * (dhat - xh * jnp.mean(dhat * xh, axis=-1, keepdims=True))
        dxo[at, :] = (d[pl.ds(row(z, c, y) + i, 16), :].astype(F32) + dxn).astype(BF16)

    rows_loop(t, grad_x)
    th = t // 2

    def dx_part(zz, yy, h):
        return dx_o.at[pl.ds(pl.multiple_of(row(zz, c, yy) + h * th, th), th)]

    def dx_own(h):
        return dxo.at[pl.ds(h * th, th)]

    def far_part(h):
        return far_o.at[pl.ds(h * th, th)]

    def dx_next(k, h):
        here = dx_part(order[k], y, h)
        return (here, here) if k == 1 else (here if k == 0 else far_part(h), far_part(h))

    def dx_across(zz, src, h, act):
        act(remote(src, dx_part(zz, y, h), S_XY + 4 * h + zz, R_XY + 4 * h + zz, across))

    def dx_along(act):
        for h in range(2):
            along(dx_own(h), dx_part(z, y, h), S_XZ + 5 * h, R_XZ + 4 * h, act)

    def dx_pair(zz, act):
        act(remote(duo(dx_o, zz, c), duo(dx_o, zz, c), S_XC + zz, R_XC + zz, partner))

    def dx_got(k, on):
        zz = order[k]
        for h in range(2):
            arrived(dx_part(zz, y, h) if k < 2 else far_part(h), R_XZ + 4 * h + zz)
            if on:
                pass_on(k, dx_next(k, h), S_XZ + 5 * h, R_XZ + 4 * h, start)
            if k < 2:
                dx_across(zz, dx_part(zz, y, h), h, start)

    def dx_hand(zz):
        for h in range(2):
            arrived(dx_part(zz, 1 - y, h), R_XY + 4 * h + zz)
        dx_pair(zz, start)

    for h in range(2):
        dx_across(z, dx_own(h), h, start)
    local(dxo, blk(dx_o, z, c, y), L_DX).start()

    @pl.when(end)
    def _():
        d_got(2)

    d_across(order[2], start)

    loop(0, PQ, lambda q: sum_part(pf, rf, 1, q))
    y_send = local(rf.at[pl.ds(far, t)], ysum_o, L_YS)
    y_send.start()

    def base(i):
        own = pl.ds(y * t + i, 16)
        yb[pl.ds(i, 16), :] = xc[own, :].astype(F32) + (pf[pl.ds(row(0, c, y) + i, 16), :] + rf[own, :])

    rows_loop(t, base)
    y_keep = local(yb, base_o, L_YB)
    y_keep.start()
    for q in range(PQ):
        part_pair(pd, rd, 0, q).wait_send()

    def unit(k):
        zz = order[k]
        arrived(blk(d, zz, c, 1 - y), R_DY + zz)
        d_pair(zz, start)
        arrived(duo(n, zz, 1 - c), R_NC + zz)
        hidden(zz, pd)
        arrived(duo(d, zz, 1 - c), R_DC + zz)
        grad_hidden(zz, pd)

    def n_rest(k, on):
        n_got(k)
        if on:
            n_on(k)
        n_pair(order[k], start)

    pl.when(middle)(lambda: n_rest(2, True))
    unit(0)
    dx_along(start)
    pl.when(end)(lambda: n_rest(1, False))
    unit(1)

    @pl.when(middle)
    def _():
        dx_got(0, True)
        dx_got(1, True)

    pl.when(end)(lambda: n_rest(2, False))
    unit(2)

    tw = 2 * t

    def stage(i, width):
        return pd.at[pl.ds(pl.multiple_of(lax.rem(i, 2) * tw, tw), tw), pl.ds(0, width)]

    def flush(i, dst):
        return local(stage(i, dst.shape[1]), dst.at[pl.ds(pl.multiple_of(i * tw, tw), tw)], L_DW + lax.rem(i, 2))

    def weight_tile(i, lhs, rhs, dst):
        @pl.when(i >= 2)
        def _():
            flush(i - 2, dst).wait()

        at = pl.ds(pl.multiple_of(i * tw, tw), tw)
        stage(i, dst.shape[1])[...] = lax.dot_general(lhs[:, at], rhs[...], TN, preferred_element_type=F32)
        flush(i, dst).start()

    n1, n2 = m // tw, f // tw
    pl.when(end)(lambda: dx_got(0, False))
    loop(0, n1 // 2, lambda i: weight_tile(i, n, dus, dw1_o))
    pl.when(end)(lambda: dx_got(1, False))
    pl.when(middle)(lambda: dx_got(2, True))
    loop(n1 // 2, n1, lambda i: weight_tile(i, n, dus, dw1_o))
    for i in (n1 - 2, n1 - 1):
        flush(i, dw1_o).wait()
    local(dxo, blk(dx_o, z, c, y), L_DX).wait()
    dx_hand(z)
    dx_hand(order[0])
    loop(0, n2 // 2 + 1, lambda i: weight_tile(i, hs, d, dw2_o))
    loop(n2 // 2 + 1, n2, lambda i: weight_tile(i, hs, d, dw2_o))
    for i in (n2 - 2, n2 - 1):
        flush(i, dw2_o).wait()
    if f % tw:
        rest = pd.at[pl.ds(0, f % tw)]
        rest[...] = lax.dot_general(hs[:, n2 * tw :], d[...], TN, preferred_element_type=F32)
        last = local(rest, dw2_o.at[pl.ds(n2 * tw, f % tw)], L_DW)
        last.start()
    dx_hand(order[1])
    pl.when(end)(lambda: dx_got(2, False))
    if f % tw:
        last.wait()

    y_send.wait()
    y_keep.wait()
    for zz in (z, *order):
        d_pair(zz, sent)
    for k in range(3):
        d_across(order[k], sent)
        n_pair(order[k], sent)
        remote(ids_ref, idl.at[z], S_IDS + k, R_IDS + z, {"data": order[k]}).wait_send()
    dx_along(sent)
    for b in range(2):
        n_along(b, sent)
        dx_across(z, dx_own(b), b, sent)
        for k in range(2):
            dx_across(order[k], dx_part(order[k], y, b), b, sent)

    @pl.when(middle)
    def _():
        for k in range(3):
            pass_on(k, blk(d, order[k], c, y), S_DZ, R_DZ, sent)
            for b in range(2):
                pass_on(k, dx_next(k, b), S_XZ + 5 * b, R_XZ + 4 * b, sent)
                pass_on(k, blk(n, order[k], c, b), S_NZ + 5 * b, R_NZ + 4 * b, sent)

    for q in range(XQ):
        xm_part(q).wait_send()
        n_own(q, sent)
    for q in range(PQ):
        part_pair(pf, rf, 1, q).wait_send()
        part_across(q).wait_send()
    for zz in (z, *order[:2]):
        arrived(duo(dx_o, zz, 1 - c), R_XC + zz)
        dx_pair(zz, sent)


def run_group(ids, xm, w1, w2, gain, d_outs, shard_rows, tall):
    t, m = d_outs[0].shape
    f = w1.shape[1]
    lines = 4 * ids.shape[0]
    any_, vmem = pl.BlockSpec(memory_space=pl.ANY), pl.BlockSpec(memory_space=pltpu.VMEM)
    V = pltpu.VMEM
    sds = jax.ShapeDtypeStruct
    dots = 2 * 4 * t * m * f
    return pl.pallas_call(
        functools.partial(group_kernel, shard_rows, tall),
        out_shape=(
            sds((t, m), F32), sds((t, m), F32), sds((lines, LANES), I32), sds((1, LANES), I32), sds((16 * t, m), BF16),
            sds((t, m), BF16), sds((m, f), F32), sds((f, m), F32),
        ),
        in_specs=[vmem, any_, any_, any_, vmem, any_, any_, any_, any_],
        out_specs=(any_, any_, vmem, vmem, any_, any_, any_, any_),
        scratch_shapes=[
            V((m, f), BF16), V((f, m), BF16), V((16 * t, m), BF16), V((16 * t, m), BF16),
            V((4 * t, m), BF16), V((2 * t, m), BF16), V((2 * t, m), BF16),
            V((16 * t, f), BF16), V((16 * t, f), BF16),
            V((4 * t, m), F32), V((4 * t, m), F32), V((2 * t, m), F32), V((2 * t, m), F32),
            V((t, m), F32), V((t, m), F32),
            V((t, m), BF16), V((4, *ids.shape), I32),
            V((lines, LANES), F32), V((lines, LANES), F32), V((lines, LANES), F32), V((1, LANES), F32),
            pltpu.SemaphoreType.DMA((N_L,)), pltpu.SemaphoreType.DMA((N_S,)), pltpu.SemaphoreType.DMA((N_R,)),
        ],
        compiler_params=pltpu.CompilerParams(collective_id=0, has_side_effects=True, vmem_limit_bytes=67043328),
        cost_estimate=pl.CostEstimate(flops=18 * dots, bytes_accessed=64 * 16 * t * m, transcendentals=16 * t * f),
        name="group_step",
    )(ids, xm, w1, w2, gain, *d_outs)


def lookup_kernel(shard_rows, ids_smem, ids_vmem, table, out_hbm, got, rows, sem, out_sem):
    total, m = out_hbm.shape
    t = total // 4
    per = 32
    chunks = total // per
    r = lax.axis_index("tensor")
    spread = (1 << (shard_rows.bit_length() - 1)) - 1

    def fetch(k):
        def some(j, carry):
            for u in range(8):
                p = k * per + j * 8 + u
                row = ids_smem[jnp.right_shift(p, 7), p & (LANES - 1)]
                near = row - r * shard_rows
                near = jnp.where((near >= 0) & (near < shard_rows), near, row & spread)
                pltpu.make_async_copy(table.at[jnp.right_shift(near, 3)], got.at[p], sem.at[k]).start()
            return carry

        lax.fori_loop(0, per // 8, some, 0)

    loop(0, chunks, fetch)
    spot = lax.broadcasted_iota(I32, (per, 8 * per), 1)
    token = lax.broadcasted_iota(I32, (per, 8 * per), 0)
    same = lax.broadcasted_iota(I32, (LANES, LANES), 0) == lax.broadcasted_iota(I32, (LANES, LANES), 1)

    def line(b):
        ids = ids_vmem[pl.ds(b, 1), :].astype(F32)
        col = jnp.sum(jnp.where(same, jnp.broadcast_to(ids, (LANES, LANES)), 0.0), axis=1, keepdims=True).astype(I32)
        row = col - r * shard_rows
        row = jnp.where((row >= 0) & (row < shard_rows), row & 7, -8 * per)
        for j in range(LANES // per):
            k = b * (LANES // per) + j
            at = pl.ds(pl.multiple_of(k * per, per), per)
            pltpu.make_async_copy(got.at[at], got.at[at], sem.at[k]).wait()
            want = row[j * per : (j + 1) * per] + 8 * token
            chosen = jnp.where(want == spot, 1.0, 0.0).astype(BF16)
            picked = jnp.dot(chosen, got[at].reshape(8 * per, m), preferred_element_type=F32)
            p = k * per
            nat = lax.div(p, t)
            to = pl.multiple_of(lax.rem(nat, 2) * (2 * t) + lax.div(nat, 2) * t + lax.rem(p, t), per)
            rows[pl.ds(to, per), :] = picked.astype(BF16)
            pltpu.make_async_copy(rows.at[pl.ds(to, per)], out_hbm.at[pl.ds(to, per)], out_sem).start()

    loop(0, total // LANES, line)
    pltpu.make_async_copy(rows, out_hbm, out_sem).wait()


def look_up(ids, table):
    shard_rows, m = table.shape
    total = ids.size
    any_ = pl.BlockSpec(memory_space=pl.ANY)
    return pl.pallas_call(
        functools.partial(lookup_kernel, shard_rows),
        out_shape=jax.ShapeDtypeStruct((total, m), BF16),
        in_specs=[pl.BlockSpec(memory_space=pltpu.SMEM), pl.BlockSpec(memory_space=pltpu.VMEM), any_],
        out_specs=any_,
        scratch_shapes=[
            pltpu.VMEM((total, 8, m), BF16), pltpu.VMEM((total, m), BF16),
            pltpu.SemaphoreType.DMA((total // 32,)), pltpu.SemaphoreType.DMA,
        ],
        compiler_params=pltpu.CompilerParams(vmem_limit_bytes=60 << 20),
        cost_estimate=pl.CostEstimate(flops=16 * total * m, bytes_accessed=20 * total * m, transcendentals=0),
        name="look_up",
    )(ids, ids, table.reshape(shard_rows // 8, 8, m))


RING = 6


def pass_kernel(dw1_in, dw2_in, dw1_o, dw2_o, w1, w2, in_sem, w_sem):
    m, f = w1.shape

    def pieces(i, back):
        for k, (src, buf, dst, n) in enumerate(((dw1_in, w1, dw1_o, m // 8), (dw2_in, w2, dw2_o, f // 8))):
            at = pl.ds(pl.multiple_of(i * n, 8), n)
            if back:
                yield pltpu.make_async_copy(buf.at[at], dst.at[at], w_sem)
            else:
                yield pltpu.make_async_copy(src.at[at], buf.at[at], in_sem.at[2 * i + k])

    def fetch(i):
        for cp in pieces(i, False):
            cp.start()

    def put(i):
        for come, go in zip(pieces(i, False), pieces(i, True)):
            come.wait()
            go.start()

    loop(0, 8, fetch)
    loop(0, 8, put)
    pltpu.make_async_copy(w1, dw1_o, w_sem).wait()
    pltpu.make_async_copy(w2, dw2_o, w_sem).wait()


def pass_on_weights(dw1, dw2):
    m, f = dw1.shape
    any_ = pl.BlockSpec(memory_space=pl.ANY)
    return pl.pallas_call(
        pass_kernel,
        out_shape=(jax.ShapeDtypeStruct((m, f), F32), jax.ShapeDtypeStruct((f, m), F32)),
        in_specs=[any_, any_],
        out_specs=[any_, any_],
        scratch_shapes=[
            pltpu.VMEM((m, f), F32), pltpu.VMEM((f, m), F32), pltpu.SemaphoreType.DMA((16,)), pltpu.SemaphoreType.DMA,
        ],
        compiler_params=pltpu.CompilerParams(vmem_limit_bytes=60 << 20),
        cost_estimate=pl.CostEstimate(flops=8000 * m * f, bytes_accessed=16 * m * f, transcendentals=0),
        name="pass_weights",
    )(dw1, dw2)


def table_kernel(tall, key_ref, first_ref, dx_in, far_own, far_across, far_partner, far_both, out_hbm, dxb, dxf, ring, dx_sem, t_sem):
    count, _ = dxb.shape
    t = count // 16
    shift = count.bit_length() - 1
    steps = out_hbm.shape[0] // tall
    z, r = lax.axis_index("data"), lax.axis_index("tensor")
    y, c = lax.div(r, 2), lax.rem(r, 2)
    late = lax.div(z, 2)

    def near(k):
        at = pl.ds(pl.multiple_of(late * (4 * t) + k * (2 * t), t), 2 * t)
        return at, pltpu.make_async_copy(dx_in.at[at], dxb.at[at], dx_sem.at[k])

    def far(k, src, cc, yy):
        at = pl.ds(pl.multiple_of((1 - late) * (12 * t) + cc * (2 * t) + yy * t, t), t)
        return at, pltpu.make_async_copy(src, dxb.at[at], dx_sem.at[6 + k])

    fars = ((far_own, c, y), (far_across, c, 1 - y), (far_partner, 1 - c, y), (far_both, 1 - c, 1 - y))
    loop(0, 6, lambda k: near(k)[1].start())
    for k, what in enumerate(fars):
        far(k, *what)[1].start()

    def widen_piece(at, cp):
        cp.wait()

        def widen(i):
            rows = pl.ds(pl.multiple_of(at.start + i, 16), 16)
            dxf[rows, :] = dxb[rows, :].astype(F32)

        rows_loop(at.size, widen)

    loop(0, 6, lambda k: widen_piece(*near(k)))
    for k, what in enumerate(fars):
        widen_piece(*far(k, *what))

    def tile_out(i):
        slot = lax.rem(i, RING)
        return pltpu.make_async_copy(ring.at[slot], out_hbm.at[pl.ds(pl.multiple_of(i * tall, 8), tall)], t_sem.at[slot])

    def tile(i):
        slot = lax.rem(i, RING)
        here = ring.at[slot]
        pl.when(i >= RING)(lambda: tile_out(i - RING).wait())
        here[...] = jnp.zeros_like(here)

        def add(j, key):
            ahead = key_ref[jnp.minimum(j + 1, count - 1)]
            to = pl.ds(jnp.right_shift(key, shift) - i * tall, 1)
            here[to, :] += dxf[pl.ds(key & (count - 1), 1), :]
            return ahead

        low = first_ref[i]
        lax.fori_loop(low, first_ref[i + 1], add, key_ref[jnp.minimum(low, count - 1)])
        tile_out(i).start()

    loop(0, steps, tile)
    loop(steps - RING, steps, lambda i: tile_out(i).wait())


def table_grad(ordered, first, dx_all, fars, shard_rows, tall):
    count, m = dx_all.shape
    any_ = pl.BlockSpec(memory_space=pl.ANY)
    V, S = pltpu.VMEM, pltpu.SemaphoreType.DMA
    return pl.pallas_call(
        functools.partial(table_kernel, tall),
        out_shape=jax.ShapeDtypeStruct((shard_rows, m), F32),
        grid_spec=pltpu.PrefetchScalarGridSpec(
            num_scalar_prefetch=2,
            grid=(1,),
            in_specs=[any_] * 5,
            out_specs=any_,
            scratch_shapes=[
                V((count, m), BF16), V((count, m), F32), V((RING, tall, m), F32), S((10,)), S((RING,)),
            ],
        ),
        compiler_params=pltpu.CompilerParams(vmem_limit_bytes=60 << 20),
        cost_estimate=pl.CostEstimate(flops=16000 * shard_rows * m // 10, bytes_accessed=4 * shard_rows * m, transcendentals=0),
        name="table_grad",
    )(ordered, first, dx_all, *fars)


def solution(mesh):
    tok_spec = P(("pod", "data", "tensor"), None)

    over_y, over_core = [(0, 2), (1, 3), (2, 0), (3, 1)], [(0, 1), (1, 0), (2, 3), (3, 2)]

    def per_device(token_ids, embed_table, norm_gain, w_in, w_out, d_out):
        shard_rows = embed_table.shape[0]
        tall = next(k for k in (160, 8) if shard_rows % k == 0)
        ids = token_ids.reshape(-1, LANES)
        do_across = lax.ppermute(d_out, "tensor", over_y)
        do_below = lax.ppermute(d_out, "data", [(0, 1), (1, 2), (2, 3)])
        do_above = lax.ppermute(d_out, "data", [(1, 0), (2, 1), (3, 2)])
        masked = look_up(ids, embed_table)
        gain = norm_gain.reshape(-1, LANES)
        base, ysum, ordered, first, dx_all, far, dw1, dw2 = run_group(
            ids, masked, w_in, w_out, gain, (d_out, do_across, do_below, do_above), shard_rows, tall
        )
        far_across = lax.ppermute(far, "tensor", over_y)
        far_partner = lax.ppermute(far, "tensor", over_core)
        other = lax.ppermute(ysum, "tensor", over_y)
        grad_w_in, grad_w_out = pass_on_weights(dw1, dw2)
        far_both = lax.ppermute(far_across, "tensor", over_core)
        fars = (far, far_across, far_partner, far_both)
        grad_table = table_grad(ordered.reshape(-1), first.reshape(-1), dx_all, fars, shard_rows, tall)
        return (base + other).astype(BF16), grad_table, grad_w_in, grad_w_out

    return jax.shard_map(
        per_device,
        mesh=mesh,
        in_specs=(P(("pod", "data")), P("tensor", None), P(None), P(None, "tensor"), P("tensor", None), tok_spec),
        out_specs=(tok_spec, P(("pod", "tensor"), None), P("pod", "tensor"), P(("pod", "tensor"), None)),
        check_vma=False,
    )
```

```python
import functools

import jax
import jax.numpy as jnp
from jax import lax
from jax.experimental import pallas as pl
from jax.experimental.pallas import tpu as pltpu
from jax.sharding import PartitionSpec as P


NORM_EPS = 1e-6
GELU_A = 0.7978845608028654
GELU_B = 0.044715
MESH = pl.DeviceIdType.MESH
NT = (((1,), (1,)), ((), ()))
TN = (((0,), (0,)), ((), ()))
F32, BF16, I32 = jnp.float32, jnp.bfloat16, jnp.int32
LANES = 128
XQ = 4
PQ = 4

R_IDS, R_DZ, R_DY, R_DC, R_NZ, R_NC, R_XZ, R_XY, R_XC = 0, 4, 8, 12, 16, 24, 28, 36, 44
R_XM, R_X, R_NO, R_PC, R_PY, N_R = 48, 52, 56, 60, 68, 72
S_IDS, S_DZ, S_DY, S_DC, S_NZ, S_NC, S_XZ, S_XY, S_XC = 0, 3, 8, 12, 16, 26, 30, 40, 48
S_XM, S_X, S_NO, S_PC, S_PY, N_S = 52, 56, 60, 64, 72, 76
L_W1, L_W2, L_XM, L_DX, L_YS, L_YB, L_DW, L_DO, L_PF, N_L = 0, 1, 2, 3, 4, 5, 6, 8, 9, 11


def loop(lo, hi, body):
    def one(j, carry):
        body(j)
        return carry

    lax.fori_loop(lo, hi, one, 0)


def tiles(total, step, body):
    full = total // step
    loop(0, full, lambda j: body(pl.multiple_of(j * step, step), step))
    if total % step:
        body(full * step, total % step)


def rows_loop(total, body):
    loop(0, total // 16, lambda j: body(pl.multiple_of(j * 16, 16)))


def sort_keys(ids, keys, place, ordered, first, shard_rows, tall, rank0):
    reps, per, _ = ids.shape
    count = reps * per * LANES
    t = per * LANES // 4
    shift = t.bit_length() - 1
    lines = reps * per
    lane = lax.broadcasted_iota(I32, (per, LANES), 1)
    spot = lax.broadcasted_iota(I32, (per, LANES), 0) * LANES + lane
    block = jnp.right_shift(spot, shift)
    kept = (block & 1) * (2 * t) + jnp.right_shift(block, 1) * t + (spot & (t - 1))
    for k in range(reps):
        row = ids[k] - rank0
        row = jnp.where((row >= 0) & (row < shard_rows), row, shard_rows)
        keys[k * per : (k + 1) * per, :] = (row * count + (k * per * LANES + kept)).astype(F32)
    place[...] = jnp.zeros_like(place)
    ordered[...] = jnp.zeros_like(ordered)
    up = lax.broadcasted_iota(I32, (LANES, LANES), 0)
    over = lax.broadcasted_iota(I32, (LANES, LANES), 1)
    same = up == over
    overf = over.astype(F32)

    def column(ref, b):
        return jnp.sum(jnp.where(same, jnp.broadcast_to(ref[pl.ds(b, 1), :], (LANES, LANES)), 0.0), axis=1, keepdims=True)

    def count_below(b):
        col = column(keys, b)

        def one(a):
            at = pl.ds(a, 1)
            place[at, :] += jnp.sum(jnp.where(col < keys[at, :], 1.0, 0.0), axis=0, keepdims=True)

        loop(0, lines, one)

    loop(0, lines, count_below)

    def put(b):
        col, spot_of = column(keys, b), column(place, b)

        def one(a):
            want = overf + (a * LANES).astype(F32)
            ordered[pl.ds(a, 1), :] += jnp.sum(jnp.where(spot_of == want, col, 0.0), axis=0, keepdims=True)

        loop(0, lines, one)
        edge = overf * float(tall * count)
        first[...] += jnp.sum(jnp.where(col < edge, 1.0, 0.0), axis=0, keepdims=True)

    first[...] = jnp.zeros_like(first)
    loop(0, lines, put)


def group_kernel(shard_rows, tall, ids_ref, xm_hbm, w1_hbm, w2_hbm, g_ref, do_hbm,
                 base_o, ysum_o, ord_o, first_o, dx_o, far_o, farx_o, dw1_o, dw2_o,
                 w1, w2, n, d, xm, xc, xy, hs, dus, pd, pf, rd, rf, yd, yb, dxo, idl, keys, place, ordered, first,
                 lsem, ssem, rsem):
    t, m = do_hbm.shape
    f = w1_hbm.shape[1]
    tq, mq = 2 * t // XQ, m // PQ
    z = lax.axis_index("data")
    r = lax.axis_index("tensor")
    y, c = lax.div(r, 2), lax.rem(r, 2)
    partner = {"tensor": 2 * y + 1 - c}
    across = {"tensor": 2 * (1 - y) + c}
    half = lax.div(z, 2)
    inner = z + half * (3 - 2 * z)
    order = [b + half * (3 - 2 * b) for b in (1 - inner, 2, 3)]
    middle, end = inner == 1, inner == 0

    def row(zz, cc, yy=0):
        return pl.multiple_of(zz * (4 * t) + cc * (2 * t) + yy * t, t)

    def blk(ref, zz, cc, yy):
        return ref.at[pl.ds(row(zz, cc, yy), t)]

    def duo(ref, zz, cc):
        return ref.at[pl.ds(row(zz, cc), 2 * t)]

    def remote(src, dst, s, q, dev):
        return pltpu.make_async_remote_copy(
            src_ref=src, dst_ref=dst, send_sem=ssem.at[s], recv_sem=rsem.at[q], device_id=dev, device_id_type=MESH
        )

    def local(src, dst, i):
        return pltpu.make_async_copy(src, dst, lsem.at[i])

    def arrived(ref, q):
        remote(ref, ref, 0, q, partner).wait_recv()

    def start(cp):
        cp.start()

    def sent(cp):
        cp.wait_send()

    def along(src, dst, s, q, act):
        for i, hop in enumerate((1, -1)):
            to = z + hop

            @pl.when((to >= 0) & (to <= 3))
            def _():
                act(remote(src, dst, s + i, q + z, {"data": to}))

    def pass_on(k, ref, s, q, act):
        src, dst = ref if isinstance(ref, tuple) else (ref, ref)
        act(remote(src, dst, s + 2 + k, q + order[k], {"data": order[1] if k == 0 else order[0]}))

    barrier = pltpu.get_barrier_semaphore()
    pl.semaphore_signal(barrier, inc=1, device_id=partner, device_id_type=MESH)
    pl.semaphore_signal(barrier, inc=1, device_id=across, device_id_type=MESH)
    for k in range(3):
        pl.semaphore_signal(barrier, inc=1, device_id={"data": order[k]}, device_id_type=MESH)

    own_d = blk(d, z, c, y)
    local(do_hbm, own_d, L_DO).start()
    local(xm_hbm, xm, L_XM).start()
    local(w1_hbm, w1, L_W1).start()
    local(w2_hbm, w2, L_W2).start()
    pl.semaphore_wait(barrier, 5)

    def piece(q):
        return pl.ds(q * tq, tq)

    local(do_hbm, own_d, L_DO).wait()
    along(own_d, own_d, S_DZ, R_DZ, start)
    local(xm_hbm, xm, L_XM).wait()

    def xm_part(q):
        return remote(xm.at[pl.ds(row(0, 1 - c) + q * tq, tq)], xc.at[piece(q)], S_XM + q, R_XM + q, partner)

    def x_part(q):
        return remote(xc.at[piece(q)], xy.at[piece(q)], S_X + q, R_X + q, across)

    def d_got(k):
        arrived(blk(d, order[k], c, y), R_DZ + order[k])

    def d_on(k):
        pass_on(k, blk(d, order[k], c, y), S_DZ, R_DZ, start)

    def d_across(zz, act):
        act(remote(blk(d, zz, c, y), blk(d, zz, c, y), S_DY + zz, R_DY + zz, across))

    def d_pair(zz, act):
        act(remote(duo(d, zz, c), duo(d, zz, c), S_DC + zz, R_DC + zz, partner))

    for q in range(XQ):
        xm_part(q).start()
    for k in range(3):
        remote(ids_ref, idl.at[z], S_IDS + k, R_IDS + z, {"data": order[k]}).start()
    idl[z] = ids_ref[...]
    for q in range(XQ):
        arrived(xc.at[piece(q)], R_XM + q)

        def join(i, q=q):
            at = pl.ds(q * tq + i, 16)
            xc[at, :] += xm[pl.ds(row(0, c) + q * tq + i, 16), :]

        rows_loop(tq, join)
        x_part(q).start()
    d_across(z, start)
    d_got(0)

    @pl.when(middle)
    def _():
        d_on(0)
        d_got(1)
        d_on(1)

    gain = jnp.concatenate([g_ref[pl.ds(i, 1), :] for i in range(m // LANES)], axis=1).astype(F32)

    def n_own(q, act):
        at = n.at[pl.ds(row(z, c) + q * tq, tq)]
        act(remote(at, at, S_NO + q, R_NO + q, partner))

    def n_along(b, act):
        ref = blk(n, z, c, b)
        along(ref, ref, S_NZ + 5 * b, R_NZ + 4 * b, act)

    for q in range(XQ):
        arrived(xy.at[piece(q)], R_X + q)
        x_part(q).wait_send()

        def norm(i, q=q):
            at = pl.ds(q * tq + i, 16)
            x16 = xc[at, :] + xy[at, :]
            xc[at, :] = x16
            x = x16.astype(F32)
            s = lax.rsqrt(jnp.mean(x * x, axis=-1, keepdims=True) + NORM_EPS)
            n[pl.ds(row(z, c) + q * tq + i, 16), :] = ((x * s) * gain).astype(BF16)

        rows_loop(tq, norm)
        n_own(q, start)
        if q == XQ // 2 - 1:
            n_along(0, start)

            @pl.when(middle)
            def _():
                d_got(2)
                d_on(2)

        if q == XQ - 1:
            n_along(1, start)
    d_across(order[0], start)

    def hidden(zz, slopes):
        at = pl.ds(row(zz, 0), 4 * t)

        def body(off, w):
            to = pl.ds(off, w)
            u = jnp.dot(n[at, :], w1[:, to], preferred_element_type=F32).astype(BF16).astype(F32)
            uu = u * u
            th = jnp.tanh(GELU_A * (u + GELU_B * (uu * u)))
            cdf = 0.5 * (1.0 + th)
            hs[at, to] = (u * cdf).astype(BF16)
            slopes[:, to] = cdf + (0.5 * GELU_A) * u * (1.0 - th * th) * (1.0 + (3.0 * GELU_B) * uu)

        tiles(f, 256, body)

    def grad_hidden(zz, slopes):
        at = pl.ds(row(zz, 0), 4 * t)

        def body(off, w):
            to = pl.ds(off, w)
            dh = lax.dot_general(d[at, :], w2[to, :], NT, preferred_element_type=F32)
            dus[at, to] = (dh * slopes[:, to]).astype(BF16)

        tiles(f, 256, body)

    for q in range(XQ):
        arrived(n.at[pl.ds(row(z, 1 - c) + q * tq, tq)], R_NO + q)
    local(w1_hbm, w1, L_W1).wait()
    hidden(z, pf)
    arrived(blk(d, z, c, 1 - y), R_DY + z)
    d_pair(z, start)
    arrived(duo(d, z, 1 - c), R_DC + z)
    local(w2_hbm, w2, L_W2).wait()
    grad_hidden(z, pf)

    own_rows = pl.ds(row(z, 0), 4 * t)
    far = pl.multiple_of((1 - y) * t, t)

    def cols(q):
        return pl.ds(pl.multiple_of(q * mq, mq), mq)

    def part_pair(src, dst, i, q):
        return remote(src.at[pl.ds(row(0, 1 - c), 2 * t), cols(q)], dst.at[:, cols(q)], S_PC + PQ * i + q, R_PC + PQ * i + q, partner)

    def part_across(q):
        return remote(rd.at[pl.ds(far, t), cols(q)], yd.at[:, cols(q)], S_PY + q, R_PY + q, across)

    def sum_part(part, got, i, q):
        arrived(got.at[:, cols(q)], R_PC + PQ * i + q)

        def add(k):
            got[pl.ds(far + k, 16), cols(q)] += part[pl.ds(row(0, c, 1 - y) + k, 16), cols(q)]

        rows_loop(t, add)

    def dn_part(q):
        pd[:, cols(q)] = lax.dot_general(dus[own_rows, :], w1[cols(q), :], NT, preferred_element_type=F32)
        part_pair(pd, rd, 0, q).start()

    def y_part(q):
        pf[:, cols(q)] = jnp.dot(hs[own_rows, :], w2[:, cols(q)], preferred_element_type=F32)
        part_pair(pf, rf, 1, q).start()

    def dn_out(q):
        sum_part(pd, rd, 0, q)
        part_across(q).start()

    loop(0, PQ, dn_part)
    loop(0, PQ, dn_out)
    loop(0, PQ, y_part)

    @pl.when(end)
    def _():
        d_got(1)

    d_across(order[1], start)

    def n_got(k):
        for b in range(2):
            arrived(blk(n, order[k], c, b), R_NZ + 4 * b + order[k])

    def n_on(k):
        for b in range(2):
            pass_on(k, blk(n, order[k], c, b), S_NZ + 5 * b, R_NZ + 4 * b, start)

    def n_pair(zz, act):
        act(remote(duo(n, zz, c), duo(n, zz, c), S_NC + zz, R_NC + zz, partner))

    n_got(0)
    n_pair(order[0], start)

    @pl.when(middle)
    def _():
        n_on(0)
        n_got(1)
        n_on(1)
        n_pair(order[1], start)

    for k in range(3):
        arrived(idl.at[order[k]], R_IDS + order[k])
    sort_keys(idl, keys, place, ordered, first, shard_rows, tall, r * shard_rows)
    ord_o[...] = ordered[...].astype(I32)
    first_o[...] = first[...].astype(I32)

    for q in range(PQ):
        arrived(yd.at[:, cols(q)], R_PY + q)

    def grad_x(i):
        at, own = pl.ds(i, 16), pl.ds(y * t + i, 16)
        dn = pd[pl.ds(row(0, c, y) + i, 16), :] + rd[own, :] + yd[at, :]
        x = xc[own, :].astype(F32)
        s = lax.rsqrt(jnp.mean(x * x, axis=-1, keepdims=True) + NORM_EPS)
        xh = x * s
        dhat = dn * gain
        dxn = s * (dhat - xh * jnp.mean(dhat * xh, axis=-1, keepdims=True))
        dxo[at, :] = (d[pl.ds(row(z, c, y) + i, 16), :].astype(F32) + dxn).astype(BF16)

    rows_loop(t, grad_x)
    th = t // 2

    def dx_part(zz, yy, h):
        return dx_o.at[pl.ds(pl.multiple_of(row(zz, c, yy) + h * th, th), th)]

    def dx_own(h):
        return dxo.at[pl.ds(h * th, th)]

    def far_part(h):
        return far_o.at[pl.ds(h * th, th)]

    def dx_next(k, h):
        here = dx_part(order[k], y, h)
        return (here, here) if k == 1 else (here if k == 0 else far_part(h), far_part(h))

    def far_out(act):
        act(remote(far_part(0), farx_o, S_XY + order[2], R_XY + order[2], across))

    def dx_across(zz, src, h, act):
        act(remote(src, dx_part(zz, y, h), S_XY + 4 * h + zz, R_XY + 4 * h + zz, across))

    def dx_along(act):
        for h in range(2):
            along(dx_own(h), dx_part(z, y, h), S_XZ + 5 * h, R_XZ + 4 * h, act)

    def dx_pair(zz, act):
        act(remote(duo(dx_o, zz, c), duo(dx_o, zz, c), S_XC + zz, R_XC + zz, partner))

    def dx_got(k, on):
        zz = order[k]
        for h in range(2):
            arrived(dx_part(zz, y, h) if k < 2 else far_part(h), R_XZ + 4 * h + zz)
            if on:
                pass_on(k, dx_next(k, h), S_XZ + 5 * h, R_XZ + 4 * h, start)
            if k < 2:
                dx_across(zz, dx_part(zz, y, h), h, start)
            elif h == 0:
                far_out(start)

    def dx_hand(zz):
        for h in range(2):
            arrived(dx_part(zz, 1 - y, h), R_XY + 4 * h + zz)
        dx_pair(zz, start)

    for h in range(2):
        dx_across(z, dx_own(h), h, start)
    local(dxo, blk(dx_o, z, c, y), L_DX).start()

    @pl.when(end)
    def _():
        d_got(2)

    d_across(order[2], start)

    loop(0, PQ, lambda q: sum_part(pf, rf, 1, q))
    y_send = local(rf.at[pl.ds(far, t)], ysum_o, L_YS)
    y_send.start()

    def base(i):
        own = pl.ds(y * t + i, 16)
        yb[pl.ds(i, 16), :] = xc[own, :].astype(F32) + (pf[pl.ds(row(0, c, y) + i, 16), :] + rf[own, :])

    rows_loop(t, base)
    y_keep = local(yb, base_o, L_YB)
    y_keep.start()
    for q in range(PQ):
        part_pair(pd, rd, 0, q).wait_send()
        part_pair(pf, rf, 1, q).wait_send()

    def unit(k):
        zz = order[k]
        arrived(blk(d, zz, c, 1 - y), R_DY + zz)
        d_pair(zz, start)
        arrived(duo(n, zz, 1 - c), R_NC + zz)
        hidden(zz, pd)
        arrived(duo(d, zz, 1 - c), R_DC + zz)
        grad_hidden(zz, pd)

    def n_rest(k, on):
        n_got(k)
        if on:
            n_on(k)
        n_pair(order[k], start)

    pl.when(middle)(lambda: n_rest(2, True))
    unit(0)
    dx_along(start)
    pl.when(end)(lambda: n_rest(1, False))
    unit(1)

    @pl.when(middle)
    def _():
        dx_got(0, True)
        dx_got(1, True)

    tw = 2 * t
    n1 = m // tw
    late_rows = pl.ds(row(order[2], 0), 4 * t)
    early_rows = pl.ds(pl.multiple_of(half * (4 * t), 4 * t), 12 * t)

    def w_at(i):
        return pl.ds(pl.multiple_of(i * tw, tw), tw)

    def slot(s):
        return pf.at[pl.ds(s * tw, tw), pl.ds(0, f)]

    def w1_tile(i, s, back):
        here, there = slot(s), dw1_o.at[w_at(i)]
        return local(here, there, L_PF + s) if back else local(there, here, L_PF + s)

    def early(j):
        for s in range(2):
            i = 2 * j + s
            pl.when(j >= 1)(lambda s=s, i=i: w1_tile(i - 2, s, True).wait())
            slot(s)[...] = lax.dot_general(n[early_rows, w_at(i)], dus[early_rows, :], TN, preferred_element_type=F32)
            w1_tile(i, s, True).start()

    loop(0, n1 // 2, early)
    for s in range(2):
        w1_tile(n1 - 2 + s, s, True).wait()
    pl.when(end)(lambda: n_rest(2, False))
    unit(2)

    def both(j):
        for s in range(2):
            i = 2 * j + s
            pl.when(j >= 1)(lambda s=s, i=i: w1_tile(i - 2, s, True).wait())
            w1_tile(i, s, False).start()
        weight_tile(j)
        for s in range(2):
            i = 2 * j + s
            w1_tile(i, s, False).wait()
            slot(s)[...] += lax.dot_general(n[late_rows, w_at(i)], dus[late_rows, :], TN, preferred_element_type=F32)
            w1_tile(i, s, True).start()

    def weight_tile(i):
        pl.when(i >= 2)(lambda: flush(i - 2).wait())
        stage(i)[...] = lax.dot_general(hs[:, w_at(i)], d[...], TN, preferred_element_type=F32)
        flush(i).start()

    def stage(i):
        return pd.at[pl.ds(pl.multiple_of(lax.rem(i, 2) * tw, tw), tw)]

    def flush(i):
        return local(stage(i), dw2_o.at[w_at(i)], L_DW + lax.rem(i, 2))

    n2, paired = f // tw, n1 // 2
    steps = min(n2, paired)
    pl.when(end)(lambda: dx_got(0, False))
    pl.when(middle)(lambda: dx_got(2, True))
    loop(0, steps // 2, both)
    pl.when(end)(lambda: dx_got(1, False))
    loop(steps // 2, steps, both)
    local(dxo, blk(dx_o, z, c, y), L_DX).wait()
    dx_hand(z)
    dx_hand(order[0])
    loop(steps, n2, weight_tile)
    for i in (n2 - 2, n2 - 1):
        flush(i).wait()
    if f % tw:
        rest = pd.at[pl.ds(0, f % tw)]
        rest[...] = lax.dot_general(hs[:, n2 * tw :], d[...], TN, preferred_element_type=F32)
        last = local(rest, dw2_o.at[pl.ds(n2 * tw, f % tw)], L_DW)
        last.start()
    dx_hand(order[1])
    pl.when(end)(lambda: dx_got(2, False))
    if f % tw:
        last.wait()
    for s in range(2):
        w1_tile(2 * paired - 2 + s, s, True).wait()

    y_send.wait()
    y_keep.wait()
    along(own_d, own_d, S_DZ, R_DZ, sent)
    for zz in (z, *order):
        d_across(zz, sent)
        d_pair(zz, sent)
    for k in range(3):
        n_pair(order[k], sent)
        remote(ids_ref, idl.at[z], S_IDS + k, R_IDS + z, {"data": order[k]}).wait_send()
    dx_along(sent)
    for b in range(2):
        n_along(b, sent)
        dx_across(z, dx_own(b), b, sent)
        for k in range(2):
            dx_across(order[k], dx_part(order[k], y, b), b, sent)

    @pl.when(middle)
    def _():
        for k in range(3):
            pass_on(k, blk(d, order[k], c, y), S_DZ, R_DZ, sent)
            for b in range(2):
                pass_on(k, dx_next(k, b), S_XZ + 5 * b, R_XZ + 4 * b, sent)
                pass_on(k, blk(n, order[k], c, b), S_NZ + 5 * b, R_NZ + 4 * b, sent)

    for q in range(XQ):
        xm_part(q).wait_send()
        n_own(q, sent)
    for q in range(PQ):
        part_across(q).wait_send()
    arrived(farx_o, R_XY + order[2])
    far_out(sent)
    for zz in (z, *order[:2]):
        arrived(duo(dx_o, zz, 1 - c), R_XC + zz)
        dx_pair(zz, sent)


def run_group(ids, xm, w1, w2, gain, d_out, shard_rows, tall):
    t, m = d_out.shape
    f = w1.shape[1]
    lines = 4 * ids.shape[0]
    any_, vmem = pl.BlockSpec(memory_space=pl.ANY), pl.BlockSpec(memory_space=pltpu.VMEM)
    V = pltpu.VMEM
    sds = jax.ShapeDtypeStruct
    dots = 2 * 4 * t * m * f
    return pl.pallas_call(
        functools.partial(group_kernel, shard_rows, tall),
        out_shape=(
            sds((t, m), F32), sds((t, m), F32), sds((lines, LANES), I32), sds((1, LANES), I32), sds((16 * t, m), BF16),
            sds((t, m), BF16), sds((t // 2, m), BF16), sds((m, f), F32), sds((f, m), F32),
        ),
        in_specs=[vmem, any_, any_, any_, vmem, any_],
        out_specs=(any_, any_, vmem, vmem, any_, any_, any_, any_, any_),
        scratch_shapes=[
            V((m, f), BF16), V((f, m), BF16), V((16 * t, m), BF16), V((16 * t, m), BF16),
            V((4 * t, m), BF16), V((2 * t, m), BF16), V((2 * t, m), BF16),
            V((16 * t, f), BF16), V((16 * t, f), BF16),
            V((4 * t, m), F32), V((4 * t, m), F32), V((2 * t, m), F32), V((2 * t, m), F32),
            V((t, m), F32), V((t, m), F32),
            V((t, m), BF16), V((4, *ids.shape), I32),
            V((lines, LANES), F32), V((lines, LANES), F32), V((lines, LANES), F32), V((1, LANES), F32),
            pltpu.SemaphoreType.DMA((N_L,)), pltpu.SemaphoreType.DMA((N_S,)), pltpu.SemaphoreType.DMA((N_R,)),
        ],
        compiler_params=pltpu.CompilerParams(collective_id=0, has_side_effects=True, vmem_limit_bytes=67043328),
        cost_estimate=pl.CostEstimate(flops=18 * dots, bytes_accessed=64 * 16 * t * m, transcendentals=16 * t * f),
        name="group_step",
    )(ids, xm, w1, w2, gain, d_out)


def lookup_kernel(shard_rows, ids_smem, ids_vmem, table, out_hbm, got, rows, sem, out_sem):
    total, m = out_hbm.shape
    t = total // 4
    per = 32
    chunks = total // per
    r = lax.axis_index("tensor")
    spread = (1 << (shard_rows.bit_length() - 1)) - 1

    def fetch(k):
        def some(j, carry):
            for u in range(8):
                p = k * per + j * 8 + u
                row = ids_smem[jnp.right_shift(p, 7), p & (LANES - 1)]
                near = row - r * shard_rows
                near = jnp.where((near >= 0) & (near < shard_rows), near, row & spread)
                pltpu.make_async_copy(table.at[jnp.right_shift(near, 3)], got.at[p], sem.at[k]).start()
            return carry

        lax.fori_loop(0, per // 8, some, 0)

    loop(0, chunks, fetch)
    spot = lax.broadcasted_iota(I32, (per, 8 * per), 1)
    token = lax.broadcasted_iota(I32, (per, 8 * per), 0)
    same = lax.broadcasted_iota(I32, (LANES, LANES), 0) == lax.broadcasted_iota(I32, (LANES, LANES), 1)

    def line(b):
        ids = ids_vmem[pl.ds(b, 1), :].astype(F32)
        col = jnp.sum(jnp.where(same, jnp.broadcast_to(ids, (LANES, LANES)), 0.0), axis=1, keepdims=True).astype(I32)
        row = col - r * shard_rows
        row = jnp.where((row >= 0) & (row < shard_rows), row & 7, -8 * per)
        for j in range(LANES // per):
            k = b * (LANES // per) + j
            at = pl.ds(pl.multiple_of(k * per, per), per)
            pltpu.make_async_copy(got.at[at], got.at[at], sem.at[k]).wait()
            want = row[j * per : (j + 1) * per] + 8 * token
            chosen = jnp.where(want == spot, 1.0, 0.0).astype(BF16)
            picked = jnp.dot(chosen, got[at].reshape(8 * per, m), preferred_element_type=F32)
            p = k * per
            nat = lax.div(p, t)
            to = pl.multiple_of(lax.rem(nat, 2) * (2 * t) + lax.div(nat, 2) * t + lax.rem(p, t), per)
            rows[pl.ds(to, per), :] = picked.astype(BF16)
            pltpu.make_async_copy(rows.at[pl.ds(to, per)], out_hbm.at[pl.ds(to, per)], out_sem).start()

    loop(0, total // LANES, line)
    pltpu.make_async_copy(rows, out_hbm, out_sem).wait()


def look_up(ids, table):
    shard_rows, m = table.shape
    total = ids.size
    any_ = pl.BlockSpec(memory_space=pl.ANY)
    return pl.pallas_call(
        functools.partial(lookup_kernel, shard_rows),
        out_shape=jax.ShapeDtypeStruct((total, m), BF16),
        in_specs=[pl.BlockSpec(memory_space=pltpu.SMEM), pl.BlockSpec(memory_space=pltpu.VMEM), any_],
        out_specs=any_,
        scratch_shapes=[
            pltpu.VMEM((total, 8, m), BF16), pltpu.VMEM((total, m), BF16),
            pltpu.SemaphoreType.DMA((total // 32,)), pltpu.SemaphoreType.DMA,
        ],
        compiler_params=pltpu.CompilerParams(vmem_limit_bytes=60 << 20),
        cost_estimate=pl.CostEstimate(flops=16 * total * m, bytes_accessed=20 * total * m, transcendentals=0),
        name="look_up",
    )(ids, ids, table.reshape(shard_rows // 8, 8, m))


RING = 6


def pass_pieces(src, buf, dst, in_sem, out_sem):
    rows = src.shape[0] // 8

    def fetch(i):
        at = pl.ds(pl.multiple_of(i * rows, 8), rows)
        return pltpu.make_async_copy(src.at[at], buf.at[at], in_sem.at[i])

    def put(i):
        at = pl.ds(pl.multiple_of(i * rows, 8), rows)
        return pltpu.make_async_copy(buf.at[at], dst.at[at], out_sem)

    def step(i):
        fetch(i).wait()
        put(i).start()

    return lambda i: fetch(i).start(), step, lambda: pltpu.make_async_copy(buf, dst, out_sem).wait()


def pass_kernel(src, dst, buf, in_sem, out_sem):
    fetch, step, drain = pass_pieces(src, buf, dst, in_sem, out_sem)
    loop(0, 8, fetch)
    loop(0, 8, step)
    drain()


def pass_on(w):
    any_ = pl.BlockSpec(memory_space=pl.ANY)
    return pl.pallas_call(
        pass_kernel,
        out_shape=jax.ShapeDtypeStruct(w.shape, w.dtype),
        in_specs=[any_],
        out_specs=any_,
        scratch_shapes=[pltpu.VMEM(w.shape, w.dtype), pltpu.SemaphoreType.DMA((8,)), pltpu.SemaphoreType.DMA],
        compiler_params=pltpu.CompilerParams(vmem_limit_bytes=60 << 20),
        cost_estimate=pl.CostEstimate(flops=8000 * w.size, bytes_accessed=8 * w.size, transcendentals=0),
        name="pass_weights",
    )(w)


def table_kernel(tall, key_ref, first_ref, w_in, dx_in, far_own, far_x0, far_x1, far_partner, far_b0, far_b1,
                 out_hbm, w_out, dxb, dxf, ring, w_buf, dx_sem, t_sem, in_sem, out_sem):
    count, _ = dxb.shape
    t = count // 16
    shift = count.bit_length() - 1
    steps = out_hbm.shape[0] // tall
    z, r = lax.axis_index("data"), lax.axis_index("tensor")
    y, c = lax.div(r, 2), lax.rem(r, 2)
    late = lax.div(z, 2)
    w_fetch, w_step, w_drain = pass_pieces(w_in, w_buf, w_out, in_sem, out_sem)

    def near(k):
        at = pl.ds(pl.multiple_of(late * (4 * t) + k * (2 * t), t), 2 * t)
        return at, pltpu.make_async_copy(dx_in.at[at], dxb.at[at], dx_sem.at[k])

    def far(k, src, cc, yy, h):
        n = src.shape[0]
        at = pl.ds(pl.multiple_of((1 - late) * (12 * t) + cc * (2 * t) + yy * t + h * n, n), n)
        return at, pltpu.make_async_copy(src, dxb.at[at], dx_sem.at[6 + k])

    fars = (
        (far_own, c, y, 0), (far_partner, 1 - c, y, 0), (far_x0, c, 1 - y, 0), (far_b0, 1 - c, 1 - y, 0),
        (far_x1, c, 1 - y, 1), (far_b1, 1 - c, 1 - y, 1),
    )
    loop(0, 6, lambda k: near(k)[1].start())
    for k, what in enumerate(fars):
        far(k, *what)[1].start()
    loop(0, 8, w_fetch)

    def widen_piece(at, cp):
        cp.wait()

        def widen(i):
            rows = pl.ds(pl.multiple_of(at.start + i, 16), 16)
            dxf[rows, :] = dxb[rows, :].astype(F32)

        rows_loop(at.size, widen)

    loop(0, 6, lambda k: widen_piece(*near(k)))
    for k, what in enumerate(fars):
        widen_piece(*far(k, *what))

    def tile_out(i):
        slot = lax.rem(i, RING)
        return pltpu.make_async_copy(ring.at[slot], out_hbm.at[pl.ds(pl.multiple_of(i * tall, 8), tall)], t_sem.at[slot])

    def tile(i):
        slot = lax.rem(i, RING)
        here = ring.at[slot]
        pl.when(i >= RING)(lambda: tile_out(i - RING).wait())
        here[...] = jnp.zeros_like(here)

        def add(j, key):
            ahead = key_ref[jnp.minimum(j + 1, count - 1)]
            to = pl.ds(jnp.right_shift(key, shift) - i * tall, 1)
            here[to, :] += dxf[pl.ds(key & (count - 1), 1), :]
            return ahead

        low = first_ref[i]
        lax.fori_loop(low, first_ref[i + 1], add, key_ref[jnp.minimum(low, count - 1)])
        tile_out(i).start()
        pl.when(i < 8)(lambda: w_step(i))

    loop(0, steps, tile)
    loop(steps - RING, steps, lambda i: tile_out(i).wait())
    w_drain()


def table_grad(ordered, first, w, dx_all, fars, shard_rows, tall):
    count, m = dx_all.shape
    any_ = pl.BlockSpec(memory_space=pl.ANY)
    V, S = pltpu.VMEM, pltpu.SemaphoreType.DMA
    return pl.pallas_call(
        functools.partial(table_kernel, tall),
        out_shape=(jax.ShapeDtypeStruct((shard_rows, m), F32), jax.ShapeDtypeStruct(w.shape, F32)),
        grid_spec=pltpu.PrefetchScalarGridSpec(
            num_scalar_prefetch=2,
            grid=(1,),
            in_specs=[any_] * 8,
            out_specs=[any_] * 2,
            scratch_shapes=[
                V((count, m), BF16), V((count, m), F32), V((RING, tall, m), F32), V(w.shape, F32),
                S((12,)), S((RING,)), S((8,)), S,
            ],
        ),
        compiler_params=pltpu.CompilerParams(vmem_limit_bytes=60 << 20),
        cost_estimate=pl.CostEstimate(flops=1600 * shard_rows * m, bytes_accessed=4 * shard_rows * m, transcendentals=0),
        name="table_grad",
    )(ordered, first, w, dx_all, *fars)


def solution(mesh):
    tok_spec = P(("pod", "data", "tensor"), None)

    over_y, over_core = [(0, 2), (1, 3), (2, 0), (3, 1)], [(0, 1), (1, 0), (2, 3), (3, 2)]

    def per_device(token_ids, embed_table, norm_gain, w_in, w_out, d_out):
        shard_rows = embed_table.shape[0]
        tall = next(k for k in (160, 8) if shard_rows % k == 0)
        ids = token_ids.reshape(-1, LANES)
        masked = look_up(ids, embed_table)
        gain = norm_gain.reshape(-1, LANES)
        base, ysum, ordered, first, dx_all, far, far_x0, dw1, dw2 = run_group(
            ids, masked, w_in, w_out, gain, d_out, shard_rows, tall
        )
        late = far[far.shape[0] // 2 :]
        far_x1 = lax.ppermute(late, "tensor", over_y)
        far_partner = lax.ppermute(far, "tensor", over_core)
        far_b0 = lax.ppermute(far_x0, "tensor", over_core)
        other = lax.ppermute(ysum, "tensor", over_y)
        grad_w_in = pass_on(dw1)
        far_b1 = lax.ppermute(far_x1, "tensor", over_core)
        fars = (far, far_x0, far_x1, far_partner, far_b0, far_b1)
        grad_table, grad_w_out = table_grad(ordered.reshape(-1), first.reshape(-1), dw2, dx_all, fars, shard_rows, tall)
        return (base + other).astype(BF16), grad_table, grad_w_in, grad_w_out

    return jax.shard_map(
        per_device,
        mesh=mesh,
        in_specs=(P(("pod", "data")), P("tensor", None), P(None), P(None, "tensor"), P("tensor", None), tok_spec),
        out_specs=(tok_spec, P(("pod", "tensor"), None), P("pod", "tensor"), P(("pod", "tensor"), None)),
        check_vma=False,
    )
```

```python
import functools

import jax
import jax.numpy as jnp
from jax import lax
from jax.experimental import pallas as pl
from jax.experimental.pallas import tpu as pltpu
from jax.sharding import PartitionSpec as P


NORM_EPS = 1e-6
GELU_A = 0.7978845608028654
GELU_B = 0.044715
MESH = pl.DeviceIdType.MESH
NT = (((1,), (1,)), ((), ()))
TN = (((0,), (0,)), ((), ()))
F32, BF16, I32 = jnp.float32, jnp.bfloat16, jnp.int32
LANES = 128
XQ = 4
PQ = 4

R_IDS, R_DZ, R_DY, R_DC, R_NZ, R_NC, R_XZ, R_XY, R_XC = 0, 4, 8, 12, 16, 24, 28, 36, 44
R_XM, R_X, R_NO, R_PC, R_PY, N_R = 48, 52, 56, 60, 68, 72
S_IDS, S_DZ, S_DY, S_DC, S_NZ, S_NC, S_XZ, S_XY, S_XC = 0, 3, 8, 12, 16, 26, 30, 40, 48
S_XM, S_X, S_NO, S_PC, S_PY, N_S = 52, 56, 60, 64, 72, 76
L_W1, L_W2, L_XM, L_DX, L_YS, L_YB, L_DW, L_DO, L_PF, N_L = 0, 1, 2, 3, 4, 5, 6, 8, 9, 11


def loop(lo, hi, body):
    def one(j, carry):
        body(j)
        return carry

    lax.fori_loop(lo, hi, one, 0)


def tiles(total, step, body):
    full = total // step
    loop(0, full, lambda j: body(pl.multiple_of(j * step, step), step))
    if total % step:
        body(full * step, total % step)


def rows_loop(total, body):
    loop(0, total // 16, lambda j: body(pl.multiple_of(j * 16, 16)))


def sort_keys(ids, keys, place, ordered, first, shard_rows, tall, rank0):
    reps, per, _ = ids.shape
    count = reps * per * LANES
    t = per * LANES // 4
    shift = t.bit_length() - 1
    lines = reps * per
    lane = lax.broadcasted_iota(I32, (per, LANES), 1)
    spot = lax.broadcasted_iota(I32, (per, LANES), 0) * LANES + lane
    block = jnp.right_shift(spot, shift)
    kept = (block & 1) * (2 * t) + jnp.right_shift(block, 1) * t + (spot & (t - 1))
    for k in range(reps):
        row = ids[k] - rank0
        row = jnp.where((row >= 0) & (row < shard_rows), row, shard_rows)
        keys[k * per : (k + 1) * per, :] = (row * count + (k * per * LANES + kept)).astype(F32)
    place[...] = jnp.zeros_like(place)
    ordered[...] = jnp.zeros_like(ordered)
    up = lax.broadcasted_iota(I32, (LANES, LANES), 0)
    over = lax.broadcasted_iota(I32, (LANES, LANES), 1)
    same = up == over
    overf = over.astype(F32)

    def column(ref, b):
        return jnp.sum(jnp.where(same, jnp.broadcast_to(ref[pl.ds(b, 1), :], (LANES, LANES)), 0.0), axis=1, keepdims=True)

    def count_below(b):
        col = column(keys, b)

        def one(a):
            at = pl.ds(a, 1)
            place[at, :] += jnp.sum(jnp.where(col < keys[at, :], 1.0, 0.0), axis=0, keepdims=True)

        loop(0, lines, one)

    loop(0, lines, count_below)

    def put(b):
        col, spot_of = column(keys, b), column(place, b)

        def one(a):
            want = overf + (a * LANES).astype(F32)
            ordered[pl.ds(a, 1), :] += jnp.sum(jnp.where(spot_of == want, col, 0.0), axis=0, keepdims=True)

        loop(0, lines, one)
        edge = overf * float(tall * count)
        first[...] += jnp.sum(jnp.where(col < edge, 1.0, 0.0), axis=0, keepdims=True)

    first[...] = jnp.zeros_like(first)
    loop(0, lines, put)


def group_kernel(shard_rows, tall, ids_ref, xm_hbm, w1_hbm, w2_hbm, g_ref, do_hbm,
                 base_o, ysum_o, ord_o, first_o, dx_o, far_o, dw1_o, dw2_o,
                 w1, w2, n, d, xm, xc, xy, hs, dus, pd, pf, rd, rf, yd, yb, dxo, idl, keys, place, ordered, first,
                 lsem, ssem, rsem):
    t, m = do_hbm.shape
    f = w1_hbm.shape[1]
    tq, mq = 2 * t // XQ, m // PQ
    z = lax.axis_index("data")
    r = lax.axis_index("tensor")
    y, c = lax.div(r, 2), lax.rem(r, 2)
    partner = {"tensor": 2 * y + 1 - c}
    across = {"tensor": 2 * (1 - y) + c}
    half = lax.div(z, 2)
    inner = z + half * (3 - 2 * z)
    order = [b + half * (3 - 2 * b) for b in (1 - inner, 2, 3)]
    middle, end = inner == 1, inner == 0

    def row(zz, cc, yy=0):
        return pl.multiple_of(zz * (4 * t) + cc * (2 * t) + yy * t, t)

    def blk(ref, zz, cc, yy):
        return ref.at[pl.ds(row(zz, cc, yy), t)]

    def duo(ref, zz, cc):
        return ref.at[pl.ds(row(zz, cc), 2 * t)]

    def remote(src, dst, s, q, dev):
        return pltpu.make_async_remote_copy(
            src_ref=src, dst_ref=dst, send_sem=ssem.at[s], recv_sem=rsem.at[q], device_id=dev, device_id_type=MESH
        )

    def local(src, dst, i):
        return pltpu.make_async_copy(src, dst, lsem.at[i])

    def arrived(ref, q):
        remote(ref, ref, 0, q, partner).wait_recv()

    def start(cp):
        cp.start()

    def sent(cp):
        cp.wait_send()

    def along(src, dst, s, q, act):
        for i, hop in enumerate((1, -1)):
            to = z + hop

            @pl.when((to >= 0) & (to <= 3))
            def _():
                act(remote(src, dst, s + i, q + z, {"data": to}))

    def pass_on(k, ref, s, q, act):
        src, dst = ref if isinstance(ref, tuple) else (ref, ref)
        act(remote(src, dst, s + 2 + k, q + order[k], {"data": order[1] if k == 0 else order[0]}))

    barrier = pltpu.get_barrier_semaphore()
    pl.semaphore_signal(barrier, inc=1, device_id=partner, device_id_type=MESH)
    pl.semaphore_signal(barrier, inc=1, device_id=across, device_id_type=MESH)
    for k in range(3):
        pl.semaphore_signal(barrier, inc=1, device_id={"data": order[k]}, device_id_type=MESH)

    own_d = blk(d, z, c, y)
    local(do_hbm, own_d, L_DO).start()
    local(xm_hbm, xm, L_XM).start()
    local(w1_hbm, w1, L_W1).start()
    local(w2_hbm, w2, L_W2).start()
    pl.semaphore_wait(barrier, 5)

    def piece(q):
        return pl.ds(q * tq, tq)

    for k in range(3):
        remote(ids_ref, idl.at[z], S_IDS + k, R_IDS + z, {"data": order[k]}).start()
    idl[z] = ids_ref[...]

    local(do_hbm, own_d, L_DO).wait()
    along(own_d, own_d, S_DZ, R_DZ, start)
    local(xm_hbm, xm, L_XM).wait()

    def xm_part(q):
        return remote(xm.at[pl.ds(row(0, 1 - c) + q * tq, tq)], xc.at[piece(q)], S_XM + q, R_XM + q, partner)

    def x_part(q):
        return remote(xc.at[piece(q)], xy.at[piece(q)], S_X + q, R_X + q, across)

    def d_got(k):
        arrived(blk(d, order[k], c, y), R_DZ + order[k])

    def d_on(k):
        pass_on(k, blk(d, order[k], c, y), S_DZ, R_DZ, start)

    def d_across(zz, act):
        act(remote(blk(d, zz, c, y), blk(d, zz, c, y), S_DY + zz, R_DY + zz, across))

    def d_pair(zz, act):
        act(remote(duo(d, zz, c), duo(d, zz, c), S_DC + zz, R_DC + zz, partner))

    for q in range(XQ):
        xm_part(q).start()
    for q in range(XQ):
        arrived(xc.at[piece(q)], R_XM + q)

        def join(i, q=q):
            at = pl.ds(q * tq + i, 16)
            xc[at, :] += xm[pl.ds(row(0, c) + q * tq + i, 16), :]

        rows_loop(tq, join)
        x_part(q).start()
    d_across(z, start)

    for k in range(3):
        arrived(idl.at[order[k]], R_IDS + order[k])
    sort_keys(idl, keys, place, ordered, first, shard_rows, tall, r * shard_rows)
    ord_o[...] = ordered[...].astype(I32)
    first_o[...] = first[...].astype(I32)
    d_got(0)

    @pl.when(middle)
    def _():
        d_on(0)
        d_got(1)
        d_on(1)

    gain = jnp.concatenate([g_ref[pl.ds(i, 1), :] for i in range(m // LANES)], axis=1).astype(F32)

    def n_own(q, act):
        at = n.at[pl.ds(row(z, c) + q * tq, tq)]
        act(remote(at, at, S_NO + q, R_NO + q, partner))

    def n_along(b, act):
        ref = blk(n, z, c, b)
        along(ref, ref, S_NZ + 5 * b, R_NZ + 4 * b, act)

    for q in range(XQ):
        arrived(xy.at[piece(q)], R_X + q)
        x_part(q).wait_send()

        def norm(i, q=q):
            at = pl.ds(q * tq + i, 16)
            x16 = xc[at, :] + xy[at, :]
            xc[at, :] = x16
            x = x16.astype(F32)
            s = lax.rsqrt(jnp.mean(x * x, axis=-1, keepdims=True) + NORM_EPS)
            n[pl.ds(row(z, c) + q * tq + i, 16), :] = ((x * s) * gain).astype(BF16)

        rows_loop(tq, norm)
        n_own(q, start)
        if q == XQ // 2 - 1:
            n_along(0, start)

            @pl.when(middle)
            def _():
                d_got(2)
                d_on(2)

        if q == XQ - 1:
            n_along(1, start)
    d_across(order[0], start)

    def hidden(zz, slopes):
        at = pl.ds(row(zz, 0), 4 * t)

        def body(off, w):
            to = pl.ds(off, w)
            u = jnp.dot(n[at, :], w1[:, to], preferred_element_type=F32).astype(BF16).astype(F32)
            uu = u * u
            th = jnp.tanh(GELU_A * (u + GELU_B * (uu * u)))
            cdf = 0.5 * (1.0 + th)
            hs[at, to] = (u * cdf).astype(BF16)
            slopes[:, to] = cdf + (0.5 * GELU_A) * u * (1.0 - th * th) * (1.0 + (3.0 * GELU_B) * uu)

        tiles(f, 256, body)

    def grad_hidden(zz, slopes):
        at = pl.ds(row(zz, 0), 4 * t)

        def body(off, w):
            to = pl.ds(off, w)
            dh = lax.dot_general(d[at, :], w2[to, :], NT, preferred_element_type=F32)
            dus[at, to] = (dh * slopes[:, to]).astype(BF16)

        tiles(f, 256, body)

    for q in range(XQ):
        arrived(n.at[pl.ds(row(z, 1 - c) + q * tq, tq)], R_NO + q)
    local(w1_hbm, w1, L_W1).wait()
    hidden(z, pf)
    arrived(blk(d, z, c, 1 - y), R_DY + z)
    d_pair(z, start)
    arrived(duo(d, z, 1 - c), R_DC + z)
    local(w2_hbm, w2, L_W2).wait()
    grad_hidden(z, pf)

    own_rows = pl.ds(row(z, 0), 4 * t)
    far = pl.multiple_of((1 - y) * t, t)

    def cols(q):
        return pl.ds(pl.multiple_of(q * mq, mq), mq)

    def part_pair(src, dst, i, q):
        return remote(src.at[pl.ds(row(0, 1 - c), 2 * t), cols(q)], dst.at[:, cols(q)], S_PC + PQ * i + q, R_PC + PQ * i + q, partner)

    def part_across(q):
        return remote(rd.at[pl.ds(far, t), cols(q)], yd.at[:, cols(q)], S_PY + q, R_PY + q, across)

    def sum_part(part, got, i, q):
        arrived(got.at[:, cols(q)], R_PC + PQ * i + q)

        def add(k):
            got[pl.ds(far + k, 16), cols(q)] += part[pl.ds(row(0, c, 1 - y) + k, 16), cols(q)]

        rows_loop(t, add)

    def dn_part(q):
        pd[:, cols(q)] = lax.dot_general(dus[own_rows, :], w1[cols(q), :], NT, preferred_element_type=F32)
        part_pair(pd, rd, 0, q).start()

    def y_part(q):
        pf[:, cols(q)] = jnp.dot(hs[own_rows, :], w2[:, cols(q)], preferred_element_type=F32)
        part_pair(pf, rf, 1, q).start()

    def dn_out(q):
        sum_part(pd, rd, 0, q)
        part_across(q).start()

    loop(0, PQ, dn_part)
    loop(0, PQ, dn_out)
    loop(0, PQ, y_part)

    @pl.when(end)
    def _():
        d_got(1)

    d_across(order[1], start)

    def n_got(k):
        for b in range(2):
            arrived(blk(n, order[k], c, b), R_NZ + 4 * b + order[k])

    def n_on(k):
        for b in range(2):
            pass_on(k, blk(n, order[k], c, b), S_NZ + 5 * b, R_NZ + 4 * b, start)

    def n_pair(zz, act):
        act(remote(duo(n, zz, c), duo(n, zz, c), S_NC + zz, R_NC + zz, partner))

    n_got(0)
    n_pair(order[0], start)

    @pl.when(middle)
    def _():
        n_on(0)
        n_got(1)
        n_on(1)
        n_pair(order[1], start)

    for q in range(PQ):
        arrived(yd.at[:, cols(q)], R_PY + q)

    def grad_x(i):
        at, own = pl.ds(i, 16), pl.ds(y * t + i, 16)
        dn = pd[pl.ds(row(0, c, y) + i, 16), :] + rd[own, :] + yd[at, :]
        x = xc[own, :].astype(F32)
        s = lax.rsqrt(jnp.mean(x * x, axis=-1, keepdims=True) + NORM_EPS)
        xh = x * s
        dhat = dn * gain
        dxn = s * (dhat - xh * jnp.mean(dhat * xh, axis=-1, keepdims=True))
        dxo[at, :] = (d[pl.ds(row(z, c, y) + i, 16), :].astype(F32) + dxn).astype(BF16)

    rows_loop(t, grad_x)
    th = t // 2

    def dx_part(zz, yy, h):
        return dx_o.at[pl.ds(pl.multiple_of(row(zz, c, yy) + h * th, th), th)]

    def dx_own(h):
        return dxo.at[pl.ds(h * th, th)]

    def far_part(h):
        return far_o.at[pl.ds(h * th, th)]

    def dx_next(k, h):
        here = dx_part(order[k], y, h)
        return (here, here) if k == 1 else (here if k == 0 else far_part(h), far_part(h))

    def dx_across(zz, src, h, act):
        act(remote(src, dx_part(zz, y, h), S_XY + 4 * h + zz, R_XY + 4 * h + zz, across))

    def dx_along(act):
        for h in range(2):
            along(dx_own(h), dx_part(z, y, h), S_XZ + 5 * h, R_XZ + 4 * h, act)

    def dx_pair(zz, act):
        act(remote(duo(dx_o, zz, c), duo(dx_o, zz, c), S_XC + zz, R_XC + zz, partner))

    def dx_got(k, on):
        zz = order[k]
        for h in range(2):
            arrived(dx_part(zz, y, h) if k < 2 else far_part(h), R_XZ + 4 * h + zz)
            if on:
                pass_on(k, dx_next(k, h), S_XZ + 5 * h, R_XZ + 4 * h, start)
            if k < 2:
                dx_across(zz, dx_part(zz, y, h), h, start)

    def dx_hand(zz):
        for h in range(2):
            arrived(dx_part(zz, 1 - y, h), R_XY + 4 * h + zz)
        dx_pair(zz, start)

    for h in range(2):
        dx_across(z, dx_own(h), h, start)
    local(dxo, blk(dx_o, z, c, y), L_DX).start()

    @pl.when(end)
    def _():
        d_got(2)

    d_across(order[2], start)

    loop(0, PQ, lambda q: sum_part(pf, rf, 1, q))
    y_send = local(rf.at[pl.ds(far, t)], ysum_o, L_YS)
    y_send.start()

    def base(i):
        own = pl.ds(y * t + i, 16)
        yb[pl.ds(i, 16), :] = xc[own, :].astype(F32) + (pf[pl.ds(row(0, c, y) + i, 16), :] + rf[own, :])

    rows_loop(t, base)
    y_keep = local(yb, base_o, L_YB)
    y_keep.start()
    for q in range(PQ):
        part_pair(pd, rd, 0, q).wait_send()
        part_pair(pf, rf, 1, q).wait_send()

    def unit(k):
        zz = order[k]
        arrived(blk(d, zz, c, 1 - y), R_DY + zz)
        d_pair(zz, start)
        arrived(duo(n, zz, 1 - c), R_NC + zz)
        hidden(zz, pd)
        arrived(duo(d, zz, 1 - c), R_DC + zz)
        grad_hidden(zz, pd)

    def n_rest(k, on):
        n_got(k)
        if on:
            n_on(k)
        n_pair(order[k], start)

    pl.when(middle)(lambda: n_rest(2, True))
    unit(0)
    dx_along(start)
    pl.when(end)(lambda: n_rest(1, False))
    unit(1)

    @pl.when(middle)
    def _():
        dx_got(0, True)
        dx_got(1, True)

    tw = 2 * t
    n1 = m // tw
    late_rows = pl.ds(row(order[2], 0), 4 * t)
    early_rows = pl.ds(pl.multiple_of(half * (4 * t), 4 * t), 12 * t)

    def w_at(i):
        return pl.ds(pl.multiple_of(i * tw, tw), tw)

    def slot(s):
        return pf.at[pl.ds(s * tw, tw), pl.ds(0, f)]

    def w1_tile(i, s, back):
        here, there = slot(s), dw1_o.at[w_at(i)]
        return local(here, there, L_PF + s) if back else local(there, here, L_PF + s)

    def early(j):
        for s in range(2):
            i = 2 * j + s
            pl.when(j >= 1)(lambda s=s, i=i: w1_tile(i - 2, s, True).wait())
            slot(s)[...] = lax.dot_general(n[early_rows, w_at(i)], dus[early_rows, :], TN, preferred_element_type=F32)
            w1_tile(i, s, True).start()

    loop(0, n1 // 2, early)
    for s in range(2):
        w1_tile(n1 - 2 + s, s, True).wait()
    pl.when(end)(lambda: n_rest(2, False))
    unit(2)

    def both(j):
        for s in range(2):
            i = 2 * j + s
            pl.when(j >= 1)(lambda s=s, i=i: w1_tile(i - 2, s, True).wait())
            w1_tile(i, s, False).start()
        weight_tile(j)
        for s in range(2):
            i = 2 * j + s
            w1_tile(i, s, False).wait()
            slot(s)[...] += lax.dot_general(n[late_rows, w_at(i)], dus[late_rows, :], TN, preferred_element_type=F32)
            w1_tile(i, s, True).start()

    def weight_tile(i):
        pl.when(i >= 2)(lambda: flush(i - 2).wait())
        stage(i)[...] = lax.dot_general(hs[:, w_at(i)], d[...], TN, preferred_element_type=F32)
        flush(i).start()

    def stage(i):
        return pd.at[pl.ds(pl.multiple_of(lax.rem(i, 2) * tw, tw), tw)]

    def flush(i):
        return local(stage(i), dw2_o.at[w_at(i)], L_DW + lax.rem(i, 2))

    n2, paired = f // tw, n1 // 2
    steps = min(n2, paired)
    pl.when(end)(lambda: dx_got(0, False))
    pl.when(middle)(lambda: dx_got(2, True))
    loop(0, steps // 2, both)
    pl.when(end)(lambda: dx_got(1, False))
    loop(steps // 2, steps, both)
    local(dxo, blk(dx_o, z, c, y), L_DX).wait()
    dx_hand(z)
    dx_hand(order[0])
    loop(steps, n2, weight_tile)
    for i in (n2 - 2, n2 - 1):
        flush(i).wait()
    if f % tw:
        rest = pd.at[pl.ds(0, f % tw)]
        rest[...] = lax.dot_general(hs[:, n2 * tw :], d[...], TN, preferred_element_type=F32)
        last = local(rest, dw2_o.at[pl.ds(n2 * tw, f % tw)], L_DW)
        last.start()
    dx_hand(order[1])
    pl.when(end)(lambda: dx_got(2, False))
    if f % tw:
        last.wait()
    for s in range(2):
        w1_tile(2 * paired - 2 + s, s, True).wait()

    y_send.wait()
    y_keep.wait()
    along(own_d, own_d, S_DZ, R_DZ, sent)
    for zz in (z, *order):
        d_across(zz, sent)
        d_pair(zz, sent)
    for k in range(3):
        n_pair(order[k], sent)
        remote(ids_ref, idl.at[z], S_IDS + k, R_IDS + z, {"data": order[k]}).wait_send()
    dx_along(sent)
    for b in range(2):
        n_along(b, sent)
        dx_across(z, dx_own(b), b, sent)
        for k in range(2):
            dx_across(order[k], dx_part(order[k], y, b), b, sent)

    @pl.when(middle)
    def _():
        for k in range(3):
            pass_on(k, blk(d, order[k], c, y), S_DZ, R_DZ, sent)
            for b in range(2):
                pass_on(k, dx_next(k, b), S_XZ + 5 * b, R_XZ + 4 * b, sent)
                pass_on(k, blk(n, order[k], c, b), S_NZ + 5 * b, R_NZ + 4 * b, sent)

    for q in range(XQ):
        xm_part(q).wait_send()
        n_own(q, sent)
    for q in range(PQ):
        part_across(q).wait_send()
    for zz in (z, *order[:2]):
        arrived(duo(dx_o, zz, 1 - c), R_XC + zz)
        dx_pair(zz, sent)


def run_group(ids, xm, w1, w2, gain, d_out, shard_rows, tall):
    t, m = d_out.shape
    f = w1.shape[1]
    lines = 4 * ids.shape[0]
    any_, vmem = pl.BlockSpec(memory_space=pl.ANY), pl.BlockSpec(memory_space=pltpu.VMEM)
    V = pltpu.VMEM
    sds = jax.ShapeDtypeStruct
    dots = 2 * 4 * t * m * f
    return pl.pallas_call(
        functools.partial(group_kernel, shard_rows, tall),
        out_shape=(
            sds((t, m), F32), sds((t, m), F32), sds((lines, LANES), I32), sds((1, LANES), I32), sds((16 * t, m), BF16),
            sds((t, m), BF16), sds((m, f), F32), sds((f, m), F32),
        ),
        in_specs=[vmem, any_, any_, any_, vmem, any_],
        out_specs=(any_, any_, vmem, vmem, any_, any_, any_, any_),
        scratch_shapes=[
            V((m, f), BF16), V((f, m), BF16), V((16 * t, m), BF16), V((16 * t, m), BF16),
            V((4 * t, m), BF16), V((2 * t, m), BF16), V((2 * t, m), BF16),
            V((16 * t, f), BF16), V((16 * t, f), BF16),
            V((4 * t, m), F32), V((4 * t, m), F32), V((2 * t, m), F32), V((2 * t, m), F32),
            V((t, m), F32), V((t, m), F32),
            V((t, m), BF16), V((4, *ids.shape), I32),
            V((lines, LANES), F32), V((lines, LANES), F32), V((lines, LANES), F32), V((1, LANES), F32),
            pltpu.SemaphoreType.DMA((N_L,)), pltpu.SemaphoreType.DMA((N_S,)), pltpu.SemaphoreType.DMA((N_R,)),
        ],
        compiler_params=pltpu.CompilerParams(collective_id=0, has_side_effects=True, vmem_limit_bytes=67043328),
        cost_estimate=pl.CostEstimate(flops=18 * dots, bytes_accessed=64 * 16 * t * m, transcendentals=16 * t * f),
        name="group_step",
    )(ids, xm, w1, w2, gain, d_out)


def lookup_kernel(shard_rows, ids_smem, ids_vmem, table, out_hbm, got, rows, sem, out_sem):
    total, m = out_hbm.shape
    t = total // 4
    per = 32
    chunks = total // per
    r = lax.axis_index("tensor")
    spread = (1 << (shard_rows.bit_length() - 1)) - 1

    def fetch(k):
        def some(j, carry):
            for u in range(8):
                p = k * per + j * 8 + u
                row = ids_smem[jnp.right_shift(p, 7), p & (LANES - 1)]
                near = row - r * shard_rows
                near = jnp.where((near >= 0) & (near < shard_rows), near, row & spread)
                pltpu.make_async_copy(table.at[jnp.right_shift(near, 3)], got.at[p], sem.at[k]).start()
            return carry

        lax.fori_loop(0, per // 8, some, 0)

    loop(0, chunks, fetch)
    spot = lax.broadcasted_iota(I32, (per, 8 * per), 1)
    token = lax.broadcasted_iota(I32, (per, 8 * per), 0)
    same = lax.broadcasted_iota(I32, (LANES, LANES), 0) == lax.broadcasted_iota(I32, (LANES, LANES), 1)

    def line(b):
        ids = ids_vmem[pl.ds(b, 1), :].astype(F32)
        col = jnp.sum(jnp.where(same, jnp.broadcast_to(ids, (LANES, LANES)), 0.0), axis=1, keepdims=True).astype(I32)
        row = col - r * shard_rows
        row = jnp.where((row >= 0) & (row < shard_rows), row & 7, -8 * per)
        for j in range(LANES // per):
            k = b * (LANES // per) + j
            at = pl.ds(pl.multiple_of(k * per, per), per)
            pltpu.make_async_copy(got.at[at], got.at[at], sem.at[k]).wait()
            want = row[j * per : (j + 1) * per] + 8 * token
            chosen = jnp.where(want == spot, 1.0, 0.0).astype(BF16)
            picked = jnp.dot(chosen, got[at].reshape(8 * per, m), preferred_element_type=F32)
            p = k * per
            nat = lax.div(p, t)
            to = pl.multiple_of(lax.rem(nat, 2) * (2 * t) + lax.div(nat, 2) * t + lax.rem(p, t), per)
            rows[pl.ds(to, per), :] = picked.astype(BF16)
            pltpu.make_async_copy(rows.at[pl.ds(to, per)], out_hbm.at[pl.ds(to, per)], out_sem).start()

    loop(0, total // LANES, line)
    pltpu.make_async_copy(rows, out_hbm, out_sem).wait()


def look_up(ids, table):
    shard_rows, m = table.shape
    total = ids.size
    any_ = pl.BlockSpec(memory_space=pl.ANY)
    return pl.pallas_call(
        functools.partial(lookup_kernel, shard_rows),
        out_shape=jax.ShapeDtypeStruct((total, m), BF16),
        in_specs=[pl.BlockSpec(memory_space=pltpu.SMEM), pl.BlockSpec(memory_space=pltpu.VMEM), any_],
        out_specs=any_,
        scratch_shapes=[
            pltpu.VMEM((total, 8, m), BF16), pltpu.VMEM((total, m), BF16),
            pltpu.SemaphoreType.DMA((total // 32,)), pltpu.SemaphoreType.DMA,
        ],
        compiler_params=pltpu.CompilerParams(vmem_limit_bytes=60 << 20),
        cost_estimate=pl.CostEstimate(flops=16 * total * m, bytes_accessed=20 * total * m, transcendentals=0),
        name="look_up",
    )(ids, ids, table.reshape(shard_rows // 8, 8, m))


RING = 6


def pass_pieces(src, buf, dst, in_sem, out_sem, first, count):
    rows = src.shape[0] // 8

    def piece(i):
        return pl.ds(pl.multiple_of((first + i) * rows, 8), rows)

    def fetch(i):
        return pltpu.make_async_copy(src.at[piece(i)], buf.at[pl.ds(pl.multiple_of(i * rows, 8), rows)], in_sem.at[i])

    def put(i):
        return pltpu.make_async_copy(buf.at[pl.ds(pl.multiple_of(i * rows, 8), rows)], dst.at[piece(i)], out_sem)

    def step(i):
        fetch(i).wait()
        put(i).start()

    def drain():
        pltpu.make_async_copy(buf, dst.at[pl.ds(first * rows, count * rows)], out_sem).wait()

    return lambda i: fetch(i).start(), step, drain


HALF = 4


def pass_kernel(w1_in, w2_in, w1_out, w2_out, buf1, buf2, in1, in2, out1, out2):
    fetch1, step1, drain1 = pass_pieces(w1_in, buf1, w1_out, in1, out1, 0, 8)
    fetch2, step2, drain2 = pass_pieces(w2_in, buf2, w2_out, in2, out2, 0, HALF)
    loop(0, 8, fetch1)
    loop(0, HALF, fetch2)
    loop(0, 8, step1)
    loop(0, HALF, step2)
    drain1()
    drain2()


def pass_on(w1, w2):
    any_ = pl.BlockSpec(memory_space=pl.ANY)
    V, S = pltpu.VMEM, pltpu.SemaphoreType.DMA
    f, m = w2.shape
    return pl.pallas_call(
        pass_kernel,
        out_shape=(jax.ShapeDtypeStruct(w1.shape, F32), jax.ShapeDtypeStruct(w2.shape, F32)),
        in_specs=[any_] * 2,
        out_specs=[any_] * 2,
        scratch_shapes=[V(w1.shape, F32), V((f * HALF // 8, m), F32), S((8,)), S((HALF,)), S, S],
        compiler_params=pltpu.CompilerParams(vmem_limit_bytes=60 << 20),
        cost_estimate=pl.CostEstimate(flops=8000 * w1.size, bytes_accessed=12 * w1.size, transcendentals=0),
        name="pass_weights",
    )(w1, w2)


def table_kernel(tall, key_ref, first_ref, w_in, w_half, dx_in, far_own, far_x, far_p, far_b,
                 out_hbm, w_out, dxb, dxf, ring, w_buf, dx_sem, t_sem, in_sem, out_sem):
    del w_half
    count, _ = dxb.shape
    t = count // 16
    shift = count.bit_length() - 1
    steps = out_hbm.shape[0] // tall
    z, r = lax.axis_index("data"), lax.axis_index("tensor")
    y, c = lax.div(r, 2), lax.rem(r, 2)
    late = lax.div(z, 2)
    w_fetch, w_step, w_drain = pass_pieces(w_in, w_buf, w_out, in_sem, out_sem, HALF, 8 - HALF)

    def near(k):
        at = pl.ds(pl.multiple_of(late * (4 * t) + k * (2 * t), t), 2 * t)
        return at, pltpu.make_async_copy(dx_in.at[at], dxb.at[at], dx_sem.at[k])

    def far(k, src, cc, yy):
        at = pl.ds(pl.multiple_of((1 - late) * (12 * t) + cc * (2 * t) + yy * t, t), t)
        return at, pltpu.make_async_copy(src, dxb.at[at], dx_sem.at[6 + k])

    fars = ((far_own, c, y), (far_p, 1 - c, y), (far_x, c, 1 - y), (far_b, 1 - c, 1 - y))
    loop(0, 6, lambda k: near(k)[1].start())
    for k, what in enumerate(fars):
        far(k, *what)[1].start()
    loop(0, 8 - HALF, w_fetch)

    def widen_piece(at, cp):
        cp.wait()

        def widen(i):
            rows = pl.ds(pl.multiple_of(at.start + i, 16), 16)
            dxf[rows, :] = dxb[rows, :].astype(F32)

        rows_loop(at.size, widen)

    for k in range(6):
        widen_piece(*near(k))
        if k >= 2:
            w_step(k - 2)
    for k, what in enumerate(fars):
        widen_piece(*far(k, *what))

    def tile_out(i):
        slot = lax.rem(i, RING)
        return pltpu.make_async_copy(ring.at[slot], out_hbm.at[pl.ds(pl.multiple_of(i * tall, 8), tall)], t_sem.at[slot])

    def tile(i):
        slot = lax.rem(i, RING)
        here = ring.at[slot]
        pl.when(i >= RING)(lambda: tile_out(i - RING).wait())
        here[...] = jnp.zeros_like(here)

        def add(j, key):
            ahead = key_ref[jnp.minimum(j + 1, count - 1)]
            to = pl.ds(jnp.right_shift(key, shift) - i * tall, 1)
            here[to, :] += dxf[pl.ds(key & (count - 1), 1), :]
            return ahead

        low = first_ref[i]
        lax.fori_loop(low, first_ref[i + 1], add, key_ref[jnp.minimum(low, count - 1)])
        tile_out(i).start()

    loop(0, steps, tile)
    loop(steps - RING, steps, lambda i: tile_out(i).wait())
    w_drain()


def table_grad(ordered, first, w, w_half, dx_all, fars, shard_rows, tall):
    count, m = dx_all.shape
    f = w.shape[0]
    any_ = pl.BlockSpec(memory_space=pl.ANY)
    V, S = pltpu.VMEM, pltpu.SemaphoreType.DMA
    return pl.pallas_call(
        functools.partial(table_kernel, tall),
        out_shape=(jax.ShapeDtypeStruct((shard_rows, m), F32), jax.ShapeDtypeStruct(w.shape, F32)),
        grid_spec=pltpu.PrefetchScalarGridSpec(
            num_scalar_prefetch=2,
            grid=(1,),
            in_specs=[any_] * 7,
            out_specs=[any_] * 2,
            scratch_shapes=[
                V((count, m), BF16), V((count, m), F32), V((RING, tall, m), F32), V((f - f * HALF // 8, m), F32),
                S((10,)), S((RING,)), S((8 - HALF,)), S,
            ],
        ),
        input_output_aliases={3: 1},
        compiler_params=pltpu.CompilerParams(vmem_limit_bytes=60 << 20),
        cost_estimate=pl.CostEstimate(flops=1600 * shard_rows * m, bytes_accessed=4 * shard_rows * m, transcendentals=0),
        name="table_grad",
    )(ordered, first, w, w_half, dx_all, *fars)


def solution(mesh):
    tok_spec = P(("pod", "data", "tensor"), None)

    over_y, over_core = [(0, 2), (1, 3), (2, 0), (3, 1)], [(0, 1), (1, 0), (2, 3), (3, 2)]

    def per_device(token_ids, embed_table, norm_gain, w_in, w_out, d_out):
        shard_rows = embed_table.shape[0]
        tall = next(k for k in (160, 8) if shard_rows % k == 0)
        ids = token_ids.reshape(-1, LANES)
        masked = look_up(ids, embed_table)
        gain = norm_gain.reshape(-1, LANES)
        base, ysum, ordered, first, dx_all, far, dw1, dw2 = run_group(
            ids, masked, w_in, w_out, gain, d_out, shard_rows, tall
        )
        far_x = lax.ppermute(far, "tensor", over_y)
        far_p = lax.ppermute(far, "tensor", over_core)
        other = lax.ppermute(ysum, "tensor", over_y)
        grad_w_in, w_half = pass_on(dw1, dw2)
        far_b = lax.ppermute(far_x, "tensor", over_core)
        grad_table, grad_w_out = table_grad(
            ordered.reshape(-1), first.reshape(-1), dw2, w_half, dx_all, (far, far_x, far_p, far_b), shard_rows, tall
        )
        return (base + other).astype(BF16), grad_table, grad_w_in, grad_w_out

    return jax.shard_map(
        per_device,
        mesh=mesh,
        in_specs=(P(("pod", "data")), P("tensor", None), P(None), P(None, "tensor"), P("tensor", None), tok_spec),
        out_specs=(tok_spec, P(("pod", "tensor"), None), P("pod", "tensor"), P(("pod", "tensor"), None)),
        check_vma=False,
    )
```

```python
import functools

import jax
import jax.numpy as jnp
from jax import lax
from jax.experimental import pallas as pl
from jax.experimental.pallas import tpu as pltpu
from jax.sharding import PartitionSpec as P


NORM_EPS = 1e-6
GELU_A = 0.7978845608028654
GELU_B = 0.044715
MESH = pl.DeviceIdType.MESH
NT = (((1,), (1,)), ((), ()))
TN = (((0,), (0,)), ((), ()))
F32, BF16, I32 = jnp.float32, jnp.bfloat16, jnp.int32
LANES = 128
XQ = 4
PQ = 4

R_IDS, R_DZ, R_DY, R_DC, R_NZ, R_NC, R_XZ, R_XY, R_XC = 0, 4, 8, 12, 16, 24, 28, 36, 44
R_XM, R_X, R_NO, R_PC, R_PY, N_R = 48, 52, 56, 60, 68, 72
S_IDS, S_DZ, S_DY, S_DC, S_NZ, S_NC, S_XZ, S_XY, S_XC = 0, 3, 8, 12, 16, 26, 30, 40, 48
S_XM, S_X, S_NO, S_PC, S_PY, N_S = 52, 56, 60, 64, 72, 76
L_W1, L_W2, L_XM, L_DX, L_YS, L_YB, L_DW, L_DO, L_K, N_L = 0, 1, 2, 3, 4, 5, 6, 8, 9, 13


def loop(lo, hi, body):
    def one(j, carry):
        body(j)
        return carry

    lax.fori_loop(lo, hi, one, 0)


def tiles(total, step, body):
    full = total // step
    loop(0, full, lambda j: body(pl.multiple_of(j * step, step), step))
    if total % step:
        body(full * step, total % step)


def rows_loop(total, body):
    loop(0, total // 16, lambda j: body(pl.multiple_of(j * 16, 16)))


def sort_keys(ids, keys, place, ordered, first, shard_rows, tall, rank0):
    reps, per, _ = ids.shape
    count = reps * per * LANES
    t = per * LANES // 4
    shift = t.bit_length() - 1
    lines = reps * per
    lane = lax.broadcasted_iota(I32, (per, LANES), 1)
    spot = lax.broadcasted_iota(I32, (per, LANES), 0) * LANES + lane
    block = jnp.right_shift(spot, shift)
    kept = (block & 1) * (2 * t) + jnp.right_shift(block, 1) * t + (spot & (t - 1))
    for k in range(reps):
        row = ids[k] - rank0
        row = jnp.where((row >= 0) & (row < shard_rows), row, shard_rows)
        keys[k * per : (k + 1) * per, :] = (row * count + (k * per * LANES + kept)).astype(F32)
    place[...] = jnp.zeros_like(place)
    ordered[...] = jnp.zeros_like(ordered)
    up = lax.broadcasted_iota(I32, (LANES, LANES), 0)
    over = lax.broadcasted_iota(I32, (LANES, LANES), 1)
    same = up == over
    overf = over.astype(F32)

    def column(ref, b):
        return jnp.sum(jnp.where(same, jnp.broadcast_to(ref[pl.ds(b, 1), :], (LANES, LANES)), 0.0), axis=1, keepdims=True)

    def count_below(b):
        col = column(keys, b)

        def one(a):
            at = pl.ds(a, 1)
            place[at, :] += jnp.sum(jnp.where(col < keys[at, :], 1.0, 0.0), axis=0, keepdims=True)

        loop(0, lines, one)

    loop(0, lines, count_below)

    def put(b):
        col, spot_of = column(keys, b), column(place, b)

        def one(a):
            want = overf + (a * LANES).astype(F32)
            ordered[pl.ds(a, 1), :] += jnp.sum(jnp.where(spot_of == want, col, 0.0), axis=0, keepdims=True)

        loop(0, lines, one)
        edge = overf * float(tall * count)
        first[...] += jnp.sum(jnp.where(col < edge, 1.0, 0.0), axis=0, keepdims=True)

    first[...] = jnp.zeros_like(first)
    loop(0, lines, put)


def group_kernel(shard_rows, tall, ids_ref, xm_hbm, w1_hbm, w2_hbm, g_ref, do_hbm,
                 base_o, ysum_o, ord_o, first_o, dx_o, far_o, dw1_o, dw2_o, nk_o, dk_o, hk_o, duk_o,
                 w1, w2, n, d, xm, xc, xy, hs, dus, pd, pf, rd, rf, yd, yb, dxo, idl, keys, place, ordered, first,
                 lsem, ssem, rsem):
    t, m = do_hbm.shape
    f = w1_hbm.shape[1]
    tq, mq = 2 * t // XQ, m // PQ
    z = lax.axis_index("data")
    r = lax.axis_index("tensor")
    y, c = lax.div(r, 2), lax.rem(r, 2)
    partner = {"tensor": 2 * y + 1 - c}
    across = {"tensor": 2 * (1 - y) + c}
    half = lax.div(z, 2)
    inner = z + half * (3 - 2 * z)
    order = [b + half * (3 - 2 * b) for b in (1 - inner, 2, 3)]
    middle, end = inner == 1, inner == 0

    def row(zz, cc, yy=0):
        return pl.multiple_of(zz * (4 * t) + cc * (2 * t) + yy * t, t)

    def blk(ref, zz, cc, yy):
        return ref.at[pl.ds(row(zz, cc, yy), t)]

    def duo(ref, zz, cc):
        return ref.at[pl.ds(row(zz, cc), 2 * t)]

    def remote(src, dst, s, q, dev):
        return pltpu.make_async_remote_copy(
            src_ref=src, dst_ref=dst, send_sem=ssem.at[s], recv_sem=rsem.at[q], device_id=dev, device_id_type=MESH
        )

    def local(src, dst, i):
        return pltpu.make_async_copy(src, dst, lsem.at[i])

    def arrived(ref, q):
        remote(ref, ref, 0, q, partner).wait_recv()

    def start(cp):
        cp.start()

    def sent(cp):
        cp.wait_send()

    def along(src, dst, s, q, act):
        for i, hop in enumerate((1, -1)):
            to = z + hop

            @pl.when((to >= 0) & (to <= 3))
            def _():
                act(remote(src, dst, s + i, q + z, {"data": to}))

    def pass_on(k, ref, s, q, act):
        src, dst = ref if isinstance(ref, tuple) else (ref, ref)
        act(remote(src, dst, s + 2 + k, q + order[k], {"data": order[1] if k == 0 else order[0]}))

    barrier = pltpu.get_barrier_semaphore()
    pl.semaphore_signal(barrier, inc=1, device_id=partner, device_id_type=MESH)
    pl.semaphore_signal(barrier, inc=1, device_id=across, device_id_type=MESH)
    for k in range(3):
        pl.semaphore_signal(barrier, inc=1, device_id={"data": order[k]}, device_id_type=MESH)

    own_d = blk(d, z, c, y)
    local(do_hbm, own_d, L_DO).start()
    local(xm_hbm, xm, L_XM).start()
    local(w1_hbm, w1, L_W1).start()
    local(w2_hbm, w2, L_W2).start()
    pl.semaphore_wait(barrier, 5)

    def piece(q):
        return pl.ds(q * tq, tq)

    for k in range(3):
        remote(ids_ref, idl.at[z], S_IDS + k, R_IDS + z, {"data": order[k]}).start()
    idl[z] = ids_ref[...]

    local(do_hbm, own_d, L_DO).wait()
    along(own_d, own_d, S_DZ, R_DZ, start)
    local(xm_hbm, xm, L_XM).wait()

    def xm_part(q):
        return remote(xm.at[pl.ds(row(0, 1 - c) + q * tq, tq)], xc.at[piece(q)], S_XM + q, R_XM + q, partner)

    def x_part(q):
        return remote(xc.at[piece(q)], xy.at[piece(q)], S_X + q, R_X + q, across)

    def d_got(k):
        arrived(blk(d, order[k], c, y), R_DZ + order[k])

    def d_on(k):
        pass_on(k, blk(d, order[k], c, y), S_DZ, R_DZ, start)

    def d_across(zz, act):
        act(remote(blk(d, zz, c, y), blk(d, zz, c, y), S_DY + zz, R_DY + zz, across))

    def d_pair(zz, act):
        act(remote(duo(d, zz, c), duo(d, zz, c), S_DC + zz, R_DC + zz, partner))

    for q in range(XQ):
        xm_part(q).start()
    for q in range(XQ):
        arrived(xc.at[piece(q)], R_XM + q)

        def join(i, q=q):
            at = pl.ds(q * tq + i, 16)
            xc[at, :] += xm[pl.ds(row(0, c) + q * tq + i, 16), :]

        rows_loop(tq, join)
        x_part(q).start()
    d_across(z, start)

    d_got(0)

    @pl.when(middle)
    def _():
        d_on(0)
        d_got(1)
        d_on(1)

    gain = jnp.concatenate([g_ref[pl.ds(i, 1), :] for i in range(m // LANES)], axis=1).astype(F32)

    def n_own(q, act):
        at = n.at[pl.ds(row(z, c) + q * tq, tq)]
        act(remote(at, at, S_NO + q, R_NO + q, partner))

    def n_along(b, act):
        ref = blk(n, z, c, b)
        along(ref, ref, S_NZ + 5 * b, R_NZ + 4 * b, act)

    for q in range(XQ):
        arrived(xy.at[piece(q)], R_X + q)
        x_part(q).wait_send()

        def norm(i, q=q):
            at = pl.ds(q * tq + i, 16)
            x16 = xc[at, :] + xy[at, :]
            xc[at, :] = x16
            x = x16.astype(F32)
            s = lax.rsqrt(jnp.mean(x * x, axis=-1, keepdims=True) + NORM_EPS)
            n[pl.ds(row(z, c) + q * tq + i, 16), :] = ((x * s) * gain).astype(BF16)

        rows_loop(tq, norm)
        n_own(q, start)
        if q == XQ // 2 - 1:
            n_along(0, start)

            @pl.when(middle)
            def _():
                d_got(2)
                d_on(2)

        if q == XQ - 1:
            n_along(1, start)
    d_across(order[0], start)

    def hidden(zz, slopes):
        at = pl.ds(row(zz, 0), 4 * t)

        def body(off, w):
            to = pl.ds(off, w)
            u = jnp.dot(n[at, :], w1[:, to], preferred_element_type=F32).astype(BF16).astype(F32)
            uu = u * u
            th = jnp.tanh(GELU_A * (u + GELU_B * (uu * u)))
            cdf = 0.5 * (1.0 + th)
            hs[at, to] = (u * cdf).astype(BF16)
            slopes[:, to] = cdf + (0.5 * GELU_A) * u * (1.0 - th * th) * (1.0 + (3.0 * GELU_B) * uu)

        tiles(f, 256, body)

    def grad_hidden(zz, slopes):
        at = pl.ds(row(zz, 0), 4 * t)

        def body(off, w):
            to = pl.ds(off, w)
            dh = lax.dot_general(d[at, :], w2[to, :], NT, preferred_element_type=F32)
            dus[at, to] = (dh * slopes[:, to]).astype(BF16)

        tiles(f, 256, body)

    for q in range(XQ):
        arrived(n.at[pl.ds(row(z, 1 - c) + q * tq, tq)], R_NO + q)
    local(w1_hbm, w1, L_W1).wait()
    hidden(z, pf)
    arrived(blk(d, z, c, 1 - y), R_DY + z)
    d_pair(z, start)
    arrived(duo(d, z, 1 - c), R_DC + z)
    local(w2_hbm, w2, L_W2).wait()
    grad_hidden(z, pf)

    own_rows = pl.ds(row(z, 0), 4 * t)
    far = pl.multiple_of((1 - y) * t, t)

    def cols(q):
        return pl.ds(pl.multiple_of(q * mq, mq), mq)

    def part_pair(src, dst, i, q):
        return remote(src.at[pl.ds(row(0, 1 - c), 2 * t), cols(q)], dst.at[:, cols(q)], S_PC + PQ * i + q, R_PC + PQ * i + q, partner)

    def part_across(q):
        return remote(rd.at[pl.ds(far, t), cols(q)], yd.at[:, cols(q)], S_PY + q, R_PY + q, across)

    def sum_part(part, got, i, q):
        arrived(got.at[:, cols(q)], R_PC + PQ * i + q)

        def add(k):
            got[pl.ds(far + k, 16), cols(q)] += part[pl.ds(row(0, c, 1 - y) + k, 16), cols(q)]

        rows_loop(t, add)

    def dn_part(q):
        pd[:, cols(q)] = lax.dot_general(dus[own_rows, :], w1[cols(q), :], NT, preferred_element_type=F32)
        part_pair(pd, rd, 0, q).start()

    def y_part(q):
        pf[:, cols(q)] = jnp.dot(hs[own_rows, :], w2[:, cols(q)], preferred_element_type=F32)
        part_pair(pf, rf, 1, q).start()

    def dn_out(q):
        sum_part(pd, rd, 0, q)
        part_across(q).start()

    loop(0, PQ, dn_part)
    loop(0, PQ, dn_out)
    loop(0, PQ, y_part)

    @pl.when(end)
    def _():
        d_got(1)

    d_across(order[1], start)

    loop(0, PQ, lambda q: sum_part(pf, rf, 1, q))
    y_send = local(rf.at[pl.ds(far, t)], ysum_o, L_YS)
    y_send.start()

    def base(i):
        own = pl.ds(y * t + i, 16)
        yb[pl.ds(i, 16), :] = xc[own, :].astype(F32) + (pf[pl.ds(row(0, c, y) + i, 16), :] + rf[own, :])

    rows_loop(t, base)
    y_keep = local(yb, base_o, L_YB)
    y_keep.start()
    for q in range(PQ):
        part_pair(pf, rf, 1, q).wait_send()

    def n_got(k):
        for b in range(2):
            arrived(blk(n, order[k], c, b), R_NZ + 4 * b + order[k])

    def n_on(k):
        for b in range(2):
            pass_on(k, blk(n, order[k], c, b), S_NZ + 5 * b, R_NZ + 4 * b, start)

    def n_pair(zz, act):
        act(remote(duo(n, zz, c), duo(n, zz, c), S_NC + zz, R_NC + zz, partner))

    n_got(0)
    n_pair(order[0], start)

    @pl.when(middle)
    def _():
        n_on(0)
        n_got(1)
        n_on(1)
        n_pair(order[1], start)

    def unit(k, slopes):
        zz = order[k]
        arrived(blk(d, zz, c, 1 - y), R_DY + zz)
        d_pair(zz, start)
        arrived(duo(n, zz, 1 - c), R_NC + zz)
        hidden(zz, slopes)
        arrived(duo(d, zz, 1 - c), R_DC + zz)
        grad_hidden(zz, slopes)

    def n_rest(k, on):
        n_got(k)
        if on:
            n_on(k)
        n_pair(order[k], start)

    unit(0, pf)

    for q in range(PQ):
        arrived(yd.at[:, cols(q)], R_PY + q)

    def grad_x(i):
        at, own = pl.ds(i, 16), pl.ds(y * t + i, 16)
        dn = pd[pl.ds(row(0, c, y) + i, 16), :] + rd[own, :] + yd[at, :]
        x = xc[own, :].astype(F32)
        s = lax.rsqrt(jnp.mean(x * x, axis=-1, keepdims=True) + NORM_EPS)
        xh = x * s
        dhat = dn * gain
        dxn = s * (dhat - xh * jnp.mean(dhat * xh, axis=-1, keepdims=True))
        dxo[at, :] = (d[pl.ds(row(z, c, y) + i, 16), :].astype(F32) + dxn).astype(BF16)

    rows_loop(t, grad_x)
    th = t // 2

    def dx_part(zz, yy, h):
        return dx_o.at[pl.ds(pl.multiple_of(row(zz, c, yy) + h * th, th), th)]

    def dx_own(h):
        return dxo.at[pl.ds(h * th, th)]

    def far_part(h):
        return far_o.at[pl.ds(h * th, th)]

    def dx_next(k, h):
        here = dx_part(order[k], y, h)
        return (here, here) if k == 1 else (here if k == 0 else far_part(h), far_part(h))

    def dx_across(zz, src, h, act):
        act(remote(src, dx_part(zz, y, h), S_XY + 4 * h + zz, R_XY + 4 * h + zz, across))

    def dx_along(act):
        for h in range(2):
            along(dx_own(h), dx_part(z, y, h), S_XZ + 5 * h, R_XZ + 4 * h, act)

    def dx_pair(zz, act):
        act(remote(duo(dx_o, zz, c), duo(dx_o, zz, c), S_XC + zz, R_XC + zz, partner))

    def dx_got(k, on):
        zz = order[k]
        for h in range(2):
            arrived(dx_part(zz, y, h) if k < 2 else far_part(h), R_XZ + 4 * h + zz)
            if on:
                pass_on(k, dx_next(k, h), S_XZ + 5 * h, R_XZ + 4 * h, start)
            if k < 2:
                dx_across(zz, dx_part(zz, y, h), h, start)

    def dx_hand(zz):
        for h in range(2):
            arrived(dx_part(zz, 1 - y, h), R_XY + 4 * h + zz)
        dx_pair(zz, start)

    for h in range(2):
        dx_across(z, dx_own(h), h, start)
    local(dxo, blk(dx_o, z, c, y), L_DX).start()

    @pl.when(end)
    def _():
        d_got(2)

    d_across(order[2], start)

    for q in range(PQ):
        part_pair(pd, rd, 0, q).wait_send()

    pl.when(middle)(lambda: n_rest(2, True))
    dx_along(start)
    pl.when(end)(lambda: n_rest(1, False))
    unit(1, pd)

    @pl.when(middle)
    def _():
        dx_got(0, True)
        dx_got(1, True)

    tw = 2 * t
    n1, n2 = m // tw, f // tw
    late_rows = pl.ds(row(order[2], 0), 4 * t)
    early_rows = pl.ds(pl.multiple_of(half * (4 * t), 4 * t), 12 * t)

    def flush(i, buf, dst):
        lines = pl.ds(pl.multiple_of(lax.rem(i, 2) * tw, tw), tw)
        here = buf.at[lines, pl.ds(0, dst.shape[1])]
        return here, local(here, dst.at[pl.ds(pl.multiple_of(i * tw, tw), tw)], L_DW + lax.rem(i, 2))

    def weight_tile(i, lhs, rhs, buf, dst):
        pl.when(i >= 2)(lambda: flush(i - 2, buf, dst)[1].wait())
        here, out = flush(i, buf, dst)
        at = pl.ds(pl.multiple_of(i * tw, tw), tw)
        here[...] = lax.dot_general(lhs[early_rows, at], rhs[early_rows, :], TN, preferred_element_type=F32)
        out.start()

    loop(0, n1, lambda i: weight_tile(i, n, dus, pf, dw1_o))
    for i in (n1 - 2, n1 - 1):
        flush(i, pf, dw1_o)[1].wait()
    pl.when(end)(lambda: n_rest(2, False))
    unit(2, pd)
    kept = [
        local(src.at[late_rows], dst, L_K + i)
        for i, (src, dst) in enumerate(((n, nk_o), (d, dk_o), (hs, hk_o), (dus, duk_o)))
    ]
    for cp in kept:
        cp.start()
    pl.when(end)(lambda: dx_got(0, False))
    pl.when(middle)(lambda: dx_got(2, True))
    loop(0, n2 // 2, lambda i: weight_tile(i, hs, d, pd, dw2_o))
    pl.when(end)(lambda: dx_got(1, False))
    loop(n2 // 2, n2, lambda i: weight_tile(i, hs, d, pd, dw2_o))
    local(dxo, blk(dx_o, z, c, y), L_DX).wait()
    dx_hand(z)
    dx_hand(order[0])

    for k in range(3):
        arrived(idl.at[order[k]], R_IDS + order[k])
    sort_keys(idl, keys, place, ordered, first, shard_rows, tall, r * shard_rows)
    ord_o[...] = ordered[...].astype(I32)
    first_o[...] = first[...].astype(I32)

    for i in (n2 - 2, n2 - 1):
        flush(i, pd, dw2_o)[1].wait()
    if f % tw:
        rest = pd.at[pl.ds(0, f % tw)]
        rest[...] = lax.dot_general(hs[early_rows, n2 * tw :], d[early_rows, :], TN, preferred_element_type=F32)
        last = local(rest, dw2_o.at[pl.ds(n2 * tw, f % tw)], L_DW)
        last.start()
    dx_hand(order[1])
    pl.when(end)(lambda: dx_got(2, False))
    if f % tw:
        last.wait()
    for cp in kept:
        cp.wait()

    y_send.wait()
    y_keep.wait()
    along(own_d, own_d, S_DZ, R_DZ, sent)
    for zz in (z, *order):
        d_across(zz, sent)
        d_pair(zz, sent)
    for k in range(3):
        n_pair(order[k], sent)
        remote(ids_ref, idl.at[z], S_IDS + k, R_IDS + z, {"data": order[k]}).wait_send()
    dx_along(sent)
    for b in range(2):
        n_along(b, sent)
        dx_across(z, dx_own(b), b, sent)
        for k in range(2):
            dx_across(order[k], dx_part(order[k], y, b), b, sent)

    @pl.when(middle)
    def _():
        for k in range(3):
            pass_on(k, blk(d, order[k], c, y), S_DZ, R_DZ, sent)
            for b in range(2):
                pass_on(k, dx_next(k, b), S_XZ + 5 * b, R_XZ + 4 * b, sent)
                pass_on(k, blk(n, order[k], c, b), S_NZ + 5 * b, R_NZ + 4 * b, sent)

    for q in range(XQ):
        xm_part(q).wait_send()
        n_own(q, sent)
    for q in range(PQ):
        part_across(q).wait_send()
    for zz in (z, *order[:2]):
        arrived(duo(dx_o, zz, 1 - c), R_XC + zz)
        dx_pair(zz, sent)


def run_group(ids, xm, w1, w2, gain, d_out, shard_rows, tall):
    t, m = d_out.shape
    f = w1.shape[1]
    lines = 4 * ids.shape[0]
    any_, vmem = pl.BlockSpec(memory_space=pl.ANY), pl.BlockSpec(memory_space=pltpu.VMEM)
    V = pltpu.VMEM
    sds = jax.ShapeDtypeStruct
    dots = 2 * 4 * t * m * f
    return pl.pallas_call(
        functools.partial(group_kernel, shard_rows, tall),
        out_shape=(
            sds((t, m), F32), sds((t, m), F32), sds((lines, LANES), I32), sds((1, LANES), I32), sds((16 * t, m), BF16),
            sds((t, m), BF16), sds((m, f), F32), sds((f, m), F32),
            sds((4 * t, m), BF16), sds((4 * t, m), BF16), sds((4 * t, f), BF16), sds((4 * t, f), BF16),
        ),
        in_specs=[vmem, any_, any_, any_, vmem, any_],
        out_specs=(any_, any_, vmem, vmem, *[any_] * 8),
        scratch_shapes=[
            V((m, f), BF16), V((f, m), BF16), V((16 * t, m), BF16), V((16 * t, m), BF16),
            V((4 * t, m), BF16), V((2 * t, m), BF16), V((2 * t, m), BF16),
            V((16 * t, f), BF16), V((16 * t, f), BF16),
            V((4 * t, m), F32), V((4 * t, m), F32), V((2 * t, m), F32), V((2 * t, m), F32),
            V((t, m), F32), V((t, m), F32),
            V((t, m), BF16), V((4, *ids.shape), I32),
            V((lines, LANES), F32), V((lines, LANES), F32), V((lines, LANES), F32), V((1, LANES), F32),
            pltpu.SemaphoreType.DMA((N_L,)), pltpu.SemaphoreType.DMA((N_S,)), pltpu.SemaphoreType.DMA((N_R,)),
        ],
        compiler_params=pltpu.CompilerParams(collective_id=0, has_side_effects=True, vmem_limit_bytes=67043328),
        cost_estimate=pl.CostEstimate(flops=18 * dots, bytes_accessed=64 * 16 * t * m, transcendentals=16 * t * f),
        name="group_step",
    )(ids, xm, w1, w2, gain, d_out)


def lookup_kernel(shard_rows, ids_smem, ids_vmem, table, out_hbm, got, rows, sem, out_sem):
    total, m = out_hbm.shape
    t = total // 4
    per = 32
    chunks = total // per
    r = lax.axis_index("tensor")
    spread = (1 << (shard_rows.bit_length() - 1)) - 1

    def fetch(k):
        def some(j, carry):
            for u in range(8):
                p = k * per + j * 8 + u
                row = ids_smem[jnp.right_shift(p, 7), p & (LANES - 1)]
                near = row - r * shard_rows
                near = jnp.where((near >= 0) & (near < shard_rows), near, row & spread)
                pltpu.make_async_copy(table.at[jnp.right_shift(near, 3)], got.at[p], sem.at[k]).start()
            return carry

        lax.fori_loop(0, per // 8, some, 0)

    loop(0, chunks, fetch)
    spot = lax.broadcasted_iota(I32, (per, 8 * per), 1)
    token = lax.broadcasted_iota(I32, (per, 8 * per), 0)
    same = lax.broadcasted_iota(I32, (LANES, LANES), 0) == lax.broadcasted_iota(I32, (LANES, LANES), 1)

    def line(b):
        ids = ids_vmem[pl.ds(b, 1), :].astype(F32)
        col = jnp.sum(jnp.where(same, jnp.broadcast_to(ids, (LANES, LANES)), 0.0), axis=1, keepdims=True).astype(I32)
        row = col - r * shard_rows
        row = jnp.where((row >= 0) & (row < shard_rows), row & 7, -8 * per)
        for j in range(LANES // per):
            k = b * (LANES // per) + j
            at = pl.ds(pl.multiple_of(k * per, per), per)
            pltpu.make_async_copy(got.at[at], got.at[at], sem.at[k]).wait()
            want = row[j * per : (j + 1) * per] + 8 * token
            chosen = jnp.where(want == spot, 1.0, 0.0).astype(BF16)
            picked = jnp.dot(chosen, got[at].reshape(8 * per, m), preferred_element_type=F32)
            p = k * per
            nat = lax.div(p, t)
            to = pl.multiple_of(lax.rem(nat, 2) * (2 * t) + lax.div(nat, 2) * t + lax.rem(p, t), per)
            rows[pl.ds(to, per), :] = picked.astype(BF16)
            pltpu.make_async_copy(rows.at[pl.ds(to, per)], out_hbm.at[pl.ds(to, per)], out_sem).start()

    loop(0, total // LANES, line)
    pltpu.make_async_copy(rows, out_hbm, out_sem).wait()


def look_up(ids, table):
    shard_rows, m = table.shape
    total = ids.size
    any_ = pl.BlockSpec(memory_space=pl.ANY)
    return pl.pallas_call(
        functools.partial(lookup_kernel, shard_rows),
        out_shape=jax.ShapeDtypeStruct((total, m), BF16),
        in_specs=[pl.BlockSpec(memory_space=pltpu.SMEM), pl.BlockSpec(memory_space=pltpu.VMEM), any_],
        out_specs=any_,
        scratch_shapes=[
            pltpu.VMEM((total, 8, m), BF16), pltpu.VMEM((total, m), BF16),
            pltpu.SemaphoreType.DMA((total // 32,)), pltpu.SemaphoreType.DMA,
        ],
        compiler_params=pltpu.CompilerParams(vmem_limit_bytes=60 << 20),
        cost_estimate=pl.CostEstimate(flops=16 * total * m, bytes_accessed=20 * total * m, transcendentals=0),
        name="look_up",
    )(ids, ids, table.reshape(shard_rows // 8, 8, m))


RING = 6


def weights_kernel(p1, p2, nk_in, dk_in, hk_in, duk_in, o1, o2, b1, b2, nk, dk, hk, duk, in_sem, out_sem, k_sem):
    m, f = b1.shape
    tw = nk.shape[0] // 2
    ins = [pltpu.make_async_copy(a, b, k_sem.at[i]) for i, (a, b) in enumerate(((nk_in, nk), (duk_in, duk), (hk_in, hk), (dk_in, dk)))]
    for cp in ins[:2]:
        cp.start()

    def part(src, buf, dst, first, i, rows=tw):
        at = pl.ds(pl.multiple_of(i * tw, 8), rows)
        fetch = pltpu.make_async_copy(src.at[at], buf.at[at], in_sem.at[first + i])
        return fetch, pltpu.make_async_copy(buf.at[at], dst.at[at], out_sem)

    def fetch_all(src, buf, dst, first):
        loop(0, src.shape[0] // tw, lambda i: part(src, buf, dst, first, i)[0].start())

    n1, n2 = m // tw, f // tw
    fetch_all(p1, b1, o1, 0)
    for cp in ins[2:]:
        cp.start()
    fetch_all(p2, b2, o2, n1)
    rest = [part(p2, b2, o2, n1, n2, f % tw)] if f % tw else []
    for come, _ in rest:
        come.start()

    def add(src, buf, dst, first, lhs, rhs, i, rows=tw):
        come, go = part(src, buf, dst, first, i, rows)
        come.wait()
        cols = pl.ds(pl.multiple_of(i * tw, tw), rows)
        buf[cols, :] += lax.dot_general(lhs[:, cols], rhs[...], TN, preferred_element_type=F32)
        go.start()

    for cp in ins[:2]:
        cp.wait()
    loop(0, n1, lambda i: add(p1, b1, o1, 0, nk, duk, i))
    for cp in ins[2:]:
        cp.wait()
    loop(0, n2, lambda i: add(p2, b2, o2, n1, hk, dk, i))
    if rest:
        add(p2, b2, o2, n1, hk, dk, n2, f % tw)
    pltpu.make_async_copy(b1, o1, out_sem).wait()
    pltpu.make_async_copy(b2, o2, out_sem).wait()


def finish_weights(p1, p2, nk, dk, hk, duk):
    any_ = pl.BlockSpec(memory_space=pl.ANY)
    V, S = pltpu.VMEM, pltpu.SemaphoreType.DMA
    arrays = (p1, p2, nk, dk, hk, duk)
    return pl.pallas_call(
        weights_kernel,
        out_shape=(jax.ShapeDtypeStruct(p1.shape, F32), jax.ShapeDtypeStruct(p2.shape, F32)),
        in_specs=[any_] * 6,
        out_specs=[any_] * 2,
        scratch_shapes=[*[V(a.shape, a.dtype) for a in arrays], S((32,)), S, S((4,))],
        compiler_params=pltpu.CompilerParams(vmem_limit_bytes=60 << 20),
        cost_estimate=pl.CostEstimate(flops=8000 * p1.size, bytes_accessed=20 * p1.size, transcendentals=0),
        name="finish_weights",
    )(*arrays)


def table_kernel(tall, key_ref, first_ref, dx_in, far_own, far_across, far_partner, far_both, out_hbm, dxb, dxf, ring, dx_sem, t_sem):
    count, _ = dxb.shape
    t = count // 16
    shift = count.bit_length() - 1
    steps = out_hbm.shape[0] // tall
    z, r = lax.axis_index("data"), lax.axis_index("tensor")
    y, c = lax.div(r, 2), lax.rem(r, 2)
    late = lax.div(z, 2)

    def near(k):
        at = pl.ds(pl.multiple_of(late * (4 * t) + k * (2 * t), t), 2 * t)
        return at, pltpu.make_async_copy(dx_in.at[at], dxb.at[at], dx_sem.at[k])

    def far(k, src, cc, yy):
        at = pl.ds(pl.multiple_of((1 - late) * (12 * t) + cc * (2 * t) + yy * t, t), t)
        return at, pltpu.make_async_copy(src, dxb.at[at], dx_sem.at[6 + k])

    fars = ((far_own, c, y), (far_across, c, 1 - y), (far_partner, 1 - c, y), (far_both, 1 - c, 1 - y))
    loop(0, 6, lambda k: near(k)[1].start())
    for k, what in enumerate(fars):
        far(k, *what)[1].start()

    def widen_piece(at, cp):
        cp.wait()

        def widen(i):
            rows = pl.ds(pl.multiple_of(at.start + i, 16), 16)
            dxf[rows, :] = dxb[rows, :].astype(F32)

        rows_loop(at.size, widen)

    loop(0, 6, lambda k: widen_piece(*near(k)))
    for k, what in enumerate(fars):
        widen_piece(*far(k, *what))

    def tile_out(i):
        slot = lax.rem(i, RING)
        return pltpu.make_async_copy(ring.at[slot], out_hbm.at[pl.ds(pl.multiple_of(i * tall, 8), tall)], t_sem.at[slot])

    def tile(i):
        slot = lax.rem(i, RING)
        here = ring.at[slot]
        pl.when(i >= RING)(lambda: tile_out(i - RING).wait())
        here[...] = jnp.zeros_like(here)

        def add(j, key):
            ahead = key_ref[jnp.minimum(j + 1, count - 1)]
            to = pl.ds(jnp.right_shift(key, shift) - i * tall, 1)
            here[to, :] += dxf[pl.ds(key & (count - 1), 1), :]
            return ahead

        low = first_ref[i]
        lax.fori_loop(low, first_ref[i + 1], add, key_ref[jnp.minimum(low, count - 1)])
        tile_out(i).start()

    loop(0, steps, tile)
    loop(steps - RING, steps, lambda i: tile_out(i).wait())


def table_grad(ordered, first, dx_all, fars, shard_rows, tall):
    count, m = dx_all.shape
    any_ = pl.BlockSpec(memory_space=pl.ANY)
    V, S = pltpu.VMEM, pltpu.SemaphoreType.DMA
    return pl.pallas_call(
        functools.partial(table_kernel, tall),
        out_shape=jax.ShapeDtypeStruct((shard_rows, m), F32),
        grid_spec=pltpu.PrefetchScalarGridSpec(
            num_scalar_prefetch=2,
            grid=(1,),
            in_specs=[any_] * 5,
            out_specs=any_,
            scratch_shapes=[
                V((count, m), BF16), V((count, m), F32), V((RING, tall, m), F32), S((10,)), S((RING,)),
            ],
        ),
        compiler_params=pltpu.CompilerParams(vmem_limit_bytes=60 << 20),
        cost_estimate=pl.CostEstimate(flops=16000 * shard_rows * m // 10, bytes_accessed=4 * shard_rows * m, transcendentals=0),
        name="table_grad",
    )(ordered, first, dx_all, *fars)


def solution(mesh):
    tok_spec = P(("pod", "data", "tensor"), None)

    over_y, over_core = [(0, 2), (1, 3), (2, 0), (3, 1)], [(0, 1), (1, 0), (2, 3), (3, 2)]

    def per_device(token_ids, embed_table, norm_gain, w_in, w_out, d_out):
        shard_rows = embed_table.shape[0]
        tall = next(k for k in (160, 8) if shard_rows % k == 0)
        ids = token_ids.reshape(-1, LANES)
        masked = look_up(ids, embed_table)
        gain = norm_gain.reshape(-1, LANES)
        base, ysum, ordered, first, dx_all, far, *weights = run_group(
            ids, masked, w_in, w_out, gain, d_out, shard_rows, tall
        )
        far_x = lax.ppermute(far, "tensor", over_y)
        far_p = lax.ppermute(far, "tensor", over_core)
        other = lax.ppermute(ysum, "tensor", over_y)
        grad_w_in, grad_w_out = finish_weights(*weights)
        far_b = lax.ppermute(far_x, "tensor", over_core)
        fars = (far, far_x, far_p, far_b)
        grad_table = table_grad(ordered.reshape(-1), first.reshape(-1), dx_all, fars, shard_rows, tall)
        return (base + other).astype(BF16), grad_table, grad_w_in, grad_w_out

    return jax.shard_map(
        per_device,
        mesh=mesh,
        in_specs=(P(("pod", "data")), P("tensor", None), P(None), P(None, "tensor"), P("tensor", None), tok_spec),
        out_specs=(tok_spec, P(("pod", "tensor"), None), P("pod", "tensor"), P(("pod", "tensor"), None)),
        check_vma=False,
    )
```

```python
import functools

import jax
import jax.numpy as jnp
from jax import lax
from jax.experimental import pallas as pl
from jax.experimental.pallas import tpu as pltpu
from jax.sharding import PartitionSpec as P


NORM_EPS = 1e-6
GELU_A = 0.7978845608028654
GELU_B = 0.044715
MESH = pl.DeviceIdType.MESH
NT = (((1,), (1,)), ((), ()))
TN = (((0,), (0,)), ((), ()))
F32, BF16, I32 = jnp.float32, jnp.bfloat16, jnp.int32
LANES = 128
XQ = 4
PQ = 4

R_IDS, R_DZ, R_DY, R_DC, R_NZ, R_NC, R_XZ, R_XY, R_XC = 0, 4, 8, 12, 16, 24, 28, 36, 44
R_XM, R_X, R_NO, R_PC, R_PY, N_R = 48, 52, 56, 60, 68, 72
S_IDS, S_DZ, S_DY, S_DC, S_NZ, S_NC, S_XZ, S_XY, S_XC = 0, 3, 8, 12, 16, 26, 30, 40, 48
S_XM, S_X, S_NO, S_PC, S_PY, N_S = 52, 56, 60, 64, 72, 76
L_W1, L_W2, L_XM, L_DX, L_YS, L_YB, L_DW, L_DO, L_K, N_L = 0, 1, 2, 3, 4, 5, 6, 8, 9, 13


def loop(lo, hi, body):
    def one(j, carry):
        body(j)
        return carry

    lax.fori_loop(lo, hi, one, 0)


def tiles(total, step, body):
    full = total // step
    loop(0, full, lambda j: body(pl.multiple_of(j * step, step), step))
    if total % step:
        body(full * step, total % step)


def rows_loop(total, body):
    loop(0, total // 16, lambda j: body(pl.multiple_of(j * 16, 16)))


def make_keys(ids, keys, shard_rows, rank0):
    reps, per, _ = ids.shape
    count = reps * per * LANES
    t = per * LANES // 4
    shift = t.bit_length() - 1
    lane = lax.broadcasted_iota(I32, (per, LANES), 1)
    spot = lax.broadcasted_iota(I32, (per, LANES), 0) * LANES + lane
    block = jnp.right_shift(spot, shift)
    kept = (block & 1) * (2 * t) + jnp.right_shift(block, 1) * t + (spot & (t - 1))
    for k in range(reps):
        row = ids[k] - rank0
        row = jnp.where((row >= 0) & (row < shard_rows), row, shard_rows)
        keys[k * per : (k + 1) * per, :] = (row * count + (k * per * LANES + kept)).astype(F32)


def columns(refs, b):
    same = lax.broadcasted_iota(I32, (LANES, LANES), 0) == lax.broadcasted_iota(I32, (LANES, LANES), 1)
    wide = (jnp.where(same, jnp.broadcast_to(ref[pl.ds(b, 1), :], (LANES, LANES)), 0.0) for ref in refs)
    return [jnp.sum(w, axis=1, keepdims=True) for w in wide]


def count_below(keys, place):
    lines = keys.shape[0]
    place[...] = jnp.zeros_like(place)

    def some(j):
        cols = [columns((keys,), 4 * j + u)[0] for u in range(4)]
        for a in range(lines):
            row = keys[a : a + 1, :]
            hits = sum(jnp.where(col < row, 1.0, 0.0) for col in cols)
            place[a : a + 1, :] += jnp.sum(hits, axis=0, keepdims=True)

    loop(0, lines // 4, some)


def put_in_order(keys, place, ordered, first, tall):
    lines = keys.shape[0]
    ordered[...] = jnp.zeros_like(ordered)
    first[...] = jnp.zeros_like(first)
    lane = lax.broadcasted_iota(I32, (1, LANES), 1).astype(F32)
    edge = lane * float(tall * lines * LANES)

    def some(j):
        cols = [columns((keys, place), 4 * j + u) for u in range(4)]
        for a in range(lines):
            want = lane + float(a * LANES)
            hits = sum(jnp.where(spot == want, key, 0.0) for key, spot in cols)
            ordered[a : a + 1, :] += jnp.sum(hits, axis=0, keepdims=True)
        first[...] += jnp.sum(sum(jnp.where(key < edge, 1.0, 0.0) for key, _ in cols), axis=0, keepdims=True)

    loop(0, lines // 4, some)


def group_kernel(shard_rows, tall, ids_ref, xm_hbm, w1_hbm, w2_hbm, g_ref, do_hbm,
                 base_o, ysum_o, ord_o, first_o, dx_o, far_o, dw1_o, dw2_o, nk_o, dk_o, hk_o, duk_o,
                 w1, w2, n, d, xm, xc, xy, hs, dus, pd, pf, rd, rf, yd, yb, dxo, idl, keys, place, ordered, first,
                 lsem, ssem, rsem):
    t, m = do_hbm.shape
    f = w1_hbm.shape[1]
    tq, mq = 2 * t // XQ, m // PQ
    z = lax.axis_index("data")
    r = lax.axis_index("tensor")
    y, c = lax.div(r, 2), lax.rem(r, 2)
    partner = {"tensor": 2 * y + 1 - c}
    across = {"tensor": 2 * (1 - y) + c}
    half = lax.div(z, 2)
    inner = z + half * (3 - 2 * z)
    order = [b + half * (3 - 2 * b) for b in (1 - inner, 2, 3)]
    middle, end = inner == 1, inner == 0

    def row(zz, cc, yy=0):
        return pl.multiple_of(zz * (4 * t) + cc * (2 * t) + yy * t, t)

    def blk(ref, zz, cc, yy):
        return ref.at[pl.ds(row(zz, cc, yy), t)]

    def duo(ref, zz, cc):
        return ref.at[pl.ds(row(zz, cc), 2 * t)]

    def remote(src, dst, s, q, dev):
        return pltpu.make_async_remote_copy(
            src_ref=src, dst_ref=dst, send_sem=ssem.at[s], recv_sem=rsem.at[q], device_id=dev, device_id_type=MESH
        )

    def local(src, dst, i):
        return pltpu.make_async_copy(src, dst, lsem.at[i])

    def arrived(ref, q):
        remote(ref, ref, 0, q, partner).wait_recv()

    def start(cp):
        cp.start()

    def sent(cp):
        cp.wait_send()

    def along(src, dst, s, q, act):
        for i, hop in enumerate((1, -1)):
            to = z + hop

            @pl.when((to >= 0) & (to <= 3))
            def _():
                act(remote(src, dst, s + i, q + z, {"data": to}))

    def pass_on(k, ref, s, q, act):
        src, dst = ref if isinstance(ref, tuple) else (ref, ref)
        act(remote(src, dst, s + 2 + k, q + order[k], {"data": order[1] if k == 0 else order[0]}))

    barrier = pltpu.get_barrier_semaphore()
    pl.semaphore_signal(barrier, inc=1, device_id=partner, device_id_type=MESH)
    pl.semaphore_signal(barrier, inc=1, device_id=across, device_id_type=MESH)
    for k in range(3):
        pl.semaphore_signal(barrier, inc=1, device_id={"data": order[k]}, device_id_type=MESH)

    own_d = blk(d, z, c, y)
    local(do_hbm, own_d, L_DO).start()
    local(xm_hbm, xm, L_XM).start()
    local(w1_hbm, w1, L_W1).start()
    local(w2_hbm, w2, L_W2).start()
    pl.semaphore_wait(barrier, 5)

    def piece(q):
        return pl.ds(q * tq, tq)

    for k in range(3):
        remote(ids_ref, idl.at[z], S_IDS + k, R_IDS + z, {"data": order[k]}).start()
    idl[z] = ids_ref[...]

    local(do_hbm, own_d, L_DO).wait()
    along(own_d, own_d, S_DZ, R_DZ, start)
    local(xm_hbm, xm, L_XM).wait()

    def xm_part(q):
        return remote(xm.at[pl.ds(row(0, 1 - c) + q * tq, tq)], xc.at[piece(q)], S_XM + q, R_XM + q, partner)

    def x_part(q):
        return remote(xc.at[piece(q)], xy.at[piece(q)], S_X + q, R_X + q, across)

    def d_got(k):
        arrived(blk(d, order[k], c, y), R_DZ + order[k])

    def d_on(k):
        pass_on(k, blk(d, order[k], c, y), S_DZ, R_DZ, start)

    def d_across(zz, act):
        act(remote(blk(d, zz, c, y), blk(d, zz, c, y), S_DY + zz, R_DY + zz, across))

    def d_pair(zz, act):
        act(remote(duo(d, zz, c), duo(d, zz, c), S_DC + zz, R_DC + zz, partner))

    for q in range(XQ):
        xm_part(q).start()
    for q in range(XQ):
        arrived(xc.at[piece(q)], R_XM + q)

        def join(i, q=q):
            at = pl.ds(q * tq + i, 16)
            xc[at, :] += xm[pl.ds(row(0, c) + q * tq + i, 16), :]

        rows_loop(tq, join)
        x_part(q).start()
    d_across(z, start)

    for k in range(3):
        arrived(idl.at[order[k]], R_IDS + order[k])
    make_keys(idl, keys, shard_rows, r * shard_rows)
    count_below(keys, place)
    d_got(0)

    @pl.when(middle)
    def _():
        d_on(0)
        d_got(1)
        d_on(1)

    gain = jnp.concatenate([g_ref[pl.ds(i, 1), :] for i in range(m // LANES)], axis=1).astype(F32)

    def n_own(q, act):
        at = n.at[pl.ds(row(z, c) + q * tq, tq)]
        act(remote(at, at, S_NO + q, R_NO + q, partner))

    def n_along(b, act):
        ref = blk(n, z, c, b)
        along(ref, ref, S_NZ + 5 * b, R_NZ + 4 * b, act)

    for q in range(XQ):
        arrived(xy.at[piece(q)], R_X + q)
        x_part(q).wait_send()

        def norm(i, q=q):
            at = pl.ds(q * tq + i, 16)
            x16 = xc[at, :] + xy[at, :]
            xc[at, :] = x16
            x = x16.astype(F32)
            s = lax.rsqrt(jnp.mean(x * x, axis=-1, keepdims=True) + NORM_EPS)
            n[pl.ds(row(z, c) + q * tq + i, 16), :] = ((x * s) * gain).astype(BF16)

        rows_loop(tq, norm)
        n_own(q, start)
        if q == XQ // 2 - 1:
            n_along(0, start)
            put_in_order(keys, place, ordered, first, tall)
            ord_o[...] = ordered[...].astype(I32)
            first_o[...] = first[...].astype(I32)

            @pl.when(middle)
            def _():
                d_got(2)
                d_on(2)

        if q == XQ - 1:
            n_along(1, start)
    d_across(order[0], start)

    def hidden(zz, slopes):
        at = pl.ds(row(zz, 0), 4 * t)

        def body(off, w):
            to = pl.ds(off, w)
            u = jnp.dot(n[at, :], w1[:, to], preferred_element_type=F32).astype(BF16).astype(F32)
            uu = u * u
            th = jnp.tanh(GELU_A * (u + GELU_B * (uu * u)))
            cdf = 0.5 * (1.0 + th)
            hs[at, to] = (u * cdf).astype(BF16)
            slopes[:, to] = cdf + (0.5 * GELU_A) * u * (1.0 - th * th) * (1.0 + (3.0 * GELU_B) * uu)

        tiles(f, 256, body)

    def grad_hidden(zz, slopes):
        at = pl.ds(row(zz, 0), 4 * t)

        def body(off, w):
            to = pl.ds(off, w)
            dh = lax.dot_general(d[at, :], w2[to, :], NT, preferred_element_type=F32)
            dus[at, to] = (dh * slopes[:, to]).astype(BF16)

        tiles(f, 256, body)

    for q in range(XQ):
        arrived(n.at[pl.ds(row(z, 1 - c) + q * tq, tq)], R_NO + q)
    local(w1_hbm, w1, L_W1).wait()
    hidden(z, pf)
    arrived(blk(d, z, c, 1 - y), R_DY + z)
    d_pair(z, start)
    arrived(duo(d, z, 1 - c), R_DC + z)
    local(w2_hbm, w2, L_W2).wait()
    grad_hidden(z, pf)

    own_rows = pl.ds(row(z, 0), 4 * t)
    far = pl.multiple_of((1 - y) * t, t)

    def cols(q):
        return pl.ds(pl.multiple_of(q * mq, mq), mq)

    def part_pair(src, dst, i, q):
        return remote(src.at[pl.ds(row(0, 1 - c), 2 * t), cols(q)], dst.at[:, cols(q)], S_PC + PQ * i + q, R_PC + PQ * i + q, partner)

    def part_across(q):
        return remote(rd.at[pl.ds(far, t), cols(q)], yd.at[:, cols(q)], S_PY + q, R_PY + q, across)

    def sum_part(part, got, i, q):
        arrived(got.at[:, cols(q)], R_PC + PQ * i + q)

        def add(k):
            got[pl.ds(far + k, 16), cols(q)] += part[pl.ds(row(0, c, 1 - y) + k, 16), cols(q)]

        rows_loop(t, add)

    def dn_part(q):
        pd[:, cols(q)] = lax.dot_general(dus[own_rows, :], w1[cols(q), :], NT, preferred_element_type=F32)
        part_pair(pd, rd, 0, q).start()

    def y_part(q):
        pf[:, cols(q)] = jnp.dot(hs[own_rows, :], w2[:, cols(q)], preferred_element_type=F32)
        part_pair(pf, rf, 1, q).start()

    def dn_out(q):
        sum_part(pd, rd, 0, q)
        part_across(q).start()

    loop(0, PQ, dn_part)
    loop(0, PQ, dn_out)
    loop(0, PQ, y_part)

    @pl.when(end)
    def _():
        d_got(1)

    d_across(order[1], start)

    loop(0, PQ, lambda q: sum_part(pf, rf, 1, q))
    y_send = local(rf.at[pl.ds(far, t)], ysum_o, L_YS)
    y_send.start()

    def base(i):
        own = pl.ds(y * t + i, 16)
        yb[pl.ds(i, 16), :] = xc[own, :].astype(F32) + (pf[pl.ds(row(0, c, y) + i, 16), :] + rf[own, :])

    rows_loop(t, base)
    y_keep = local(yb, base_o, L_YB)
    y_keep.start()
    for q in range(PQ):
        part_pair(pf, rf, 1, q).wait_send()

    def n_got(k):
        for b in range(2):
            arrived(blk(n, order[k], c, b), R_NZ + 4 * b + order[k])

    def n_on(k):
        for b in range(2):
            pass_on(k, blk(n, order[k], c, b), S_NZ + 5 * b, R_NZ + 4 * b, start)

    def n_pair(zz, act):
        act(remote(duo(n, zz, c), duo(n, zz, c), S_NC + zz, R_NC + zz, partner))

    n_got(0)
    n_pair(order[0], start)

    @pl.when(middle)
    def _():
        n_on(0)
        n_got(1)
        n_on(1)
        n_pair(order[1], start)

    def unit(k, slopes):
        zz = order[k]
        arrived(blk(d, zz, c, 1 - y), R_DY + zz)
        d_pair(zz, start)
        arrived(duo(n, zz, 1 - c), R_NC + zz)
        hidden(zz, slopes)
        arrived(duo(d, zz, 1 - c), R_DC + zz)
        grad_hidden(zz, slopes)

    def n_rest(k, on):
        n_got(k)
        if on:
            n_on(k)
        n_pair(order[k], start)

    unit(0, pf)

    for q in range(PQ):
        arrived(yd.at[:, cols(q)], R_PY + q)

    def grad_x(i):
        at, own = pl.ds(i, 16), pl.ds(y * t + i, 16)
        dn = pd[pl.ds(row(0, c, y) + i, 16), :] + rd[own, :] + yd[at, :]
        x = xc[own, :].astype(F32)
        s = lax.rsqrt(jnp.mean(x * x, axis=-1, keepdims=True) + NORM_EPS)
        xh = x * s
        dhat = dn * gain
        dxn = s * (dhat - xh * jnp.mean(dhat * xh, axis=-1, keepdims=True))
        dxo[at, :] = (d[pl.ds(row(z, c, y) + i, 16), :].astype(F32) + dxn).astype(BF16)

    rows_loop(t, grad_x)
    th = t // 2

    def dx_part(zz, yy, h):
        return dx_o.at[pl.ds(pl.multiple_of(row(zz, c, yy) + h * th, th), th)]

    def dx_own(h):
        return dxo.at[pl.ds(h * th, th)]

    def far_part(h):
        return far_o.at[pl.ds(h * th, th)]

    def dx_next(k, h):
        here = dx_part(order[k], y, h)
        return (here, here) if k == 1 else (here if k == 0 else far_part(h), far_part(h))

    def dx_across(zz, src, h, act):
        act(remote(src, dx_part(zz, y, h), S_XY + 4 * h + zz, R_XY + 4 * h + zz, across))

    def dx_along(act):
        for h in range(2):
            along(dx_own(h), dx_part(z, y, h), S_XZ + 5 * h, R_XZ + 4 * h, act)

    def dx_pair(zz, act):
        act(remote(duo(dx_o, zz, c), duo(dx_o, zz, c), S_XC + zz, R_XC + zz, partner))

    def dx_got(k, on):
        zz = order[k]
        for h in range(2):
            arrived(dx_part(zz, y, h) if k < 2 else far_part(h), R_XZ + 4 * h + zz)
            if on:
                pass_on(k, dx_next(k, h), S_XZ + 5 * h, R_XZ + 4 * h, start)
            if k < 2:
                dx_across(zz, dx_part(zz, y, h), h, start)

    def dx_hand(zz):
        for h in range(2):
            arrived(dx_part(zz, 1 - y, h), R_XY + 4 * h + zz)
        dx_pair(zz, start)

    for h in range(2):
        dx_across(z, dx_own(h), h, start)
    local(dxo, blk(dx_o, z, c, y), L_DX).start()

    @pl.when(end)
    def _():
        d_got(2)

    d_across(order[2], start)

    for q in range(PQ):
        part_pair(pd, rd, 0, q).wait_send()

    pl.when(middle)(lambda: n_rest(2, True))
    dx_along(start)
    pl.when(end)(lambda: n_rest(1, False))
    unit(1, pd)

    @pl.when(middle)
    def _():
        dx_got(0, True)
        dx_got(1, True)

    tw = 2 * t
    n1, n2 = m // tw, f // tw
    late_rows = pl.ds(row(order[2], 0), 4 * t)
    early_rows = pl.ds(pl.multiple_of(half * (4 * t), 4 * t), 12 * t)

    def flush(i, buf, dst):
        lines = pl.ds(pl.multiple_of(lax.rem(i, 2) * tw, tw), tw)
        here = buf.at[lines, pl.ds(0, dst.shape[1])]
        return here, local(here, dst.at[pl.ds(pl.multiple_of(i * tw, tw), tw)], L_DW + lax.rem(i, 2))

    def weight_tile(i, lhs, rhs, buf, dst):
        pl.when(i >= 2)(lambda: flush(i - 2, buf, dst)[1].wait())
        here, out = flush(i, buf, dst)
        at = pl.ds(pl.multiple_of(i * tw, tw), tw)
        here[...] = lax.dot_general(lhs[early_rows, at], rhs[early_rows, :], TN, preferred_element_type=F32)
        out.start()

    loop(0, n1, lambda i: weight_tile(i, n, dus, pf, dw1_o))
    for i in (n1 - 2, n1 - 1):
        flush(i, pf, dw1_o)[1].wait()
    pl.when(end)(lambda: n_rest(2, False))
    unit(2, pd)
    kept = [
        local(src.at[late_rows], dst, L_K + i)
        for i, (src, dst) in enumerate(((n, nk_o), (d, dk_o), (hs, hk_o), (dus, duk_o)))
    ]
    for cp in kept:
        cp.start()
    pl.when(end)(lambda: dx_got(0, False))
    pl.when(middle)(lambda: dx_got(2, True))
    loop(0, n2 // 2, lambda i: weight_tile(i, hs, d, pd, dw2_o))
    pl.when(end)(lambda: dx_got(1, False))
    loop(n2 // 2, n2, lambda i: weight_tile(i, hs, d, pd, dw2_o))
    local(dxo, blk(dx_o, z, c, y), L_DX).wait()
    dx_hand(z)
    dx_hand(order[0])
    for i in (n2 - 2, n2 - 1):
        flush(i, pd, dw2_o)[1].wait()
    if f % tw:
        rest = pd.at[pl.ds(0, f % tw)]
        rest[...] = lax.dot_general(hs[early_rows, n2 * tw :], d[early_rows, :], TN, preferred_element_type=F32)
        last = local(rest, dw2_o.at[pl.ds(n2 * tw, f % tw)], L_DW)
        last.start()
    dx_hand(order[1])
    pl.when(end)(lambda: dx_got(2, False))
    if f % tw:
        last.wait()
    for cp in kept:
        cp.wait()

    y_send.wait()
    y_keep.wait()
    along(own_d, own_d, S_DZ, R_DZ, sent)
    for zz in (z, *order):
        d_across(zz, sent)
        d_pair(zz, sent)
    for k in range(3):
        n_pair(order[k], sent)
        remote(ids_ref, idl.at[z], S_IDS + k, R_IDS + z, {"data": order[k]}).wait_send()
    dx_along(sent)
    for b in range(2):
        n_along(b, sent)
        dx_across(z, dx_own(b), b, sent)
        for k in range(2):
            dx_across(order[k], dx_part(order[k], y, b), b, sent)

    @pl.when(middle)
    def _():
        for k in range(3):
            pass_on(k, blk(d, order[k], c, y), S_DZ, R_DZ, sent)
            for b in range(2):
                pass_on(k, dx_next(k, b), S_XZ + 5 * b, R_XZ + 4 * b, sent)
                pass_on(k, blk(n, order[k], c, b), S_NZ + 5 * b, R_NZ + 4 * b, sent)

    for q in range(XQ):
        xm_part(q).wait_send()
        n_own(q, sent)
    for q in range(PQ):
        part_across(q).wait_send()
    for zz in (z, *order[:2]):
        arrived(duo(dx_o, zz, 1 - c), R_XC + zz)
        dx_pair(zz, sent)


def run_group(ids, xm, w1, w2, gain, d_out, shard_rows, tall):
    t, m = d_out.shape
    f = w1.shape[1]
    lines = 4 * ids.shape[0]
    any_, vmem = pl.BlockSpec(memory_space=pl.ANY), pl.BlockSpec(memory_space=pltpu.VMEM)
    V = pltpu.VMEM
    sds = jax.ShapeDtypeStruct
    dots = 2 * 4 * t * m * f
    return pl.pallas_call(
        functools.partial(group_kernel, shard_rows, tall),
        out_shape=(
            sds((t, m), F32), sds((t, m), F32), sds((lines, LANES), I32), sds((1, LANES), I32), sds((16 * t, m), BF16),
            sds((t, m), BF16), sds((m, f), F32), sds((f, m), F32),
            sds((4 * t, m), BF16), sds((4 * t, m), BF16), sds((4 * t, f), BF16), sds((4 * t, f), BF16),
        ),
        in_specs=[vmem, any_, any_, any_, vmem, any_],
        out_specs=(any_, any_, vmem, vmem, *[any_] * 8),
        scratch_shapes=[
            V((m, f), BF16), V((f, m), BF16), V((16 * t, m), BF16), V((16 * t, m), BF16),
            V((4 * t, m), BF16), V((2 * t, m), BF16), V((2 * t, m), BF16),
            V((16 * t, f), BF16), V((16 * t, f), BF16),
            V((4 * t, m), F32), V((4 * t, m), F32), V((2 * t, m), F32), V((2 * t, m), F32),
            V((t, m), F32), V((t, m), F32),
            V((t, m), BF16), V((4, *ids.shape), I32),
            V((lines, LANES), F32), V((lines, LANES), F32), V((lines, LANES), F32), V((1, LANES), F32),
            pltpu.SemaphoreType.DMA((N_L,)), pltpu.SemaphoreType.DMA((N_S,)), pltpu.SemaphoreType.DMA((N_R,)),
        ],
        compiler_params=pltpu.CompilerParams(collective_id=0, has_side_effects=True, vmem_limit_bytes=67043328),
        cost_estimate=pl.CostEstimate(flops=18 * dots, bytes_accessed=64 * 16 * t * m, transcendentals=16 * t * f),
        name="group_step",
    )(ids, xm, w1, w2, gain, d_out)


def lookup_kernel(shard_rows, ids_smem, ids_vmem, table, out_hbm, got, rows, sem, out_sem):
    total, m = out_hbm.shape
    t = total // 4
    per = 32
    chunks = total // per
    r = lax.axis_index("tensor")
    spread = (1 << (shard_rows.bit_length() - 1)) - 1

    def fetch(k):
        def some(j, carry):
            for u in range(8):
                p = k * per + j * 8 + u
                row = ids_smem[jnp.right_shift(p, 7), p & (LANES - 1)]
                near = row - r * shard_rows
                near = jnp.where((near >= 0) & (near < shard_rows), near, row & spread)
                pltpu.make_async_copy(table.at[jnp.right_shift(near, 3)], got.at[p], sem.at[k]).start()
            return carry

        lax.fori_loop(0, per // 8, some, 0)

    loop(0, chunks, fetch)
    spot = lax.broadcasted_iota(I32, (per, 8 * per), 1)
    token = lax.broadcasted_iota(I32, (per, 8 * per), 0)
    same = lax.broadcasted_iota(I32, (LANES, LANES), 0) == lax.broadcasted_iota(I32, (LANES, LANES), 1)

    def line(b):
        ids = ids_vmem[pl.ds(b, 1), :].astype(F32)
        col = jnp.sum(jnp.where(same, jnp.broadcast_to(ids, (LANES, LANES)), 0.0), axis=1, keepdims=True).astype(I32)
        row = col - r * shard_rows
        row = jnp.where((row >= 0) & (row < shard_rows), row & 7, -8 * per)
        for j in range(LANES // per):
            k = b * (LANES // per) + j
            at = pl.ds(pl.multiple_of(k * per, per), per)
            pltpu.make_async_copy(got.at[at], got.at[at], sem.at[k]).wait()
            want = row[j * per : (j + 1) * per] + 8 * token
            chosen = jnp.where(want == spot, 1.0, 0.0).astype(BF16)
            picked = jnp.dot(chosen, got[at].reshape(8 * per, m), preferred_element_type=F32)
            p = k * per
            nat = lax.div(p, t)
            to = pl.multiple_of(lax.rem(nat, 2) * (2 * t) + lax.div(nat, 2) * t + lax.rem(p, t), per)
            rows[pl.ds(to, per), :] = picked.astype(BF16)
            pltpu.make_async_copy(rows.at[pl.ds(to, per)], out_hbm.at[pl.ds(to, per)], out_sem).start()

    loop(0, total // LANES, line)
    pltpu.make_async_copy(rows, out_hbm, out_sem).wait()


def look_up(ids, table):
    shard_rows, m = table.shape
    total = ids.size
    any_ = pl.BlockSpec(memory_space=pl.ANY)
    return pl.pallas_call(
        functools.partial(lookup_kernel, shard_rows),
        out_shape=jax.ShapeDtypeStruct((total, m), BF16),
        in_specs=[pl.BlockSpec(memory_space=pltpu.SMEM), pl.BlockSpec(memory_space=pltpu.VMEM), any_],
        out_specs=any_,
        scratch_shapes=[
            pltpu.VMEM((total, 8, m), BF16), pltpu.VMEM((total, m), BF16),
            pltpu.SemaphoreType.DMA((total // 32,)), pltpu.SemaphoreType.DMA,
        ],
        compiler_params=pltpu.CompilerParams(vmem_limit_bytes=60 << 20),
        cost_estimate=pl.CostEstimate(flops=16 * total * m, bytes_accessed=20 * total * m, transcendentals=0),
        name="look_up",
    )(ids, ids, table.reshape(shard_rows // 8, 8, m))


RING = 6


def weights_kernel(p1, p2, nk_in, dk_in, hk_in, duk_in, o1, o2, b1, b2, nk, dk, hk, duk, in_sem, out_sem, k_sem):
    m, f = b1.shape
    tw = nk.shape[0] // 2
    ins = [pltpu.make_async_copy(a, b, k_sem.at[i]) for i, (a, b) in enumerate(((nk_in, nk), (duk_in, duk), (hk_in, hk), (dk_in, dk)))]
    for cp in ins[:2]:
        cp.start()

    def part(src, buf, dst, first, i, rows=tw):
        at = pl.ds(pl.multiple_of(i * tw, 8), rows)
        fetch = pltpu.make_async_copy(src.at[at], buf.at[at], in_sem.at[first + i])
        return fetch, pltpu.make_async_copy(buf.at[at], dst.at[at], out_sem)

    def fetch_all(src, buf, dst, first):
        loop(0, src.shape[0] // tw, lambda i: part(src, buf, dst, first, i)[0].start())

    n1, n2 = m // tw, f // tw
    fetch_all(p1, b1, o1, 0)
    for cp in ins[2:]:
        cp.start()
    fetch_all(p2, b2, o2, n1)
    rest = [part(p2, b2, o2, n1, n2, f % tw)] if f % tw else []
    for come, _ in rest:
        come.start()

    def add(src, buf, dst, first, lhs, rhs, i, rows=tw):
        come, go = part(src, buf, dst, first, i, rows)
        come.wait()
        cols = pl.ds(pl.multiple_of(i * tw, tw), rows)
        buf[cols, :] += lax.dot_general(lhs[:, cols], rhs[...], TN, preferred_element_type=F32)
        go.start()

    for cp in ins[:2]:
        cp.wait()
    loop(0, n1, lambda i: add(p1, b1, o1, 0, nk, duk, i))
    for cp in ins[2:]:
        cp.wait()
    loop(0, n2, lambda i: add(p2, b2, o2, n1, hk, dk, i))
    if rest:
        add(p2, b2, o2, n1, hk, dk, n2, f % tw)
    pltpu.make_async_copy(b1, o1, out_sem).wait()
    pltpu.make_async_copy(b2, o2, out_sem).wait()


def finish_weights(p1, p2, nk, dk, hk, duk):
    any_ = pl.BlockSpec(memory_space=pl.ANY)
    V, S = pltpu.VMEM, pltpu.SemaphoreType.DMA
    arrays = (p1, p2, nk, dk, hk, duk)
    return pl.pallas_call(
        weights_kernel,
        out_shape=(jax.ShapeDtypeStruct(p1.shape, F32), jax.ShapeDtypeStruct(p2.shape, F32)),
        in_specs=[any_] * 6,
        out_specs=[any_] * 2,
        scratch_shapes=[*[V(a.shape, a.dtype) for a in arrays], S((32,)), S, S((4,))],
        compiler_params=pltpu.CompilerParams(vmem_limit_bytes=60 << 20),
        cost_estimate=pl.CostEstimate(flops=8000 * p1.size, bytes_accessed=20 * p1.size, transcendentals=0),
        name="finish_weights",
    )(*arrays)


def table_kernel(tall, key_ref, first_ref, dx_in, far_own, far_across, far_partner, far_both, out_hbm, dxb, dxf, ring, dx_sem, t_sem):
    count, _ = dxb.shape
    t = count // 16
    shift = count.bit_length() - 1
    steps = out_hbm.shape[0] // tall
    z, r = lax.axis_index("data"), lax.axis_index("tensor")
    y, c = lax.div(r, 2), lax.rem(r, 2)
    late = lax.div(z, 2)

    def near(k):
        at = pl.ds(pl.multiple_of(late * (4 * t) + k * (2 * t), t), 2 * t)
        return at, pltpu.make_async_copy(dx_in.at[at], dxb.at[at], dx_sem.at[k])

    def far(k, src, cc, yy):
        at = pl.ds(pl.multiple_of((1 - late) * (12 * t) + cc * (2 * t) + yy * t, t), t)
        return at, pltpu.make_async_copy(src, dxb.at[at], dx_sem.at[6 + k])

    fars = ((far_own, c, y), (far_across, c, 1 - y), (far_partner, 1 - c, y), (far_both, 1 - c, 1 - y))
    loop(0, 6, lambda k: near(k)[1].start())
    for k, what in enumerate(fars):
        far(k, *what)[1].start()

    def widen_piece(at, cp):
        cp.wait()

        def widen(i):
            rows = pl.ds(pl.multiple_of(at.start + i, 16), 16)
            dxf[rows, :] = dxb[rows, :].astype(F32)

        rows_loop(at.size, widen)

    loop(0, 6, lambda k: widen_piece(*near(k)))
    for k, what in enumerate(fars):
        widen_piece(*far(k, *what))

    def tile_out(i):
        slot = lax.rem(i, RING)
        return pltpu.make_async_copy(ring.at[slot], out_hbm.at[pl.ds(pl.multiple_of(i * tall, 8), tall)], t_sem.at[slot])

    def tile(i):
        slot = lax.rem(i, RING)
        here = ring.at[slot]
        pl.when(i >= RING)(lambda: tile_out(i - RING).wait())
        here[...] = jnp.zeros_like(here)

        def add(j, key):
            ahead = key_ref[jnp.minimum(j + 1, count - 1)]
            to = pl.ds(jnp.right_shift(key, shift) - i * tall, 1)
            here[to, :] += dxf[pl.ds(key & (count - 1), 1), :]
            return ahead

        low = first_ref[i]
        lax.fori_loop(low, first_ref[i + 1], add, key_ref[jnp.minimum(low, count - 1)])
        tile_out(i).start()

    loop(0, steps, tile)
    loop(steps - RING, steps, lambda i: tile_out(i).wait())


def table_grad(ordered, first, dx_all, fars, shard_rows, tall):
    count, m = dx_all.shape
    any_ = pl.BlockSpec(memory_space=pl.ANY)
    V, S = pltpu.VMEM, pltpu.SemaphoreType.DMA
    return pl.pallas_call(
        functools.partial(table_kernel, tall),
        out_shape=jax.ShapeDtypeStruct((shard_rows, m), F32),
        grid_spec=pltpu.PrefetchScalarGridSpec(
            num_scalar_prefetch=2,
            grid=(1,),
            in_specs=[any_] * 5,
            out_specs=any_,
            scratch_shapes=[
                V((count, m), BF16), V((count, m), F32), V((RING, tall, m), F32), S((10,)), S((RING,)),
            ],
        ),
        compiler_params=pltpu.CompilerParams(vmem_limit_bytes=60 << 20),
        cost_estimate=pl.CostEstimate(flops=16000 * shard_rows * m // 10, bytes_accessed=4 * shard_rows * m, transcendentals=0),
        name="table_grad",
    )(ordered, first, dx_all, *fars)


def solution(mesh):
    tok_spec = P(("pod", "data", "tensor"), None)

    over_y, over_core = [(0, 2), (1, 3), (2, 0), (3, 1)], [(0, 1), (1, 0), (2, 3), (3, 2)]

    def per_device(token_ids, embed_table, norm_gain, w_in, w_out, d_out):
        shard_rows = embed_table.shape[0]
        tall = next(k for k in (160, 8) if shard_rows % k == 0)
        ids = token_ids.reshape(-1, LANES)
        masked = look_up(ids, embed_table)
        gain = norm_gain.reshape(-1, LANES)
        base, ysum, ordered, first, dx_all, far, *weights = run_group(
            ids, masked, w_in, w_out, gain, d_out, shard_rows, tall
        )
        far_x = lax.ppermute(far, "tensor", over_y)
        far_p = lax.ppermute(far, "tensor", over_core)
        other = lax.ppermute(ysum, "tensor", over_y)
        grad_w_in, grad_w_out = finish_weights(*weights)
        far_b = lax.ppermute(far_x, "tensor", over_core)
        fars = (far, far_x, far_p, far_b)
        grad_table = table_grad(ordered.reshape(-1), first.reshape(-1), dx_all, fars, shard_rows, tall)
        return (base + other).astype(BF16), grad_table, grad_w_in, grad_w_out

    return jax.shard_map(
        per_device,
        mesh=mesh,
        in_specs=(P(("pod", "data")), P("tensor", None), P(None), P(None, "tensor"), P("tensor", None), tok_spec),
        out_specs=(tok_spec, P(("pod", "tensor"), None), P("pod", "tensor"), P(("pod", "tensor"), None)),
        check_vma=False,
    )
```

```python
import functools

import jax
import jax.numpy as jnp
from jax import lax
from jax.experimental import pallas as pl
from jax.experimental.pallas import tpu as pltpu
from jax.sharding import PartitionSpec as P


NORM_EPS = 1e-6
GELU_A = 0.7978845608028654
GELU_B = 0.044715
MESH = pl.DeviceIdType.MESH
NT = (((1,), (1,)), ((), ()))
TN = (((0,), (0,)), ((), ()))
F32, BF16, I32 = jnp.float32, jnp.bfloat16, jnp.int32
LANES = 128
XQ = 4
PQ = 4

R_IDS, R_DZ, R_DY, R_DC, R_NZ, R_NC, R_XZ, R_XY, R_XC = 0, 4, 8, 12, 16, 24, 28, 36, 44
R_XM, R_X, R_NO, R_PC, R_PY, R_NY, N_R = 48, 52, 56, 60, 68, 72, 73
S_IDS, S_DZ, S_DY, S_DC, S_NZ, S_NC, S_XZ, S_XY, S_XC = 0, 3, 8, 12, 16, 26, 30, 40, 48
S_XM, S_X, S_NO, S_PC, S_PY, S_NY, N_S = 52, 56, 60, 64, 72, 76, 77
L_W1, L_W2, L_XM, L_DX, L_YS, L_YB, L_DW, L_DO, L_K, N_L = 0, 1, 2, 3, 4, 5, 6, 8, 9, 13


def loop(lo, hi, body):
    def one(j, carry):
        body(j)
        return carry

    lax.fori_loop(lo, hi, one, 0)


def tiles(total, step, body):
    full = total // step
    loop(0, full, lambda j: body(pl.multiple_of(j * step, step), step))
    if total % step:
        body(full * step, total % step)


def rows_loop(total, body):
    loop(0, total // 16, lambda j: body(pl.multiple_of(j * 16, 16)))


def make_keys(ids, keys, shard_rows, rank0):
    reps, per, _ = ids.shape
    count = reps * per * LANES
    t = per * LANES // 4
    shift = t.bit_length() - 1
    lane = lax.broadcasted_iota(I32, (per, LANES), 1)
    spot = lax.broadcasted_iota(I32, (per, LANES), 0) * LANES + lane
    block = jnp.right_shift(spot, shift)
    kept = (block & 1) * (2 * t) + jnp.right_shift(block, 1) * t + (spot & (t - 1))
    for k in range(reps):
        row = ids[k] - rank0
        row = jnp.where((row >= 0) & (row < shard_rows), row, shard_rows)
        keys[k * per : (k + 1) * per, :] = (row * count + (k * per * LANES + kept)).astype(F32)


def columns(refs, b):
    same = lax.broadcasted_iota(I32, (LANES, LANES), 0) == lax.broadcasted_iota(I32, (LANES, LANES), 1)
    wide = (jnp.where(same, jnp.broadcast_to(ref[pl.ds(b, 1), :], (LANES, LANES)), 0.0) for ref in refs)
    return [jnp.sum(w, axis=1, keepdims=True) for w in wide]


def count_below(keys, place):
    lines = keys.shape[0]
    place[...] = jnp.zeros_like(place)

    def some(j):
        cols = [columns((keys,), 4 * j + u)[0] for u in range(4)]
        for a in range(lines):
            row = keys[a : a + 1, :]
            hits = sum(jnp.where(col < row, 1.0, 0.0) for col in cols)
            place[a : a + 1, :] += jnp.sum(hits, axis=0, keepdims=True)

    loop(0, lines // 4, some)


def put_in_order(keys, place, ordered, first, tall):
    lines = keys.shape[0]
    ordered[...] = jnp.zeros_like(ordered)
    first[...] = jnp.zeros_like(first)
    lane = lax.broadcasted_iota(I32, (1, LANES), 1).astype(F32)
    edge = lane * float(tall * lines * LANES)

    def some(j):
        cols = [columns((keys, place), 4 * j + u) for u in range(4)]
        for a in range(lines):
            want = lane + float(a * LANES)
            hits = sum(jnp.where(spot == want, key, 0.0) for key, spot in cols)
            ordered[a : a + 1, :] += jnp.sum(hits, axis=0, keepdims=True)
        first[...] += jnp.sum(sum(jnp.where(key < edge, 1.0, 0.0) for key, _ in cols), axis=0, keepdims=True)

    loop(0, lines // 4, some)


def group_kernel(shard_rows, tall, ids_ref, xm_hbm, w1_hbm, w2_hbm, g_ref, do_hbm,
                 base_o, ysum_o, ord_o, first_o, dx_o, far_o, dw1_o, dw2_o, nk_o, dk_o, hk_o, duk_o,
                 w1, w2, n, d, xm, xc, xy, hs, dus, pd, pf, rd, rf, yd, yb, dxo, idl, keys, place, ordered, first,
                 lsem, ssem, rsem):
    t, m = do_hbm.shape
    f = w1_hbm.shape[1]
    tq, mq = 2 * t // XQ, m // PQ
    z = lax.axis_index("data")
    r = lax.axis_index("tensor")
    y, c = lax.div(r, 2), lax.rem(r, 2)
    partner = {"tensor": 2 * y + 1 - c}
    across = {"tensor": 2 * (1 - y) + c}
    half = lax.div(z, 2)
    inner = z + half * (3 - 2 * z)
    order = [b + half * (3 - 2 * b) for b in (1 - inner, 2, 3)]
    middle, end = inner == 1, inner == 0

    def row(zz, cc, yy=0):
        return pl.multiple_of(zz * (4 * t) + cc * (2 * t) + yy * t, t)

    def blk(ref, zz, cc, yy):
        return ref.at[pl.ds(row(zz, cc, yy), t)]

    def duo(ref, zz, cc):
        return ref.at[pl.ds(row(zz, cc), 2 * t)]

    def remote(src, dst, s, q, dev):
        return pltpu.make_async_remote_copy(
            src_ref=src, dst_ref=dst, send_sem=ssem.at[s], recv_sem=rsem.at[q], device_id=dev, device_id_type=MESH
        )

    def local(src, dst, i):
        return pltpu.make_async_copy(src, dst, lsem.at[i])

    def arrived(ref, q):
        remote(ref, ref, 0, q, partner).wait_recv()

    def start(cp):
        cp.start()

    def sent(cp):
        cp.wait_send()

    def along(src, dst, s, q, act):
        for i, hop in enumerate((1, -1)):
            to = z + hop

            @pl.when((to >= 0) & (to <= 3))
            def _():
                act(remote(src, dst, s + i, q + z, {"data": to}))

    def pass_on(k, ref, s, q, act):
        src, dst = ref if isinstance(ref, tuple) else (ref, ref)
        act(remote(src, dst, s + 2 + k, q + order[k], {"data": order[1] if k == 0 else order[0]}))

    barrier = pltpu.get_barrier_semaphore()
    pl.semaphore_signal(barrier, inc=1, device_id=partner, device_id_type=MESH)
    pl.semaphore_signal(barrier, inc=1, device_id=across, device_id_type=MESH)
    for k in range(3):
        pl.semaphore_signal(barrier, inc=1, device_id={"data": order[k]}, device_id_type=MESH)

    own_d = blk(d, z, c, y)
    local(do_hbm, own_d, L_DO).start()
    local(xm_hbm, xm, L_XM).start()
    local(w1_hbm, w1, L_W1).start()
    local(w2_hbm, w2, L_W2).start()
    pl.semaphore_wait(barrier, 5)

    def piece(q):
        return pl.ds(q * tq, tq)

    for k in range(3):
        remote(ids_ref, idl.at[z], S_IDS + k, R_IDS + z, {"data": order[k]}).start()
    idl[z] = ids_ref[...]

    local(do_hbm, own_d, L_DO).wait()
    along(own_d, own_d, S_DZ, R_DZ, start)
    local(xm_hbm, xm, L_XM).wait()

    def xm_part(q):
        return remote(xm.at[pl.ds(row(0, 1 - c) + q * tq, tq)], xc.at[piece(q)], S_XM + q, R_XM + q, partner)

    def x_part(q):
        return remote(xc.at[piece(q)], xy.at[piece(q)], S_X + q, R_X + q, across)

    def d_got(k):
        arrived(blk(d, order[k], c, y), R_DZ + order[k])

    def d_on(k):
        pass_on(k, blk(d, order[k], c, y), S_DZ, R_DZ, start)

    def d_across(zz, act):
        act(remote(blk(d, zz, c, y), blk(d, zz, c, y), S_DY + zz, R_DY + zz, across))

    def d_pair(zz, act):
        act(remote(duo(d, zz, c), duo(d, zz, c), S_DC + zz, R_DC + zz, partner))

    for q in range(XQ):
        xm_part(q).start()
    for q in range(XQ):
        arrived(xc.at[piece(q)], R_XM + q)

        def join(i, q=q):
            at = pl.ds(q * tq + i, 16)
            xc[at, :] += xm[pl.ds(row(0, c) + q * tq + i, 16), :]

        rows_loop(tq, join)
        x_part(q).start()
    d_across(z, start)

    for k in range(3):
        arrived(idl.at[order[k]], R_IDS + order[k])
    make_keys(idl, keys, shard_rows, r * shard_rows)
    count_below(keys, place)
    d_got(0)

    @pl.when(middle)
    def _():
        d_on(0)
        d_got(1)
        d_on(1)

    gain = jnp.concatenate([g_ref[pl.ds(i, 1), :] for i in range(m // LANES)], axis=1).astype(F32)

    def n_own(q, act):
        at = n.at[pl.ds(row(z, c) + q * tq, tq)]
        act(remote(at, at, S_NO + q, R_NO + q, partner))

    def n_along(b, act):
        ref = blk(n, z, c, b)
        along(ref, ref, S_NZ + 5 * b, R_NZ + 4 * b, act)

    for q in range(XQ):
        arrived(xy.at[piece(q)], R_X + q)
        x_part(q).wait_send()

        def norm(i, q=q):
            at = pl.ds(q * tq + i, 16)
            x16 = xc[at, :] + xy[at, :]
            xc[at, :] = x16
            x = x16.astype(F32)
            s = lax.rsqrt(jnp.mean(x * x, axis=-1, keepdims=True) + NORM_EPS)
            n[pl.ds(row(z, c) + q * tq + i, 16), :] = ((x * s) * gain).astype(BF16)

        rows_loop(tq, norm)
        n_own(q, start)
        if q == XQ // 2 - 1:
            n_along(0, start)
            put_in_order(keys, place, ordered, first, tall)
            ord_o[...] = ordered[...].astype(I32)
            first_o[...] = first[...].astype(I32)

            @pl.when(middle)
            def _():
                d_got(2)
                d_on(2)

        if q == XQ - 1:
            n_along(1, start)
    d_across(order[0], start)

    def hidden(zz, slopes):
        at = pl.ds(row(zz, 0), 4 * t)

        def body(off, w):
            to = pl.ds(off, w)
            u = jnp.dot(n[at, :], w1[:, to], preferred_element_type=F32).astype(BF16).astype(F32)
            uu = u * u
            th = jnp.tanh(GELU_A * (u + GELU_B * (uu * u)))
            cdf = 0.5 * (1.0 + th)
            hs[at, to] = (u * cdf).astype(BF16)
            slopes[:, to] = cdf + (0.5 * GELU_A) * u * (1.0 - th * th) * (1.0 + (3.0 * GELU_B) * uu)

        tiles(f, 256, body)

    def grad_hidden(zz, slopes):
        at = pl.ds(row(zz, 0), 4 * t)

        def body(off, w):
            to = pl.ds(off, w)
            dh = lax.dot_general(d[at, :], w2[to, :], NT, preferred_element_type=F32)
            dus[at, to] = (dh * slopes[:, to]).astype(BF16)

        tiles(f, 256, body)

    for q in range(XQ):
        arrived(n.at[pl.ds(row(z, 1 - c) + q * tq, tq)], R_NO + q)
    local(w1_hbm, w1, L_W1).wait()
    hidden(z, pf)
    arrived(blk(d, z, c, 1 - y), R_DY + z)
    d_pair(z, start)
    arrived(duo(d, z, 1 - c), R_DC + z)
    local(w2_hbm, w2, L_W2).wait()
    grad_hidden(z, pf)

    own_rows = pl.ds(row(z, 0), 4 * t)
    far = pl.multiple_of((1 - y) * t, t)

    def cols(q):
        return pl.ds(pl.multiple_of(q * mq, mq), mq)

    def part_pair(src, dst, i, q):
        return remote(src.at[pl.ds(row(0, 1 - c), 2 * t), cols(q)], dst.at[:, cols(q)], S_PC + PQ * i + q, R_PC + PQ * i + q, partner)

    def part_across(q):
        return remote(rd.at[pl.ds(far, t), cols(q)], yd.at[:, cols(q)], S_PY + q, R_PY + q, across)

    def sum_part(part, got, i, q):
        arrived(got.at[:, cols(q)], R_PC + PQ * i + q)

        def add(k):
            got[pl.ds(far + k, 16), cols(q)] += part[pl.ds(row(0, c, 1 - y) + k, 16), cols(q)]

        rows_loop(t, add)

    def dn_part(q):
        pd[:, cols(q)] = lax.dot_general(dus[own_rows, :], w1[cols(q), :], NT, preferred_element_type=F32)
        part_pair(pd, rd, 0, q).start()

    def y_part(q):
        pf[:, cols(q)] = jnp.dot(hs[own_rows, :], w2[:, cols(q)], preferred_element_type=F32)
        part_pair(pf, rf, 1, q).start()

    def dn_out(q):
        sum_part(pd, rd, 0, q)
        part_across(q).start()

    loop(0, PQ, dn_part)
    loop(0, PQ, dn_out)
    loop(0, PQ, y_part)

    @pl.when(end)
    def _():
        d_got(1)

    d_across(order[1], start)

    loop(0, PQ, lambda q: sum_part(pf, rf, 1, q))
    y_send = local(rf.at[pl.ds(far, t)], ysum_o, L_YS)
    y_send.start()

    def base(i):
        own = pl.ds(y * t + i, 16)
        yb[pl.ds(i, 16), :] = xc[own, :].astype(F32) + (pf[pl.ds(row(0, c, y) + i, 16), :] + rf[own, :])

    rows_loop(t, base)
    y_keep = local(yb, base_o, L_YB)
    y_keep.start()
    for q in range(PQ):
        part_pair(pf, rf, 1, q).wait_send()

    th = t // 2

    def n_parts(k, lands):
        own, other = blk(n, order[k], c, y), blk(n, order[k], c, 1 - y)
        if lands == 2:
            other = other.at[pl.ds(0, th)]
        return (own, y), (other, 1 - y)

    def n_got(k):
        for ref, b in n_parts(k, k):
            arrived(ref, R_NZ + 4 * b + order[k])

    def n_on(k, act):
        for ref, b in n_parts(k, 1 if k == 1 else 2):
            pass_on(k, ref, S_NZ + 5 * b, R_NZ + 4 * b, act)

    def n_cross(act):
        half_own = blk(n, order[2], c, y).at[pl.ds(th, th)]
        act(remote(half_own, half_own, S_NY, R_NY, across))

    def n_pair(zz, act):
        act(remote(duo(n, zz, c), duo(n, zz, c), S_NC + zz, R_NC + zz, partner))

    n_got(0)
    n_pair(order[0], start)

    @pl.when(middle)
    def _():
        n_on(0, start)
        n_got(1)
        n_on(1, start)
        n_pair(order[1], start)

    def unit(k, slopes):
        zz = order[k]
        arrived(blk(d, zz, c, 1 - y), R_DY + zz)
        d_pair(zz, start)
        arrived(duo(n, zz, 1 - c), R_NC + zz)
        hidden(zz, slopes)
        arrived(duo(d, zz, 1 - c), R_DC + zz)
        grad_hidden(zz, slopes)

    def n_far(on):
        n_got(2)
        if on:
            n_on(2, start)
        n_cross(start)

    def n_far_pair():
        arrived(blk(n, order[2], c, 1 - y).at[pl.ds(th, th)], R_NY)
        n_pair(order[2], start)

    unit(0, pf)

    for q in range(PQ):
        arrived(yd.at[:, cols(q)], R_PY + q)

    def grad_x(i):
        at, own = pl.ds(i, 16), pl.ds(y * t + i, 16)
        dn = pd[pl.ds(row(0, c, y) + i, 16), :] + rd[own, :] + yd[at, :]
        x = xc[own, :].astype(F32)
        s = lax.rsqrt(jnp.mean(x * x, axis=-1, keepdims=True) + NORM_EPS)
        xh = x * s
        dhat = dn * gain
        dxn = s * (dhat - xh * jnp.mean(dhat * xh, axis=-1, keepdims=True))
        dxo[at, :] = (d[pl.ds(row(z, c, y) + i, 16), :].astype(F32) + dxn).astype(BF16)

    rows_loop(t, grad_x)

    def dx_part(zz, yy, h):
        return dx_o.at[pl.ds(pl.multiple_of(row(zz, c, yy) + h * th, th), th)]

    def dx_own(h):
        return dxo.at[pl.ds(h * th, th)]

    def far_part(h):
        return far_o.at[pl.ds(h * th, th)]

    def dx_next(k, h):
        here = dx_part(order[k], y, h)
        return (here, here) if k == 1 else (here if k == 0 else far_part(h), far_part(h))

    def dx_across(zz, src, h, act):
        act(remote(src, dx_part(zz, y, h), S_XY + 4 * h + zz, R_XY + 4 * h + zz, across))

    def dx_along(act):
        for h in range(2):
            along(dx_own(h), dx_part(z, y, h), S_XZ + 5 * h, R_XZ + 4 * h, act)

    def dx_pair(zz, act):
        act(remote(duo(dx_o, zz, c), duo(dx_o, zz, c), S_XC + zz, R_XC + zz, partner))

    def dx_got(k, on):
        zz = order[k]
        for h in range(2):
            arrived(dx_part(zz, y, h) if k < 2 else far_part(h), R_XZ + 4 * h + zz)
            if on:
                pass_on(k, dx_next(k, h), S_XZ + 5 * h, R_XZ + 4 * h, start)
            if k < 2:
                dx_across(zz, dx_part(zz, y, h), h, start)

    def dx_hand(zz):
        for h in range(2):
            arrived(dx_part(zz, 1 - y, h), R_XY + 4 * h + zz)
        dx_pair(zz, start)

    for h in range(2):
        dx_across(z, dx_own(h), h, start)
    local(dxo, blk(dx_o, z, c, y), L_DX).start()

    @pl.when(end)
    def _():
        d_got(2)

    d_across(order[2], start)

    for q in range(PQ):
        part_pair(pd, rd, 0, q).wait_send()

    pl.when(middle)(lambda: n_far(True))
    dx_along(start)

    @pl.when(end)
    def _():
        n_got(1)
        n_pair(order[1], start)

    unit(1, pd)

    @pl.when(middle)
    def _():
        dx_got(0, True)
        dx_got(1, True)

    tw = 2 * t
    n1, n2 = m // tw, f // tw
    late_rows = pl.ds(row(order[2], 0), 4 * t)
    early_rows = pl.ds(pl.multiple_of(half * (4 * t), 4 * t), 12 * t)

    def flush(i, buf, dst):
        lines = pl.ds(pl.multiple_of(lax.rem(i, 2) * tw, tw), tw)
        here = buf.at[lines, pl.ds(0, dst.shape[1])]
        return here, local(here, dst.at[pl.ds(pl.multiple_of(i * tw, tw), tw)], L_DW + lax.rem(i, 2))

    def weight_tile(i, lhs, rhs, buf, dst):
        pl.when(i >= 2)(lambda: flush(i - 2, buf, dst)[1].wait())
        here, out = flush(i, buf, dst)
        at = pl.ds(pl.multiple_of(i * tw, tw), tw)
        here[...] = lax.dot_general(lhs[early_rows, at], rhs[early_rows, :], TN, preferred_element_type=F32)
        out.start()

    loop(0, n1 // 2, lambda i: weight_tile(i, n, dus, pf, dw1_o))
    pl.when(end)(lambda: n_far(False))
    loop(n1 // 2, n1, lambda i: weight_tile(i, n, dus, pf, dw1_o))
    for i in (n1 - 2, n1 - 1):
        flush(i, pf, dw1_o)[1].wait()
    n_far_pair()
    unit(2, pd)
    kept = [
        local(src.at[late_rows], dst, L_K + i)
        for i, (src, dst) in enumerate(((n, nk_o), (d, dk_o), (hs, hk_o), (dus, duk_o)))
    ]
    for cp in kept:
        cp.start()
    pl.when(end)(lambda: dx_got(0, False))
    pl.when(middle)(lambda: dx_got(2, True))
    loop(0, n2 // 2, lambda i: weight_tile(i, hs, d, pd, dw2_o))
    pl.when(end)(lambda: dx_got(1, False))
    loop(n2 // 2, n2, lambda i: weight_tile(i, hs, d, pd, dw2_o))
    local(dxo, blk(dx_o, z, c, y), L_DX).wait()
    dx_hand(z)
    dx_hand(order[0])
    for i in (n2 - 2, n2 - 1):
        flush(i, pd, dw2_o)[1].wait()
    if f % tw:
        rest = pd.at[pl.ds(0, f % tw)]
        rest[...] = lax.dot_general(hs[early_rows, n2 * tw :], d[early_rows, :], TN, preferred_element_type=F32)
        last = local(rest, dw2_o.at[pl.ds(n2 * tw, f % tw)], L_DW)
        last.start()
    dx_hand(order[1])
    pl.when(end)(lambda: dx_got(2, False))
    if f % tw:
        last.wait()
    for cp in kept:
        cp.wait()

    y_send.wait()
    y_keep.wait()
    along(own_d, own_d, S_DZ, R_DZ, sent)
    for zz in (z, *order):
        d_across(zz, sent)
        d_pair(zz, sent)
    for k in range(3):
        n_pair(order[k], sent)
        remote(ids_ref, idl.at[z], S_IDS + k, R_IDS + z, {"data": order[k]}).wait_send()
    dx_along(sent)
    for b in range(2):
        n_along(b, sent)
        dx_across(z, dx_own(b), b, sent)
        for k in range(2):
            dx_across(order[k], dx_part(order[k], y, b), b, sent)

    @pl.when(middle)
    def _():
        for k in range(3):
            pass_on(k, blk(d, order[k], c, y), S_DZ, R_DZ, sent)
            n_on(k, sent)
            for b in range(2):
                pass_on(k, dx_next(k, b), S_XZ + 5 * b, R_XZ + 4 * b, sent)

    for q in range(XQ):
        xm_part(q).wait_send()
        n_own(q, sent)
    n_cross(sent)
    for q in range(PQ):
        part_across(q).wait_send()
    for zz in (z, *order[:2]):
        arrived(duo(dx_o, zz, 1 - c), R_XC + zz)
        dx_pair(zz, sent)


def run_group(ids, xm, w1, w2, gain, d_out, shard_rows, tall):
    t, m = d_out.shape
    f = w1.shape[1]
    lines = 4 * ids.shape[0]
    any_, vmem = pl.BlockSpec(memory_space=pl.ANY), pl.BlockSpec(memory_space=pltpu.VMEM)
    V = pltpu.VMEM
    sds = jax.ShapeDtypeStruct
    dots = 2 * 4 * t * m * f
    return pl.pallas_call(
        functools.partial(group_kernel, shard_rows, tall),
        out_shape=(
            sds((t, m), F32), sds((t, m), F32), sds((lines, LANES), I32), sds((1, LANES), I32), sds((16 * t, m), BF16),
            sds((t, m), BF16), sds((m, f), F32), sds((f, m), F32),
            sds((4 * t, m), BF16), sds((4 * t, m), BF16), sds((4 * t, f), BF16), sds((4 * t, f), BF16),
        ),
        in_specs=[vmem, any_, any_, any_, vmem, any_],
        out_specs=(any_, any_, vmem, vmem, *[any_] * 8),
        scratch_shapes=[
            V((m, f), BF16), V((f, m), BF16), V((16 * t, m), BF16), V((16 * t, m), BF16),
            V((4 * t, m), BF16), V((2 * t, m), BF16), V((2 * t, m), BF16),
            V((16 * t, f), BF16), V((16 * t, f), BF16),
            V((4 * t, m), F32), V((4 * t, m), F32), V((2 * t, m), F32), V((2 * t, m), F32),
            V((t, m), F32), V((t, m), F32),
            V((t, m), BF16), V((4, *ids.shape), I32),
            V((lines, LANES), F32), V((lines, LANES), F32), V((lines, LANES), F32), V((1, LANES), F32),
            pltpu.SemaphoreType.DMA((N_L,)), pltpu.SemaphoreType.DMA((N_S,)), pltpu.SemaphoreType.DMA((N_R,)),
        ],
        compiler_params=pltpu.CompilerParams(collective_id=0, has_side_effects=True, vmem_limit_bytes=67043328),
        cost_estimate=pl.CostEstimate(flops=18 * dots, bytes_accessed=64 * 16 * t * m, transcendentals=16 * t * f),
        name="group_step",
    )(ids, xm, w1, w2, gain, d_out)


def lookup_kernel(shard_rows, ids_smem, ids_vmem, table, out_hbm, got, rows, sem, out_sem):
    total, m = out_hbm.shape
    t = total // 4
    per = 32
    chunks = total // per
    r = lax.axis_index("tensor")
    spread = (1 << (shard_rows.bit_length() - 1)) - 1

    def fetch(k):
        def some(j, carry):
            for u in range(8):
                p = k * per + j * 8 + u
                row = ids_smem[jnp.right_shift(p, 7), p & (LANES - 1)]
                near = row - r * shard_rows
                near = jnp.where((near >= 0) & (near < shard_rows), near, row & spread)
                pltpu.make_async_copy(table.at[jnp.right_shift(near, 3)], got.at[p], sem.at[k]).start()
            return carry

        lax.fori_loop(0, per // 8, some, 0)

    loop(0, chunks, fetch)
    spot = lax.broadcasted_iota(I32, (per, 8 * per), 1)
    token = lax.broadcasted_iota(I32, (per, 8 * per), 0)
    same = lax.broadcasted_iota(I32, (LANES, LANES), 0) == lax.broadcasted_iota(I32, (LANES, LANES), 1)

    def line(b):
        ids = ids_vmem[pl.ds(b, 1), :].astype(F32)
        col = jnp.sum(jnp.where(same, jnp.broadcast_to(ids, (LANES, LANES)), 0.0), axis=1, keepdims=True).astype(I32)
        row = col - r * shard_rows
        row = jnp.where((row >= 0) & (row < shard_rows), row & 7, -8 * per)
        for j in range(LANES // per):
            k = b * (LANES // per) + j
            at = pl.ds(pl.multiple_of(k * per, per), per)
            pltpu.make_async_copy(got.at[at], got.at[at], sem.at[k]).wait()
            want = row[j * per : (j + 1) * per] + 8 * token
            chosen = jnp.where(want == spot, 1.0, 0.0).astype(BF16)
            picked = jnp.dot(chosen, got[at].reshape(8 * per, m), preferred_element_type=F32)
            p = k * per
            nat = lax.div(p, t)
            to = pl.multiple_of(lax.rem(nat, 2) * (2 * t) + lax.div(nat, 2) * t + lax.rem(p, t), per)
            rows[pl.ds(to, per), :] = picked.astype(BF16)
            pltpu.make_async_copy(rows.at[pl.ds(to, per)], out_hbm.at[pl.ds(to, per)], out_sem).start()

    loop(0, total // LANES, line)
    pltpu.make_async_copy(rows, out_hbm, out_sem).wait()


def look_up(ids, table):
    shard_rows, m = table.shape
    total = ids.size
    any_ = pl.BlockSpec(memory_space=pl.ANY)
    return pl.pallas_call(
        functools.partial(lookup_kernel, shard_rows),
        out_shape=jax.ShapeDtypeStruct((total, m), BF16),
        in_specs=[pl.BlockSpec(memory_space=pltpu.SMEM), pl.BlockSpec(memory_space=pltpu.VMEM), any_],
        out_specs=any_,
        scratch_shapes=[
            pltpu.VMEM((total, 8, m), BF16), pltpu.VMEM((total, m), BF16),
            pltpu.SemaphoreType.DMA((total // 32,)), pltpu.SemaphoreType.DMA,
        ],
        compiler_params=pltpu.CompilerParams(vmem_limit_bytes=60 << 20),
        cost_estimate=pl.CostEstimate(flops=16 * total * m, bytes_accessed=20 * total * m, transcendentals=0),
        name="look_up",
    )(ids, ids, table.reshape(shard_rows // 8, 8, m))


RING = 6


def weights_kernel(p1, p2, nk_in, dk_in, hk_in, duk_in, o1, o2, b1, b2, nk, dk, hk, duk, in_sem, out_sem, k_sem):
    m, f = b1.shape
    tw = nk.shape[0] // 2
    ins = [pltpu.make_async_copy(a, b, k_sem.at[i]) for i, (a, b) in enumerate(((nk_in, nk), (duk_in, duk), (hk_in, hk), (dk_in, dk)))]
    for cp in ins[:2]:
        cp.start()

    def part(src, buf, dst, first, i, rows=tw):
        at = pl.ds(pl.multiple_of(i * tw, 8), rows)
        fetch = pltpu.make_async_copy(src.at[at], buf.at[at], in_sem.at[first + i])
        return fetch, pltpu.make_async_copy(buf.at[at], dst.at[at], out_sem)

    def fetch_all(src, buf, dst, first):
        loop(0, src.shape[0] // tw, lambda i: part(src, buf, dst, first, i)[0].start())

    n1, n2 = m // tw, f // tw
    fetch_all(p1, b1, o1, 0)
    for cp in ins[2:]:
        cp.start()
    fetch_all(p2, b2, o2, n1)
    rest = [part(p2, b2, o2, n1, n2, f % tw)] if f % tw else []
    for come, _ in rest:
        come.start()

    def add(src, buf, dst, first, lhs, rhs, i, rows=tw):
        come, go = part(src, buf, dst, first, i, rows)
        come.wait()
        cols = pl.ds(pl.multiple_of(i * tw, tw), rows)
        buf[cols, :] += lax.dot_general(lhs[:, cols], rhs[...], TN, preferred_element_type=F32)
        go.start()

    for cp in ins[:2]:
        cp.wait()
    loop(0, n1, lambda i: add(p1, b1, o1, 0, nk, duk, i))
    for cp in ins[2:]:
        cp.wait()
    loop(0, n2, lambda i: add(p2, b2, o2, n1, hk, dk, i))
    if rest:
        add(p2, b2, o2, n1, hk, dk, n2, f % tw)
    pltpu.make_async_copy(b1, o1, out_sem).wait()
    pltpu.make_async_copy(b2, o2, out_sem).wait()


def finish_weights(p1, p2, nk, dk, hk, duk):
    any_ = pl.BlockSpec(memory_space=pl.ANY)
    V, S = pltpu.VMEM, pltpu.SemaphoreType.DMA
    arrays = (p1, p2, nk, dk, hk, duk)
    return pl.pallas_call(
        weights_kernel,
        out_shape=(jax.ShapeDtypeStruct(p1.shape, F32), jax.ShapeDtypeStruct(p2.shape, F32)),
        in_specs=[any_] * 6,
        out_specs=[any_] * 2,
        scratch_shapes=[*[V(a.shape, a.dtype) for a in arrays], S((32,)), S, S((4,))],
        compiler_params=pltpu.CompilerParams(vmem_limit_bytes=60 << 20),
        cost_estimate=pl.CostEstimate(flops=8000 * p1.size, bytes_accessed=20 * p1.size, transcendentals=0),
        name="finish_weights",
    )(*arrays)


def table_kernel(tall, key_ref, first_ref, dx_in, far_own, far_across, far_partner, far_both, out_hbm, dxb, dxf, ring, dx_sem, t_sem):
    count, _ = dxb.shape
    t = count // 16
    shift = count.bit_length() - 1
    steps = out_hbm.shape[0] // tall
    z, r = lax.axis_index("data"), lax.axis_index("tensor")
    y, c = lax.div(r, 2), lax.rem(r, 2)
    late = lax.div(z, 2)

    def near(k):
        at = pl.ds(pl.multiple_of(late * (4 * t) + k * (2 * t), t), 2 * t)
        return at, pltpu.make_async_copy(dx_in.at[at], dxb.at[at], dx_sem.at[k])

    def far(cc, yy):
        return pl.multiple_of((1 - late) * (12 * t) + cc * (2 * t) + yy * t, t)

    loop(0, 6, lambda k: near(k)[1].start())
    for src, cc, yy in ((far_own, c, y), (far_across, c, 1 - y), (far_partner, 1 - c, y), (far_both, 1 - c, 1 - y)):
        to = far(cc, yy)

        def widen_far(i, src=src, to=to):
            dxf[pl.ds(to + i, 16), :] = src[pl.ds(i, 16), :].astype(F32)

        rows_loop(t, widen_far)

    def widen_piece(at, cp):
        cp.wait()

        def widen(i):
            rows = pl.ds(pl.multiple_of(at.start + i, 16), 16)
            dxf[rows, :] = dxb[rows, :].astype(F32)

        rows_loop(at.size, widen)

    loop(0, 6, lambda k: widen_piece(*near(k)))

    def tile_out(i):
        slot = lax.rem(i, RING)
        return pltpu.make_async_copy(ring.at[slot], out_hbm.at[pl.ds(pl.multiple_of(i * tall, 8), tall)], t_sem.at[slot])

    def tile(i):
        slot = lax.rem(i, RING)
        here = ring.at[slot]
        pl.when(i >= RING)(lambda: tile_out(i - RING).wait())
        here[...] = jnp.zeros_like(here)

        def add(j, key):
            ahead = key_ref[jnp.minimum(j + 1, count - 1)]
            to = pl.ds(jnp.right_shift(key, shift) - i * tall, 1)
            here[to, :] += dxf[pl.ds(key & (count - 1), 1), :]
            return ahead

        low = first_ref[i]
        lax.fori_loop(low, first_ref[i + 1], add, key_ref[jnp.minimum(low, count - 1)])
        tile_out(i).start()

    loop(0, steps, tile)
    loop(steps - RING, steps, lambda i: tile_out(i).wait())


def table_grad(ordered, first, dx_all, fars, shard_rows, tall):
    count, m = dx_all.shape
    any_ = pl.BlockSpec(memory_space=pl.ANY)
    V, S = pltpu.VMEM, pltpu.SemaphoreType.DMA
    return pl.pallas_call(
        functools.partial(table_kernel, tall),
        out_shape=jax.ShapeDtypeStruct((shard_rows, m), F32),
        grid_spec=pltpu.PrefetchScalarGridSpec(
            num_scalar_prefetch=2,
            grid=(1,),
            in_specs=[any_, *[pl.BlockSpec(memory_space=pltpu.VMEM)] * 4],
            out_specs=any_,
            scratch_shapes=[
                V((count, m), BF16), V((count, m), F32), V((RING, tall, m), F32), S((6,)), S((RING,)),
            ],
        ),
        compiler_params=pltpu.CompilerParams(vmem_limit_bytes=44 << 20),
        cost_estimate=pl.CostEstimate(flops=16000 * shard_rows * m // 10, bytes_accessed=4 * shard_rows * m, transcendentals=0),
        name="table_grad",
    )(ordered, first, dx_all, *fars)


def solution(mesh):
    tok_spec = P(("pod", "data", "tensor"), None)

    over_y, over_core = [(0, 2), (1, 3), (2, 0), (3, 1)], [(0, 1), (1, 0), (2, 3), (3, 2)]

    def per_device(token_ids, embed_table, norm_gain, w_in, w_out, d_out):
        shard_rows = embed_table.shape[0]
        tall = next(k for k in (160, 8) if shard_rows % k == 0)
        ids = token_ids.reshape(-1, LANES)
        masked = look_up(ids, embed_table)
        gain = norm_gain.reshape(-1, LANES)
        base, ysum, ordered, first, dx_all, far, *weights = run_group(
            ids, masked, w_in, w_out, gain, d_out, shard_rows, tall
        )
        far_x = lax.ppermute(far, "tensor", over_y)
        far_p = lax.ppermute(far, "tensor", over_core)
        other = lax.ppermute(ysum, "tensor", over_y)
        grad_w_in, grad_w_out = finish_weights(*weights)
        far_b = lax.ppermute(far_x, "tensor", over_core)
        fars = (far, far_x, far_p, far_b)
        grad_table = table_grad(ordered.reshape(-1), first.reshape(-1), dx_all, fars, shard_rows, tall)
        return (base + other).astype(BF16), grad_table, grad_w_in, grad_w_out

    return jax.shard_map(
        per_device,
        mesh=mesh,
        in_specs=(P(("pod", "data")), P("tensor", None), P(None), P(None, "tensor"), P("tensor", None), tok_spec),
        out_specs=(tok_spec, P(("pod", "tensor"), None), P("pod", "tensor"), P(("pod", "tensor"), None)),
        check_vma=False,
    )
```

```python
import functools

import jax
import jax.numpy as jnp
from jax import lax
from jax.experimental import pallas as pl
from jax.experimental.pallas import tpu as pltpu
from jax.sharding import PartitionSpec as P


NORM_EPS = 1e-6
GELU_A = 0.7978845608028654
GELU_B = 0.044715
MESH = pl.DeviceIdType.MESH
NT = (((1,), (1,)), ((), ()))
TN = (((0,), (0,)), ((), ()))
F32, BF16, I32 = jnp.float32, jnp.bfloat16, jnp.int32
LANES = 128
XQ = 4
PQ = 4

R_IDS, R_DZ, R_DY, R_DC, R_NZ, R_NC, R_XZ, R_XY, R_XC = 0, 4, 8, 12, 16, 24, 28, 36, 44
R_XM, R_X, R_NO, R_PC, R_PY, R_NY, N_R = 48, 52, 56, 60, 68, 72, 73
S_IDS, S_DZ, S_DY, S_DC, S_NZ, S_NC, S_XZ, S_XY, S_XC = 0, 3, 8, 12, 16, 26, 30, 40, 48
S_XM, S_X, S_NO, S_PC, S_PY, S_NY, N_S = 52, 56, 60, 64, 72, 76, 77
L_W1, L_W2, L_XM, L_DX, L_YS, L_YB, L_DW, L_DO, L_K, N_L = 0, 1, 2, 3, 4, 5, 6, 8, 9, 13


def loop(lo, hi, body):
    def one(j, carry):
        body(j)
        return carry

    lax.fori_loop(lo, hi, one, 0)


def tiles(total, step, body):
    full = total // step
    loop(0, full, lambda j: body(pl.multiple_of(j * step, step), step))
    if total % step:
        body(full * step, total % step)


def rows_loop(total, body):
    loop(0, total // 16, lambda j: body(pl.multiple_of(j * 16, 16)))


def make_keys(ids, keys, shard_rows, rank0):
    reps, per, _ = ids.shape
    count = reps * per * LANES
    t = per * LANES // 4
    shift = t.bit_length() - 1
    lane = lax.broadcasted_iota(I32, (per, LANES), 1)
    spot = lax.broadcasted_iota(I32, (per, LANES), 0) * LANES + lane
    block = jnp.right_shift(spot, shift)
    kept = (block & 1) * (2 * t) + jnp.right_shift(block, 1) * t + (spot & (t - 1))
    for k in range(reps):
        row = ids[k] - rank0
        row = jnp.where((row >= 0) & (row < shard_rows), row, shard_rows)
        keys[k * per : (k + 1) * per, :] = (row * count + (k * per * LANES + kept)).astype(F32)


def columns(refs, b):
    same = lax.broadcasted_iota(I32, (LANES, LANES), 0) == lax.broadcasted_iota(I32, (LANES, LANES), 1)
    wide = (jnp.where(same, jnp.broadcast_to(ref[pl.ds(b, 1), :], (LANES, LANES)), 0.0) for ref in refs)
    return [jnp.sum(w, axis=1, keepdims=True) for w in wide]


def count_below(keys, place):
    lines = keys.shape[0]
    place[...] = jnp.zeros_like(place)

    def some(j):
        cols = [columns((keys,), 4 * j + u)[0] for u in range(4)]
        for a in range(lines):
            row = keys[a : a + 1, :]
            hits = sum(jnp.where(col < row, 1.0, 0.0) for col in cols)
            place[a : a + 1, :] += jnp.sum(hits, axis=0, keepdims=True)

    loop(0, lines // 4, some)


def put_in_order(keys, place, ordered, first, tall):
    lines = keys.shape[0]
    ordered[...] = jnp.zeros_like(ordered)
    first[...] = jnp.zeros_like(first)
    lane = lax.broadcasted_iota(I32, (1, LANES), 1).astype(F32)
    edge = lane * float(tall * lines * LANES)

    def some(j):
        cols = [columns((keys, place), 4 * j + u) for u in range(4)]
        for a in range(lines):
            want = lane + float(a * LANES)
            hits = sum(jnp.where(spot == want, key, 0.0) for key, spot in cols)
            ordered[a : a + 1, :] += jnp.sum(hits, axis=0, keepdims=True)
        first[...] += jnp.sum(sum(jnp.where(key < edge, 1.0, 0.0) for key, _ in cols), axis=0, keepdims=True)

    loop(0, lines // 4, some)


def group_kernel(shard_rows, tall, ids_ref, xm_hbm, w1_hbm, w2_hbm, g_ref, do_hbm,
                 base_o, ysum_o, ord_o, first_o, dx_o, far_o, dw1_o, dw2_o, nk_o, dk_o, hk_o, duk_o,
                 w1, w2, n, d, xm, xc, xy, hs, dus, pd, pf, rd, rf, yd, yb, dxo, idl, keys, place, ordered, first,
                 lsem, ssem, rsem):
    t, m = do_hbm.shape
    f = w1_hbm.shape[1]
    tq, mq = 2 * t // XQ, m // PQ
    z = lax.axis_index("data")
    r = lax.axis_index("tensor")
    y, c = lax.div(r, 2), lax.rem(r, 2)
    partner = {"tensor": 2 * y + 1 - c}
    across = {"tensor": 2 * (1 - y) + c}
    half = lax.div(z, 2)
    inner = z + half * (3 - 2 * z)
    order = [b + half * (3 - 2 * b) for b in (1 - inner, 2, 3)]
    middle, end = inner == 1, inner == 0

    def row(zz, cc, yy=0):
        return pl.multiple_of(zz * (4 * t) + cc * (2 * t) + yy * t, t)

    def blk(ref, zz, cc, yy):
        return ref.at[pl.ds(row(zz, cc, yy), t)]

    def duo(ref, zz, cc):
        return ref.at[pl.ds(row(zz, cc), 2 * t)]

    def remote(src, dst, s, q, dev):
        return pltpu.make_async_remote_copy(
            src_ref=src, dst_ref=dst, send_sem=ssem.at[s], recv_sem=rsem.at[q], device_id=dev, device_id_type=MESH
        )

    def local(src, dst, i):
        return pltpu.make_async_copy(src, dst, lsem.at[i])

    def arrived(ref, q):
        remote(ref, ref, 0, q, partner).wait_recv()

    def start(cp):
        cp.start()

    def sent(cp):
        cp.wait_send()

    def along(src, dst, s, q, act):
        for i, hop in enumerate((1, -1)):
            to = z + hop

            @pl.when((to >= 0) & (to <= 3))
            def _():
                act(remote(src, dst, s + i, q + z, {"data": to}))

    def pass_on(k, ref, s, q, act):
        src, dst = ref if isinstance(ref, tuple) else (ref, ref)
        act(remote(src, dst, s + 2 + k, q + order[k], {"data": order[1] if k == 0 else order[0]}))

    barrier = pltpu.get_barrier_semaphore()
    pl.semaphore_signal(barrier, inc=1, device_id=partner, device_id_type=MESH)
    pl.semaphore_signal(barrier, inc=1, device_id=across, device_id_type=MESH)
    for k in range(3):
        pl.semaphore_signal(barrier, inc=1, device_id={"data": order[k]}, device_id_type=MESH)

    own_d = blk(d, z, c, y)
    local(do_hbm, own_d, L_DO).start()
    local(xm_hbm, xm, L_XM).start()
    local(w1_hbm, w1, L_W1).start()
    local(w2_hbm, w2, L_W2).start()
    pl.semaphore_wait(barrier, 5)

    def piece(q):
        return pl.ds(q * tq, tq)

    for k in range(3):
        remote(ids_ref, idl.at[z], S_IDS + k, R_IDS + z, {"data": order[k]}).start()
    idl[z] = ids_ref[...]

    local(do_hbm, own_d, L_DO).wait()
    along(own_d, own_d, S_DZ, R_DZ, start)
    local(xm_hbm, xm, L_XM).wait()

    def xm_part(q):
        return remote(xm.at[pl.ds(row(0, 1 - c) + q * tq, tq)], xc.at[piece(q)], S_XM + q, R_XM + q, partner)

    def x_part(q):
        return remote(xc.at[piece(q)], xy.at[piece(q)], S_X + q, R_X + q, across)

    def d_got(k):
        arrived(blk(d, order[k], c, y), R_DZ + order[k])

    def d_on(k):
        pass_on(k, blk(d, order[k], c, y), S_DZ, R_DZ, start)

    def d_across(zz, act):
        act(remote(blk(d, zz, c, y), blk(d, zz, c, y), S_DY + zz, R_DY + zz, across))

    def d_pair(zz, act):
        act(remote(duo(d, zz, c), duo(d, zz, c), S_DC + zz, R_DC + zz, partner))

    for q in range(XQ):
        xm_part(q).start()
    for q in range(XQ):
        arrived(xc.at[piece(q)], R_XM + q)

        def join(i, q=q):
            at = pl.ds(q * tq + i, 16)
            xc[at, :] += xm[pl.ds(row(0, c) + q * tq + i, 16), :]

        rows_loop(tq, join)
        x_part(q).start()
    d_across(z, start)

    for k in range(3):
        arrived(idl.at[order[k]], R_IDS + order[k])
    make_keys(idl, keys, shard_rows, r * shard_rows)
    count_below(keys, place)
    d_got(0)

    @pl.when(middle)
    def _():
        d_on(0)
        d_got(1)
        d_on(1)

    gain = jnp.concatenate([g_ref[pl.ds(i, 1), :] for i in range(m // LANES)], axis=1).astype(F32)

    def n_own(q, act):
        at = n.at[pl.ds(row(z, c) + q * tq, tq)]
        act(remote(at, at, S_NO + q, R_NO + q, partner))

    def n_along(b, act):
        ref = blk(n, z, c, b)
        along(ref, ref, S_NZ + 5 * b, R_NZ + 4 * b, act)

    for q in range(XQ):
        arrived(xy.at[piece(q)], R_X + q)
        x_part(q).wait_send()

        def norm(i, q=q):
            at = pl.ds(q * tq + i, 16)
            x16 = xc[at, :] + xy[at, :]
            xc[at, :] = x16
            x = x16.astype(F32)
            s = lax.rsqrt(jnp.mean(x * x, axis=-1, keepdims=True) + NORM_EPS)
            n[pl.ds(row(z, c) + q * tq + i, 16), :] = ((x * s) * gain).astype(BF16)

        rows_loop(tq, norm)
        n_own(q, start)
        if q == XQ // 2 - 1:
            n_along(0, start)
            put_in_order(keys, place, ordered, first, tall)
            ord_o[...] = ordered[...].astype(I32)
            first_o[...] = first[...].astype(I32)

            @pl.when(middle)
            def _():
                d_got(2)
                d_on(2)

        if q == XQ - 1:
            n_along(1, start)
    d_across(order[0], start)

    def hidden(zz, slopes):
        at = pl.ds(row(zz, 0), 4 * t)

        def body(off, w):
            to = pl.ds(off, w)
            u = jnp.dot(n[at, :], w1[:, to], preferred_element_type=F32).astype(BF16).astype(F32)
            uu = u * u
            th = jnp.tanh(GELU_A * (u + GELU_B * (uu * u)))
            cdf = 0.5 * (1.0 + th)
            hs[at, to] = (u * cdf).astype(BF16)
            slopes[:, to] = cdf + (0.5 * GELU_A) * u * (1.0 - th * th) * (1.0 + (3.0 * GELU_B) * uu)

        tiles(f, 256, body)

    def grad_hidden(zz, slopes):
        at = pl.ds(row(zz, 0), 4 * t)

        def body(off, w):
            to = pl.ds(off, w)
            dh = lax.dot_general(d[at, :], w2[to, :], NT, preferred_element_type=F32)
            dus[at, to] = (dh * slopes[:, to]).astype(BF16)

        tiles(f, 256, body)

    for q in range(XQ):
        arrived(n.at[pl.ds(row(z, 1 - c) + q * tq, tq)], R_NO + q)
    local(w1_hbm, w1, L_W1).wait()
    hidden(z, pf)
    arrived(blk(d, z, c, 1 - y), R_DY + z)
    d_pair(z, start)
    arrived(duo(d, z, 1 - c), R_DC + z)
    local(w2_hbm, w2, L_W2).wait()
    grad_hidden(z, pf)

    own_rows = pl.ds(row(z, 0), 4 * t)
    far = pl.multiple_of((1 - y) * t, t)

    def cols(q):
        return pl.ds(pl.multiple_of(q * mq, mq), mq)

    def part_pair(src, dst, i, q):
        return remote(src.at[pl.ds(row(0, 1 - c), 2 * t), cols(q)], dst.at[:, cols(q)], S_PC + PQ * i + q, R_PC + PQ * i + q, partner)

    def part_across(q):
        return remote(rd.at[pl.ds(far, t), cols(q)], yd.at[:, cols(q)], S_PY + q, R_PY + q, across)

    def sum_part(part, got, i, q):
        arrived(got.at[:, cols(q)], R_PC + PQ * i + q)

        def add(k):
            got[pl.ds(far + k, 16), cols(q)] += part[pl.ds(row(0, c, 1 - y) + k, 16), cols(q)]

        rows_loop(t, add)

    def dn_part(q):
        pd[:, cols(q)] = lax.dot_general(dus[own_rows, :], w1[cols(q), :], NT, preferred_element_type=F32)
        part_pair(pd, rd, 0, q).start()

    def y_part(q):
        pf[:, cols(q)] = jnp.dot(hs[own_rows, :], w2[:, cols(q)], preferred_element_type=F32)
        part_pair(pf, rf, 1, q).start()

    def dn_out(q):
        sum_part(pd, rd, 0, q)
        part_across(q).start()

    loop(0, PQ, dn_part)
    loop(0, PQ, dn_out)
    loop(0, PQ, y_part)

    @pl.when(end)
    def _():
        d_got(1)

    d_across(order[1], start)

    loop(0, PQ, lambda q: sum_part(pf, rf, 1, q))
    y_send = local(rf.at[pl.ds(far, t)], ysum_o, L_YS)
    y_send.start()

    def base(i):
        own = pl.ds(y * t + i, 16)
        yb[pl.ds(i, 16), :] = xc[own, :].astype(F32) + (pf[pl.ds(row(0, c, y) + i, 16), :] + rf[own, :])

    rows_loop(t, base)
    y_keep = local(yb, base_o, L_YB)
    y_keep.start()
    for q in range(PQ):
        part_pair(pf, rf, 1, q).wait_send()

    th = t // 2

    def n_parts(k, lands):
        own, other = blk(n, order[k], c, y), blk(n, order[k], c, 1 - y)
        if lands == 2:
            other = other.at[pl.ds(0, th)]
        return (own, y), (other, 1 - y)

    def n_got(k):
        for ref, b in n_parts(k, k):
            arrived(ref, R_NZ + 4 * b + order[k])

    def n_on(k, act):
        for ref, b in n_parts(k, 1 if k == 1 else 2):
            pass_on(k, ref, S_NZ + 5 * b, R_NZ + 4 * b, act)

    def n_cross(act):
        half_own = blk(n, order[2], c, y).at[pl.ds(th, th)]
        act(remote(half_own, half_own, S_NY, R_NY, across))

    def n_pair(zz, act):
        act(remote(duo(n, zz, c), duo(n, zz, c), S_NC + zz, R_NC + zz, partner))

    n_got(0)
    n_pair(order[0], start)

    @pl.when(middle)
    def _():
        n_on(0, start)
        n_got(1)
        n_on(1, start)
        n_pair(order[1], start)

    def unit(k, slopes, between=None):
        zz = order[k]
        arrived(blk(d, zz, c, 1 - y), R_DY + zz)
        d_pair(zz, start)
        arrived(duo(n, zz, 1 - c), R_NC + zz)
        if between:
            between()
        hidden(zz, slopes)
        arrived(duo(d, zz, 1 - c), R_DC + zz)
        grad_hidden(zz, slopes)

    def n_far(part, on):
        ref, b = n_parts(2, 2)[part]
        arrived(ref, R_NZ + 4 * b + order[2])
        if on:
            pass_on(2, ref, S_NZ + 5 * b, R_NZ + 4 * b, start)
        if part == 0:
            n_cross(start)

    def n_far_pair():
        arrived(blk(n, order[2], c, 1 - y).at[pl.ds(th, th)], R_NY)
        n_pair(order[2], start)

    unit(0, pf)

    for q in range(PQ):
        arrived(yd.at[:, cols(q)], R_PY + q)

    def grad_x(i):
        at, own = pl.ds(i, 16), pl.ds(y * t + i, 16)
        dn = pd[pl.ds(row(0, c, y) + i, 16), :] + rd[own, :] + yd[at, :]
        x = xc[own, :].astype(F32)
        s = lax.rsqrt(jnp.mean(x * x, axis=-1, keepdims=True) + NORM_EPS)
        xh = x * s
        dhat = dn * gain
        dxn = s * (dhat - xh * jnp.mean(dhat * xh, axis=-1, keepdims=True))
        dxo[at, :] = (d[pl.ds(row(z, c, y) + i, 16), :].astype(F32) + dxn).astype(BF16)

    rows_loop(t, grad_x)

    def dx_part(zz, yy, h):
        return dx_o.at[pl.ds(pl.multiple_of(row(zz, c, yy) + h * th, th), th)]

    def dx_own(h):
        return dxo.at[pl.ds(h * th, th)]

    def far_part(h):
        return far_o.at[pl.ds(h * th, th)]

    def dx_next(k, h):
        here = dx_part(order[k], y, h)
        return (here, here) if k == 1 else (here if k == 0 else far_part(h), far_part(h))

    def dx_across(zz, src, h, act):
        act(remote(src, dx_part(zz, y, h), S_XY + 4 * h + zz, R_XY + 4 * h + zz, across))

    def dx_along(act):
        for h in range(2):
            along(dx_own(h), dx_part(z, y, h), S_XZ + 5 * h, R_XZ + 4 * h, act)

    def dx_pair(zz, act):
        act(remote(duo(dx_o, zz, c), duo(dx_o, zz, c), S_XC + zz, R_XC + zz, partner))

    def dx_got(k, on):
        zz = order[k]
        for h in range(2):
            arrived(dx_part(zz, y, h) if k < 2 else far_part(h), R_XZ + 4 * h + zz)
            if on:
                pass_on(k, dx_next(k, h), S_XZ + 5 * h, R_XZ + 4 * h, start)
            if k < 2:
                dx_across(zz, dx_part(zz, y, h), h, start)

    def dx_hand(zz):
        for h in range(2):
            arrived(dx_part(zz, 1 - y, h), R_XY + 4 * h + zz)
        dx_pair(zz, start)

    for h in range(2):
        dx_across(z, dx_own(h), h, start)
    local(dxo, blk(dx_o, z, c, y), L_DX).start()

    @pl.when(end)
    def _():
        d_got(2)

    d_across(order[2], start)

    for q in range(PQ):
        part_pair(pd, rd, 0, q).wait_send()


    @pl.when(middle)
    def _():
        n_far(0, True)
        n_far(1, True)

    dx_along(start)

    @pl.when(end)
    def _():
        n_got(1)
        n_pair(order[1], start)

    unit(1, pd)
    pl.when(end)(lambda: n_far(0, False))

    @pl.when(middle)
    def _():
        dx_got(0, True)
        dx_got(1, True)

    tw = 2 * t
    n1, n2 = m // tw, f // tw
    late_rows = pl.ds(row(order[2], 0), 4 * t)
    early_rows = pl.ds(pl.multiple_of(half * (4 * t), 4 * t), 12 * t)

    def flush(i, buf, dst):
        lines = pl.ds(pl.multiple_of(lax.rem(i, 2) * tw, tw), tw)
        here = buf.at[lines, pl.ds(0, dst.shape[1])]
        return here, local(here, dst.at[pl.ds(pl.multiple_of(i * tw, tw), tw)], L_DW + lax.rem(i, 2))

    def weight_tile(i, lhs, rhs, buf, dst):
        pl.when(i >= 2)(lambda: flush(i - 2, buf, dst)[1].wait())
        here, out = flush(i, buf, dst)
        at = pl.ds(pl.multiple_of(i * tw, tw), tw)
        here[...] = lax.dot_general(lhs[early_rows, at], rhs[early_rows, :], TN, preferred_element_type=F32)
        out.start()

    loop(0, n1 // 2, lambda i: weight_tile(i, n, dus, pf, dw1_o))
    pl.when(end)(lambda: n_far(1, False))
    loop(n1 // 2, n1, lambda i: weight_tile(i, n, dus, pf, dw1_o))
    for i in (n1 - 2, n1 - 1):
        flush(i, pf, dw1_o)[1].wait()
    n_far_pair()
    unit(2, pd, lambda: pl.when(end)(lambda: dx_got(0, False)))
    kept = [
        local(src.at[late_rows], dst, L_K + i)
        for i, (src, dst) in enumerate(((n, nk_o), (d, dk_o), (hs, hk_o), (dus, duk_o)))
    ]
    for cp in kept:
        cp.start()
    pl.when(middle)(lambda: dx_got(2, True))
    loop(0, n2 // 2, lambda i: weight_tile(i, hs, d, pd, dw2_o))
    pl.when(end)(lambda: dx_got(1, False))
    loop(n2 // 2, n2, lambda i: weight_tile(i, hs, d, pd, dw2_o))
    local(dxo, blk(dx_o, z, c, y), L_DX).wait()
    dx_hand(z)
    dx_hand(order[0])
    for i in (n2 - 2, n2 - 1):
        flush(i, pd, dw2_o)[1].wait()
    if f % tw:
        rest = pd.at[pl.ds(0, f % tw)]
        rest[...] = lax.dot_general(hs[early_rows, n2 * tw :], d[early_rows, :], TN, preferred_element_type=F32)
        last = local(rest, dw2_o.at[pl.ds(n2 * tw, f % tw)], L_DW)
        last.start()
    dx_hand(order[1])
    pl.when(end)(lambda: dx_got(2, False))
    if f % tw:
        last.wait()
    for cp in kept:
        cp.wait()

    y_send.wait()
    y_keep.wait()
    along(own_d, own_d, S_DZ, R_DZ, sent)
    for zz in (z, *order):
        d_across(zz, sent)
        d_pair(zz, sent)
    for k in range(3):
        n_pair(order[k], sent)
        remote(ids_ref, idl.at[z], S_IDS + k, R_IDS + z, {"data": order[k]}).wait_send()
    dx_along(sent)
    for b in range(2):
        n_along(b, sent)
        dx_across(z, dx_own(b), b, sent)
        for k in range(2):
            dx_across(order[k], dx_part(order[k], y, b), b, sent)

    @pl.when(middle)
    def _():
        for k in range(3):
            pass_on(k, blk(d, order[k], c, y), S_DZ, R_DZ, sent)
            n_on(k, sent)
            for b in range(2):
                pass_on(k, dx_next(k, b), S_XZ + 5 * b, R_XZ + 4 * b, sent)

    for q in range(XQ):
        xm_part(q).wait_send()
        n_own(q, sent)
    n_cross(sent)
    for q in range(PQ):
        part_across(q).wait_send()
    for zz in (z, *order[:2]):
        arrived(duo(dx_o, zz, 1 - c), R_XC + zz)
        dx_pair(zz, sent)


def run_group(ids, xm, w1, w2, gain, d_out, shard_rows, tall):
    t, m = d_out.shape
    f = w1.shape[1]
    lines = 4 * ids.shape[0]
    any_, vmem = pl.BlockSpec(memory_space=pl.ANY), pl.BlockSpec(memory_space=pltpu.VMEM)
    V = pltpu.VMEM
    sds = jax.ShapeDtypeStruct
    dots = 2 * 4 * t * m * f
    return pl.pallas_call(
        functools.partial(group_kernel, shard_rows, tall),
        out_shape=(
            sds((t, m), F32), sds((t, m), F32), sds((lines, LANES), I32), sds((1, LANES), I32), sds((16 * t, m), BF16),
            sds((t, m), BF16), sds((m, f), F32), sds((f, m), F32),
            sds((4 * t, m), BF16), sds((4 * t, m), BF16), sds((4 * t, f), BF16), sds((4 * t, f), BF16),
        ),
        in_specs=[vmem, any_, any_, any_, vmem, any_],
        out_specs=(any_, any_, vmem, vmem, *[any_] * 8),
        scratch_shapes=[
            V((m, f), BF16), V((f, m), BF16), V((16 * t, m), BF16), V((16 * t, m), BF16),
            V((4 * t, m), BF16), V((2 * t, m), BF16), V((2 * t, m), BF16),
            V((16 * t, f), BF16), V((16 * t, f), BF16),
            V((4 * t, m), F32), V((4 * t, m), F32), V((2 * t, m), F32), V((2 * t, m), F32),
            V((t, m), F32), V((t, m), F32),
            V((t, m), BF16), V((4, *ids.shape), I32),
            V((lines, LANES), F32), V((lines, LANES), F32), V((lines, LANES), F32), V((1, LANES), F32),
            pltpu.SemaphoreType.DMA((N_L,)), pltpu.SemaphoreType.DMA((N_S,)), pltpu.SemaphoreType.DMA((N_R,)),
        ],
        compiler_params=pltpu.CompilerParams(collective_id=0, has_side_effects=True, vmem_limit_bytes=67043328),
        cost_estimate=pl.CostEstimate(flops=18 * dots, bytes_accessed=64 * 16 * t * m, transcendentals=16 * t * f),
        name="group_step",
    )(ids, xm, w1, w2, gain, d_out)


def lookup_kernel(shard_rows, ids_smem, ids_vmem, table, out_hbm, got, rows, sem, out_sem):
    total, m = out_hbm.shape
    t = total // 4
    per = 32
    chunks = total // per
    r = lax.axis_index("tensor")
    spread = (1 << (shard_rows.bit_length() - 1)) - 1

    def fetch(k):
        def some(j, carry):
            for u in range(8):
                p = k * per + j * 8 + u
                row = ids_smem[jnp.right_shift(p, 7), p & (LANES - 1)]
                near = row - r * shard_rows
                near = jnp.where((near >= 0) & (near < shard_rows), near, row & spread)
                pltpu.make_async_copy(table.at[jnp.right_shift(near, 3)], got.at[p], sem.at[k]).start()
            return carry

        lax.fori_loop(0, per // 8, some, 0)

    loop(0, chunks, fetch)
    spot = lax.broadcasted_iota(I32, (per, 8 * per), 1)
    token = lax.broadcasted_iota(I32, (per, 8 * per), 0)
    same = lax.broadcasted_iota(I32, (LANES, LANES), 0) == lax.broadcasted_iota(I32, (LANES, LANES), 1)

    def line(b):
        ids = ids_vmem[pl.ds(b, 1), :].astype(F32)
        col = jnp.sum(jnp.where(same, jnp.broadcast_to(ids, (LANES, LANES)), 0.0), axis=1, keepdims=True).astype(I32)
        row = col - r * shard_rows
        row = jnp.where((row >= 0) & (row < shard_rows), row & 7, -8 * per)
        for j in range(LANES // per):
            k = b * (LANES // per) + j
            at = pl.ds(pl.multiple_of(k * per, per), per)
            pltpu.make_async_copy(got.at[at], got.at[at], sem.at[k]).wait()
            want = row[j * per : (j + 1) * per] + 8 * token
            chosen = jnp.where(want == spot, 1.0, 0.0).astype(BF16)
            picked = jnp.dot(chosen, got[at].reshape(8 * per, m), preferred_element_type=F32)
            p = k * per
            nat = lax.div(p, t)
            to = pl.multiple_of(lax.rem(nat, 2) * (2 * t) + lax.div(nat, 2) * t + lax.rem(p, t), per)
            rows[pl.ds(to, per), :] = picked.astype(BF16)
            pltpu.make_async_copy(rows.at[pl.ds(to, per)], out_hbm.at[pl.ds(to, per)], out_sem).start()

    loop(0, total // LANES, line)
    pltpu.make_async_copy(rows, out_hbm, out_sem).wait()


def look_up(ids, table):
    shard_rows, m = table.shape
    total = ids.size
    any_ = pl.BlockSpec(memory_space=pl.ANY)
    return pl.pallas_call(
        functools.partial(lookup_kernel, shard_rows),
        out_shape=jax.ShapeDtypeStruct((total, m), BF16),
        in_specs=[pl.BlockSpec(memory_space=pltpu.SMEM), pl.BlockSpec(memory_space=pltpu.VMEM), any_],
        out_specs=any_,
        scratch_shapes=[
            pltpu.VMEM((total, 8, m), BF16), pltpu.VMEM((total, m), BF16),
            pltpu.SemaphoreType.DMA((total // 32,)), pltpu.SemaphoreType.DMA,
        ],
        compiler_params=pltpu.CompilerParams(vmem_limit_bytes=60 << 20),
        cost_estimate=pl.CostEstimate(flops=16 * total * m, bytes_accessed=20 * total * m, transcendentals=0),
        name="look_up",
    )(ids, ids, table.reshape(shard_rows // 8, 8, m))


RING = 6


def weights_kernel(p1, p2, nk_in, dk_in, hk_in, duk_in, o1, o2, b1, b2, nk, dk, hk, duk, in_sem, out_sem, k_sem):
    m, f = b1.shape
    tw = nk.shape[0] // 2
    ins = [pltpu.make_async_copy(a, b, k_sem.at[i]) for i, (a, b) in enumerate(((nk_in, nk), (duk_in, duk), (hk_in, hk), (dk_in, dk)))]
    for cp in ins[:2]:
        cp.start()

    def part(src, buf, dst, first, i, rows=tw):
        at = pl.ds(pl.multiple_of(i * tw, 8), rows)
        fetch = pltpu.make_async_copy(src.at[at], buf.at[at], in_sem.at[first + i])
        return fetch, pltpu.make_async_copy(buf.at[at], dst.at[at], out_sem)

    def fetch_all(src, buf, dst, first):
        loop(0, src.shape[0] // tw, lambda i: part(src, buf, dst, first, i)[0].start())

    n1, n2 = m // tw, f // tw
    fetch_all(p1, b1, o1, 0)
    for cp in ins[2:]:
        cp.start()
    fetch_all(p2, b2, o2, n1)
    rest = [part(p2, b2, o2, n1, n2, f % tw)] if f % tw else []
    for come, _ in rest:
        come.start()

    def add(src, buf, dst, first, lhs, rhs, i, rows=tw):
        come, go = part(src, buf, dst, first, i, rows)
        come.wait()
        cols = pl.ds(pl.multiple_of(i * tw, tw), rows)
        buf[cols, :] += lax.dot_general(lhs[:, cols], rhs[...], TN, preferred_element_type=F32)
        go.start()

    for cp in ins[:2]:
        cp.wait()
    loop(0, n1, lambda i: add(p1, b1, o1, 0, nk, duk, i))
    for cp in ins[2:]:
        cp.wait()
    loop(0, n2, lambda i: add(p2, b2, o2, n1, hk, dk, i))
    if rest:
        add(p2, b2, o2, n1, hk, dk, n2, f % tw)
    pltpu.make_async_copy(b1, o1, out_sem).wait()
    pltpu.make_async_copy(b2, o2, out_sem).wait()


def finish_weights(p1, p2, nk, dk, hk, duk):
    any_ = pl.BlockSpec(memory_space=pl.ANY)
    V, S = pltpu.VMEM, pltpu.SemaphoreType.DMA
    arrays = (p1, p2, nk, dk, hk, duk)
    return pl.pallas_call(
        weights_kernel,
        out_shape=(jax.ShapeDtypeStruct(p1.shape, F32), jax.ShapeDtypeStruct(p2.shape, F32)),
        in_specs=[any_] * 6,
        out_specs=[any_] * 2,
        scratch_shapes=[*[V(a.shape, a.dtype) for a in arrays], S((32,)), S, S((4,))],
        compiler_params=pltpu.CompilerParams(vmem_limit_bytes=60 << 20),
        cost_estimate=pl.CostEstimate(flops=8000 * p1.size, bytes_accessed=20 * p1.size, transcendentals=0),
        name="finish_weights",
    )(*arrays)


def table_kernel(tall, key_ref, first_ref, dx_in, far_own, far_across, far_partner, far_both, out_hbm, dxb, dxf, ring, dx_sem, t_sem):
    count, _ = dxb.shape
    t = count // 16
    shift = count.bit_length() - 1
    steps = out_hbm.shape[0] // tall
    z, r = lax.axis_index("data"), lax.axis_index("tensor")
    y, c = lax.div(r, 2), lax.rem(r, 2)
    late = lax.div(z, 2)

    def near(k):
        at = pl.ds(pl.multiple_of(late * (4 * t) + k * (2 * t), t), 2 * t)
        return at, pltpu.make_async_copy(dx_in.at[at], dxb.at[at], dx_sem.at[k])

    def far(cc, yy):
        return pl.multiple_of((1 - late) * (12 * t) + cc * (2 * t) + yy * t, t)

    loop(0, 6, lambda k: near(k)[1].start())
    for src, cc, yy in ((far_own, c, y), (far_across, c, 1 - y), (far_partner, 1 - c, y), (far_both, 1 - c, 1 - y)):
        to = far(cc, yy)

        def widen_far(i, src=src, to=to):
            dxf[pl.ds(to + i, 16), :] = src[pl.ds(i, 16), :].astype(F32)

        rows_loop(t, widen_far)

    def widen_piece(at, cp):
        cp.wait()

        def widen(i):
            rows = pl.ds(pl.multiple_of(at.start + i, 16), 16)
            dxf[rows, :] = dxb[rows, :].astype(F32)

        rows_loop(at.size, widen)

    loop(0, 6, lambda k: widen_piece(*near(k)))

    def tile_out(i):
        slot = lax.rem(i, RING)
        return pltpu.make_async_copy(ring.at[slot], out_hbm.at[pl.ds(pl.multiple_of(i * tall, 8), tall)], t_sem.at[slot])

    def tile(i):
        slot = lax.rem(i, RING)
        here = ring.at[slot]
        pl.when(i >= RING)(lambda: tile_out(i - RING).wait())
        here[...] = jnp.zeros_like(here)

        def add(j, key):
            ahead = key_ref[jnp.minimum(j + 1, count - 1)]
            to = pl.ds(jnp.right_shift(key, shift) - i * tall, 1)
            here[to, :] += dxf[pl.ds(key & (count - 1), 1), :]
            return ahead

        low = first_ref[i]
        lax.fori_loop(low, first_ref[i + 1], add, key_ref[jnp.minimum(low, count - 1)])
        tile_out(i).start()

    loop(0, steps, tile)
    loop(steps - RING, steps, lambda i: tile_out(i).wait())


def table_grad(ordered, first, dx_all, fars, shard_rows, tall):
    count, m = dx_all.shape
    any_ = pl.BlockSpec(memory_space=pl.ANY)
    V, S = pltpu.VMEM, pltpu.SemaphoreType.DMA
    return pl.pallas_call(
        functools.partial(table_kernel, tall),
        out_shape=jax.ShapeDtypeStruct((shard_rows, m), F32),
        grid_spec=pltpu.PrefetchScalarGridSpec(
            num_scalar_prefetch=2,
            grid=(1,),
            in_specs=[any_, *[pl.BlockSpec(memory_space=pltpu.VMEM)] * 4],
            out_specs=any_,
            scratch_shapes=[
                V((count, m), BF16), V((count, m), F32), V((RING, tall, m), F32), S((6,)), S((RING,)),
            ],
        ),
        compiler_params=pltpu.CompilerParams(vmem_limit_bytes=44 << 20),
        cost_estimate=pl.CostEstimate(flops=16000 * shard_rows * m // 10, bytes_accessed=4 * shard_rows * m, transcendentals=0),
        name="table_grad",
    )(ordered, first, dx_all, *fars)


def solution(mesh):
    tok_spec = P(("pod", "data", "tensor"), None)

    over_y, over_core = [(0, 2), (1, 3), (2, 0), (3, 1)], [(0, 1), (1, 0), (2, 3), (3, 2)]

    def per_device(token_ids, embed_table, norm_gain, w_in, w_out, d_out):
        shard_rows = embed_table.shape[0]
        tall = next(k for k in (160, 8) if shard_rows % k == 0)
        ids = token_ids.reshape(-1, LANES)
        masked = look_up(ids, embed_table)
        gain = norm_gain.reshape(-1, LANES)
        base, ysum, ordered, first, dx_all, far, *weights = run_group(
            ids, masked, w_in, w_out, gain, d_out, shard_rows, tall
        )
        far_x = lax.ppermute(far, "tensor", over_y)
        far_p = lax.ppermute(far, "tensor", over_core)
        other = lax.ppermute(ysum, "tensor", over_y)
        grad_w_in, grad_w_out = finish_weights(*weights)
        far_b = lax.ppermute(far_x, "tensor", over_core)
        fars = (far, far_x, far_p, far_b)
        grad_table = table_grad(ordered.reshape(-1), first.reshape(-1), dx_all, fars, shard_rows, tall)
        return (base + other).astype(BF16), grad_table, grad_w_in, grad_w_out

    return jax.shard_map(
        per_device,
        mesh=mesh,
        in_specs=(P(("pod", "data")), P("tensor", None), P(None), P(None, "tensor"), P("tensor", None), tok_spec),
        out_specs=(tok_spec, P(("pod", "tensor"), None), P("pod", "tensor"), P(("pod", "tensor"), None)),
        check_vma=False,
    )
```

```python
import functools

import jax
import jax.numpy as jnp
from jax import lax
from jax.experimental import pallas as pl
from jax.experimental.pallas import tpu as pltpu
from jax.sharding import PartitionSpec as P


NORM_EPS = 1e-6
GELU_A = 0.7978845608028654
GELU_B = 0.044715
MESH = pl.DeviceIdType.MESH
NT = (((1,), (1,)), ((), ()))
TN = (((0,), (0,)), ((), ()))
F32, BF16, I32 = jnp.float32, jnp.bfloat16, jnp.int32
LANES = 128
XQ = 4
PQ = 4

R_IDS, R_DZ, R_DY, R_DC, R_NZ, R_NC, R_XZ, R_XY, R_XC = 0, 4, 8, 12, 16, 24, 28, 36, 44
R_XM, R_X, R_NO, R_PC, R_PY, R_NY, N_R = 48, 52, 56, 60, 68, 72, 73
S_IDS, S_DZ, S_DY, S_DC, S_NZ, S_NC, S_XZ, S_XY, S_XC = 0, 3, 8, 12, 16, 26, 30, 40, 48
S_XM, S_X, S_NO, S_PC, S_PY, S_NY, N_S = 52, 56, 60, 64, 72, 76, 77
L_W1, L_W2, L_XM, L_DX, L_YS, L_YB, L_DW, L_DO, L_K, N_L = 0, 1, 2, 3, 4, 5, 6, 8, 9, 13


def loop(lo, hi, body):
    def one(j, carry):
        body(j)
        return carry

    lax.fori_loop(lo, hi, one, 0)


def tiles(total, step, body):
    full = total // step
    loop(0, full, lambda j: body(pl.multiple_of(j * step, step), step))
    if total % step:
        body(full * step, total % step)


def rows_loop(total, body):
    loop(0, total // 16, lambda j: body(pl.multiple_of(j * 16, 16)))


def make_keys(ids, keys, shard_rows, rank0):
    reps, per, _ = ids.shape
    count = reps * per * LANES
    t = per * LANES // 4
    shift = t.bit_length() - 1
    lane = lax.broadcasted_iota(I32, (per, LANES), 1)
    spot = lax.broadcasted_iota(I32, (per, LANES), 0) * LANES + lane
    block = jnp.right_shift(spot, shift)
    kept = (block & 1) * (2 * t) + jnp.right_shift(block, 1) * t + (spot & (t - 1))
    for k in range(reps):
        row = ids[k] - rank0
        row = jnp.where((row >= 0) & (row < shard_rows), row, shard_rows)
        keys[k * per : (k + 1) * per, :] = (row * count + (k * per * LANES + kept)).astype(F32)


def columns(refs, b):
    same = lax.broadcasted_iota(I32, (LANES, LANES), 0) == lax.broadcasted_iota(I32, (LANES, LANES), 1)
    wide = (jnp.where(same, jnp.broadcast_to(ref[pl.ds(b, 1), :], (LANES, LANES)), 0.0) for ref in refs)
    return [jnp.sum(w, axis=1, keepdims=True) for w in wide]


def count_below(keys, place):
    lines = keys.shape[0]
    place[...] = jnp.zeros_like(place)

    def some(j):
        cols = [columns((keys,), 4 * j + u)[0] for u in range(4)]
        for a in range(lines):
            row = keys[a : a + 1, :]
            hits = sum(jnp.where(col < row, 1.0, 0.0) for col in cols)
            place[a : a + 1, :] += jnp.sum(hits, axis=0, keepdims=True)

    loop(0, lines // 4, some)


def put_in_order(keys, place, ordered, first, tall):
    lines = keys.shape[0]
    ordered[...] = jnp.zeros_like(ordered)
    first[...] = jnp.zeros_like(first)
    lane = lax.broadcasted_iota(I32, (1, LANES), 1).astype(F32)
    edge = lane * float(tall * lines * LANES)

    def some(j):
        cols = [columns((keys, place), 4 * j + u) for u in range(4)]
        for a in range(lines):
            want = lane + float(a * LANES)
            hits = sum(jnp.where(spot == want, key, 0.0) for key, spot in cols)
            ordered[a : a + 1, :] += jnp.sum(hits, axis=0, keepdims=True)
        first[...] += jnp.sum(sum(jnp.where(key < edge, 1.0, 0.0) for key, _ in cols), axis=0, keepdims=True)

    loop(0, lines // 4, some)


def group_kernel(shard_rows, tall, ids_ref, xm_hbm, w1_hbm, w2_hbm, g_ref, do_hbm,
                 base_o, ysum_o, ord_o, first_o, dx_o, far_o, dw1_o, dw2_o, nk_o, dk_o, hk_o, duk_o,
                 w1, w2, n, d, xm, xc, xy, hs, dus, pd, pf, rd, rf, yd, yb, dxo, idl, keys, place, ordered, first,
                 lsem, ssem, rsem):
    t, m = do_hbm.shape
    f = w1_hbm.shape[1]
    tq, mq = 2 * t // XQ, m // PQ
    z = lax.axis_index("data")
    r = lax.axis_index("tensor")
    y, c = lax.div(r, 2), lax.rem(r, 2)
    partner = {"tensor": 2 * y + 1 - c}
    across = {"tensor": 2 * (1 - y) + c}
    half = lax.div(z, 2)
    inner = z + half * (3 - 2 * z)
    order = [b + half * (3 - 2 * b) for b in (1 - inner, 2, 3)]
    middle, end = inner == 1, inner == 0

    def row(zz, cc, yy=0):
        return pl.multiple_of(zz * (4 * t) + cc * (2 * t) + yy * t, t)

    def blk(ref, zz, cc, yy):
        return ref.at[pl.ds(row(zz, cc, yy), t)]

    def duo(ref, zz, cc):
        return ref.at[pl.ds(row(zz, cc), 2 * t)]

    def remote(src, dst, s, q, dev):
        return pltpu.make_async_remote_copy(
            src_ref=src, dst_ref=dst, send_sem=ssem.at[s], recv_sem=rsem.at[q], device_id=dev, device_id_type=MESH
        )

    def local(src, dst, i):
        return pltpu.make_async_copy(src, dst, lsem.at[i])

    def arrived(ref, q):
        remote(ref, ref, 0, q, partner).wait_recv()

    def start(cp):
        cp.start()

    def sent(cp):
        cp.wait_send()

    def along(src, dst, s, q, act):
        for i, hop in enumerate((1, -1)):
            to = z + hop

            @pl.when((to >= 0) & (to <= 3))
            def _():
                act(remote(src, dst, s + i, q + z, {"data": to}))

    def pass_on(k, ref, s, q, act):
        src, dst = ref if isinstance(ref, tuple) else (ref, ref)
        act(remote(src, dst, s + 2 + k, q + order[k], {"data": order[1] if k == 0 else order[0]}))

    barrier = pltpu.get_barrier_semaphore()
    pl.semaphore_signal(barrier, inc=1, device_id=partner, device_id_type=MESH)
    pl.semaphore_signal(barrier, inc=1, device_id=across, device_id_type=MESH)
    for k in range(3):
        pl.semaphore_signal(barrier, inc=1, device_id={"data": order[k]}, device_id_type=MESH)

    own_d = blk(d, z, c, y)
    local(do_hbm, own_d, L_DO).start()
    local(xm_hbm, xm, L_XM).start()
    local(w1_hbm, w1, L_W1).start()
    local(w2_hbm, w2, L_W2).start()
    pl.semaphore_wait(barrier, 5)

    def piece(q):
        return pl.ds(q * tq, tq)

    for k in range(3):
        remote(ids_ref, idl.at[z], S_IDS + k, R_IDS + z, {"data": order[k]}).start()
    idl[z] = ids_ref[...]

    local(do_hbm, own_d, L_DO).wait()
    along(own_d, own_d, S_DZ, R_DZ, start)
    local(xm_hbm, xm, L_XM).wait()

    def xm_part(q):
        return remote(xm.at[pl.ds(row(0, 1 - c) + q * tq, tq)], xc.at[piece(q)], S_XM + q, R_XM + q, partner)

    def x_part(q):
        return remote(xc.at[piece(q)], xy.at[piece(q)], S_X + q, R_X + q, across)

    def d_got(k):
        arrived(blk(d, order[k], c, y), R_DZ + order[k])

    def d_on(k):
        pass_on(k, blk(d, order[k], c, y), S_DZ, R_DZ, start)

    def d_across(zz, act):
        act(remote(blk(d, zz, c, y), blk(d, zz, c, y), S_DY + zz, R_DY + zz, across))

    def d_pair(zz, act):
        act(remote(duo(d, zz, c), duo(d, zz, c), S_DC + zz, R_DC + zz, partner))

    for q in range(XQ):
        xm_part(q).start()
    for q in range(XQ):
        arrived(xc.at[piece(q)], R_XM + q)

        def join(i, q=q):
            at = pl.ds(q * tq + i, 16)
            xc[at, :] += xm[pl.ds(row(0, c) + q * tq + i, 16), :]

        rows_loop(tq, join)
        x_part(q).start()
    d_across(z, start)

    for k in range(3):
        arrived(idl.at[order[k]], R_IDS + order[k])
    make_keys(idl, keys, shard_rows, r * shard_rows)
    count_below(keys, place)
    d_got(0)

    @pl.when(middle)
    def _():
        d_on(0)
        d_got(1)
        d_on(1)

    gain = jnp.concatenate([g_ref[pl.ds(i, 1), :] for i in range(m // LANES)], axis=1).astype(F32)

    def n_own(q, act):
        at = n.at[pl.ds(row(z, c) + q * tq, tq)]
        act(remote(at, at, S_NO + q, R_NO + q, partner))

    def n_along(b, act):
        ref = blk(n, z, c, b)
        along(ref, ref, S_NZ + 5 * b, R_NZ + 4 * b, act)

    for q in range(XQ):
        arrived(xy.at[piece(q)], R_X + q)
        x_part(q).wait_send()

        def norm(i, q=q):
            at = pl.ds(q * tq + i, 16)
            x16 = xc[at, :] + xy[at, :]
            xc[at, :] = x16
            x = x16.astype(F32)
            s = lax.rsqrt(jnp.mean(x * x, axis=-1, keepdims=True) + NORM_EPS)
            n[pl.ds(row(z, c) + q * tq + i, 16), :] = ((x * s) * gain).astype(BF16)

        rows_loop(tq, norm)
        n_own(q, start)
        if q == XQ // 2 - 1:
            n_along(0, start)
            put_in_order(keys, place, ordered, first, tall)
            ord_o[...] = ordered[...].astype(I32)
            first_o[...] = first[...].astype(I32)

            @pl.when(middle)
            def _():
                d_got(2)
                d_on(2)

        if q == XQ - 1:
            n_along(1, start)
    d_across(order[0], start)

    def hidden(zz, slopes):
        at = pl.ds(row(zz, 0), 4 * t)

        def body(off, w):
            to = pl.ds(off, w)
            u = jnp.dot(n[at, :], w1[:, to], preferred_element_type=F32).astype(BF16).astype(F32)
            uu = u * u
            th = jnp.tanh(GELU_A * (u + GELU_B * (uu * u)))
            cdf = 0.5 * (1.0 + th)
            hs[at, to] = (u * cdf).astype(BF16)
            slopes[:, to] = cdf + (0.5 * GELU_A) * u * (1.0 - th * th) * (1.0 + (3.0 * GELU_B) * uu)

        tiles(f, 256, body)

    def grad_hidden(zz, slopes):
        at = pl.ds(row(zz, 0), 4 * t)

        def body(off, w):
            to = pl.ds(off, w)
            dh = lax.dot_general(d[at, :], w2[to, :], NT, preferred_element_type=F32)
            dus[at, to] = (dh * slopes[:, to]).astype(BF16)

        tiles(f, 256, body)

    for q in range(XQ):
        arrived(n.at[pl.ds(row(z, 1 - c) + q * tq, tq)], R_NO + q)
    local(w1_hbm, w1, L_W1).wait()
    hidden(z, pf)
    arrived(blk(d, z, c, 1 - y), R_DY + z)
    d_pair(z, start)
    arrived(duo(d, z, 1 - c), R_DC + z)
    local(w2_hbm, w2, L_W2).wait()
    grad_hidden(z, pf)

    own_rows = pl.ds(row(z, 0), 4 * t)
    far = pl.multiple_of((1 - y) * t, t)

    def cols(q):
        return pl.ds(pl.multiple_of(q * mq, mq), mq)

    def part_pair(src, dst, i, q):
        return remote(src.at[pl.ds(row(0, 1 - c), 2 * t), cols(q)], dst.at[:, cols(q)], S_PC + PQ * i + q, R_PC + PQ * i + q, partner)

    def part_across(q):
        return remote(rd.at[pl.ds(far, t), cols(q)], yd.at[:, cols(q)], S_PY + q, R_PY + q, across)

    def sum_part(part, got, i, q):
        arrived(got.at[:, cols(q)], R_PC + PQ * i + q)

        def add(k):
            got[pl.ds(far + k, 16), cols(q)] += part[pl.ds(row(0, c, 1 - y) + k, 16), cols(q)]

        rows_loop(t, add)

    def dn_part(q):
        pd[:, cols(q)] = lax.dot_general(dus[own_rows, :], w1[cols(q), :], NT, preferred_element_type=F32)
        part_pair(pd, rd, 0, q).start()

    def y_part(q):
        pf[:, cols(q)] = jnp.dot(hs[own_rows, :], w2[:, cols(q)], preferred_element_type=F32)
        part_pair(pf, rf, 1, q).start()

    def dn_out(q):
        sum_part(pd, rd, 0, q)
        part_across(q).start()

    loop(0, PQ, dn_part)
    loop(0, PQ, dn_out)
    loop(0, PQ, y_part)

    @pl.when(end)
    def _():
        d_got(1)

    d_across(order[1], start)

    loop(0, PQ, lambda q: sum_part(pf, rf, 1, q))
    y_send = local(rf.at[pl.ds(far, t)], ysum_o, L_YS)
    y_send.start()

    def base(i):
        own = pl.ds(y * t + i, 16)
        yb[pl.ds(i, 16), :] = xc[own, :].astype(F32) + (pf[pl.ds(row(0, c, y) + i, 16), :] + rf[own, :])

    rows_loop(t, base)
    y_keep = local(yb, base_o, L_YB)
    y_keep.start()
    for q in range(PQ):
        part_pair(pf, rf, 1, q).wait_send()

    th = t // 2

    def n_parts(k, lands):
        own, other = blk(n, order[k], c, y), blk(n, order[k], c, 1 - y)
        if lands == 2:
            other = other.at[pl.ds(0, th)]
        return (own, y), (other, 1 - y)

    def n_got(k):
        for ref, b in n_parts(k, k):
            arrived(ref, R_NZ + 4 * b + order[k])

    def n_on(k, act):
        for ref, b in n_parts(k, 1 if k == 1 else 2):
            pass_on(k, ref, S_NZ + 5 * b, R_NZ + 4 * b, act)

    def n_cross(act):
        half_own = blk(n, order[2], c, y).at[pl.ds(th, th)]
        act(remote(half_own, half_own, S_NY, R_NY, across))

    def n_pair(zz, act):
        act(remote(duo(n, zz, c), duo(n, zz, c), S_NC + zz, R_NC + zz, partner))

    n_got(0)
    n_pair(order[0], start)

    @pl.when(middle)
    def _():
        n_on(0, start)
        n_got(1)
        n_on(1, start)
        n_pair(order[1], start)

    def unit(k, slopes):
        zz = order[k]
        arrived(blk(d, zz, c, 1 - y), R_DY + zz)
        d_pair(zz, start)
        arrived(duo(n, zz, 1 - c), R_NC + zz)
        hidden(zz, slopes)
        arrived(duo(d, zz, 1 - c), R_DC + zz)
        grad_hidden(zz, slopes)

    def n_far(part, on):
        ref, b = n_parts(2, 2)[part]
        arrived(ref, R_NZ + 4 * b + order[2])
        if on:
            pass_on(2, ref, S_NZ + 5 * b, R_NZ + 4 * b, start)
        if part == 0:
            n_cross(start)

    def n_far_pair():
        arrived(blk(n, order[2], c, 1 - y).at[pl.ds(th, th)], R_NY)
        n_pair(order[2], start)

    unit(0, pf)

    for q in range(PQ):
        arrived(yd.at[:, cols(q)], R_PY + q)

    def grad_x(i):
        at, own = pl.ds(i, 16), pl.ds(y * t + i, 16)
        dn = pd[pl.ds(row(0, c, y) + i, 16), :] + rd[own, :] + yd[at, :]
        x = xc[own, :].astype(F32)
        s = lax.rsqrt(jnp.mean(x * x, axis=-1, keepdims=True) + NORM_EPS)
        xh = x * s
        dhat = dn * gain
        dxn = s * (dhat - xh * jnp.mean(dhat * xh, axis=-1, keepdims=True))
        dxo[at, :] = (d[pl.ds(row(z, c, y) + i, 16), :].astype(F32) + dxn).astype(BF16)

    rows_loop(t, grad_x)

    def dx_part(zz, yy, h):
        return dx_o.at[pl.ds(pl.multiple_of(row(zz, c, yy) + h * th, th), th)]

    def dx_own(h):
        return dxo.at[pl.ds(h * th, th)]

    def far_part(h):
        return far_o.at[pl.ds(h * th, th)]

    def dx_next(k, h):
        here = dx_part(order[k], y, h)
        return (here, here) if k == 1 else (here if k == 0 else far_part(h), far_part(h))

    def dx_across(zz, src, h, act):
        act(remote(src, dx_part(zz, y, h), S_XY + 4 * h + zz, R_XY + 4 * h + zz, across))

    def dx_along(act):
        for h in range(2):
            along(dx_own(h), dx_part(z, y, h), S_XZ + 5 * h, R_XZ + 4 * h, act)

    def dx_pair(zz, act):
        act(remote(duo(dx_o, zz, c), duo(dx_o, zz, c), S_XC + zz, R_XC + zz, partner))

    def dx_got(k, on):
        zz = order[k]
        for h in range(2):
            arrived(dx_part(zz, y, h) if k < 2 else far_part(h), R_XZ + 4 * h + zz)
            if on:
                pass_on(k, dx_next(k, h), S_XZ + 5 * h, R_XZ + 4 * h, start)
            if k < 2:
                dx_across(zz, dx_part(zz, y, h), h, start)

    def dx_hand(zz):
        for h in range(2):
            arrived(dx_part(zz, 1 - y, h), R_XY + 4 * h + zz)
        dx_pair(zz, start)

    for h in range(2):
        dx_across(z, dx_own(h), h, start)
    local(dxo, blk(dx_o, z, c, y), L_DX).start()

    @pl.when(end)
    def _():
        d_got(2)

    d_across(order[2], start)

    for q in range(PQ):
        part_pair(pd, rd, 0, q).wait_send()


    @pl.when(middle)
    def _():
        n_far(0, True)
        n_far(1, True)

    dx_along(start)

    @pl.when(end)
    def _():
        n_got(1)
        n_pair(order[1], start)

    unit(1, pd)
    pl.when(end)(lambda: n_far(0, False))

    @pl.when(middle)
    def _():
        dx_got(0, True)
        dx_got(1, True)

    tw = 2 * t
    n1, n2 = m // tw, f // tw
    late_rows = pl.ds(row(order[2], 0), 4 * t)
    early_rows = pl.ds(pl.multiple_of(half * (4 * t), 4 * t), 12 * t)

    def flush(i, buf, dst):
        lines = pl.ds(pl.multiple_of(lax.rem(i, 2) * tw, tw), tw)
        here = buf.at[lines, pl.ds(0, dst.shape[1])]
        return here, local(here, dst.at[pl.ds(pl.multiple_of(i * tw, tw), tw)], L_DW + lax.rem(i, 2))

    def weight_tile(i, lhs, rhs, buf, dst):
        pl.when(i >= 2)(lambda: flush(i - 2, buf, dst)[1].wait())
        here, out = flush(i, buf, dst)
        at = pl.ds(pl.multiple_of(i * tw, tw), tw)
        here[...] = lax.dot_general(lhs[early_rows, at], rhs[early_rows, :], TN, preferred_element_type=F32)
        out.start()

    loop(0, n1 // 2, lambda i: weight_tile(i, n, dus, pf, dw1_o))
    pl.when(end)(lambda: n_far(1, False))
    loop(n1 // 2, n1, lambda i: weight_tile(i, n, dus, pf, dw1_o))
    for i in (n1 - 2, n1 - 1):
        flush(i, pf, dw1_o)[1].wait()
    pl.when(end)(lambda: dx_got(0, False))
    n_far_pair()
    local(dxo, blk(dx_o, z, c, y), L_DX).wait()
    dx_hand(z)
    pl.when(middle)(lambda: dx_got(2, True))
    unit(2, pd)
    pl.when(end)(lambda: dx_got(1, False))
    kept = [
        local(src.at[late_rows], dst, L_K + i)
        for i, (src, dst) in enumerate(((n, nk_o), (d, dk_o), (hs, hk_o), (dus, duk_o)))
    ]
    for cp in kept:
        cp.start()
    loop(0, n2 // 2, lambda i: weight_tile(i, hs, d, pd, dw2_o))
    dx_hand(order[0])
    loop(n2 // 2, n2, lambda i: weight_tile(i, hs, d, pd, dw2_o))
    for i in (n2 - 2, n2 - 1):
        flush(i, pd, dw2_o)[1].wait()
    if f % tw:
        rest = pd.at[pl.ds(0, f % tw)]
        rest[...] = lax.dot_general(hs[early_rows, n2 * tw :], d[early_rows, :], TN, preferred_element_type=F32)
        last = local(rest, dw2_o.at[pl.ds(n2 * tw, f % tw)], L_DW)
        last.start()
    dx_hand(order[1])
    pl.when(end)(lambda: dx_got(2, False))
    if f % tw:
        last.wait()
    for cp in kept:
        cp.wait()

    y_send.wait()
    y_keep.wait()
    along(own_d, own_d, S_DZ, R_DZ, sent)
    for zz in (z, *order):
        d_across(zz, sent)
        d_pair(zz, sent)
    for k in range(3):
        n_pair(order[k], sent)
        remote(ids_ref, idl.at[z], S_IDS + k, R_IDS + z, {"data": order[k]}).wait_send()
    dx_along(sent)
    for b in range(2):
        n_along(b, sent)
        dx_across(z, dx_own(b), b, sent)
        for k in range(2):
            dx_across(order[k], dx_part(order[k], y, b), b, sent)

    @pl.when(middle)
    def _():
        for k in range(3):
            pass_on(k, blk(d, order[k], c, y), S_DZ, R_DZ, sent)
            n_on(k, sent)
            for b in range(2):
                pass_on(k, dx_next(k, b), S_XZ + 5 * b, R_XZ + 4 * b, sent)

    for q in range(XQ):
        xm_part(q).wait_send()
        n_own(q, sent)
    n_cross(sent)
    for q in range(PQ):
        part_across(q).wait_send()
    for zz in (z, *order[:2]):
        arrived(duo(dx_o, zz, 1 - c), R_XC + zz)
        dx_pair(zz, sent)


def run_group(ids, xm, w1, w2, gain, d_out, shard_rows, tall):
    t, m = d_out.shape
    f = w1.shape[1]
    lines = 4 * ids.shape[0]
    any_, vmem = pl.BlockSpec(memory_space=pl.ANY), pl.BlockSpec(memory_space=pltpu.VMEM)
    V = pltpu.VMEM
    sds = jax.ShapeDtypeStruct
    dots = 2 * 4 * t * m * f
    return pl.pallas_call(
        functools.partial(group_kernel, shard_rows, tall),
        out_shape=(
            sds((t, m), F32), sds((t, m), F32), sds((lines, LANES), I32), sds((1, LANES), I32), sds((16 * t, m), BF16),
            sds((t, m), BF16), sds((m, f), F32), sds((f, m), F32),
            sds((4 * t, m), BF16), sds((4 * t, m), BF16), sds((4 * t, f), BF16), sds((4 * t, f), BF16),
        ),
        in_specs=[vmem, any_, any_, any_, vmem, any_],
        out_specs=(any_, any_, vmem, vmem, *[any_] * 8),
        scratch_shapes=[
            V((m, f), BF16), V((f, m), BF16), V((16 * t, m), BF16), V((16 * t, m), BF16),
            V((4 * t, m), BF16), V((2 * t, m), BF16), V((2 * t, m), BF16),
            V((16 * t, f), BF16), V((16 * t, f), BF16),
            V((4 * t, m), F32), V((4 * t, m), F32), V((2 * t, m), F32), V((2 * t, m), F32),
            V((t, m), F32), V((t, m), F32),
            V((t, m), BF16), V((4, *ids.shape), I32),
            V((lines, LANES), F32), V((lines, LANES), F32), V((lines, LANES), F32), V((1, LANES), F32),
            pltpu.SemaphoreType.DMA((N_L,)), pltpu.SemaphoreType.DMA((N_S,)), pltpu.SemaphoreType.DMA((N_R,)),
        ],
        compiler_params=pltpu.CompilerParams(collective_id=0, has_side_effects=True, vmem_limit_bytes=67043328),
        cost_estimate=pl.CostEstimate(flops=18 * dots, bytes_accessed=64 * 16 * t * m, transcendentals=16 * t * f),
        name="group_step",
    )(ids, xm, w1, w2, gain, d_out)


def lookup_kernel(shard_rows, ids_smem, ids_vmem, table, out_hbm, got, rows, sem, out_sem):
    total, m = out_hbm.shape
    t = total // 4
    per = 32
    chunks = total // per
    r = lax.axis_index("tensor")
    spread = (1 << (shard_rows.bit_length() - 1)) - 1

    def fetch(k):
        def some(j, carry):
            for u in range(8):
                p = k * per + j * 8 + u
                row = ids_smem[jnp.right_shift(p, 7), p & (LANES - 1)]
                near = row - r * shard_rows
                near = jnp.where((near >= 0) & (near < shard_rows), near, row & spread)
                pltpu.make_async_copy(table.at[jnp.right_shift(near, 3)], got.at[p], sem.at[k]).start()
            return carry

        lax.fori_loop(0, per // 8, some, 0)

    loop(0, chunks, fetch)
    spot = lax.broadcasted_iota(I32, (per, 8 * per), 1)
    token = lax.broadcasted_iota(I32, (per, 8 * per), 0)
    same = lax.broadcasted_iota(I32, (LANES, LANES), 0) == lax.broadcasted_iota(I32, (LANES, LANES), 1)

    def line(b):
        ids = ids_vmem[pl.ds(b, 1), :].astype(F32)
        col = jnp.sum(jnp.where(same, jnp.broadcast_to(ids, (LANES, LANES)), 0.0), axis=1, keepdims=True).astype(I32)
        row = col - r * shard_rows
        row = jnp.where((row >= 0) & (row < shard_rows), row & 7, -8 * per)
        for j in range(LANES // per):
            k = b * (LANES // per) + j
            at = pl.ds(pl.multiple_of(k * per, per), per)
            pltpu.make_async_copy(got.at[at], got.at[at], sem.at[k]).wait()
            want = row[j * per : (j + 1) * per] + 8 * token
            chosen = jnp.where(want == spot, 1.0, 0.0).astype(BF16)
            picked = jnp.dot(chosen, got[at].reshape(8 * per, m), preferred_element_type=F32)
            p = k * per
            nat = lax.div(p, t)
            to = pl.multiple_of(lax.rem(nat, 2) * (2 * t) + lax.div(nat, 2) * t + lax.rem(p, t), per)
            rows[pl.ds(to, per), :] = picked.astype(BF16)
            pltpu.make_async_copy(rows.at[pl.ds(to, per)], out_hbm.at[pl.ds(to, per)], out_sem).start()

    loop(0, total // LANES, line)
    pltpu.make_async_copy(rows, out_hbm, out_sem).wait()


def look_up(ids, table):
    shard_rows, m = table.shape
    total = ids.size
    any_ = pl.BlockSpec(memory_space=pl.ANY)
    return pl.pallas_call(
        functools.partial(lookup_kernel, shard_rows),
        out_shape=jax.ShapeDtypeStruct((total, m), BF16),
        in_specs=[pl.BlockSpec(memory_space=pltpu.SMEM), pl.BlockSpec(memory_space=pltpu.VMEM), any_],
        out_specs=any_,
        scratch_shapes=[
            pltpu.VMEM((total, 8, m), BF16), pltpu.VMEM((total, m), BF16),
            pltpu.SemaphoreType.DMA((total // 32,)), pltpu.SemaphoreType.DMA,
        ],
        compiler_params=pltpu.CompilerParams(vmem_limit_bytes=60 << 20),
        cost_estimate=pl.CostEstimate(flops=16 * total * m, bytes_accessed=20 * total * m, transcendentals=0),
        name="look_up",
    )(ids, ids, table.reshape(shard_rows // 8, 8, m))


RING = 6


def weights_kernel(p1, p2, nk_in, dk_in, hk_in, duk_in, o1, o2, b1, b2, nk, dk, hk, duk, in_sem, out_sem, k_sem):
    m, f = b1.shape
    tw = nk.shape[0] // 2
    ins = [pltpu.make_async_copy(a, b, k_sem.at[i]) for i, (a, b) in enumerate(((nk_in, nk), (duk_in, duk), (hk_in, hk), (dk_in, dk)))]
    for cp in ins[:2]:
        cp.start()

    def part(src, buf, dst, first, i, rows=tw):
        at = pl.ds(pl.multiple_of(i * tw, 8), rows)
        fetch = pltpu.make_async_copy(src.at[at], buf.at[at], in_sem.at[first + i])
        return fetch, pltpu.make_async_copy(buf.at[at], dst.at[at], out_sem)

    def fetch_all(src, buf, dst, first):
        loop(0, src.shape[0] // tw, lambda i: part(src, buf, dst, first, i)[0].start())

    n1, n2 = m // tw, f // tw
    fetch_all(p1, b1, o1, 0)
    for cp in ins[2:]:
        cp.start()
    fetch_all(p2, b2, o2, n1)
    rest = [part(p2, b2, o2, n1, n2, f % tw)] if f % tw else []
    for come, _ in rest:
        come.start()

    def add(src, buf, dst, first, lhs, rhs, i, rows=tw):
        come, go = part(src, buf, dst, first, i, rows)
        come.wait()
        cols = pl.ds(pl.multiple_of(i * tw, tw), rows)
        buf[cols, :] += lax.dot_general(lhs[:, cols], rhs[...], TN, preferred_element_type=F32)
        go.start()

    for cp in ins[:2]:
        cp.wait()
    loop(0, n1, lambda i: add(p1, b1, o1, 0, nk, duk, i))
    for cp in ins[2:]:
        cp.wait()
    loop(0, n2, lambda i: add(p2, b2, o2, n1, hk, dk, i))
    if rest:
        add(p2, b2, o2, n1, hk, dk, n2, f % tw)
    pltpu.make_async_copy(b1, o1, out_sem).wait()
    pltpu.make_async_copy(b2, o2, out_sem).wait()


def finish_weights(p1, p2, nk, dk, hk, duk):
    any_ = pl.BlockSpec(memory_space=pl.ANY)
    V, S = pltpu.VMEM, pltpu.SemaphoreType.DMA
    arrays = (p1, p2, nk, dk, hk, duk)
    return pl.pallas_call(
        weights_kernel,
        out_shape=(jax.ShapeDtypeStruct(p1.shape, F32), jax.ShapeDtypeStruct(p2.shape, F32)),
        in_specs=[any_] * 6,
        out_specs=[any_] * 2,
        scratch_shapes=[*[V(a.shape, a.dtype) for a in arrays], S((32,)), S, S((4,))],
        compiler_params=pltpu.CompilerParams(vmem_limit_bytes=60 << 20),
        cost_estimate=pl.CostEstimate(flops=8000 * p1.size, bytes_accessed=20 * p1.size, transcendentals=0),
        name="finish_weights",
    )(*arrays)


def table_kernel(tall, key_ref, first_ref, dx_in, far_own, far_across, far_partner, far_both, out_hbm, dxb, dxf, ring, dx_sem, t_sem):
    count, _ = dxb.shape
    t = count // 16
    shift = count.bit_length() - 1
    steps = out_hbm.shape[0] // tall
    z, r = lax.axis_index("data"), lax.axis_index("tensor")
    y, c = lax.div(r, 2), lax.rem(r, 2)
    late = lax.div(z, 2)

    def near(k):
        at = pl.ds(pl.multiple_of(late * (4 * t) + k * (2 * t), t), 2 * t)
        return at, pltpu.make_async_copy(dx_in.at[at], dxb.at[at], dx_sem.at[k])

    def far(cc, yy):
        return pl.multiple_of((1 - late) * (12 * t) + cc * (2 * t) + yy * t, t)

    loop(0, 6, lambda k: near(k)[1].start())
    for src, cc, yy in ((far_own, c, y), (far_across, c, 1 - y), (far_partner, 1 - c, y), (far_both, 1 - c, 1 - y)):
        to = far(cc, yy)

        def widen_far(i, src=src, to=to):
            dxf[pl.ds(to + i, 16), :] = src[pl.ds(i, 16), :].astype(F32)

        rows_loop(t, widen_far)

    def widen_piece(at, cp):
        cp.wait()

        def widen(i):
            rows = pl.ds(pl.multiple_of(at.start + i, 16), 16)
            dxf[rows, :] = dxb[rows, :].astype(F32)

        rows_loop(at.size, widen)

    loop(0, 6, lambda k: widen_piece(*near(k)))

    def tile_out(i):
        slot = lax.rem(i, RING)
        return pltpu.make_async_copy(ring.at[slot], out_hbm.at[pl.ds(pl.multiple_of(i * tall, 8), tall)], t_sem.at[slot])

    def tile(i):
        slot = lax.rem(i, RING)
        here = ring.at[slot]
        pl.when(i >= RING)(lambda: tile_out(i - RING).wait())
        here[...] = jnp.zeros_like(here)

        def add(j, key):
            ahead = key_ref[jnp.minimum(j + 1, count - 1)]
            to = pl.ds(jnp.right_shift(key, shift) - i * tall, 1)
            here[to, :] += dxf[pl.ds(key & (count - 1), 1), :]
            return ahead

        low = first_ref[i]
        lax.fori_loop(low, first_ref[i + 1], add, key_ref[jnp.minimum(low, count - 1)])
        tile_out(i).start()

    loop(0, steps, tile)
    loop(steps - RING, steps, lambda i: tile_out(i).wait())


def table_grad(ordered, first, dx_all, fars, shard_rows, tall):
    count, m = dx_all.shape
    any_ = pl.BlockSpec(memory_space=pl.ANY)
    V, S = pltpu.VMEM, pltpu.SemaphoreType.DMA
    return pl.pallas_call(
        functools.partial(table_kernel, tall),
        out_shape=jax.ShapeDtypeStruct((shard_rows, m), F32),
        grid_spec=pltpu.PrefetchScalarGridSpec(
            num_scalar_prefetch=2,
            grid=(1,),
            in_specs=[any_, *[pl.BlockSpec(memory_space=pltpu.VMEM)] * 4],
            out_specs=any_,
            scratch_shapes=[
                V((count, m), BF16), V((count, m), F32), V((RING, tall, m), F32), S((6,)), S((RING,)),
            ],
        ),
        compiler_params=pltpu.CompilerParams(vmem_limit_bytes=44 << 20),
        cost_estimate=pl.CostEstimate(flops=16000 * shard_rows * m // 10, bytes_accessed=4 * shard_rows * m, transcendentals=0),
        name="table_grad",
    )(ordered, first, dx_all, *fars)


def solution(mesh):
    tok_spec = P(("pod", "data", "tensor"), None)

    over_y, over_core = [(0, 2), (1, 3), (2, 0), (3, 1)], [(0, 1), (1, 0), (2, 3), (3, 2)]

    def per_device(token_ids, embed_table, norm_gain, w_in, w_out, d_out):
        shard_rows = embed_table.shape[0]
        tall = next(k for k in (160, 8) if shard_rows % k == 0)
        ids = token_ids.reshape(-1, LANES)
        masked = look_up(ids, embed_table)
        gain = norm_gain.reshape(-1, LANES)
        base, ysum, ordered, first, dx_all, far, *weights = run_group(
            ids, masked, w_in, w_out, gain, d_out, shard_rows, tall
        )
        far_x = lax.ppermute(far, "tensor", over_y)
        far_p = lax.ppermute(far, "tensor", over_core)
        other = lax.ppermute(ysum, "tensor", over_y)
        grad_w_in, grad_w_out = finish_weights(*weights)
        far_b = lax.ppermute(far_x, "tensor", over_core)
        fars = (far, far_x, far_p, far_b)
        grad_table = table_grad(ordered.reshape(-1), first.reshape(-1), dx_all, fars, shard_rows, tall)
        return (base + other).astype(BF16), grad_table, grad_w_in, grad_w_out

    return jax.shard_map(
        per_device,
        mesh=mesh,
        in_specs=(P(("pod", "data")), P("tensor", None), P(None), P(None, "tensor"), P("tensor", None), tok_spec),
        out_specs=(tok_spec, P(("pod", "tensor"), None), P("pod", "tensor"), P(("pod", "tensor"), None)),
        check_vma=False,
    )
```

```python
import functools

import jax
import jax.numpy as jnp
from jax import lax
from jax.experimental import pallas as pl
from jax.experimental.pallas import tpu as pltpu
from jax.sharding import PartitionSpec as P


NORM_EPS = 1e-6
GELU_A = 0.7978845608028654
GELU_B = 0.044715
MESH = pl.DeviceIdType.MESH
NT = (((1,), (1,)), ((), ()))
TN = (((0,), (0,)), ((), ()))
F32, BF16, I32 = jnp.float32, jnp.bfloat16, jnp.int32
LANES = 128
XQ = 4
PQ = 4

R_IDS, R_DZ, R_DY, R_DC, R_NZ, R_NC, R_XZ, R_XY, R_XC = 0, 4, 8, 12, 16, 24, 28, 36, 44
R_XM, R_X, R_NO, R_PC, R_PY, R_NY, R_X2, N_R = 48, 52, 56, 60, 68, 72, 73, 74
S_IDS, S_DZ, S_DY, S_DC, S_NZ, S_NC, S_XZ, S_XY, S_XC = 0, 3, 8, 12, 16, 26, 30, 40, 48
S_XM, S_X, S_NO, S_PC, S_PY, S_NY, S_X2, N_S = 52, 56, 60, 64, 72, 76, 77, 78
L_W1, L_W2, L_XM, L_DX, L_YS, L_YB, L_DW, L_DO, L_K, N_L = 0, 1, 2, 3, 4, 5, 6, 8, 9, 13


def loop(lo, hi, body):
    def one(j, carry):
        body(j)
        return carry

    lax.fori_loop(lo, hi, one, 0)


def tiles(total, step, body):
    full = total // step
    loop(0, full, lambda j: body(pl.multiple_of(j * step, step), step))
    if total % step:
        body(full * step, total % step)


def rows_loop(total, body):
    loop(0, total // 16, lambda j: body(pl.multiple_of(j * 16, 16)))


def make_keys(ids, keys, shard_rows, rank0):
    reps, per, _ = ids.shape
    count = reps * per * LANES
    t = per * LANES // 4
    shift = t.bit_length() - 1
    lane = lax.broadcasted_iota(I32, (per, LANES), 1)
    spot = lax.broadcasted_iota(I32, (per, LANES), 0) * LANES + lane
    block = jnp.right_shift(spot, shift)
    kept = (block & 1) * (2 * t) + jnp.right_shift(block, 1) * t + (spot & (t - 1))
    for k in range(reps):
        row = ids[k] - rank0
        row = jnp.where((row >= 0) & (row < shard_rows), row, shard_rows)
        keys[k * per : (k + 1) * per, :] = (row * count + (k * per * LANES + kept)).astype(F32)


def columns(refs, b):
    same = lax.broadcasted_iota(I32, (LANES, LANES), 0) == lax.broadcasted_iota(I32, (LANES, LANES), 1)
    wide = (jnp.where(same, jnp.broadcast_to(ref[pl.ds(b, 1), :], (LANES, LANES)), 0.0) for ref in refs)
    return [jnp.sum(w, axis=1, keepdims=True) for w in wide]


def count_below(keys, place):
    lines = keys.shape[0]
    place[...] = jnp.zeros_like(place)

    def some(j):
        cols = [columns((keys,), 4 * j + u)[0] for u in range(4)]
        for a in range(lines):
            row = keys[a : a + 1, :]
            hits = sum(jnp.where(col < row, 1.0, 0.0) for col in cols)
            place[a : a + 1, :] += jnp.sum(hits, axis=0, keepdims=True)

    loop(0, lines // 4, some)


def put_in_order(keys, place, ordered, first, tall):
    lines = keys.shape[0]
    ordered[...] = jnp.zeros_like(ordered)
    first[...] = jnp.zeros_like(first)
    lane = lax.broadcasted_iota(I32, (1, LANES), 1).astype(F32)
    edge = lane * float(tall * lines * LANES)

    def some(j):
        cols = [columns((keys, place), 4 * j + u) for u in range(4)]
        for a in range(lines):
            want = lane + float(a * LANES)
            hits = sum(jnp.where(spot == want, key, 0.0) for key, spot in cols)
            ordered[a : a + 1, :] += jnp.sum(hits, axis=0, keepdims=True)
        first[...] += jnp.sum(sum(jnp.where(key < edge, 1.0, 0.0) for key, _ in cols), axis=0, keepdims=True)

    loop(0, lines // 4, some)


def group_kernel(shard_rows, tall, ids_ref, xm_hbm, w1_hbm, w2_hbm, g_ref, do_hbm,
                 base_o, ysum_o, ord_o, first_o, dx_o, far_o, dw1_o, dw2_o, nk_o, dk_o, hk_o, duk_o,
                 w1, w2, n, d, xm, xc, xy, hs, dus, pd, pf, rd, rf, yd, yb, dxo, idl, keys, place, ordered, first,
                 lsem, ssem, rsem):
    t, m = do_hbm.shape
    f = w1_hbm.shape[1]
    tq, mq = 2 * t // XQ, m // PQ
    z = lax.axis_index("data")
    r = lax.axis_index("tensor")
    y, c = lax.div(r, 2), lax.rem(r, 2)
    partner = {"tensor": 2 * y + 1 - c}
    across = {"tensor": 2 * (1 - y) + c}
    half = lax.div(z, 2)
    inner = z + half * (3 - 2 * z)
    order = [b + half * (3 - 2 * b) for b in (1 - inner, 2, 3)]
    middle, end = inner == 1, inner == 0

    def row(zz, cc, yy=0):
        return pl.multiple_of(zz * (4 * t) + cc * (2 * t) + yy * t, t)

    def blk(ref, zz, cc, yy):
        return ref.at[pl.ds(row(zz, cc, yy), t)]

    def duo(ref, zz, cc):
        return ref.at[pl.ds(row(zz, cc), 2 * t)]

    def remote(src, dst, s, q, dev):
        return pltpu.make_async_remote_copy(
            src_ref=src, dst_ref=dst, send_sem=ssem.at[s], recv_sem=rsem.at[q], device_id=dev, device_id_type=MESH
        )

    def local(src, dst, i):
        return pltpu.make_async_copy(src, dst, lsem.at[i])

    def arrived(ref, q):
        remote(ref, ref, 0, q, partner).wait_recv()

    def start(cp):
        cp.start()

    def sent(cp):
        cp.wait_send()

    def along(src, dst, s, q, act):
        for i, hop in enumerate((1, -1)):
            to = z + hop

            @pl.when((to >= 0) & (to <= 3))
            def _():
                act(remote(src, dst, s + i, q + z, {"data": to}))

    def pass_on(k, ref, s, q, act):
        src, dst = ref if isinstance(ref, tuple) else (ref, ref)
        act(remote(src, dst, s + 2 + k, q + order[k], {"data": order[1] if k == 0 else order[0]}))

    barrier = pltpu.get_barrier_semaphore()
    pl.semaphore_signal(barrier, inc=1, device_id=partner, device_id_type=MESH)
    pl.semaphore_signal(barrier, inc=1, device_id=across, device_id_type=MESH)
    for k in range(3):
        pl.semaphore_signal(barrier, inc=1, device_id={"data": order[k]}, device_id_type=MESH)

    own_d = blk(d, z, c, y)
    local(do_hbm, own_d, L_DO).start()
    local(xm_hbm, xm, L_XM).start()
    local(w1_hbm, w1, L_W1).start()
    local(w2_hbm, w2, L_W2).start()
    pl.semaphore_wait(barrier, 5)

    def piece(q):
        return pl.ds(q * tq, tq)

    for k in range(3):
        remote(ids_ref, idl.at[z], S_IDS + k, R_IDS + z, {"data": order[k]}).start()
    idl[z] = ids_ref[...]

    local(do_hbm, own_d, L_DO).wait()
    along(own_d, own_d, S_DZ, R_DZ, start)
    local(xm_hbm, xm, L_XM).wait()

    def xm_part(q):
        return remote(xm.at[pl.ds(row(0, 1 - c) + q * tq, tq)], xc.at[piece(q)], S_XM + q, R_XM + q, partner)

    def x_part(q):
        return remote(xc.at[piece(q)], xy.at[piece(q)], S_X + q, R_X + q, across)

    def d_got(k):
        arrived(blk(d, order[k], c, y), R_DZ + order[k])

    def d_on(k):
        pass_on(k, blk(d, order[k], c, y), S_DZ, R_DZ, start)

    def d_across(zz, act):
        act(remote(blk(d, zz, c, y), blk(d, zz, c, y), S_DY + zz, R_DY + zz, across))

    def d_pair(zz, act):
        act(remote(duo(d, zz, c), duo(d, zz, c), S_DC + zz, R_DC + zz, partner))

    for q in range(XQ):
        xm_part(q).start()
    for q in range(XQ):
        arrived(xc.at[piece(q)], R_XM + q)

        def join(i, q=q):
            at = pl.ds(q * tq + i, 16)
            xc[at, :] += xm[pl.ds(row(0, c) + q * tq + i, 16), :]

        rows_loop(tq, join)
        x_part(q).start()
    d_across(z, start)

    for k in range(3):
        arrived(idl.at[order[k]], R_IDS + order[k])
    make_keys(idl, keys, shard_rows, r * shard_rows)
    count_below(keys, place)
    d_got(0)

    @pl.when(middle)
    def _():
        d_on(0)
        d_got(1)
        d_on(1)

    gain = jnp.concatenate([g_ref[pl.ds(i, 1), :] for i in range(m // LANES)], axis=1).astype(F32)

    def n_own(q, act):
        at = n.at[pl.ds(row(z, c) + q * tq, tq)]
        act(remote(at, at, S_NO + q, R_NO + q, partner))

    def n_along(b, act):
        ref = blk(n, z, c, b)
        along(ref, ref, S_NZ + 5 * b, R_NZ + 4 * b, act)

    for q in range(XQ):
        arrived(xy.at[piece(q)], R_X + q)
        x_part(q).wait_send()

        def norm(i, q=q):
            at = pl.ds(q * tq + i, 16)
            x16 = xc[at, :] + xy[at, :]
            xc[at, :] = x16
            x = x16.astype(F32)
            s = lax.rsqrt(jnp.mean(x * x, axis=-1, keepdims=True) + NORM_EPS)
            n[pl.ds(row(z, c) + q * tq + i, 16), :] = ((x * s) * gain).astype(BF16)

        rows_loop(tq, norm)
        n_own(q, start)
        if q == XQ // 2 - 1:
            n_along(0, start)
            put_in_order(keys, place, ordered, first, tall)
            ord_o[...] = ordered[...].astype(I32)
            first_o[...] = first[...].astype(I32)

            @pl.when(middle)
            def _():
                d_got(2)
                d_on(2)

        if q == XQ - 1:
            n_along(1, start)
    d_across(order[0], start)

    def hidden(zz, slopes):
        at = pl.ds(row(zz, 0), 4 * t)

        def body(off, w):
            to = pl.ds(off, w)
            u = jnp.dot(n[at, :], w1[:, to], preferred_element_type=F32).astype(BF16).astype(F32)
            uu = u * u
            th = jnp.tanh(GELU_A * (u + GELU_B * (uu * u)))
            cdf = 0.5 * (1.0 + th)
            hs[at, to] = (u * cdf).astype(BF16)
            slopes[:, to] = cdf + (0.5 * GELU_A) * u * (1.0 - th * th) * (1.0 + (3.0 * GELU_B) * uu)

        tiles(f, 256, body)

    def grad_hidden(zz, slopes):
        at = pl.ds(row(zz, 0), 4 * t)

        def body(off, w):
            to = pl.ds(off, w)
            dh = lax.dot_general(d[at, :], w2[to, :], NT, preferred_element_type=F32)
            dus[at, to] = (dh * slopes[:, to]).astype(BF16)

        tiles(f, 256, body)

    for q in range(XQ):
        arrived(n.at[pl.ds(row(z, 1 - c) + q * tq, tq)], R_NO + q)
    local(w1_hbm, w1, L_W1).wait()
    hidden(z, pf)
    arrived(blk(d, z, c, 1 - y), R_DY + z)
    d_pair(z, start)
    arrived(duo(d, z, 1 - c), R_DC + z)
    local(w2_hbm, w2, L_W2).wait()
    grad_hidden(z, pf)

    own_rows = pl.ds(row(z, 0), 4 * t)
    far = pl.multiple_of((1 - y) * t, t)

    def cols(q):
        return pl.ds(pl.multiple_of(q * mq, mq), mq)

    def part_pair(src, dst, i, q):
        return remote(src.at[pl.ds(row(0, 1 - c), 2 * t), cols(q)], dst.at[:, cols(q)], S_PC + PQ * i + q, R_PC + PQ * i + q, partner)

    def part_across(q):
        return remote(rd.at[pl.ds(far, t), cols(q)], yd.at[:, cols(q)], S_PY + q, R_PY + q, across)

    def sum_part(part, got, i, q):
        arrived(got.at[:, cols(q)], R_PC + PQ * i + q)

        def add(k):
            got[pl.ds(far + k, 16), cols(q)] += part[pl.ds(row(0, c, 1 - y) + k, 16), cols(q)]

        rows_loop(t, add)

    def dn_part(q):
        pd[:, cols(q)] = lax.dot_general(dus[own_rows, :], w1[cols(q), :], NT, preferred_element_type=F32)
        part_pair(pd, rd, 0, q).start()

    def y_part(q):
        pf[:, cols(q)] = jnp.dot(hs[own_rows, :], w2[:, cols(q)], preferred_element_type=F32)
        part_pair(pf, rf, 1, q).start()

    def dn_out(q):
        sum_part(pd, rd, 0, q)
        part_across(q).start()

    loop(0, PQ, dn_part)
    loop(0, PQ, dn_out)
    loop(0, PQ, y_part)

    @pl.when(end)
    def _():
        d_got(1)

    d_across(order[1], start)

    loop(0, PQ, lambda q: sum_part(pf, rf, 1, q))
    y_send = local(rf.at[pl.ds(far, t)], ysum_o, L_YS)
    y_send.start()

    def base(i):
        own = pl.ds(y * t + i, 16)
        yb[pl.ds(i, 16), :] = xc[own, :].astype(F32) + (pf[pl.ds(row(0, c, y) + i, 16), :] + rf[own, :])

    rows_loop(t, base)
    y_keep = local(yb, base_o, L_YB)
    y_keep.start()
    for q in range(PQ):
        part_pair(pf, rf, 1, q).wait_send()

    th = t // 2

    def n_parts(k, lands):
        own, other = blk(n, order[k], c, y), blk(n, order[k], c, 1 - y)
        if lands == 2:
            other = other.at[pl.ds(0, th)]
        return (own, y), (other, 1 - y)

    def n_got(k):
        for ref, b in n_parts(k, k):
            arrived(ref, R_NZ + 4 * b + order[k])

    def n_on(k, act):
        for ref, b in n_parts(k, 1 if k == 1 else 2):
            pass_on(k, ref, S_NZ + 5 * b, R_NZ + 4 * b, act)

    def n_cross(act):
        half_own = blk(n, order[2], c, y).at[pl.ds(th, th)]
        act(remote(half_own, half_own, S_NY, R_NY, across))

    def n_pair(zz, act):
        act(remote(duo(n, zz, c), duo(n, zz, c), S_NC + zz, R_NC + zz, partner))

    n_got(0)
    n_pair(order[0], start)

    @pl.when(middle)
    def _():
        n_on(0, start)
        n_got(1)
        n_on(1, start)
        n_pair(order[1], start)

    def unit(k, slopes):
        zz = order[k]
        arrived(blk(d, zz, c, 1 - y), R_DY + zz)
        d_pair(zz, start)
        arrived(duo(n, zz, 1 - c), R_NC + zz)
        hidden(zz, slopes)
        arrived(duo(d, zz, 1 - c), R_DC + zz)
        grad_hidden(zz, slopes)

    def n_far(part, on):
        ref, b = n_parts(2, 2)[part]
        arrived(ref, R_NZ + 4 * b + order[2])
        if on:
            pass_on(2, ref, S_NZ + 5 * b, R_NZ + 4 * b, start)
        if part == 0:
            n_cross(start)

    def n_far_pair():
        arrived(blk(n, order[2], c, 1 - y).at[pl.ds(th, th)], R_NY)
        n_pair(order[2], start)

    unit(0, pf)

    for q in range(PQ):
        arrived(yd.at[:, cols(q)], R_PY + q)

    def grad_x(i):
        at, own = pl.ds(i, 16), pl.ds(y * t + i, 16)
        dn = pd[pl.ds(row(0, c, y) + i, 16), :] + rd[own, :] + yd[at, :]
        x = xc[own, :].astype(F32)
        s = lax.rsqrt(jnp.mean(x * x, axis=-1, keepdims=True) + NORM_EPS)
        xh = x * s
        dhat = dn * gain
        dxn = s * (dhat - xh * jnp.mean(dhat * xh, axis=-1, keepdims=True))
        dxo[at, :] = (d[pl.ds(row(z, c, y) + i, 16), :].astype(F32) + dxn).astype(BF16)

    rows_loop(t, grad_x)

    def dx_part(zz, yy, h, cc=c):
        return dx_o.at[pl.ds(pl.multiple_of(row(zz, cc, yy) + h * th, th), th)]

    def dx_own(h):
        return dxo.at[pl.ds(h * th, th)]

    def far_part(h):
        return far_o.at[pl.ds(h * th, th)]

    def dx_at(k, h):
        if k == 2:
            return far_part(h)
        return far_part(2) if k == 1 and h == 1 else dx_part(order[k], y, h)

    def dx_next(k, h):
        return dx_at(k, h), far_part(h) if k == 0 else dx_at(k, h)

    def dx_across(zz, src, h, act):
        act(remote(src, dx_part(zz, y, h), S_XY + 4 * h + zz, R_XY + 4 * h + zz, across))

    def dx_along(act):
        for h in range(2):
            for i, hop in enumerate((1, -1)):
                to = z + hop
                inside = middle & (to >= 1) & (to <= 2)

                def go(dst, h=h, i=i, to=to):
                    act(remote(dx_own(h), dst, S_XZ + 5 * h + i, R_XZ + 4 * h + z, {"data": to}))

                there = (to >= 0) & (to <= 3)
                if h == 0:
                    pl.when(there)(lambda go=go: go(dx_part(z, y, 0)))
                else:
                    pl.when(there & jnp.logical_not(inside))(lambda go=go: go(dx_part(z, y, 1)))
                    pl.when(inside)(lambda go=go: go(far_part(2)))

    def dx_pair(zz, act):
        act(remote(duo(dx_o, zz, c), duo(dx_o, zz, c), S_XC + zz, R_XC + zz, partner))

    def dx_got(k, on):
        zz = order[k]
        for h in range(2):
            arrived(dx_at(k, h), R_XZ + 4 * h + zz)
            if on:
                pass_on(k, dx_next(k, h), S_XZ + 5 * h, R_XZ + 4 * h, start)
            if k + h < 2 and k < 2:
                dx_across(zz, dx_part(zz, y, h), h, start)

    def dx_first(zz, act):
        for yy, s, q in ((y, S_XC + zz, R_XC + zz), (1 - y, S_X2, R_X2)):
            act(remote(dx_part(zz, yy, 0), dx_part(zz, yy, 0), s, q, partner))

    def dx_hand(zz):
        for h in range(2):
            arrived(dx_part(zz, 1 - y, h), R_XY + 4 * h + zz)
        dx_pair(zz, start)

    for h in range(2):
        dx_across(z, dx_own(h), h, start)
    local(dxo, blk(dx_o, z, c, y), L_DX).start()

    for q in range(PQ):
        part_pair(pd, rd, 0, q).wait_send()


    @pl.when(middle)
    def _():
        n_far(0, True)
        n_far(1, True)
        d_across(order[2], start)

    dx_along(start)

    @pl.when(end)
    def _():
        n_got(1)
        n_pair(order[1], start)

    unit(1, pd)

    @pl.when(end)
    def _():
        n_far(0, False)
        d_got(2)
        d_across(order[2], start)


    @pl.when(middle)
    def _():
        dx_got(0, True)
        dx_got(1, True)

    tw = 2 * t
    n1, n2 = m // tw, f // tw
    late_rows = pl.ds(row(order[2], 0), 4 * t)
    early_rows = pl.ds(pl.multiple_of(half * (4 * t), 4 * t), 12 * t)

    def flush(i, buf, dst):
        lines = pl.ds(pl.multiple_of(lax.rem(i, 2) * tw, tw), tw)
        here = buf.at[lines, pl.ds(0, dst.shape[1])]
        return here, local(here, dst.at[pl.ds(pl.multiple_of(i * tw, tw), tw)], L_DW + lax.rem(i, 2))

    def weight_tile(i, lhs, rhs, buf, dst):
        pl.when(i >= 2)(lambda: flush(i - 2, buf, dst)[1].wait())
        here, out = flush(i, buf, dst)
        at = pl.ds(pl.multiple_of(i * tw, tw), tw)
        here[...] = lax.dot_general(lhs[early_rows, at], rhs[early_rows, :], TN, preferred_element_type=F32)
        out.start()

    loop(0, n1 // 2, lambda i: weight_tile(i, n, dus, pf, dw1_o))
    pl.when(end)(lambda: n_far(1, False))
    loop(n1 // 2, n1, lambda i: weight_tile(i, n, dus, pf, dw1_o))
    for i in (n1 - 2, n1 - 1):
        flush(i, pf, dw1_o)[1].wait()
    pl.when(end)(lambda: dx_got(0, False))
    n_far_pair()
    local(dxo, blk(dx_o, z, c, y), L_DX).wait()
    dx_hand(z)
    pl.when(middle)(lambda: dx_got(2, True))
    unit(2, pd)
    pl.when(end)(lambda: dx_got(1, False))
    kept = [
        local(src.at[late_rows], dst, L_K + i)
        for i, (src, dst) in enumerate(((n, nk_o), (d, dk_o), (hs, hk_o), (dus, duk_o)))
    ]
    for cp in kept:
        cp.start()
    loop(0, n2 // 2, lambda i: weight_tile(i, hs, d, pd, dw2_o))
    dx_hand(order[0])
    loop(n2 // 2, n2, lambda i: weight_tile(i, hs, d, pd, dw2_o))
    for i in (n2 - 2, n2 - 1):
        flush(i, pd, dw2_o)[1].wait()
    if f % tw:
        rest = pd.at[pl.ds(0, f % tw)]
        rest[...] = lax.dot_general(hs[early_rows, n2 * tw :], d[early_rows, :], TN, preferred_element_type=F32)
        last = local(rest, dw2_o.at[pl.ds(n2 * tw, f % tw)], L_DW)
        last.start()
    arrived(dx_part(order[1], 1 - y, 0), R_XY + order[1])
    dx_first(order[1], start)
    pl.when(end)(lambda: dx_got(2, False))
    if f % tw:
        last.wait()
    for cp in kept:
        cp.wait()

    y_send.wait()
    y_keep.wait()
    along(own_d, own_d, S_DZ, R_DZ, sent)
    for zz in (z, *order):
        d_across(zz, sent)
        d_pair(zz, sent)
    for k in range(3):
        n_pair(order[k], sent)
        remote(ids_ref, idl.at[z], S_IDS + k, R_IDS + z, {"data": order[k]}).wait_send()
    dx_along(sent)
    for b in range(2):
        n_along(b, sent)
        dx_across(z, dx_own(b), b, sent)
        dx_across(order[b], dx_part(order[b], y, 0), 0, sent)
    dx_across(order[0], dx_part(order[0], y, 1), 1, sent)

    @pl.when(middle)
    def _():
        for k in range(3):
            pass_on(k, blk(d, order[k], c, y), S_DZ, R_DZ, sent)
            n_on(k, sent)
            for b in range(2):
                pass_on(k, dx_next(k, b), S_XZ + 5 * b, R_XZ + 4 * b, sent)

    for q in range(XQ):
        xm_part(q).wait_send()
        n_own(q, sent)
    n_cross(sent)
    for q in range(PQ):
        part_across(q).wait_send()
    for zz in (z, order[0]):
        arrived(duo(dx_o, zz, 1 - c), R_XC + zz)
        dx_pair(zz, sent)
    arrived(dx_part(order[1], y, 0, 1 - c), R_XC + order[1])
    arrived(dx_part(order[1], 1 - y, 0, 1 - c), R_X2)
    dx_first(order[1], sent)


def run_group(ids, xm, w1, w2, gain, d_out, shard_rows, tall):
    t, m = d_out.shape
    f = w1.shape[1]
    lines = 4 * ids.shape[0]
    any_, vmem = pl.BlockSpec(memory_space=pl.ANY), pl.BlockSpec(memory_space=pltpu.VMEM)
    V = pltpu.VMEM
    sds = jax.ShapeDtypeStruct
    dots = 2 * 4 * t * m * f
    return pl.pallas_call(
        functools.partial(group_kernel, shard_rows, tall),
        out_shape=(
            sds((t, m), F32), sds((t, m), F32), sds((lines, LANES), I32), sds((1, LANES), I32), sds((16 * t, m), BF16),
            sds((3 * t // 2, m), BF16), sds((m, f), F32), sds((f, m), F32),
            sds((4 * t, m), BF16), sds((4 * t, m), BF16), sds((4 * t, f), BF16), sds((4 * t, f), BF16),
        ),
        in_specs=[vmem, any_, any_, any_, vmem, any_],
        out_specs=(any_, any_, vmem, vmem, *[any_] * 8),
        scratch_shapes=[
            V((m, f), BF16), V((f, m), BF16), V((16 * t, m), BF16), V((16 * t, m), BF16),
            V((4 * t, m), BF16), V((2 * t, m), BF16), V((2 * t, m), BF16),
            V((16 * t, f), BF16), V((16 * t, f), BF16),
            V((4 * t, m), F32), V((4 * t, m), F32), V((2 * t, m), F32), V((2 * t, m), F32),
            V((t, m), F32), V((t, m), F32),
            V((t, m), BF16), V((4, *ids.shape), I32),
            V((lines, LANES), F32), V((lines, LANES), F32), V((lines, LANES), F32), V((1, LANES), F32),
            pltpu.SemaphoreType.DMA((N_L,)), pltpu.SemaphoreType.DMA((N_S,)), pltpu.SemaphoreType.DMA((N_R,)),
        ],
        compiler_params=pltpu.CompilerParams(collective_id=0, has_side_effects=True, vmem_limit_bytes=67043328),
        cost_estimate=pl.CostEstimate(flops=18 * dots, bytes_accessed=64 * 16 * t * m, transcendentals=16 * t * f),
        name="group_step",
    )(ids, xm, w1, w2, gain, d_out)


def lookup_kernel(shard_rows, ids_smem, ids_vmem, table, out_hbm, got, rows, sem, out_sem):
    total, m = out_hbm.shape
    t = total // 4
    per = 32
    chunks = total // per
    r = lax.axis_index("tensor")
    spread = (1 << (shard_rows.bit_length() - 1)) - 1

    def fetch(k):
        def some(j, carry):
            for u in range(8):
                p = k * per + j * 8 + u
                row = ids_smem[jnp.right_shift(p, 7), p & (LANES - 1)]
                near = row - r * shard_rows
                near = jnp.where((near >= 0) & (near < shard_rows), near, row & spread)
                pltpu.make_async_copy(table.at[jnp.right_shift(near, 3)], got.at[p], sem.at[k]).start()
            return carry

        lax.fori_loop(0, per // 8, some, 0)

    loop(0, chunks, fetch)
    spot = lax.broadcasted_iota(I32, (per, 8 * per), 1)
    token = lax.broadcasted_iota(I32, (per, 8 * per), 0)
    same = lax.broadcasted_iota(I32, (LANES, LANES), 0) == lax.broadcasted_iota(I32, (LANES, LANES), 1)

    def line(b):
        ids = ids_vmem[pl.ds(b, 1), :].astype(F32)
        col = jnp.sum(jnp.where(same, jnp.broadcast_to(ids, (LANES, LANES)), 0.0), axis=1, keepdims=True).astype(I32)
        row = col - r * shard_rows
        row = jnp.where((row >= 0) & (row < shard_rows), row & 7, -8 * per)
        for j in range(LANES // per):
            k = b * (LANES // per) + j
            at = pl.ds(pl.multiple_of(k * per, per), per)
            pltpu.make_async_copy(got.at[at], got.at[at], sem.at[k]).wait()
            want = row[j * per : (j + 1) * per] + 8 * token
            chosen = jnp.where(want == spot, 1.0, 0.0).astype(BF16)
            picked = jnp.dot(chosen, got[at].reshape(8 * per, m), preferred_element_type=F32)
            p = k * per
            nat = lax.div(p, t)
            to = pl.multiple_of(lax.rem(nat, 2) * (2 * t) + lax.div(nat, 2) * t + lax.rem(p, t), per)
            rows[pl.ds(to, per), :] = picked.astype(BF16)
            pltpu.make_async_copy(rows.at[pl.ds(to, per)], out_hbm.at[pl.ds(to, per)], out_sem).start()

    loop(0, total // LANES, line)
    pltpu.make_async_copy(rows, out_hbm, out_sem).wait()


def look_up(ids, table):
    shard_rows, m = table.shape
    total = ids.size
    any_ = pl.BlockSpec(memory_space=pl.ANY)
    return pl.pallas_call(
        functools.partial(lookup_kernel, shard_rows),
        out_shape=jax.ShapeDtypeStruct((total, m), BF16),
        in_specs=[pl.BlockSpec(memory_space=pltpu.SMEM), pl.BlockSpec(memory_space=pltpu.VMEM), any_],
        out_specs=any_,
        scratch_shapes=[
            pltpu.VMEM((total, 8, m), BF16), pltpu.VMEM((total, m), BF16),
            pltpu.SemaphoreType.DMA((total // 32,)), pltpu.SemaphoreType.DMA,
        ],
        compiler_params=pltpu.CompilerParams(vmem_limit_bytes=60 << 20),
        cost_estimate=pl.CostEstimate(flops=16 * total * m, bytes_accessed=20 * total * m, transcendentals=0),
        name="look_up",
    )(ids, ids, table.reshape(shard_rows // 8, 8, m))


RING = 6


def weights_kernel(p1, p2, nk_in, dk_in, hk_in, duk_in, o1, o2, b1, b2, nk, dk, hk, duk, in_sem, out_sem, k_sem):
    m, f = b1.shape
    tw = nk.shape[0] // 2
    ins = [pltpu.make_async_copy(a, b, k_sem.at[i]) for i, (a, b) in enumerate(((nk_in, nk), (duk_in, duk), (hk_in, hk), (dk_in, dk)))]
    for cp in ins[:2]:
        cp.start()

    def part(src, buf, dst, first, i, rows=tw):
        at = pl.ds(pl.multiple_of(i * tw, 8), rows)
        fetch = pltpu.make_async_copy(src.at[at], buf.at[at], in_sem.at[first + i])
        return fetch, pltpu.make_async_copy(buf.at[at], dst.at[at], out_sem)

    def fetch_all(src, buf, dst, first):
        loop(0, src.shape[0] // tw, lambda i: part(src, buf, dst, first, i)[0].start())

    n1, n2 = m // tw, f // tw
    fetch_all(p1, b1, o1, 0)
    for cp in ins[2:]:
        cp.start()
    fetch_all(p2, b2, o2, n1)
    rest = [part(p2, b2, o2, n1, n2, f % tw)] if f % tw else []
    for come, _ in rest:
        come.start()

    def add(src, buf, dst, first, lhs, rhs, i, rows=tw):
        come, go = part(src, buf, dst, first, i, rows)
        come.wait()
        cols = pl.ds(pl.multiple_of(i * tw, tw), rows)
        buf[cols, :] += lax.dot_general(lhs[:, cols], rhs[...], TN, preferred_element_type=F32)
        go.start()

    for cp in ins[:2]:
        cp.wait()
    loop(0, n1, lambda i: add(p1, b1, o1, 0, nk, duk, i))
    for cp in ins[2:]:
        cp.wait()
    loop(0, n2, lambda i: add(p2, b2, o2, n1, hk, dk, i))
    if rest:
        add(p2, b2, o2, n1, hk, dk, n2, f % tw)
    pltpu.make_async_copy(b1, o1, out_sem).wait()
    pltpu.make_async_copy(b2, o2, out_sem).wait()


def finish_weights(p1, p2, nk, dk, hk, duk):
    any_ = pl.BlockSpec(memory_space=pl.ANY)
    V, S = pltpu.VMEM, pltpu.SemaphoreType.DMA
    arrays = (p1, p2, nk, dk, hk, duk)
    return pl.pallas_call(
        weights_kernel,
        out_shape=(jax.ShapeDtypeStruct(p1.shape, F32), jax.ShapeDtypeStruct(p2.shape, F32)),
        in_specs=[any_] * 6,
        out_specs=[any_] * 2,
        scratch_shapes=[*[V(a.shape, a.dtype) for a in arrays], S((32,)), S, S((4,))],
        compiler_params=pltpu.CompilerParams(vmem_limit_bytes=60 << 20),
        cost_estimate=pl.CostEstimate(flops=8000 * p1.size, bytes_accessed=20 * p1.size, transcendentals=0),
        name="finish_weights",
    )(*arrays)


def table_kernel(tall, key_ref, first_ref, dx_in, far_own, far_across, far_partner, far_both, out_hbm, dxb, dxf, ring, dx_sem, t_sem):
    count, _ = dxb.shape
    t = count // 16
    shift = count.bit_length() - 1
    steps = out_hbm.shape[0] // tall
    z, r = lax.axis_index("data"), lax.axis_index("tensor")
    y, c = lax.div(r, 2), lax.rem(r, 2)
    late = lax.div(z, 2)

    def near(k):
        at = pl.ds(pl.multiple_of(late * (4 * t) + k * (2 * t), t), 2 * t)
        return at, pltpu.make_async_copy(dx_in.at[at], dxb.at[at], dx_sem.at[k])

    def far(cc, yy):
        return pl.multiple_of((1 - late) * (12 * t) + cc * (2 * t) + yy * t, t)

    def second(cc, yy):
        return pl.multiple_of((2 - late) * (4 * t) + cc * (2 * t) + yy * t + t // 2, t // 2)

    loop(0, 6, lambda k: near(k)[1].start())
    fars = ((far_own, c, y), (far_across, c, 1 - y), (far_partner, 1 - c, y), (far_both, 1 - c, 1 - y))

    def widen_from(src, begin, to, rows):
        def widen(i):
            dxf[pl.ds(to + i, 16), :] = src[pl.ds(begin + i, 16), :].astype(F32)

        rows_loop(rows, widen)

    for src, cc, yy in fars:
        widen_from(src, 0, far(cc, yy), t)

    def widen_piece(at, cp):
        cp.wait()

        def widen(i):
            rows = pl.ds(pl.multiple_of(at.start + i, 16), 16)
            dxf[rows, :] = dxb[rows, :].astype(F32)

        rows_loop(at.size, widen)

    loop(0, 6, lambda k: widen_piece(*near(k)))
    for src, cc, yy in fars:
        widen_from(src, t, second(cc, yy), t // 2)

    def tile_out(i):
        slot = lax.rem(i, RING)
        return pltpu.make_async_copy(ring.at[slot], out_hbm.at[pl.ds(pl.multiple_of(i * tall, 8), tall)], t_sem.at[slot])

    def tile(i):
        slot = lax.rem(i, RING)
        here = ring.at[slot]
        pl.when(i >= RING)(lambda: tile_out(i - RING).wait())
        here[...] = jnp.zeros_like(here)

        def add(j, key):
            ahead = key_ref[jnp.minimum(j + 1, count - 1)]
            to = pl.ds(jnp.right_shift(key, shift) - i * tall, 1)
            here[to, :] += dxf[pl.ds(key & (count - 1), 1), :]
            return ahead

        low = first_ref[i]
        lax.fori_loop(low, first_ref[i + 1], add, key_ref[jnp.minimum(low, count - 1)])
        tile_out(i).start()

    loop(0, steps, tile)
    loop(steps - RING, steps, lambda i: tile_out(i).wait())


def table_grad(ordered, first, dx_all, fars, shard_rows, tall):
    count, m = dx_all.shape
    any_ = pl.BlockSpec(memory_space=pl.ANY)
    V, S = pltpu.VMEM, pltpu.SemaphoreType.DMA
    return pl.pallas_call(
        functools.partial(table_kernel, tall),
        out_shape=jax.ShapeDtypeStruct((shard_rows, m), F32),
        grid_spec=pltpu.PrefetchScalarGridSpec(
            num_scalar_prefetch=2,
            grid=(1,),
            in_specs=[any_, *[pl.BlockSpec(memory_space=pltpu.VMEM)] * 4],
            out_specs=any_,
            scratch_shapes=[
                V((count, m), BF16), V((count, m), F32), V((RING, tall, m), F32), S((6,)), S((RING,)),
            ],
        ),
        compiler_params=pltpu.CompilerParams(vmem_limit_bytes=44 << 20),
        cost_estimate=pl.CostEstimate(flops=16000 * shard_rows * m // 10, bytes_accessed=4 * shard_rows * m, transcendentals=0),
        name="table_grad",
    )(ordered, first, dx_all, *fars)


def solution(mesh):
    tok_spec = P(("pod", "data", "tensor"), None)

    over_y, over_core = [(0, 2), (1, 3), (2, 0), (3, 1)], [(0, 1), (1, 0), (2, 3), (3, 2)]

    def per_device(token_ids, embed_table, norm_gain, w_in, w_out, d_out):
        shard_rows = embed_table.shape[0]
        tall = next(k for k in (160, 8) if shard_rows % k == 0)
        ids = token_ids.reshape(-1, LANES)
        masked = look_up(ids, embed_table)
        gain = norm_gain.reshape(-1, LANES)
        base, ysum, ordered, first, dx_all, far, *weights = run_group(
            ids, masked, w_in, w_out, gain, d_out, shard_rows, tall
        )
        far_x = lax.ppermute(far, "tensor", over_y)
        far_p = lax.ppermute(far, "tensor", over_core)
        other = lax.ppermute(ysum, "tensor", over_y)
        grad_w_in, grad_w_out = finish_weights(*weights)
        far_b = lax.ppermute(far_x, "tensor", over_core)
        fars = (far, far_x, far_p, far_b)
        grad_table = table_grad(ordered.reshape(-1), first.reshape(-1), dx_all, fars, shard_rows, tall)
        return (base + other).astype(BF16), grad_table, grad_w_in, grad_w_out

    return jax.shard_map(
        per_device,
        mesh=mesh,
        in_specs=(P(("pod", "data")), P("tensor", None), P(None), P(None, "tensor"), P("tensor", None), tok_spec),
        out_specs=(tok_spec, P(("pod", "tensor"), None), P("pod", "tensor"), P(("pod", "tensor"), None)),
        check_vma=False,
    )
```

```python
import functools

import jax
import jax.numpy as jnp
from jax import lax
from jax.experimental import pallas as pl
from jax.experimental.pallas import tpu as pltpu
from jax.sharding import PartitionSpec as P


NORM_EPS = 1e-6
GELU_A = 0.7978845608028654
GELU_B = 0.044715
MESH = pl.DeviceIdType.MESH
NT = (((1,), (1,)), ((), ()))
TN = (((0,), (0,)), ((), ()))
F32, BF16, I32 = jnp.float32, jnp.bfloat16, jnp.int32
LANES = 128
XQ = 4
PQ = 4

R_IDS, R_DZ, R_DY, R_DC, R_NZ, R_NC, R_XZ, R_XY, R_XC = 0, 4, 8, 12, 16, 24, 28, 36, 44
R_XM, R_X, R_NO, R_PC, R_PY, R_NY, R_X2, N_R = 48, 52, 56, 60, 68, 72, 73, 74
S_IDS, S_DZ, S_DY, S_DC, S_NZ, S_NC, S_XZ, S_XY, S_XC = 0, 3, 8, 12, 16, 26, 30, 40, 48
S_XM, S_X, S_NO, S_PC, S_PY, S_NY, S_X2, N_S = 52, 56, 60, 64, 72, 76, 77, 78
L_W1, L_W2, L_XM, L_DX, L_YS, L_YB, L_DW, L_DO, L_K, N_L = 0, 1, 2, 3, 4, 5, 6, 8, 9, 13


def loop(lo, hi, body):
    def one(j, carry):
        body(j)
        return carry

    lax.fori_loop(lo, hi, one, 0)


def tiles(total, step, body):
    full = total // step
    loop(0, full, lambda j: body(pl.multiple_of(j * step, step), step))
    if total % step:
        body(full * step, total % step)


def rows_loop(total, body):
    loop(0, total // 16, lambda j: body(pl.multiple_of(j * 16, 16)))


def make_keys(ids, keys, shard_rows, rank0):
    reps, per, _ = ids.shape
    count = reps * per * LANES
    t = per * LANES // 4
    shift = t.bit_length() - 1
    lane = lax.broadcasted_iota(I32, (per, LANES), 1)
    spot = lax.broadcasted_iota(I32, (per, LANES), 0) * LANES + lane
    block = jnp.right_shift(spot, shift)
    kept = (block & 1) * (2 * t) + jnp.right_shift(block, 1) * t + (spot & (t - 1))
    for k in range(reps):
        row = ids[k] - rank0
        row = jnp.where((row >= 0) & (row < shard_rows), row, shard_rows)
        keys[k * per : (k + 1) * per, :] = (row * count + (k * per * LANES + kept)).astype(F32)


def columns(refs, b):
    same = lax.broadcasted_iota(I32, (LANES, LANES), 0) == lax.broadcasted_iota(I32, (LANES, LANES), 1)
    wide = (jnp.where(same, jnp.broadcast_to(ref[pl.ds(b, 1), :], (LANES, LANES)), 0.0) for ref in refs)
    return [jnp.sum(w, axis=1, keepdims=True) for w in wide]


def count_below(keys, place):
    lines = keys.shape[0]
    place[...] = jnp.zeros_like(place)

    def some(j):
        cols = [columns((keys,), 4 * j + u)[0] for u in range(4)]
        for a in range(lines):
            row = keys[a : a + 1, :]
            hits = sum(jnp.where(col < row, 1.0, 0.0) for col in cols)
            place[a : a + 1, :] += jnp.sum(hits, axis=0, keepdims=True)

    loop(0, lines // 4, some)


def put_in_order(keys, place, ordered, first, tall):
    lines = keys.shape[0]
    ordered[...] = jnp.zeros_like(ordered)
    first[...] = jnp.zeros_like(first)
    lane = lax.broadcasted_iota(I32, (1, LANES), 1).astype(F32)
    edge = lane * float(tall * lines * LANES)

    def some(j):
        cols = [columns((keys, place), 4 * j + u) for u in range(4)]
        for a in range(lines):
            want = lane + float(a * LANES)
            hits = sum(jnp.where(spot == want, key, 0.0) for key, spot in cols)
            ordered[a : a + 1, :] += jnp.sum(hits, axis=0, keepdims=True)
        first[...] += jnp.sum(sum(jnp.where(key < edge, 1.0, 0.0) for key, _ in cols), axis=0, keepdims=True)

    loop(0, lines // 4, some)


def group_kernel(shard_rows, tall, ids_ref, xm_hbm, w1_hbm, w2_hbm, g_ref, do_hbm,
                 base_o, ysum_o, ord_o, first_o, dx_o, far_o, dw1_o, dw2_o, nk_o, dk_o, hk_o, duk_o,
                 w1, w2, n, d, xm, xc, xy, hs, dus, pd, pf, rd, rf, yd, yb, dxo, idl, keys, place, ordered, first,
                 lsem, ssem, rsem):
    t, m = do_hbm.shape
    f = w1_hbm.shape[1]
    tq, mq = 2 * t // XQ, m // PQ
    z = lax.axis_index("data")
    r = lax.axis_index("tensor")
    y, c = lax.div(r, 2), lax.rem(r, 2)
    partner = {"tensor": 2 * y + 1 - c}
    across = {"tensor": 2 * (1 - y) + c}
    half = lax.div(z, 2)
    inner = z + half * (3 - 2 * z)
    order = [b + half * (3 - 2 * b) for b in (1 - inner, 2, 3)]
    middle, end = inner == 1, inner == 0

    def row(zz, cc, yy=0):
        return pl.multiple_of(zz * (4 * t) + cc * (2 * t) + yy * t, t)

    def blk(ref, zz, cc, yy):
        return ref.at[pl.ds(row(zz, cc, yy), t)]

    def duo(ref, zz, cc):
        return ref.at[pl.ds(row(zz, cc), 2 * t)]

    def remote(src, dst, s, q, dev):
        return pltpu.make_async_remote_copy(
            src_ref=src, dst_ref=dst, send_sem=ssem.at[s], recv_sem=rsem.at[q], device_id=dev, device_id_type=MESH
        )

    def local(src, dst, i):
        return pltpu.make_async_copy(src, dst, lsem.at[i])

    def arrived(ref, q):
        remote(ref, ref, 0, q, partner).wait_recv()

    def start(cp):
        cp.start()

    def sent(cp):
        cp.wait_send()

    def along(src, dst, s, q, act):
        for i, hop in enumerate((1, -1)):
            to = z + hop

            @pl.when((to >= 0) & (to <= 3))
            def _():
                act(remote(src, dst, s + i, q + z, {"data": to}))

    def pass_on(k, ref, s, q, act):
        src, dst = ref if isinstance(ref, tuple) else (ref, ref)
        act(remote(src, dst, s + 2 + k, q + order[k], {"data": order[1] if k == 0 else order[0]}))

    barrier = pltpu.get_barrier_semaphore()
    pl.semaphore_signal(barrier, inc=1, device_id=partner, device_id_type=MESH)
    pl.semaphore_signal(barrier, inc=1, device_id=across, device_id_type=MESH)
    for k in range(3):
        pl.semaphore_signal(barrier, inc=1, device_id={"data": order[k]}, device_id_type=MESH)

    own_d = blk(d, z, c, y)
    local(do_hbm, own_d, L_DO).start()
    local(xm_hbm, xm, L_XM).start()
    local(w1_hbm, w1, L_W1).start()
    local(w2_hbm, w2, L_W2).start()
    pl.semaphore_wait(barrier, 5)

    def piece(q):
        return pl.ds(q * tq, tq)

    for k in range(3):
        remote(ids_ref, idl.at[z], S_IDS + k, R_IDS + z, {"data": order[k]}).start()
    idl[z] = ids_ref[...]

    local(do_hbm, own_d, L_DO).wait()
    along(own_d, own_d, S_DZ, R_DZ, start)
    local(xm_hbm, xm, L_XM).wait()

    def xm_part(q):
        return remote(xm.at[pl.ds(row(0, 1 - c) + q * tq, tq)], xc.at[piece(q)], S_XM + q, R_XM + q, partner)

    def x_part(q):
        return remote(xc.at[piece(q)], xy.at[piece(q)], S_X + q, R_X + q, across)

    def d_got(k):
        arrived(blk(d, order[k], c, y), R_DZ + order[k])

    def d_on(k):
        pass_on(k, blk(d, order[k], c, y), S_DZ, R_DZ, start)

    def d_across(zz, act):
        act(remote(blk(d, zz, c, y), blk(d, zz, c, y), S_DY + zz, R_DY + zz, across))

    def d_pair(zz, act):
        act(remote(duo(d, zz, c), duo(d, zz, c), S_DC + zz, R_DC + zz, partner))

    for q in range(XQ):
        xm_part(q).start()
    for q in range(XQ):
        arrived(xc.at[piece(q)], R_XM + q)

        def join(i, q=q):
            at = pl.ds(q * tq + i, 16)
            xc[at, :] += xm[pl.ds(row(0, c) + q * tq + i, 16), :]

        rows_loop(tq, join)
        x_part(q).start()
    d_across(z, start)

    for k in range(3):
        arrived(idl.at[order[k]], R_IDS + order[k])
    make_keys(idl, keys, shard_rows, r * shard_rows)
    count_below(keys, place)
    d_got(0)

    @pl.when(middle)
    def _():
        d_on(0)
        d_got(1)
        d_on(1)

    gain = jnp.concatenate([g_ref[pl.ds(i, 1), :] for i in range(m // LANES)], axis=1).astype(F32)

    def n_own(q, act):
        at = n.at[pl.ds(row(z, c) + q * tq, tq)]
        act(remote(at, at, S_NO + q, R_NO + q, partner))

    def n_along(b, act):
        ref = blk(n, z, c, b)
        along(ref, ref, S_NZ + 5 * b, R_NZ + 4 * b, act)

    for q in range(XQ):
        arrived(xy.at[piece(q)], R_X + q)
        x_part(q).wait_send()

        def norm(i, q=q):
            at = pl.ds(q * tq + i, 16)
            x16 = xc[at, :] + xy[at, :]
            xc[at, :] = x16
            x = x16.astype(F32)
            s = lax.rsqrt(jnp.mean(x * x, axis=-1, keepdims=True) + NORM_EPS)
            n[pl.ds(row(z, c) + q * tq + i, 16), :] = ((x * s) * gain).astype(BF16)

        rows_loop(tq, norm)
        n_own(q, start)
        if q == XQ // 2 - 1:
            n_along(0, start)
            put_in_order(keys, place, ordered, first, tall)
            ord_o[...] = ordered[...].astype(I32)
            first_o[...] = first[...].astype(I32)

            @pl.when(middle)
            def _():
                d_got(2)
                d_on(2)

        if q == XQ - 1:
            n_along(1, start)
    d_across(order[0], start)

    def hidden(zz, slopes):
        at = pl.ds(row(zz, 0), 4 * t)

        def body(off, w):
            to = pl.ds(off, w)
            u = jnp.dot(n[at, :], w1[:, to], preferred_element_type=F32).astype(BF16).astype(F32)
            uu = u * u
            th = jnp.tanh(GELU_A * (u + GELU_B * (uu * u)))
            cdf = 0.5 * (1.0 + th)
            hs[at, to] = (u * cdf).astype(BF16)
            slopes[:, to] = cdf + (0.5 * GELU_A) * u * (1.0 - th * th) * (1.0 + (3.0 * GELU_B) * uu)

        tiles(f, 256, body)

    def grad_hidden(zz, slopes):
        at = pl.ds(row(zz, 0), 4 * t)

        def body(off, w):
            to = pl.ds(off, w)
            dh = lax.dot_general(d[at, :], w2[to, :], NT, preferred_element_type=F32)
            dus[at, to] = (dh * slopes[:, to]).astype(BF16)

        tiles(f, 256, body)

    for q in range(XQ):
        arrived(n.at[pl.ds(row(z, 1 - c) + q * tq, tq)], R_NO + q)
    local(w1_hbm, w1, L_W1).wait()
    hidden(z, pf)
    arrived(blk(d, z, c, 1 - y), R_DY + z)
    d_pair(z, start)
    arrived(duo(d, z, 1 - c), R_DC + z)
    local(w2_hbm, w2, L_W2).wait()
    grad_hidden(z, pf)

    own_rows = pl.ds(row(z, 0), 4 * t)
    far = pl.multiple_of((1 - y) * t, t)

    def cols(q):
        return pl.ds(pl.multiple_of(q * mq, mq), mq)

    def part_pair(src, dst, i, q):
        return remote(src.at[pl.ds(row(0, 1 - c), 2 * t), cols(q)], dst.at[:, cols(q)], S_PC + PQ * i + q, R_PC + PQ * i + q, partner)

    def part_across(q):
        return remote(rd.at[pl.ds(far, t), cols(q)], yd.at[:, cols(q)], S_PY + q, R_PY + q, across)

    def sum_part(part, got, i, q):
        arrived(got.at[:, cols(q)], R_PC + PQ * i + q)

        def add(k):
            got[pl.ds(far + k, 16), cols(q)] += part[pl.ds(row(0, c, 1 - y) + k, 16), cols(q)]

        rows_loop(t, add)

    def dn_part(q):
        pd[:, cols(q)] = lax.dot_general(dus[own_rows, :], w1[cols(q), :], NT, preferred_element_type=F32)
        part_pair(pd, rd, 0, q).start()

    def y_part(q):
        pf[:, cols(q)] = jnp.dot(hs[own_rows, :], w2[:, cols(q)], preferred_element_type=F32)
        part_pair(pf, rf, 1, q).start()

    def dn_out(q):
        sum_part(pd, rd, 0, q)
        part_across(q).start()

    loop(0, PQ, dn_part)
    loop(0, PQ, dn_out)
    loop(0, PQ, y_part)

    @pl.when(end)
    def _():
        d_got(1)

    d_across(order[1], start)

    loop(0, PQ, lambda q: sum_part(pf, rf, 1, q))
    y_send = local(rf.at[pl.ds(far, t)], ysum_o, L_YS)
    y_send.start()

    def base(i):
        own = pl.ds(y * t + i, 16)
        yb[pl.ds(i, 16), :] = xc[own, :].astype(F32) + (pf[pl.ds(row(0, c, y) + i, 16), :] + rf[own, :])

    rows_loop(t, base)
    y_keep = local(yb, base_o, L_YB)
    y_keep.start()
    for q in range(PQ):
        part_pair(pf, rf, 1, q).wait_send()

    th = t // 2

    def n_parts(k, lands):
        own, other = blk(n, order[k], c, y), blk(n, order[k], c, 1 - y)
        if lands == 2:
            other = other.at[pl.ds(0, th)]
        return (own, y), (other, 1 - y)

    def n_got(k):
        for ref, b in n_parts(k, k):
            arrived(ref, R_NZ + 4 * b + order[k])

    def n_on(k, act):
        for ref, b in n_parts(k, 1 if k == 1 else 2):
            pass_on(k, ref, S_NZ + 5 * b, R_NZ + 4 * b, act)

    def n_cross(act):
        half_own = blk(n, order[2], c, y).at[pl.ds(th, th)]
        act(remote(half_own, half_own, S_NY, R_NY, across))

    def n_pair(zz, act):
        act(remote(duo(n, zz, c), duo(n, zz, c), S_NC + zz, R_NC + zz, partner))

    n_got(0)
    n_pair(order[0], start)

    @pl.when(middle)
    def _():
        n_on(0, start)
        n_got(1)
        n_on(1, start)
        n_pair(order[1], start)

    def unit(k, slopes, between=lambda: None):
        zz = order[k]
        arrived(blk(d, zz, c, 1 - y), R_DY + zz)
        d_pair(zz, start)
        arrived(duo(n, zz, 1 - c), R_NC + zz)
        hidden(zz, slopes)
        between()
        arrived(duo(d, zz, 1 - c), R_DC + zz)
        grad_hidden(zz, slopes)

    def n_far(part, on):
        ref, b = n_parts(2, 2)[part]
        arrived(ref, R_NZ + 4 * b + order[2])
        if on:
            pass_on(2, ref, S_NZ + 5 * b, R_NZ + 4 * b, start)
        if part == 0:
            n_cross(start)

    def n_far_pair():
        arrived(blk(n, order[2], c, 1 - y).at[pl.ds(th, th)], R_NY)
        n_pair(order[2], start)

    unit(0, pf)

    for q in range(PQ):
        arrived(yd.at[:, cols(q)], R_PY + q)

    def grad_x(i):
        at, own = pl.ds(i, 16), pl.ds(y * t + i, 16)
        dn = pd[pl.ds(row(0, c, y) + i, 16), :] + rd[own, :] + yd[at, :]
        x = xc[own, :].astype(F32)
        s = lax.rsqrt(jnp.mean(x * x, axis=-1, keepdims=True) + NORM_EPS)
        xh = x * s
        dhat = dn * gain
        dxn = s * (dhat - xh * jnp.mean(dhat * xh, axis=-1, keepdims=True))
        dxo[at, :] = (d[pl.ds(row(z, c, y) + i, 16), :].astype(F32) + dxn).astype(BF16)

    rows_loop(t, grad_x)

    def dx_part(zz, yy, h, cc=c):
        return dx_o.at[pl.ds(pl.multiple_of(row(zz, cc, yy) + h * th, th), th)]

    def dx_own(h):
        return dxo.at[pl.ds(h * th, th)]

    def far_part(h):
        return far_o.at[pl.ds(h * th, th)]

    def dx_at(k, h):
        if k == 2:
            return far_part(h)
        return far_part(2) if k == 1 and h == 1 else dx_part(order[k], y, h)

    def dx_next(k, h):
        return dx_at(k, h), far_part(h) if k == 0 else dx_at(k, h)

    def dx_across(zz, src, h, act):
        act(remote(src, dx_part(zz, y, h), S_XY + 4 * h + zz, R_XY + 4 * h + zz, across))

    def dx_along(act):
        for h in range(2):
            for i, hop in enumerate((1, -1)):
                to = z + hop
                inside = middle & (to >= 1) & (to <= 2)

                def go(dst, h=h, i=i, to=to):
                    act(remote(dx_own(h), dst, S_XZ + 5 * h + i, R_XZ + 4 * h + z, {"data": to}))

                there = (to >= 0) & (to <= 3)
                if h == 0:
                    pl.when(there)(lambda go=go: go(dx_part(z, y, 0)))
                else:
                    pl.when(there & jnp.logical_not(inside))(lambda go=go: go(dx_part(z, y, 1)))
                    pl.when(inside)(lambda go=go: go(far_part(2)))

    def dx_pair(zz, act):
        act(remote(duo(dx_o, zz, c), duo(dx_o, zz, c), S_XC + zz, R_XC + zz, partner))

    def dx_got(k, on, halves=(0, 1)):
        zz = order[k]
        for h in halves:
            arrived(dx_at(k, h), R_XZ + 4 * h + zz)
            if on:
                pass_on(k, dx_next(k, h), S_XZ + 5 * h, R_XZ + 4 * h, start)
            if k + h < 2 and k < 2:
                dx_across(zz, dx_part(zz, y, h), h, start)

    def dx_first(zz, act):
        for yy, s, q in ((y, S_XC + zz, R_XC + zz), (1 - y, S_X2, R_X2)):
            act(remote(dx_part(zz, yy, 0), dx_part(zz, yy, 0), s, q, partner))

    def dx_hand(zz):
        for h in range(2):
            arrived(dx_part(zz, 1 - y, h), R_XY + 4 * h + zz)
        dx_pair(zz, start)

    for h in range(2):
        dx_across(z, dx_own(h), h, start)
    local(dxo, blk(dx_o, z, c, y), L_DX).start()

    for q in range(PQ):
        part_pair(pd, rd, 0, q).wait_send()


    @pl.when(middle)
    def _():
        n_far(0, True)
        n_far(1, True)
        d_across(order[2], start)

    dx_along(start)

    @pl.when(end)
    def _():
        n_got(1)
        n_pair(order[1], start)

    unit(1, pd)

    @pl.when(end)
    def _():
        n_far(0, False)
        d_got(2)
        d_across(order[2], start)


    @pl.when(middle)
    def _():
        dx_got(0, True)
        dx_got(1, True)

    tw = 2 * t
    n1, n2 = m // tw, f // tw
    late_rows = pl.ds(row(order[2], 0), 4 * t)
    early_rows = pl.ds(pl.multiple_of(half * (4 * t), 4 * t), 12 * t)

    def flush(i, buf, dst):
        lines = pl.ds(pl.multiple_of(lax.rem(i, 2) * tw, tw), tw)
        here = buf.at[lines, pl.ds(0, dst.shape[1])]
        return here, local(here, dst.at[pl.ds(pl.multiple_of(i * tw, tw), tw)], L_DW + lax.rem(i, 2))

    def weight_tile(i, lhs, rhs, buf, dst):
        here, out = flush(i, buf, dst)
        at = pl.ds(pl.multiple_of(i * tw, tw), tw)
        here[...] = lax.dot_general(lhs[early_rows, at], rhs[early_rows, :], TN, preferred_element_type=F32)
        out.start()

    def dw1_tile(i):
        pl.when(i >= 2)(lambda: flush(i - 2, pf, dw1_o)[1].wait())
        weight_tile(i, n, dus, pf, dw1_o)

    def dw2_tile(i):
        pl.when(i < 2)(lambda: flush(n1 - 2 + i, pf, dw1_o)[1].wait())
        pl.when(i >= 2)(lambda: flush(i - 2, pf, dw2_o)[1].wait())
        weight_tile(i, hs, d, pf, dw2_o)

    loop(0, n1 // 2, dw1_tile)
    pl.when(end)(lambda: n_far(1, False))
    loop(n1 // 2, n1, dw1_tile)
    n_far_pair()
    local(dxo, blk(dx_o, z, c, y), L_DX).wait()
    dx_hand(z)
    loop(0, 2, dw2_tile)
    pl.when(end)(lambda: dx_got(0, False))
    pl.when(middle)(lambda: dx_got(2, True))
    loop(2, n2 - 2, dw2_tile)
    unit(2, pd, lambda: pl.when(end)(lambda: dx_got(1, False, (0,))))
    pl.when(end)(lambda: dx_got(1, False, (1,)))
    kept = [
        local(src.at[late_rows], dst, L_K + i)
        for i, (src, dst) in enumerate(((n, nk_o), (d, dk_o), (hs, hk_o), (dus, duk_o)))
    ]
    for cp in kept:
        cp.start()
    dx_hand(order[0])
    loop(n2 - 2, n2, dw2_tile)
    arrived(dx_part(order[1], 1 - y, 0), R_XY + order[1])
    dx_first(order[1], start)
    if f % tw:
        rest = pd.at[pl.ds(0, f % tw)]
        rest[...] = lax.dot_general(hs[early_rows, n2 * tw :], d[early_rows, :], TN, preferred_element_type=F32)
        last = local(rest, dw2_o.at[pl.ds(n2 * tw, f % tw)], L_DO)
        last.start()
    pl.when(end)(lambda: dx_got(2, False))
    for i in (n2 - 2, n2 - 1):
        flush(i, pf, dw2_o)[1].wait()
    if f % tw:
        last.wait()
    for cp in kept:
        cp.wait()

    y_send.wait()
    y_keep.wait()
    along(own_d, own_d, S_DZ, R_DZ, sent)
    for zz in (z, *order):
        d_across(zz, sent)
        d_pair(zz, sent)
    for k in range(3):
        n_pair(order[k], sent)
        remote(ids_ref, idl.at[z], S_IDS + k, R_IDS + z, {"data": order[k]}).wait_send()
    dx_along(sent)
    for b in range(2):
        n_along(b, sent)
        dx_across(z, dx_own(b), b, sent)
        dx_across(order[b], dx_part(order[b], y, 0), 0, sent)
    dx_across(order[0], dx_part(order[0], y, 1), 1, sent)

    @pl.when(middle)
    def _():
        for k in range(3):
            pass_on(k, blk(d, order[k], c, y), S_DZ, R_DZ, sent)
            n_on(k, sent)
            for b in range(2):
                pass_on(k, dx_next(k, b), S_XZ + 5 * b, R_XZ + 4 * b, sent)

    for q in range(XQ):
        xm_part(q).wait_send()
        n_own(q, sent)
    n_cross(sent)
    for q in range(PQ):
        part_across(q).wait_send()
    for zz in (z, order[0]):
        arrived(duo(dx_o, zz, 1 - c), R_XC + zz)
        dx_pair(zz, sent)
    arrived(dx_part(order[1], y, 0, 1 - c), R_XC + order[1])
    arrived(dx_part(order[1], 1 - y, 0, 1 - c), R_X2)
    dx_first(order[1], sent)


def run_group(ids, xm, w1, w2, gain, d_out, shard_rows, tall):
    t, m = d_out.shape
    f = w1.shape[1]
    lines = 4 * ids.shape[0]
    any_, vmem = pl.BlockSpec(memory_space=pl.ANY), pl.BlockSpec(memory_space=pltpu.VMEM)
    V = pltpu.VMEM
    sds = jax.ShapeDtypeStruct
    dots = 2 * 4 * t * m * f
    return pl.pallas_call(
        functools.partial(group_kernel, shard_rows, tall),
        out_shape=(
            sds((t, m), F32), sds((t, m), F32), sds((lines, LANES), I32), sds((1, LANES), I32), sds((16 * t, m), BF16),
            sds((3 * t // 2, m), BF16), sds((m, f), F32), sds((f, m), F32),
            sds((4 * t, m), BF16), sds((4 * t, m), BF16), sds((4 * t, f), BF16), sds((4 * t, f), BF16),
        ),
        in_specs=[vmem, any_, any_, any_, vmem, any_],
        out_specs=(any_, any_, vmem, vmem, *[any_] * 8),
        scratch_shapes=[
            V((m, f), BF16), V((f, m), BF16), V((16 * t, m), BF16), V((16 * t, m), BF16),
            V((4 * t, m), BF16), V((2 * t, m), BF16), V((2 * t, m), BF16),
            V((16 * t, f), BF16), V((16 * t, f), BF16),
            V((4 * t, m), F32), V((4 * t, m), F32), V((2 * t, m), F32), V((2 * t, m), F32),
            V((t, m), F32), V((t, m), F32),
            V((t, m), BF16), V((4, *ids.shape), I32),
            V((lines, LANES), F32), V((lines, LANES), F32), V((lines, LANES), F32), V((1, LANES), F32),
            pltpu.SemaphoreType.DMA((N_L,)), pltpu.SemaphoreType.DMA((N_S,)), pltpu.SemaphoreType.DMA((N_R,)),
        ],
        compiler_params=pltpu.CompilerParams(collective_id=0, has_side_effects=True, vmem_limit_bytes=67043328),
        cost_estimate=pl.CostEstimate(flops=18 * dots, bytes_accessed=64 * 16 * t * m, transcendentals=16 * t * f),
        name="group_step",
    )(ids, xm, w1, w2, gain, d_out)


def lookup_kernel(shard_rows, ids_smem, ids_vmem, table, out_hbm, got, rows, sem, out_sem):
    total, m = out_hbm.shape
    t = total // 4
    per = 32
    chunks = total // per
    r = lax.axis_index("tensor")
    spread = (1 << (shard_rows.bit_length() - 1)) - 1

    def fetch(k):
        def some(j, carry):
            for u in range(8):
                p = k * per + j * 8 + u
                row = ids_smem[jnp.right_shift(p, 7), p & (LANES - 1)]
                near = row - r * shard_rows
                near = jnp.where((near >= 0) & (near < shard_rows), near, row & spread)
                pltpu.make_async_copy(table.at[jnp.right_shift(near, 3)], got.at[p], sem.at[k]).start()
            return carry

        lax.fori_loop(0, per // 8, some, 0)

    loop(0, chunks, fetch)
    spot = lax.broadcasted_iota(I32, (per, 8 * per), 1)
    token = lax.broadcasted_iota(I32, (per, 8 * per), 0)
    same = lax.broadcasted_iota(I32, (LANES, LANES), 0) == lax.broadcasted_iota(I32, (LANES, LANES), 1)

    def line(b):
        ids = ids_vmem[pl.ds(b, 1), :].astype(F32)
        col = jnp.sum(jnp.where(same, jnp.broadcast_to(ids, (LANES, LANES)), 0.0), axis=1, keepdims=True).astype(I32)
        row = col - r * shard_rows
        row = jnp.where((row >= 0) & (row < shard_rows), row & 7, -8 * per)
        for j in range(LANES // per):
            k = b * (LANES // per) + j
            at = pl.ds(pl.multiple_of(k * per, per), per)
            pltpu.make_async_copy(got.at[at], got.at[at], sem.at[k]).wait()
            want = row[j * per : (j + 1) * per] + 8 * token
            chosen = jnp.where(want == spot, 1.0, 0.0).astype(BF16)
            picked = jnp.dot(chosen, got[at].reshape(8 * per, m), preferred_element_type=F32)
            p = k * per
            nat = lax.div(p, t)
            to = pl.multiple_of(lax.rem(nat, 2) * (2 * t) + lax.div(nat, 2) * t + lax.rem(p, t), per)
            rows[pl.ds(to, per), :] = picked.astype(BF16)
            pltpu.make_async_copy(rows.at[pl.ds(to, per)], out_hbm.at[pl.ds(to, per)], out_sem).start()

    loop(0, total // LANES, line)
    pltpu.make_async_copy(rows, out_hbm, out_sem).wait()


def look_up(ids, table):
    shard_rows, m = table.shape
    total = ids.size
    any_ = pl.BlockSpec(memory_space=pl.ANY)
    return pl.pallas_call(
        functools.partial(lookup_kernel, shard_rows),
        out_shape=jax.ShapeDtypeStruct((total, m), BF16),
        in_specs=[pl.BlockSpec(memory_space=pltpu.SMEM), pl.BlockSpec(memory_space=pltpu.VMEM), any_],
        out_specs=any_,
        scratch_shapes=[
            pltpu.VMEM((total, 8, m), BF16), pltpu.VMEM((total, m), BF16),
            pltpu.SemaphoreType.DMA((total // 32,)), pltpu.SemaphoreType.DMA,
        ],
        compiler_params=pltpu.CompilerParams(vmem_limit_bytes=60 << 20),
        cost_estimate=pl.CostEstimate(flops=16 * total * m, bytes_accessed=20 * total * m, transcendentals=0),
        name="look_up",
    )(ids, ids, table.reshape(shard_rows // 8, 8, m))


RING = 6


def weights_kernel(p1, p2, nk_in, dk_in, hk_in, duk_in, o1, o2, b1, b2, nk, dk, hk, duk, in_sem, out_sem, k_sem):
    m, f = b1.shape
    tw = nk.shape[0] // 2
    ins = [pltpu.make_async_copy(a, b, k_sem.at[i]) for i, (a, b) in enumerate(((nk_in, nk), (duk_in, duk), (hk_in, hk), (dk_in, dk)))]
    for cp in ins[:2]:
        cp.start()

    def part(src, buf, dst, first, i, rows=tw):
        at = pl.ds(pl.multiple_of(i * tw, 8), rows)
        fetch = pltpu.make_async_copy(src.at[at], buf.at[at], in_sem.at[first + i])
        return fetch, pltpu.make_async_copy(buf.at[at], dst.at[at], out_sem)

    def fetch_all(src, buf, dst, first):
        loop(0, src.shape[0] // tw, lambda i: part(src, buf, dst, first, i)[0].start())

    n1, n2 = m // tw, f // tw
    fetch_all(p1, b1, o1, 0)
    for cp in ins[2:]:
        cp.start()
    fetch_all(p2, b2, o2, n1)
    rest = [part(p2, b2, o2, n1, n2, f % tw)] if f % tw else []
    for come, _ in rest:
        come.start()

    def add(src, buf, dst, first, lhs, rhs, i, rows=tw):
        come, go = part(src, buf, dst, first, i, rows)
        come.wait()
        cols = pl.ds(pl.multiple_of(i * tw, tw), rows)
        buf[cols, :] += lax.dot_general(lhs[:, cols], rhs[...], TN, preferred_element_type=F32)
        go.start()

    for cp in ins[:2]:
        cp.wait()
    loop(0, n1, lambda i: add(p1, b1, o1, 0, nk, duk, i))
    for cp in ins[2:]:
        cp.wait()
    loop(0, n2, lambda i: add(p2, b2, o2, n1, hk, dk, i))
    if rest:
        add(p2, b2, o2, n1, hk, dk, n2, f % tw)
    pltpu.make_async_copy(b1, o1, out_sem).wait()
    pltpu.make_async_copy(b2, o2, out_sem).wait()


def finish_weights(p1, p2, nk, dk, hk, duk):
    any_ = pl.BlockSpec(memory_space=pl.ANY)
    V, S = pltpu.VMEM, pltpu.SemaphoreType.DMA
    arrays = (p1, p2, nk, dk, hk, duk)
    return pl.pallas_call(
        weights_kernel,
        out_shape=(jax.ShapeDtypeStruct(p1.shape, F32), jax.ShapeDtypeStruct(p2.shape, F32)),
        in_specs=[any_] * 6,
        out_specs=[any_] * 2,
        scratch_shapes=[*[V(a.shape, a.dtype) for a in arrays], S((32,)), S, S((4,))],
        compiler_params=pltpu.CompilerParams(vmem_limit_bytes=60 << 20),
        cost_estimate=pl.CostEstimate(flops=8000 * p1.size, bytes_accessed=20 * p1.size, transcendentals=0),
        name="finish_weights",
    )(*arrays)


def table_kernel(tall, key_ref, first_ref, dx_in, far_own, far_across, far_partner, far_both, out_hbm, dxb, dxf, ring, dx_sem, t_sem):
    count, _ = dxb.shape
    t = count // 16
    shift = count.bit_length() - 1
    steps = out_hbm.shape[0] // tall
    z, r = lax.axis_index("data"), lax.axis_index("tensor")
    y, c = lax.div(r, 2), lax.rem(r, 2)
    late = lax.div(z, 2)

    def near(k):
        at = pl.ds(pl.multiple_of(late * (4 * t) + k * (2 * t), t), 2 * t)
        return at, pltpu.make_async_copy(dx_in.at[at], dxb.at[at], dx_sem.at[k])

    def far(cc, yy):
        return pl.multiple_of((1 - late) * (12 * t) + cc * (2 * t) + yy * t, t)

    def second(cc, yy):
        return pl.multiple_of((2 - late) * (4 * t) + cc * (2 * t) + yy * t + t // 2, t // 2)

    loop(0, 6, lambda k: near(k)[1].start())
    fars = ((far_own, c, y), (far_across, c, 1 - y), (far_partner, 1 - c, y), (far_both, 1 - c, 1 - y))

    def widen_from(src, begin, to, rows):
        def widen(i):
            dxf[pl.ds(to + i, 16), :] = src[pl.ds(begin + i, 16), :].astype(F32)

        rows_loop(rows, widen)

    for src, cc, yy in fars:
        widen_from(src, 0, far(cc, yy), t)

    def widen_piece(at, cp):
        cp.wait()

        def widen(i):
            rows = pl.ds(pl.multiple_of(at.start + i, 16), 16)
            dxf[rows, :] = dxb[rows, :].astype(F32)

        rows_loop(at.size, widen)

    loop(0, 6, lambda k: widen_piece(*near(k)))
    for src, cc, yy in fars:
        widen_from(src, t, second(cc, yy), t // 2)

    def tile_out(i):
        slot = lax.rem(i, RING)
        return pltpu.make_async_copy(ring.at[slot], out_hbm.at[pl.ds(pl.multiple_of(i * tall, 8), tall)], t_sem.at[slot])

    def tile(i):
        slot = lax.rem(i, RING)
        here = ring.at[slot]
        pl.when(i >= RING)(lambda: tile_out(i - RING).wait())
        here[...] = jnp.zeros_like(here)

        def add(j, key):
            ahead = key_ref[jnp.minimum(j + 1, count - 1)]
            to = pl.ds(jnp.right_shift(key, shift) - i * tall, 1)
            here[to, :] += dxf[pl.ds(key & (count - 1), 1), :]
            return ahead

        low = first_ref[i]
        lax.fori_loop(low, first_ref[i + 1], add, key_ref[jnp.minimum(low, count - 1)])
        tile_out(i).start()

    loop(0, steps, tile)
    loop(steps - RING, steps, lambda i: tile_out(i).wait())


def table_grad(ordered, first, dx_all, fars, shard_rows, tall):
    count, m = dx_all.shape
    any_ = pl.BlockSpec(memory_space=pl.ANY)
    V, S = pltpu.VMEM, pltpu.SemaphoreType.DMA
    return pl.pallas_call(
        functools.partial(table_kernel, tall),
        out_shape=jax.ShapeDtypeStruct((shard_rows, m), F32),
        grid_spec=pltpu.PrefetchScalarGridSpec(
            num_scalar_prefetch=2,
            grid=(1,),
            in_specs=[any_, *[pl.BlockSpec(memory_space=pltpu.VMEM)] * 4],
            out_specs=any_,
            scratch_shapes=[
                V((count, m), BF16), V((count, m), F32), V((RING, tall, m), F32), S((6,)), S((RING,)),
            ],
        ),
        compiler_params=pltpu.CompilerParams(vmem_limit_bytes=44 << 20),
        cost_estimate=pl.CostEstimate(flops=16000 * shard_rows * m // 10, bytes_accessed=4 * shard_rows * m, transcendentals=0),
        name="table_grad",
    )(ordered, first, dx_all, *fars)


def solution(mesh):
    tok_spec = P(("pod", "data", "tensor"), None)

    over_y, over_core = [(0, 2), (1, 3), (2, 0), (3, 1)], [(0, 1), (1, 0), (2, 3), (3, 2)]

    def per_device(token_ids, embed_table, norm_gain, w_in, w_out, d_out):
        shard_rows = embed_table.shape[0]
        tall = next(k for k in (160, 8) if shard_rows % k == 0)
        ids = token_ids.reshape(-1, LANES)
        masked = look_up(ids, embed_table)
        gain = norm_gain.reshape(-1, LANES)
        base, ysum, ordered, first, dx_all, far, *weights = run_group(
            ids, masked, w_in, w_out, gain, d_out, shard_rows, tall
        )
        far_x = lax.ppermute(far, "tensor", over_y)
        far_p = lax.ppermute(far, "tensor", over_core)
        other = lax.ppermute(ysum, "tensor", over_y)
        grad_w_in, grad_w_out = finish_weights(*weights)
        far_b = lax.ppermute(far_x, "tensor", over_core)
        fars = (far, far_x, far_p, far_b)
        grad_table = table_grad(ordered.reshape(-1), first.reshape(-1), dx_all, fars, shard_rows, tall)
        return (base + other).astype(BF16), grad_table, grad_w_in, grad_w_out

    return jax.shard_map(
        per_device,
        mesh=mesh,
        in_specs=(P(("pod", "data")), P("tensor", None), P(None), P(None, "tensor"), P("tensor", None), tok_spec),
        out_specs=(tok_spec, P(("pod", "tensor"), None), P("pod", "tensor"), P(("pod", "tensor"), None)),
        check_vma=False,
    )
```

```python
import functools

import jax
import jax.numpy as jnp
from jax import lax
from jax.experimental import pallas as pl
from jax.experimental.pallas import tpu as pltpu
from jax.sharding import PartitionSpec as P


NORM_EPS = 1e-6
GELU_A = 0.7978845608028654
GELU_B = 0.044715
MESH = pl.DeviceIdType.MESH
NT = (((1,), (1,)), ((), ()))
TN = (((0,), (0,)), ((), ()))
F32, BF16, I32 = jnp.float32, jnp.bfloat16, jnp.int32
LANES = 128
XQ = 4
PQ = 4

R_IDS, R_DZ, R_DY, R_DC, R_NZ, R_NC, R_XZ, R_XY, R_XC = 0, 4, 8, 12, 16, 24, 28, 36, 44
R_XM, R_X, R_NO, R_PC, R_PY, R_NY, R_X2, N_R = 48, 52, 56, 60, 68, 72, 73, 74
S_IDS, S_DZ, S_DY, S_DC, S_NZ, S_NC, S_XZ, S_XY, S_XC = 0, 3, 8, 12, 16, 26, 30, 40, 48
S_XM, S_X, S_NO, S_PC, S_PY, S_NY, S_X2, N_S = 52, 56, 60, 64, 72, 76, 77, 78
L_W1, L_W2, L_XM, L_DX, L_YS, L_YB, L_DW, L_DO, L_K, N_L = 0, 1, 2, 3, 4, 5, 6, 8, 9, 13


def loop(lo, hi, body):
    def one(j, carry):
        body(j)
        return carry

    lax.fori_loop(lo, hi, one, 0)


def tiles(total, step, body):
    full = total // step
    loop(0, full, lambda j: body(pl.multiple_of(j * step, step), step))
    if total % step:
        body(full * step, total % step)


def rows_loop(total, body):
    loop(0, total // 16, lambda j: body(pl.multiple_of(j * 16, 16)))


def make_keys(ids, keys, shard_rows, rank0):
    reps, per, _ = ids.shape
    count = reps * per * LANES
    t = per * LANES // 4
    shift = t.bit_length() - 1
    lane = lax.broadcasted_iota(I32, (per, LANES), 1)
    spot = lax.broadcasted_iota(I32, (per, LANES), 0) * LANES + lane
    block = jnp.right_shift(spot, shift)
    kept = (block & 1) * (2 * t) + jnp.right_shift(block, 1) * t + (spot & (t - 1))
    for k in range(reps):
        row = ids[k] - rank0
        row = jnp.where((row >= 0) & (row < shard_rows), row, shard_rows)
        keys[k * per : (k + 1) * per, :] = (row * count + (k * per * LANES + kept)).astype(F32)


def columns(refs, b):
    same = lax.broadcasted_iota(I32, (LANES, LANES), 0) == lax.broadcasted_iota(I32, (LANES, LANES), 1)
    wide = (jnp.where(same, jnp.broadcast_to(ref[pl.ds(b, 1), :], (LANES, LANES)), 0.0) for ref in refs)
    return [jnp.sum(w, axis=1, keepdims=True) for w in wide]


def count_below(keys, place):
    lines = keys.shape[0]
    place[...] = jnp.zeros_like(place)

    def some(j):
        cols = [columns((keys,), 4 * j + u)[0] for u in range(4)]
        for a in range(lines):
            row = keys[a : a + 1, :]
            hits = sum(jnp.where(col < row, 1.0, 0.0) for col in cols)
            place[a : a + 1, :] += jnp.sum(hits, axis=0, keepdims=True)

    loop(0, lines // 4, some)


def put_in_order(keys, place, ordered, first, tall):
    lines = keys.shape[0]
    ordered[...] = jnp.zeros_like(ordered)
    first[...] = jnp.zeros_like(first)
    lane = lax.broadcasted_iota(I32, (1, LANES), 1).astype(F32)
    edge = lane * float(tall * lines * LANES)

    def some(j):
        cols = [columns((keys, place), 4 * j + u) for u in range(4)]
        for a in range(lines):
            want = lane + float(a * LANES)
            hits = sum(jnp.where(spot == want, key, 0.0) for key, spot in cols)
            ordered[a : a + 1, :] += jnp.sum(hits, axis=0, keepdims=True)
        first[...] += jnp.sum(sum(jnp.where(key < edge, 1.0, 0.0) for key, _ in cols), axis=0, keepdims=True)

    loop(0, lines // 4, some)


def group_kernel(shard_rows, tall, ids_ref, xm_hbm, w1_hbm, w2_hbm, g_ref, do_hbm,
                 base_o, ysum_o, ord_o, first_o, dx_o, far_o, dw1_o, dw2_o, nk_o, dk_o, hk_o, duk_o,
                 w1, w2, n, d, xm, xc, xy, hs, dus, pd, pf, rd, rf, yd, yb, dxo, idl, keys, place, ordered, first,
                 lsem, ssem, rsem):
    t, m = do_hbm.shape
    f = w1_hbm.shape[1]
    tq, mq = 2 * t // XQ, m // PQ
    z = lax.axis_index("data")
    r = lax.axis_index("tensor")
    y, c = lax.div(r, 2), lax.rem(r, 2)
    partner = {"tensor": 2 * y + 1 - c}
    across = {"tensor": 2 * (1 - y) + c}
    half = lax.div(z, 2)
    inner = z + half * (3 - 2 * z)
    order = [b + half * (3 - 2 * b) for b in (1 - inner, 2, 3)]
    middle, end = inner == 1, inner == 0

    def row(zz, cc, yy=0):
        return pl.multiple_of(zz * (4 * t) + cc * (2 * t) + yy * t, t)

    def blk(ref, zz, cc, yy):
        return ref.at[pl.ds(row(zz, cc, yy), t)]

    def duo(ref, zz, cc):
        return ref.at[pl.ds(row(zz, cc), 2 * t)]

    def remote(src, dst, s, q, dev):
        return pltpu.make_async_remote_copy(
            src_ref=src, dst_ref=dst, send_sem=ssem.at[s], recv_sem=rsem.at[q], device_id=dev, device_id_type=MESH
        )

    def local(src, dst, i):
        return pltpu.make_async_copy(src, dst, lsem.at[i])

    def arrived(ref, q):
        remote(ref, ref, 0, q, partner).wait_recv()

    def start(cp):
        cp.start()

    def sent(cp):
        cp.wait_send()

    def along(src, dst, s, q, act):
        for i, hop in enumerate((1, -1)):
            to = z + hop

            @pl.when((to >= 0) & (to <= 3))
            def _():
                act(remote(src, dst, s + i, q + z, {"data": to}))

    def pass_on(k, ref, s, q, act):
        src, dst = ref if isinstance(ref, tuple) else (ref, ref)
        act(remote(src, dst, s + 2 + k, q + order[k], {"data": order[1] if k == 0 else order[0]}))

    barrier = pltpu.get_barrier_semaphore()
    pl.semaphore_signal(barrier, inc=1, device_id=partner, device_id_type=MESH)
    pl.semaphore_signal(barrier, inc=1, device_id=across, device_id_type=MESH)
    for k in range(3):
        pl.semaphore_signal(barrier, inc=1, device_id={"data": order[k]}, device_id_type=MESH)

    own_d = blk(d, z, c, y)
    local(do_hbm, own_d, L_DO).start()
    local(xm_hbm, xm, L_XM).start()
    local(w1_hbm, w1, L_W1).start()
    local(w2_hbm, w2, L_W2).start()
    pl.semaphore_wait(barrier, 5)

    def piece(q):
        return pl.ds(q * tq, tq)

    for k in range(3):
        remote(ids_ref, idl.at[z], S_IDS + k, R_IDS + z, {"data": order[k]}).start()
    idl[z] = ids_ref[...]

    local(do_hbm, own_d, L_DO).wait()
    along(own_d, own_d, S_DZ, R_DZ, start)
    local(xm_hbm, xm, L_XM).wait()

    def xm_part(q):
        return remote(xm.at[pl.ds(row(0, 1 - c) + q * tq, tq)], xc.at[piece(q)], S_XM + q, R_XM + q, partner)

    def x_part(q):
        return remote(xc.at[piece(q)], xy.at[piece(q)], S_X + q, R_X + q, across)

    def d_got(k):
        arrived(blk(d, order[k], c, y), R_DZ + order[k])

    def d_on(k):
        pass_on(k, blk(d, order[k], c, y), S_DZ, R_DZ, start)

    def d_across(zz, act):
        act(remote(blk(d, zz, c, y), blk(d, zz, c, y), S_DY + zz, R_DY + zz, across))

    def d_pair(zz, act):
        act(remote(duo(d, zz, c), duo(d, zz, c), S_DC + zz, R_DC + zz, partner))

    for q in range(XQ):
        xm_part(q).start()
    for q in range(XQ):
        arrived(xc.at[piece(q)], R_XM + q)

        def join(i, q=q):
            at = pl.ds(q * tq + i, 16)
            xc[at, :] += xm[pl.ds(row(0, c) + q * tq + i, 16), :]

        rows_loop(tq, join)
        x_part(q).start()
    d_across(z, start)

    for k in range(3):
        arrived(idl.at[order[k]], R_IDS + order[k])
    make_keys(idl, keys, shard_rows, r * shard_rows)
    count_below(keys, place)
    d_got(0)

    @pl.when(middle)
    def _():
        d_on(0)
        d_got(1)
        d_on(1)

    gain = jnp.concatenate([g_ref[pl.ds(i, 1), :] for i in range(m // LANES)], axis=1).astype(F32)

    def n_own(q, act):
        at = n.at[pl.ds(row(z, c) + q * tq, tq)]
        act(remote(at, at, S_NO + q, R_NO + q, partner))

    def n_along(b, act):
        ref = blk(n, z, c, b)
        along(ref, ref, S_NZ + 5 * b, R_NZ + 4 * b, act)

    for q in range(XQ):
        arrived(xy.at[piece(q)], R_X + q)
        x_part(q).wait_send()

        def norm(i, q=q):
            at = pl.ds(q * tq + i, 16)
            x16 = xc[at, :] + xy[at, :]
            xc[at, :] = x16
            x = x16.astype(F32)
            s = lax.rsqrt(jnp.mean(x * x, axis=-1, keepdims=True) + NORM_EPS)
            n[pl.ds(row(z, c) + q * tq + i, 16), :] = ((x * s) * gain).astype(BF16)

        rows_loop(tq, norm)
        n_own(q, start)
        if q == XQ // 2 - 1:
            n_along(0, start)
            put_in_order(keys, place, ordered, first, tall)
            ord_o[...] = ordered[...].astype(I32)
            first_o[...] = first[...].astype(I32)

            @pl.when(middle)
            def _():
                d_got(2)
                d_on(2)

        if q == XQ - 1:
            n_along(1, start)
    d_across(order[0], start)

    def hidden(zz, slopes):
        at = pl.ds(row(zz, 0), 4 * t)

        def body(off, w):
            to = pl.ds(off, w)
            u = jnp.dot(n[at, :], w1[:, to], preferred_element_type=F32).astype(BF16).astype(F32)
            uu = u * u
            th = jnp.tanh(GELU_A * (u + GELU_B * (uu * u)))
            cdf = 0.5 * (1.0 + th)
            hs[at, to] = (u * cdf).astype(BF16)
            slopes[:, to] = cdf + (0.5 * GELU_A) * u * (1.0 - th * th) * (1.0 + (3.0 * GELU_B) * uu)

        tiles(f, 256, body)

    def grad_hidden(zz, slopes):
        at = pl.ds(row(zz, 0), 4 * t)

        def body(off, w):
            to = pl.ds(off, w)
            dh = lax.dot_general(d[at, :], w2[to, :], NT, preferred_element_type=F32)
            dus[at, to] = (dh * slopes[:, to]).astype(BF16)

        tiles(f, 256, body)

    for q in range(XQ):
        arrived(n.at[pl.ds(row(z, 1 - c) + q * tq, tq)], R_NO + q)
    local(w1_hbm, w1, L_W1).wait()
    hidden(z, pf)
    arrived(blk(d, z, c, 1 - y), R_DY + z)
    d_pair(z, start)
    arrived(duo(d, z, 1 - c), R_DC + z)
    local(w2_hbm, w2, L_W2).wait()
    grad_hidden(z, pf)

    own_rows = pl.ds(row(z, 0), 4 * t)
    far = pl.multiple_of((1 - y) * t, t)

    def cols(q):
        return pl.ds(pl.multiple_of(q * mq, mq), mq)

    def part_pair(src, dst, i, q):
        return remote(src.at[pl.ds(row(0, 1 - c), 2 * t), cols(q)], dst.at[:, cols(q)], S_PC + PQ * i + q, R_PC + PQ * i + q, partner)

    def part_across(q):
        return remote(rd.at[pl.ds(far, t), cols(q)], yd.at[:, cols(q)], S_PY + q, R_PY + q, across)

    def sum_part(part, got, i, q):
        arrived(got.at[:, cols(q)], R_PC + PQ * i + q)

        def add(k):
            got[pl.ds(far + k, 16), cols(q)] += part[pl.ds(row(0, c, 1 - y) + k, 16), cols(q)]

        rows_loop(t, add)

    def dn_part(q):
        pd[:, cols(q)] = lax.dot_general(dus[own_rows, :], w1[cols(q), :], NT, preferred_element_type=F32)
        part_pair(pd, rd, 0, q).start()

    def y_part(q):
        pf[:, cols(q)] = jnp.dot(hs[own_rows, :], w2[:, cols(q)], preferred_element_type=F32)
        part_pair(pf, rf, 1, q).start()

    def dn_out(q):
        sum_part(pd, rd, 0, q)
        part_across(q).start()

    loop(0, PQ, dn_part)
    loop(0, PQ, dn_out)
    loop(0, PQ, y_part)

    @pl.when(end)
    def _():
        d_got(1)

    d_across(order[1], start)

    loop(0, PQ, lambda q: sum_part(pf, rf, 1, q))
    y_send = local(rf.at[pl.ds(far, t)], ysum_o, L_YS)
    y_send.start()

    def base(i):
        own = pl.ds(y * t + i, 16)
        yb[pl.ds(i, 16), :] = xc[own, :].astype(F32) + (pf[pl.ds(row(0, c, y) + i, 16), :] + rf[own, :])

    rows_loop(t, base)
    y_keep = local(yb, base_o, L_YB)
    y_keep.start()
    for q in range(PQ):
        part_pair(pf, rf, 1, q).wait_send()

    th, tz = t // 2, t // 4

    def n_parts(k, lands):
        own, other = blk(n, order[k], c, y), blk(n, order[k], c, 1 - y)
        if lands == 2:
            other = other.at[pl.ds(0, tz)]
        return (own, y), (other, 1 - y)

    def n_got(k):
        for ref, b in n_parts(k, k):
            arrived(ref, R_NZ + 4 * b + order[k])

    def n_on(k, act):
        for ref, b in n_parts(k, 1 if k == 1 else 2):
            pass_on(k, ref, S_NZ + 5 * b, R_NZ + 4 * b, act)

    def n_cross(act):
        most = blk(n, order[2], c, y).at[pl.ds(tz, t - tz)]
        act(remote(most, most, S_NY, R_NY, across))

    def n_pair(zz, act):
        act(remote(duo(n, zz, c), duo(n, zz, c), S_NC + zz, R_NC + zz, partner))

    n_got(0)
    n_pair(order[0], start)

    @pl.when(middle)
    def _():
        n_on(0, start)
        n_got(1)
        n_on(1, start)
        n_pair(order[1], start)

    def unit(k, slopes, between=lambda: None):
        zz = order[k]

        def pair():
            arrived(blk(d, zz, c, 1 - y), R_DY + zz)
            d_pair(zz, start)

        if k < 2:
            pair()
        arrived(duo(n, zz, 1 - c), R_NC + zz)
        hidden(zz, slopes)
        if k == 2:
            pair()
        between()
        arrived(duo(d, zz, 1 - c), R_DC + zz)
        grad_hidden(zz, slopes)

    def n_far(part, on):
        ref, b = n_parts(2, 2)[part]
        arrived(ref, R_NZ + 4 * b + order[2])
        if on:
            pass_on(2, ref, S_NZ + 5 * b, R_NZ + 4 * b, start)
        if part == 0:
            n_cross(start)

    def n_far_pair():
        arrived(blk(n, order[2], c, 1 - y).at[pl.ds(tz, t - tz)], R_NY)
        n_pair(order[2], start)

    unit(0, pf)

    for q in range(PQ):
        arrived(yd.at[:, cols(q)], R_PY + q)

    def grad_x(i):
        at, own = pl.ds(i, 16), pl.ds(y * t + i, 16)
        dn = pd[pl.ds(row(0, c, y) + i, 16), :] + rd[own, :] + yd[at, :]
        x = xc[own, :].astype(F32)
        s = lax.rsqrt(jnp.mean(x * x, axis=-1, keepdims=True) + NORM_EPS)
        xh = x * s
        dhat = dn * gain
        dxn = s * (dhat - xh * jnp.mean(dhat * xh, axis=-1, keepdims=True))
        dxo[at, :] = (d[pl.ds(row(z, c, y) + i, 16), :].astype(F32) + dxn).astype(BF16)

    rows_loop(t, grad_x)

    def dx_part(zz, yy, h, cc=c):
        return dx_o.at[pl.ds(pl.multiple_of(row(zz, cc, yy) + h * th, th), th)]

    def dx_own(h):
        return dxo.at[pl.ds(h * th, th)]

    def far_part(h):
        return far_o.at[pl.ds(h * th, th)]

    def dx_at(k, h):
        if k == 2:
            return far_part(h)
        return far_part(2) if k == 1 and h == 1 else dx_part(order[k], y, h)

    def dx_next(k, h):
        return dx_at(k, h), far_part(h) if k == 0 else dx_at(k, h)

    def dx_across(zz, src, h, act):
        act(remote(src, dx_part(zz, y, h), S_XY + 4 * h + zz, R_XY + 4 * h + zz, across))

    def dx_along(act):
        for h in range(2):
            for i, hop in enumerate((1, -1)):
                to = z + hop
                inside = middle & (to >= 1) & (to <= 2)

                def go(dst, h=h, i=i, to=to):
                    act(remote(dx_own(h), dst, S_XZ + 5 * h + i, R_XZ + 4 * h + z, {"data": to}))

                there = (to >= 0) & (to <= 3)
                if h == 0:
                    pl.when(there)(lambda go=go: go(dx_part(z, y, 0)))
                else:
                    pl.when(there & jnp.logical_not(inside))(lambda go=go: go(dx_part(z, y, 1)))
                    pl.when(inside)(lambda go=go: go(far_part(2)))

    def dx_pair(zz, act):
        act(remote(duo(dx_o, zz, c), duo(dx_o, zz, c), S_XC + zz, R_XC + zz, partner))

    def dx_got(k, on, halves=(0, 1)):
        zz = order[k]
        for h in halves:
            arrived(dx_at(k, h), R_XZ + 4 * h + zz)
            if on:
                pass_on(k, dx_next(k, h), S_XZ + 5 * h, R_XZ + 4 * h, start)
            if k + h < 2 and k < 2:
                dx_across(zz, dx_part(zz, y, h), h, start)

    def dx_first(zz, act):
        for yy, s, q in ((y, S_XC + zz, R_XC + zz), (1 - y, S_X2, R_X2)):
            act(remote(dx_part(zz, yy, 0), dx_part(zz, yy, 0), s, q, partner))

    def dx_hand(zz):
        for h in range(2):
            arrived(dx_part(zz, 1 - y, h), R_XY + 4 * h + zz)
        dx_pair(zz, start)

    for h in range(2):
        dx_across(z, dx_own(h), h, start)
    local(dxo, blk(dx_o, z, c, y), L_DX).start()

    for q in range(PQ):
        part_pair(pd, rd, 0, q).wait_send()


    @pl.when(middle)
    def _():
        n_far(0, True)
        n_far(1, True)
        d_across(order[2], start)

    dx_along(start)

    @pl.when(end)
    def _():
        n_got(1)
        n_pair(order[1], start)

    unit(1, pd)

    @pl.when(end)
    def _():
        n_far(0, False)
        d_got(2)
        d_across(order[2], start)


    @pl.when(middle)
    def _():
        dx_got(0, True)
        dx_got(1, True)

    tw = 2 * t
    n1, n2 = m // tw, f // tw
    late_rows = pl.ds(row(order[2], 0), 4 * t)
    early_rows = pl.ds(pl.multiple_of(half * (4 * t), 4 * t), 12 * t)

    def flush(i, buf, dst):
        lines = pl.ds(pl.multiple_of(lax.rem(i, 2) * tw, tw), tw)
        here = buf.at[lines, pl.ds(0, dst.shape[1])]
        return here, local(here, dst.at[pl.ds(pl.multiple_of(i * tw, tw), tw)], L_DW + lax.rem(i, 2))

    def weight_tile(i, lhs, rhs, buf, dst):
        here, out = flush(i, buf, dst)
        at = pl.ds(pl.multiple_of(i * tw, tw), tw)
        here[...] = lax.dot_general(lhs[early_rows, at], rhs[early_rows, :], TN, preferred_element_type=F32)
        out.start()

    def dw1_tile(i):
        pl.when(i >= 2)(lambda: flush(i - 2, pf, dw1_o)[1].wait())
        weight_tile(i, n, dus, pf, dw1_o)

    def dw2_tile(i):
        pl.when(i < 2)(lambda: flush(n1 - 2 + i, pf, dw1_o)[1].wait())
        pl.when(i >= 2)(lambda: flush(i - 2, pf, dw2_o)[1].wait())
        weight_tile(i, hs, d, pf, dw2_o)

    loop(0, n1 // 2, dw1_tile)
    pl.when(end)(lambda: n_far(1, False))
    loop(n1 // 2, n1, dw1_tile)
    n_far_pair()
    local(dxo, blk(dx_o, z, c, y), L_DX).wait()
    dx_hand(z)
    loop(0, 2, dw2_tile)
    pl.when(end)(lambda: dx_got(0, False))
    pl.when(middle)(lambda: dx_got(2, True))
    loop(2, n2 - 2, dw2_tile)
    unit(2, pd, lambda: pl.when(end)(lambda: dx_got(1, False, (0,))))
    pl.when(end)(lambda: dx_got(1, False, (1,)))
    kept = [
        local(src.at[late_rows], dst, L_K + i)
        for i, (src, dst) in enumerate(((n, nk_o), (d, dk_o), (hs, hk_o), (dus, duk_o)))
    ]
    for cp in kept:
        cp.start()
    dx_hand(order[0])
    loop(n2 - 2, n2, dw2_tile)
    arrived(dx_part(order[1], 1 - y, 0), R_XY + order[1])
    dx_first(order[1], start)
    if f % tw:
        rest = pd.at[pl.ds(0, f % tw)]
        rest[...] = lax.dot_general(hs[early_rows, n2 * tw :], d[early_rows, :], TN, preferred_element_type=F32)
        last = local(rest, dw2_o.at[pl.ds(n2 * tw, f % tw)], L_DO)
        last.start()
    pl.when(end)(lambda: dx_got(2, False))
    for i in (n2 - 2, n2 - 1):
        flush(i, pf, dw2_o)[1].wait()
    if f % tw:
        last.wait()
    for cp in kept:
        cp.wait()

    y_send.wait()
    y_keep.wait()
    along(own_d, own_d, S_DZ, R_DZ, sent)
    for zz in (z, *order):
        d_across(zz, sent)
        d_pair(zz, sent)
    for k in range(3):
        n_pair(order[k], sent)
        remote(ids_ref, idl.at[z], S_IDS + k, R_IDS + z, {"data": order[k]}).wait_send()
    dx_along(sent)
    for b in range(2):
        n_along(b, sent)
        dx_across(z, dx_own(b), b, sent)
        dx_across(order[b], dx_part(order[b], y, 0), 0, sent)
    dx_across(order[0], dx_part(order[0], y, 1), 1, sent)

    @pl.when(middle)
    def _():
        for k in range(3):
            pass_on(k, blk(d, order[k], c, y), S_DZ, R_DZ, sent)
            n_on(k, sent)
            for b in range(2):
                pass_on(k, dx_next(k, b), S_XZ + 5 * b, R_XZ + 4 * b, sent)

    for q in range(XQ):
        xm_part(q).wait_send()
        n_own(q, sent)
    n_cross(sent)
    for q in range(PQ):
        part_across(q).wait_send()
    for zz in (z, order[0]):
        arrived(duo(dx_o, zz, 1 - c), R_XC + zz)
        dx_pair(zz, sent)
    arrived(dx_part(order[1], y, 0, 1 - c), R_XC + order[1])
    arrived(dx_part(order[1], 1 - y, 0, 1 - c), R_X2)
    dx_first(order[1], sent)


def run_group(ids, xm, w1, w2, gain, d_out, shard_rows, tall):
    t, m = d_out.shape
    f = w1.shape[1]
    lines = 4 * ids.shape[0]
    any_, vmem = pl.BlockSpec(memory_space=pl.ANY), pl.BlockSpec(memory_space=pltpu.VMEM)
    V = pltpu.VMEM
    sds = jax.ShapeDtypeStruct
    dots = 2 * 4 * t * m * f
    return pl.pallas_call(
        functools.partial(group_kernel, shard_rows, tall),
        out_shape=(
            sds((t, m), F32), sds((t, m), F32), sds((lines, LANES), I32), sds((1, LANES), I32), sds((16 * t, m), BF16),
            sds((3 * t // 2, m), BF16), sds((m, f), F32), sds((f, m), F32),
            sds((4 * t, m), BF16), sds((4 * t, m), BF16), sds((4 * t, f), BF16), sds((4 * t, f), BF16),
        ),
        in_specs=[vmem, any_, any_, any_, vmem, any_],
        out_specs=(any_, any_, vmem, vmem, *[any_] * 8),
        scratch_shapes=[
            V((m, f), BF16), V((f, m), BF16), V((16 * t, m), BF16), V((16 * t, m), BF16),
            V((4 * t, m), BF16), V((2 * t, m), BF16), V((2 * t, m), BF16),
            V((16 * t, f), BF16), V((16 * t, f), BF16),
            V((4 * t, m), F32), V((4 * t, m), F32), V((2 * t, m), F32), V((2 * t, m), F32),
            V((t, m), F32), V((t, m), F32),
            V((t, m), BF16), V((4, *ids.shape), I32),
            V((lines, LANES), F32), V((lines, LANES), F32), V((lines, LANES), F32), V((1, LANES), F32),
            pltpu.SemaphoreType.DMA((N_L,)), pltpu.SemaphoreType.DMA((N_S,)), pltpu.SemaphoreType.DMA((N_R,)),
        ],
        compiler_params=pltpu.CompilerParams(collective_id=0, has_side_effects=True, vmem_limit_bytes=67043328),
        cost_estimate=pl.CostEstimate(flops=18 * dots, bytes_accessed=64 * 16 * t * m, transcendentals=16 * t * f),
        name="group_step",
    )(ids, xm, w1, w2, gain, d_out)


def lookup_kernel(shard_rows, ids_smem, ids_vmem, table, out_hbm, got, rows, sem, out_sem):
    total, m = out_hbm.shape
    t = total // 4
    per = 32
    r = lax.axis_index("tensor")
    spread = (1 << (shard_rows.bit_length() - 1)) - 1

    def fetch(b):
        for u in range(LANES):
            row = ids_smem[b, u]
            near = row - r * shard_rows
            near = jnp.where((near >= 0) & (near < shard_rows), near, row & spread)
            to = got.at[b * LANES + u]
            pltpu.make_async_copy(table.at[jnp.right_shift(near, 3)], to, sem.at[b * (LANES // per) + u // per]).start()

    loop(0, total // LANES, fetch)
    spot = lax.broadcasted_iota(I32, (per, 8 * per), 1)
    token = lax.broadcasted_iota(I32, (per, 8 * per), 0)
    same = lax.broadcasted_iota(I32, (LANES, LANES), 0) == lax.broadcasted_iota(I32, (LANES, LANES), 1)

    def line(b):
        ids = ids_vmem[pl.ds(b, 1), :].astype(F32)
        col = jnp.sum(jnp.where(same, jnp.broadcast_to(ids, (LANES, LANES)), 0.0), axis=1, keepdims=True).astype(I32)
        row = col - r * shard_rows
        row = jnp.where((row >= 0) & (row < shard_rows), row & 7, -8 * per)
        for j in range(LANES // per):
            k = b * (LANES // per) + j
            at = pl.ds(pl.multiple_of(k * per, per), per)
            pltpu.make_async_copy(got.at[at], got.at[at], sem.at[k]).wait()
            want = row[j * per : (j + 1) * per] + 8 * token
            chosen = jnp.where(want == spot, 1.0, 0.0).astype(BF16)
            picked = jnp.dot(chosen, got[at].reshape(8 * per, m), preferred_element_type=F32)
            p = k * per
            nat = lax.div(p, t)
            to = pl.multiple_of(lax.rem(nat, 2) * (2 * t) + lax.div(nat, 2) * t + lax.rem(p, t), per)
            rows[pl.ds(to, per), :] = picked.astype(BF16)
            pltpu.make_async_copy(rows.at[pl.ds(to, per)], out_hbm.at[pl.ds(to, per)], out_sem).start()

    loop(0, total // LANES, line)
    pltpu.make_async_copy(rows, out_hbm, out_sem).wait()


def look_up(ids, table):
    shard_rows, m = table.shape
    total = ids.size
    any_ = pl.BlockSpec(memory_space=pl.ANY)
    return pl.pallas_call(
        functools.partial(lookup_kernel, shard_rows),
        out_shape=jax.ShapeDtypeStruct((total, m), BF16),
        in_specs=[pl.BlockSpec(memory_space=pltpu.SMEM), pl.BlockSpec(memory_space=pltpu.VMEM), any_],
        out_specs=any_,
        scratch_shapes=[
            pltpu.VMEM((total, 8, m), BF16), pltpu.VMEM((total, m), BF16),
            pltpu.SemaphoreType.DMA((total // 32,)), pltpu.SemaphoreType.DMA,
        ],
        compiler_params=pltpu.CompilerParams(vmem_limit_bytes=60 << 20),
        cost_estimate=pl.CostEstimate(flops=16 * total * m, bytes_accessed=20 * total * m, transcendentals=0),
        name="look_up",
    )(ids, ids, table.reshape(shard_rows // 8, 8, m))


RING = 6


def weights_kernel(p1, p2, nk_in, dk_in, hk_in, duk_in, o1, o2, b1, b2, nk, dk, hk, duk, in_sem, out_sem, k_sem):
    m, f = b1.shape
    tw = nk.shape[0] // 2
    ins = [pltpu.make_async_copy(a, b, k_sem.at[i]) for i, (a, b) in enumerate(((nk_in, nk), (duk_in, duk), (hk_in, hk), (dk_in, dk)))]
    for cp in ins[:2]:
        cp.start()

    def part(src, buf, dst, first, i, rows=tw):
        at = pl.ds(pl.multiple_of(i * tw, 8), rows)
        fetch = pltpu.make_async_copy(src.at[at], buf.at[at], in_sem.at[first + i])
        return fetch, pltpu.make_async_copy(buf.at[at], dst.at[at], out_sem)

    def fetch_all(src, buf, dst, first):
        loop(0, src.shape[0] // tw, lambda i: part(src, buf, dst, first, i)[0].start())

    n1, n2 = m // tw, f // tw
    fetch_all(p1, b1, o1, 0)
    for cp in ins[2:]:
        cp.start()
    fetch_all(p2, b2, o2, n1)
    rest = [part(p2, b2, o2, n1, n2, f % tw)] if f % tw else []
    for come, _ in rest:
        come.start()

    def add(src, buf, dst, first, lhs, rhs, i, rows=tw):
        come, go = part(src, buf, dst, first, i, rows)
        come.wait()
        cols = pl.ds(pl.multiple_of(i * tw, tw), rows)
        buf[cols, :] += lax.dot_general(lhs[:, cols], rhs[...], TN, preferred_element_type=F32)
        go.start()

    for cp in ins[:2]:
        cp.wait()
    loop(0, n1, lambda i: add(p1, b1, o1, 0, nk, duk, i))
    for cp in ins[2:]:
        cp.wait()
    loop(0, n2, lambda i: add(p2, b2, o2, n1, hk, dk, i))
    if rest:
        add(p2, b2, o2, n1, hk, dk, n2, f % tw)
    pltpu.make_async_copy(b1, o1, out_sem).wait()
    pltpu.make_async_copy(b2, o2, out_sem).wait()


def finish_weights(p1, p2, nk, dk, hk, duk):
    any_ = pl.BlockSpec(memory_space=pl.ANY)
    V, S = pltpu.VMEM, pltpu.SemaphoreType.DMA
    arrays = (p1, p2, nk, dk, hk, duk)
    return pl.pallas_call(
        weights_kernel,
        out_shape=(jax.ShapeDtypeStruct(p1.shape, F32), jax.ShapeDtypeStruct(p2.shape, F32)),
        in_specs=[any_] * 6,
        out_specs=[any_] * 2,
        scratch_shapes=[*[V(a.shape, a.dtype) for a in arrays], S((32,)), S, S((4,))],
        compiler_params=pltpu.CompilerParams(vmem_limit_bytes=60 << 20),
        cost_estimate=pl.CostEstimate(flops=8000 * p1.size, bytes_accessed=20 * p1.size, transcendentals=0),
        name="finish_weights",
    )(*arrays)


def table_kernel(tall, key_ref, first_ref, dx_in, far_own, far_across, far_partner, far_both, out_hbm, dxb, dxf, ring, dx_sem, t_sem):
    count, _ = dxb.shape
    t = count // 16
    shift = count.bit_length() - 1
    steps = out_hbm.shape[0] // tall
    z, r = lax.axis_index("data"), lax.axis_index("tensor")
    y, c = lax.div(r, 2), lax.rem(r, 2)
    late = lax.div(z, 2)

    def near(k):
        at = pl.ds(pl.multiple_of(late * (4 * t) + k * (2 * t), t), 2 * t)
        return at, pltpu.make_async_copy(dx_in.at[at], dxb.at[at], dx_sem.at[k])

    def far(cc, yy):
        return pl.multiple_of((1 - late) * (12 * t) + cc * (2 * t) + yy * t, t)

    def second(cc, yy):
        return pl.multiple_of((2 - late) * (4 * t) + cc * (2 * t) + yy * t + t // 2, t // 2)

    loop(0, 6, lambda k: near(k)[1].start())
    fars = ((far_own, c, y), (far_across, c, 1 - y), (far_partner, 1 - c, y), (far_both, 1 - c, 1 - y))

    def widen_from(src, begin, to, rows):
        def widen(i):
            dxf[pl.ds(to + i, 16), :] = src[pl.ds(begin + i, 16), :].astype(F32)

        rows_loop(rows, widen)

    for src, cc, yy in fars:
        widen_from(src, 0, far(cc, yy), t)

    def widen_piece(at, cp):
        cp.wait()

        def widen(i):
            rows = pl.ds(pl.multiple_of(at.start + i, 16), 16)
            dxf[rows, :] = dxb[rows, :].astype(F32)

        rows_loop(at.size, widen)

    loop(0, 6, lambda k: widen_piece(*near(k)))
    for src, cc, yy in fars:
        widen_from(src, t, second(cc, yy), t // 2)

    def tile_out(i):
        slot = lax.rem(i, RING)
        return pltpu.make_async_copy(ring.at[slot], out_hbm.at[pl.ds(pl.multiple_of(i * tall, 8), tall)], t_sem.at[slot])

    def tile(i):
        slot = lax.rem(i, RING)
        here = ring.at[slot]
        pl.when(i >= RING)(lambda: tile_out(i - RING).wait())
        here[...] = jnp.zeros_like(here)

        def add(j, key):
            ahead = key_ref[jnp.minimum(j + 1, count - 1)]
            to = pl.ds(jnp.right_shift(key, shift) - i * tall, 1)
            here[to, :] += dxf[pl.ds(key & (count - 1), 1), :]
            return ahead

        low = first_ref[i]
        lax.fori_loop(low, first_ref[i + 1], add, key_ref[jnp.minimum(low, count - 1)])
        tile_out(i).start()

    loop(0, steps, tile)
    loop(steps - RING, steps, lambda i: tile_out(i).wait())


def table_grad(ordered, first, dx_all, fars, shard_rows, tall):
    count, m = dx_all.shape
    any_ = pl.BlockSpec(memory_space=pl.ANY)
    V, S = pltpu.VMEM, pltpu.SemaphoreType.DMA
    return pl.pallas_call(
        functools.partial(table_kernel, tall),
        out_shape=jax.ShapeDtypeStruct((shard_rows, m), F32),
        grid_spec=pltpu.PrefetchScalarGridSpec(
            num_scalar_prefetch=2,
            grid=(1,),
            in_specs=[any_, *[pl.BlockSpec(memory_space=pltpu.VMEM)] * 4],
            out_specs=any_,
            scratch_shapes=[
                V((count, m), BF16), V((count, m), F32), V((RING, tall, m), F32), S((6,)), S((RING,)),
            ],
        ),
        compiler_params=pltpu.CompilerParams(vmem_limit_bytes=44 << 20),
        cost_estimate=pl.CostEstimate(flops=16000 * shard_rows * m // 10, bytes_accessed=4 * shard_rows * m, transcendentals=0),
        name="table_grad",
    )(ordered, first, dx_all, *fars)


def solution(mesh):
    tok_spec = P(("pod", "data", "tensor"), None)

    over_y, over_core = [(0, 2), (1, 3), (2, 0), (3, 1)], [(0, 1), (1, 0), (2, 3), (3, 2)]

    def per_device(token_ids, embed_table, norm_gain, w_in, w_out, d_out):
        shard_rows = embed_table.shape[0]
        tall = next(k for k in (160, 8) if shard_rows % k == 0)
        ids = token_ids.reshape(-1, LANES)
        masked = look_up(ids, embed_table)
        gain = norm_gain.reshape(-1, LANES)
        base, ysum, ordered, first, dx_all, far, *weights = run_group(
            ids, masked, w_in, w_out, gain, d_out, shard_rows, tall
        )
        far_x = lax.ppermute(far, "tensor", over_y)
        far_p = lax.ppermute(far, "tensor", over_core)
        other = lax.ppermute(ysum, "tensor", over_y)
        grad_w_in, grad_w_out = finish_weights(*weights)
        far_b = lax.ppermute(far_x, "tensor", over_core)
        fars = (far, far_x, far_p, far_b)
        grad_table = table_grad(ordered.reshape(-1), first.reshape(-1), dx_all, fars, shard_rows, tall)
        return (base + other).astype(BF16), grad_table, grad_w_in, grad_w_out

    return jax.shard_map(
        per_device,
        mesh=mesh,
        in_specs=(P(("pod", "data")), P("tensor", None), P(None), P(None, "tensor"), P("tensor", None), tok_spec),
        out_specs=(tok_spec, P(("pod", "tensor"), None), P("pod", "tensor"), P(("pod", "tensor"), None)),
        check_vma=False,
    )
```

```python
import functools

import jax
import jax.numpy as jnp
from jax import lax
from jax.experimental import pallas as pl
from jax.experimental.pallas import tpu as pltpu
from jax.sharding import PartitionSpec as P


NORM_EPS = 1e-6
GELU_A = 0.7978845608028654
GELU_B = 0.044715
MESH = pl.DeviceIdType.MESH
NT = (((1,), (1,)), ((), ()))
TN = (((0,), (0,)), ((), ()))
F32, BF16, I32 = jnp.float32, jnp.bfloat16, jnp.int32
LANES = 128
XQ = 4
PQ = 4

R_IDS, R_DZ, R_DY, R_DC, R_NZ, R_NC, R_XZ, R_XY, R_XC = 0, 4, 8, 12, 16, 24, 28, 36, 44
R_XM, R_X, R_NO, R_PC, R_PY, R_NY, R_X2, N_R = 48, 52, 56, 60, 68, 72, 73, 74
S_IDS, S_DZ, S_DY, S_DC, S_NZ, S_NC, S_XZ, S_XY, S_XC = 0, 3, 8, 12, 16, 26, 30, 40, 48
S_XM, S_X, S_NO, S_PC, S_PY, S_NY, S_X2, N_S = 52, 56, 60, 64, 72, 76, 77, 78
L_W1, L_W2, L_XM, L_DX, L_YS, L_YB, L_DW, L_DO, L_K, N_L = 0, 1, 2, 3, 4, 5, 6, 8, 9, 13


def loop(lo, hi, body):
    def one(j, carry):
        body(j)
        return carry

    lax.fori_loop(lo, hi, one, 0)


def tiles(total, step, body):
    full = total // step
    loop(0, full, lambda j: body(pl.multiple_of(j * step, step), step))
    if total % step:
        body(full * step, total % step)


def rows_loop(total, body):
    loop(0, total // 16, lambda j: body(pl.multiple_of(j * 16, 16)))


def make_keys(ids, keys, shard_rows, rank0):
    reps, per, _ = ids.shape
    count = reps * per * LANES
    t = per * LANES // 4
    shift = t.bit_length() - 1
    lane = lax.broadcasted_iota(I32, (per, LANES), 1)
    spot = lax.broadcasted_iota(I32, (per, LANES), 0) * LANES + lane
    block = jnp.right_shift(spot, shift)
    kept = (block & 1) * (2 * t) + jnp.right_shift(block, 1) * t + (spot & (t - 1))
    for k in range(reps):
        row = ids[k] - rank0
        row = jnp.where((row >= 0) & (row < shard_rows), row, shard_rows)
        keys[k * per : (k + 1) * per, :] = (row * count + (k * per * LANES + kept)).astype(F32)


def columns(refs, b):
    same = lax.broadcasted_iota(I32, (LANES, LANES), 0) == lax.broadcasted_iota(I32, (LANES, LANES), 1)
    wide = (jnp.where(same, jnp.broadcast_to(ref[pl.ds(b, 1), :], (LANES, LANES)), 0.0) for ref in refs)
    return [jnp.sum(w, axis=1, keepdims=True) for w in wide]


def count_below(keys, place):
    lines = keys.shape[0]
    place[...] = jnp.zeros_like(place)

    def some(j):
        cols = [columns((keys,), 4 * j + u)[0] for u in range(4)]
        for a in range(lines):
            row = keys[a : a + 1, :]
            hits = sum(jnp.where(col < row, 1.0, 0.0) for col in cols)
            place[a : a + 1, :] += jnp.sum(hits, axis=0, keepdims=True)

    loop(0, lines // 4, some)


def put_in_order(keys, place, ordered, first, tall):
    lines = keys.shape[0]
    ordered[...] = jnp.zeros_like(ordered)
    first[...] = jnp.zeros_like(first)
    lane = lax.broadcasted_iota(I32, (1, LANES), 1).astype(F32)
    edge = lane * float(tall * lines * LANES)

    def some(j):
        cols = [columns((keys, place), 4 * j + u) for u in range(4)]
        for a in range(lines):
            want = lane + float(a * LANES)
            hits = sum(jnp.where(spot == want, key, 0.0) for key, spot in cols)
            ordered[a : a + 1, :] += jnp.sum(hits, axis=0, keepdims=True)
        first[...] += jnp.sum(sum(jnp.where(key < edge, 1.0, 0.0) for key, _ in cols), axis=0, keepdims=True)

    loop(0, lines // 4, some)


def group_kernel(shard_rows, tall, ids_ref, xm_hbm, w1_hbm, w2_hbm, g_ref, do_hbm,
                 base_o, ysum_o, ord_o, first_o, dx_o, far_o, dw1_o, dw2_o, nk_o, dk_o, hk_o, duk_o,
                 w1, w2, n, d, xm, xc, xy, hs, dus, pd, pf, rd, rf, yd, yb, dxo, idl, keys, place, ordered, first,
                 lsem, ssem, rsem):
    t, m = do_hbm.shape
    f = w1_hbm.shape[1]
    tq, mq = 2 * t // XQ, m // PQ
    z = lax.axis_index("data")
    r = lax.axis_index("tensor")
    y, c = lax.div(r, 2), lax.rem(r, 2)
    partner = {"tensor": 2 * y + 1 - c}
    across = {"tensor": 2 * (1 - y) + c}
    half = lax.div(z, 2)
    inner = z + half * (3 - 2 * z)
    order = [b + half * (3 - 2 * b) for b in (1 - inner, 2, 3)]
    middle, end = inner == 1, inner == 0

    def row(zz, cc, yy=0):
        return pl.multiple_of(zz * (4 * t) + cc * (2 * t) + yy * t, t)

    def blk(ref, zz, cc, yy):
        return ref.at[pl.ds(row(zz, cc, yy), t)]

    def duo(ref, zz, cc):
        return ref.at[pl.ds(row(zz, cc), 2 * t)]

    def remote(src, dst, s, q, dev):
        return pltpu.make_async_remote_copy(
            src_ref=src, dst_ref=dst, send_sem=ssem.at[s], recv_sem=rsem.at[q], device_id=dev, device_id_type=MESH
        )

    def local(src, dst, i):
        return pltpu.make_async_copy(src, dst, lsem.at[i])

    def arrived(ref, q):
        remote(ref, ref, 0, q, partner).wait_recv()

    def start(cp):
        cp.start()

    def sent(cp):
        cp.wait_send()

    def along(src, dst, s, q, act):
        for i, hop in enumerate((1, -1)):
            to = z + hop

            @pl.when((to >= 0) & (to <= 3))
            def _():
                act(remote(src, dst, s + i, q + z, {"data": to}))

    def pass_on(k, ref, s, q, act):
        src, dst = ref if isinstance(ref, tuple) else (ref, ref)
        act(remote(src, dst, s + 2 + k, q + order[k], {"data": order[1] if k == 0 else order[0]}))

    barrier = pltpu.get_barrier_semaphore()
    pl.semaphore_signal(barrier, inc=1, device_id=partner, device_id_type=MESH)
    pl.semaphore_signal(barrier, inc=1, device_id=across, device_id_type=MESH)
    for k in range(3):
        pl.semaphore_signal(barrier, inc=1, device_id={"data": order[k]}, device_id_type=MESH)

    own_d = blk(d, z, c, y)
    local(do_hbm, own_d, L_DO).start()
    local(xm_hbm, xm, L_XM).start()
    local(w1_hbm, w1, L_W1).start()
    local(w2_hbm, w2, L_W2).start()
    pl.semaphore_wait(barrier, 5)

    def piece(q):
        return pl.ds(q * tq, tq)

    for k in range(3):
        remote(ids_ref, idl.at[z], S_IDS + k, R_IDS + z, {"data": order[k]}).start()
    idl[z] = ids_ref[...]

    local(do_hbm, own_d, L_DO).wait()
    along(own_d, own_d, S_DZ, R_DZ, start)
    local(xm_hbm, xm, L_XM).wait()

    def xm_part(q):
        return remote(xm.at[pl.ds(row(0, 1 - c) + q * tq, tq)], xc.at[piece(q)], S_XM + q, R_XM + q, partner)

    def x_part(q):
        return remote(xc.at[piece(q)], xy.at[piece(q)], S_X + q, R_X + q, across)

    def d_got(k):
        arrived(blk(d, order[k], c, y), R_DZ + order[k])

    def d_on(k):
        pass_on(k, blk(d, order[k], c, y), S_DZ, R_DZ, start)

    def d_across(zz, act):
        act(remote(blk(d, zz, c, y), blk(d, zz, c, y), S_DY + zz, R_DY + zz, across))

    def d_pair(zz, act):
        act(remote(duo(d, zz, c), duo(d, zz, c), S_DC + zz, R_DC + zz, partner))

    for q in range(XQ):
        xm_part(q).start()
    for q in range(XQ):
        arrived(xc.at[piece(q)], R_XM + q)

        def join(i, q=q):
            at = pl.ds(q * tq + i, 16)
            xc[at, :] += xm[pl.ds(row(0, c) + q * tq + i, 16), :]

        rows_loop(tq, join)
        x_part(q).start()
    d_across(z, start)

    for k in range(3):
        arrived(idl.at[order[k]], R_IDS + order[k])
    make_keys(idl, keys, shard_rows, r * shard_rows)
    count_below(keys, place)
    d_got(0)

    @pl.when(middle)
    def _():
        d_on(0)
        d_got(1)
        d_on(1)

    gain = jnp.concatenate([g_ref[pl.ds(i, 1), :] for i in range(m // LANES)], axis=1).astype(F32)

    def n_own(q, act):
        at = n.at[pl.ds(row(z, c) + q * tq, tq)]
        act(remote(at, at, S_NO + q, R_NO + q, partner))

    def n_along(b, act):
        ref = blk(n, z, c, b)
        along(ref, ref, S_NZ + 5 * b, R_NZ + 4 * b, act)

    for q in range(XQ):
        arrived(xy.at[piece(q)], R_X + q)
        x_part(q).wait_send()

        def norm(i, q=q):
            at = pl.ds(q * tq + i, 16)
            x16 = xc[at, :] + xy[at, :]
            xc[at, :] = x16
            x = x16.astype(F32)
            s = lax.rsqrt(jnp.mean(x * x, axis=-1, keepdims=True) + NORM_EPS)
            n[pl.ds(row(z, c) + q * tq + i, 16), :] = ((x * s) * gain).astype(BF16)

        rows_loop(tq, norm)
        n_own(q, start)
        if q == XQ // 2 - 1:
            n_along(0, start)
            put_in_order(keys, place, ordered, first, tall)
            ord_o[...] = ordered[...].astype(I32)
            first_o[...] = first[...].astype(I32)

            @pl.when(middle)
            def _():
                d_got(2)
                d_on(2)

        if q == XQ - 1:
            n_along(1, start)
    d_across(order[0], start)

    def hidden(zz, slopes):
        at = pl.ds(row(zz, 0), 4 * t)

        def body(off, w):
            to = pl.ds(off, w)
            u = jnp.dot(n[at, :], w1[:, to], preferred_element_type=F32).astype(BF16).astype(F32)
            uu = u * u
            half_th = 0.5 * jnp.tanh(u * (GELU_A + (GELU_A * GELU_B) * uu))
            cdf = 0.5 + half_th
            hs[at, to] = (u * cdf).astype(BF16)
            slopes[:, to] = cdf + (u * (cdf * (0.5 - half_th))) * (2.0 * GELU_A + (6.0 * GELU_A * GELU_B) * uu)

        tiles(f, 256, body)

    def grad_hidden(zz, slopes):
        at = pl.ds(row(zz, 0), 4 * t)

        def body(off, w):
            to = pl.ds(off, w)
            dh = lax.dot_general(d[at, :], w2[to, :], NT, preferred_element_type=F32)
            dus[at, to] = (dh * slopes[:, to]).astype(BF16)

        tiles(f, 256, body)

    for q in range(XQ):
        arrived(n.at[pl.ds(row(z, 1 - c) + q * tq, tq)], R_NO + q)
    local(w1_hbm, w1, L_W1).wait()
    hidden(z, pf)
    arrived(blk(d, z, c, 1 - y), R_DY + z)
    d_pair(z, start)
    arrived(duo(d, z, 1 - c), R_DC + z)
    local(w2_hbm, w2, L_W2).wait()
    grad_hidden(z, pf)

    own_rows = pl.ds(row(z, 0), 4 * t)
    far = pl.multiple_of((1 - y) * t, t)

    def cols(q):
        return pl.ds(pl.multiple_of(q * mq, mq), mq)

    def part_pair(src, dst, i, q):
        return remote(src.at[pl.ds(row(0, 1 - c), 2 * t), cols(q)], dst.at[:, cols(q)], S_PC + PQ * i + q, R_PC + PQ * i + q, partner)

    def part_across(q):
        return remote(rd.at[pl.ds(far, t), cols(q)], yd.at[:, cols(q)], S_PY + q, R_PY + q, across)

    def sum_part(part, got, i, q):
        arrived(got.at[:, cols(q)], R_PC + PQ * i + q)

        def add(k):
            got[pl.ds(far + k, 16), cols(q)] += part[pl.ds(row(0, c, 1 - y) + k, 16), cols(q)]

        rows_loop(t, add)

    def dn_part(q):
        pd[:, cols(q)] = lax.dot_general(dus[own_rows, :], w1[cols(q), :], NT, preferred_element_type=F32)
        part_pair(pd, rd, 0, q).start()

    def y_part(q):
        pf[:, cols(q)] = jnp.dot(hs[own_rows, :], w2[:, cols(q)], preferred_element_type=F32)
        part_pair(pf, rf, 1, q).start()

    def dn_out(q):
        sum_part(pd, rd, 0, q)
        part_across(q).start()

    loop(0, PQ, dn_part)
    loop(0, PQ, dn_out)
    loop(0, PQ, y_part)

    @pl.when(end)
    def _():
        d_got(1)

    d_across(order[1], start)

    loop(0, PQ, lambda q: sum_part(pf, rf, 1, q))
    y_send = local(rf.at[pl.ds(far, t)], ysum_o, L_YS)
    y_send.start()

    def base(i):
        own = pl.ds(y * t + i, 16)
        yb[pl.ds(i, 16), :] = xc[own, :].astype(F32) + (pf[pl.ds(row(0, c, y) + i, 16), :] + rf[own, :])

    rows_loop(t, base)
    y_keep = local(yb, base_o, L_YB)
    y_keep.start()
    for q in range(PQ):
        part_pair(pf, rf, 1, q).wait_send()

    th, tz = t // 2, 3 * t // 4

    def n_parts(k, lands):
        own, other = blk(n, order[k], c, y), blk(n, order[k], c, 1 - y)
        if lands == 2:
            other = other.at[pl.ds(0, tz)]
        return (own, y), (other, 1 - y)

    def n_got(k):
        for ref, b in n_parts(k, k):
            arrived(ref, R_NZ + 4 * b + order[k])

    def n_on(k, act):
        for ref, b in n_parts(k, 1 if k == 1 else 2):
            pass_on(k, ref, S_NZ + 5 * b, R_NZ + 4 * b, act)

    def n_cross(act):
        most = blk(n, order[2], c, y).at[pl.ds(tz, t - tz)]
        act(remote(most, most, S_NY, R_NY, across))

    def n_pair(zz, act):
        act(remote(duo(n, zz, c), duo(n, zz, c), S_NC + zz, R_NC + zz, partner))

    n_got(0)
    n_pair(order[0], start)

    @pl.when(middle)
    def _():
        n_on(0, start)
        n_got(1)
        n_on(1, start)
        n_pair(order[1], start)

    def unit(k, slopes, between=lambda: None):
        zz = order[k]
        arrived(blk(d, zz, c, 1 - y), R_DY + zz)
        d_pair(zz, start)
        arrived(duo(n, zz, 1 - c), R_NC + zz)
        hidden(zz, slopes)
        between()
        arrived(duo(d, zz, 1 - c), R_DC + zz)
        grad_hidden(zz, slopes)

    def n_far(part, on):
        ref, b = n_parts(2, 2)[part]
        arrived(ref, R_NZ + 4 * b + order[2])
        if on:
            pass_on(2, ref, S_NZ + 5 * b, R_NZ + 4 * b, start)
        if part == 0:
            n_cross(start)

    def n_far_pair():
        arrived(blk(n, order[2], c, 1 - y).at[pl.ds(tz, t - tz)], R_NY)
        n_pair(order[2], start)

    unit(0, pf)

    for q in range(PQ):
        arrived(yd.at[:, cols(q)], R_PY + q)

    def grad_x(i):
        at, own = pl.ds(i, 16), pl.ds(y * t + i, 16)
        dn = pd[pl.ds(row(0, c, y) + i, 16), :] + rd[own, :] + yd[at, :]
        x = xc[own, :].astype(F32)
        s = lax.rsqrt(jnp.mean(x * x, axis=-1, keepdims=True) + NORM_EPS)
        xh = x * s
        dhat = dn * gain
        dxn = s * (dhat - xh * jnp.mean(dhat * xh, axis=-1, keepdims=True))
        dxo[at, :] = (d[pl.ds(row(z, c, y) + i, 16), :].astype(F32) + dxn).astype(BF16)

    rows_loop(t, grad_x)

    def dx_part(zz, yy, h, cc=c):
        return dx_o.at[pl.ds(pl.multiple_of(row(zz, cc, yy) + h * th, th), th)]

    def dx_own(h):
        return dxo.at[pl.ds(h * th, th)]

    def far_part(h):
        return far_o.at[pl.ds(h * th, th)]

    def dx_at(k, h):
        if k == 2:
            return far_part(h)
        return far_part(2) if k == 1 and h == 1 else dx_part(order[k], y, h)

    def dx_next(k, h):
        return dx_at(k, h), far_part(h) if k == 0 else dx_at(k, h)

    def dx_across(zz, src, h, act):
        act(remote(src, dx_part(zz, y, h), S_XY + 4 * h + zz, R_XY + 4 * h + zz, across))

    def dx_along(act):
        for h in range(2):
            for i, hop in enumerate((1, -1)):
                to = z + hop
                inside = middle & (to >= 1) & (to <= 2)

                def go(dst, h=h, i=i, to=to):
                    act(remote(dx_own(h), dst, S_XZ + 5 * h + i, R_XZ + 4 * h + z, {"data": to}))

                there = (to >= 0) & (to <= 3)
                if h == 0:
                    pl.when(there)(lambda go=go: go(dx_part(z, y, 0)))
                else:
                    pl.when(there & jnp.logical_not(inside))(lambda go=go: go(dx_part(z, y, 1)))
                    pl.when(inside)(lambda go=go: go(far_part(2)))

    def dx_pair(zz, act):
        act(remote(duo(dx_o, zz, c), duo(dx_o, zz, c), S_XC + zz, R_XC + zz, partner))

    def dx_got(k, on, halves=(0, 1)):
        zz = order[k]
        for h in halves:
            arrived(dx_at(k, h), R_XZ + 4 * h + zz)
            if on:
                pass_on(k, dx_next(k, h), S_XZ + 5 * h, R_XZ + 4 * h, start)
            if k + h < 2 and k < 2:
                dx_across(zz, dx_part(zz, y, h), h, start)

    def dx_first(zz, act):
        for yy, s, q in ((y, S_XC + zz, R_XC + zz), (1 - y, S_X2, R_X2)):
            act(remote(dx_part(zz, yy, 0), dx_part(zz, yy, 0), s, q, partner))

    def dx_hand(zz):
        for h in range(2):
            arrived(dx_part(zz, 1 - y, h), R_XY + 4 * h + zz)
        dx_pair(zz, start)

    for h in range(2):
        dx_across(z, dx_own(h), h, start)
    local(dxo, blk(dx_o, z, c, y), L_DX).start()

    for q in range(PQ):
        part_pair(pd, rd, 0, q).wait_send()


    @pl.when(middle)
    def _():
        n_far(0, True)
        n_far(1, True)
        d_across(order[2], start)

    dx_along(start)

    @pl.when(end)
    def _():
        n_got(1)
        n_pair(order[1], start)

    unit(1, pd)

    @pl.when(end)
    def _():
        n_far(0, False)
        d_got(2)
        d_across(order[2], start)


    @pl.when(middle)
    def _():
        dx_got(0, True)
        dx_got(1, True)

    tw = 2 * t
    n1, n2 = m // tw, f // tw
    late_rows = pl.ds(row(order[2], 0), 4 * t)
    early_rows = pl.ds(pl.multiple_of(half * (4 * t), 4 * t), 12 * t)

    def flush(i, buf, dst):
        lines = pl.ds(pl.multiple_of(lax.rem(i, 2) * tw, tw), tw)
        here = buf.at[lines, pl.ds(0, dst.shape[1])]
        return here, local(here, dst.at[pl.ds(pl.multiple_of(i * tw, tw), tw)], L_DW + lax.rem(i, 2))

    def weight_tile(i, lhs, rhs, buf, dst):
        here, out = flush(i, buf, dst)
        at = pl.ds(pl.multiple_of(i * tw, tw), tw)
        here[...] = lax.dot_general(lhs[early_rows, at], rhs[early_rows, :], TN, preferred_element_type=F32)
        out.start()

    def dw1_tile(i):
        pl.when(i >= 2)(lambda: flush(i - 2, pf, dw1_o)[1].wait())
        weight_tile(i, n, dus, pf, dw1_o)

    def dw2_tile(i):
        pl.when(i < 2)(lambda: flush(n1 - 2 + i, pf, dw1_o)[1].wait())
        pl.when(i >= 2)(lambda: flush(i - 2, pf, dw2_o)[1].wait())
        weight_tile(i, hs, d, pf, dw2_o)

    loop(0, n1 // 2, dw1_tile)
    pl.when(end)(lambda: n_far(1, False))
    loop(n1 // 2, n1, dw1_tile)
    n_far_pair()
    local(dxo, blk(dx_o, z, c, y), L_DX).wait()
    dx_hand(z)
    loop(0, 2, dw2_tile)
    pl.when(end)(lambda: dx_got(0, False))
    pl.when(middle)(lambda: dx_got(2, True))
    loop(2, n2 - 2, dw2_tile)
    unit(2, pd, lambda: pl.when(end)(lambda: dx_got(1, False, (0,))))
    pl.when(end)(lambda: dx_got(1, False, (1,)))
    kept = [
        local(src.at[late_rows], dst, L_K + i)
        for i, (src, dst) in enumerate(((n, nk_o), (d, dk_o), (hs, hk_o), (dus, duk_o)))
    ]
    for cp in kept:
        cp.start()
    dx_hand(order[0])
    loop(n2 - 2, n2, dw2_tile)
    arrived(dx_part(order[1], 1 - y, 0), R_XY + order[1])
    dx_first(order[1], start)
    if f % tw:
        rest = pd.at[pl.ds(0, f % tw)]
        rest[...] = lax.dot_general(hs[early_rows, n2 * tw :], d[early_rows, :], TN, preferred_element_type=F32)
        last = local(rest, dw2_o.at[pl.ds(n2 * tw, f % tw)], L_DO)
        last.start()
    pl.when(end)(lambda: dx_got(2, False))
    for i in (n2 - 2, n2 - 1):
        flush(i, pf, dw2_o)[1].wait()
    if f % tw:
        last.wait()
    for cp in kept:
        cp.wait()

    y_send.wait()
    y_keep.wait()
    along(own_d, own_d, S_DZ, R_DZ, sent)
    for zz in (z, *order):
        d_across(zz, sent)
        d_pair(zz, sent)
    for k in range(3):
        n_pair(order[k], sent)
        remote(ids_ref, idl.at[z], S_IDS + k, R_IDS + z, {"data": order[k]}).wait_send()
    dx_along(sent)
    for b in range(2):
        n_along(b, sent)
        dx_across(z, dx_own(b), b, sent)
        dx_across(order[b], dx_part(order[b], y, 0), 0, sent)
    dx_across(order[0], dx_part(order[0], y, 1), 1, sent)

    @pl.when(middle)
    def _():
        for k in range(3):
            pass_on(k, blk(d, order[k], c, y), S_DZ, R_DZ, sent)
            n_on(k, sent)
            for b in range(2):
                pass_on(k, dx_next(k, b), S_XZ + 5 * b, R_XZ + 4 * b, sent)

    for q in range(XQ):
        xm_part(q).wait_send()
        n_own(q, sent)
    n_cross(sent)
    for q in range(PQ):
        part_across(q).wait_send()
    for zz in (z, order[0]):
        arrived(duo(dx_o, zz, 1 - c), R_XC + zz)
        dx_pair(zz, sent)
    arrived(dx_part(order[1], y, 0, 1 - c), R_XC + order[1])
    arrived(dx_part(order[1], 1 - y, 0, 1 - c), R_X2)
    dx_first(order[1], sent)


def run_group(ids, xm, w1, w2, gain, d_out, shard_rows, tall):
    t, m = d_out.shape
    f = w1.shape[1]
    lines = 4 * ids.shape[0]
    any_, vmem = pl.BlockSpec(memory_space=pl.ANY), pl.BlockSpec(memory_space=pltpu.VMEM)
    V = pltpu.VMEM
    sds = jax.ShapeDtypeStruct
    dots = 2 * 4 * t * m * f
    return pl.pallas_call(
        functools.partial(group_kernel, shard_rows, tall),
        out_shape=(
            sds((t, m), F32), sds((t, m), F32), sds((lines, LANES), I32), sds((1, LANES), I32), sds((16 * t, m), BF16),
            sds((3 * t // 2, m), BF16), sds((m, f), F32), sds((f, m), F32),
            sds((4 * t, m), BF16), sds((4 * t, m), BF16), sds((4 * t, f), BF16), sds((4 * t, f), BF16),
        ),
        in_specs=[vmem, any_, any_, any_, vmem, any_],
        out_specs=(any_, any_, vmem, vmem, *[any_] * 8),
        scratch_shapes=[
            V((m, f), BF16), V((f, m), BF16), V((16 * t, m), BF16), V((16 * t, m), BF16),
            V((4 * t, m), BF16), V((2 * t, m), BF16), V((2 * t, m), BF16),
            V((16 * t, f), BF16), V((16 * t, f), BF16),
            V((4 * t, m), F32), V((4 * t, m), F32), V((2 * t, m), F32), V((2 * t, m), F32),
            V((t, m), F32), V((t, m), F32),
            V((t, m), BF16), V((4, *ids.shape), I32),
            V((lines, LANES), F32), V((lines, LANES), F32), V((lines, LANES), F32), V((1, LANES), F32),
            pltpu.SemaphoreType.DMA((N_L,)), pltpu.SemaphoreType.DMA((N_S,)), pltpu.SemaphoreType.DMA((N_R,)),
        ],
        compiler_params=pltpu.CompilerParams(collective_id=0, has_side_effects=True, vmem_limit_bytes=67043328),
        cost_estimate=pl.CostEstimate(flops=18 * dots, bytes_accessed=64 * 16 * t * m, transcendentals=16 * t * f),
        name="group_step",
    )(ids, xm, w1, w2, gain, d_out)


def lookup_kernel(shard_rows, ids_smem, ids_vmem, table, out_hbm, got, rows, sem, out_sem):
    total, m = out_hbm.shape
    t = total // 4
    per = 32
    chunks = total // per
    r = lax.axis_index("tensor")
    spread = (1 << (shard_rows.bit_length() - 1)) - 1

    def fetch(k):
        def some(j, carry):
            for u in range(8):
                p = k * per + j * 8 + u
                row = ids_smem[jnp.right_shift(p, 7), p & (LANES - 1)]
                near = row - r * shard_rows
                near = jnp.where((near >= 0) & (near < shard_rows), near, row & spread)
                pltpu.make_async_copy(table.at[jnp.right_shift(near, 3)], got.at[p], sem.at[k]).start()
            return carry

        lax.fori_loop(0, per // 8, some, 0)

    loop(0, chunks, fetch)
    spot = lax.broadcasted_iota(I32, (per, 8 * per), 1)
    token = lax.broadcasted_iota(I32, (per, 8 * per), 0)
    same = lax.broadcasted_iota(I32, (LANES, LANES), 0) == lax.broadcasted_iota(I32, (LANES, LANES), 1)

    def line(b):
        ids = ids_vmem[pl.ds(b, 1), :].astype(F32)
        col = jnp.sum(jnp.where(same, jnp.broadcast_to(ids, (LANES, LANES)), 0.0), axis=1, keepdims=True).astype(I32)
        row = col - r * shard_rows
        row = jnp.where((row >= 0) & (row < shard_rows), row & 7, -8 * per)
        for j in range(LANES // per):
            k = b * (LANES // per) + j
            at = pl.ds(pl.multiple_of(k * per, per), per)
            pltpu.make_async_copy(got.at[at], got.at[at], sem.at[k]).wait()
            want = row[j * per : (j + 1) * per] + 8 * token
            chosen = jnp.where(want == spot, 1.0, 0.0).astype(BF16)
            picked = jnp.dot(chosen, got[at].reshape(8 * per, m), preferred_element_type=F32)
            p = k * per
            nat = lax.div(p, t)
            to = pl.multiple_of(lax.rem(nat, 2) * (2 * t) + lax.div(nat, 2) * t + lax.rem(p, t), per)
            rows[pl.ds(to, per), :] = picked.astype(BF16)
            pltpu.make_async_copy(rows.at[pl.ds(to, per)], out_hbm.at[pl.ds(to, per)], out_sem).start()

    loop(0, total // LANES, line)
    pltpu.make_async_copy(rows, out_hbm, out_sem).wait()


def look_up(ids, table):
    shard_rows, m = table.shape
    total = ids.size
    any_ = pl.BlockSpec(memory_space=pl.ANY)
    return pl.pallas_call(
        functools.partial(lookup_kernel, shard_rows),
        out_shape=jax.ShapeDtypeStruct((total, m), BF16),
        in_specs=[pl.BlockSpec(memory_space=pltpu.SMEM), pl.BlockSpec(memory_space=pltpu.VMEM), any_],
        out_specs=any_,
        scratch_shapes=[
            pltpu.VMEM((total, 8, m), BF16), pltpu.VMEM((total, m), BF16),
            pltpu.SemaphoreType.DMA((total // 32,)), pltpu.SemaphoreType.DMA,
        ],
        compiler_params=pltpu.CompilerParams(vmem_limit_bytes=60 << 20),
        cost_estimate=pl.CostEstimate(flops=16 * total * m, bytes_accessed=20 * total * m, transcendentals=0),
        name="look_up",
    )(ids, ids, table.reshape(shard_rows // 8, 8, m))


RING = 6


def weights_kernel(p1, p2, nk_in, dk_in, hk_in, duk_in, o1, o2, b1, b2, nk, dk, hk, duk, in_sem, out_sem, k_sem):
    m, f = b1.shape
    tw = nk.shape[0] // 2
    ins = [pltpu.make_async_copy(a, b, k_sem.at[i]) for i, (a, b) in enumerate(((nk_in, nk), (duk_in, duk), (hk_in, hk), (dk_in, dk)))]
    for cp in ins[:2]:
        cp.start()

    def part(src, buf, dst, first, i, rows=tw):
        at = pl.ds(pl.multiple_of(i * tw, 8), rows)
        fetch = pltpu.make_async_copy(src.at[at], buf.at[at], in_sem.at[first + i])
        return fetch, pltpu.make_async_copy(buf.at[at], dst.at[at], out_sem)

    def fetch_all(src, buf, dst, first):
        loop(0, src.shape[0] // tw, lambda i: part(src, buf, dst, first, i)[0].start())

    n1, n2 = m // tw, f // tw
    fetch_all(p1, b1, o1, 0)
    for cp in ins[2:]:
        cp.start()
    fetch_all(p2, b2, o2, n1)
    rest = [part(p2, b2, o2, n1, n2, f % tw)] if f % tw else []
    for come, _ in rest:
        come.start()

    def add(src, buf, dst, first, lhs, rhs, i, rows=tw):
        come, go = part(src, buf, dst, first, i, rows)
        come.wait()
        cols = pl.ds(pl.multiple_of(i * tw, tw), rows)
        buf[cols, :] += lax.dot_general(lhs[:, cols], rhs[...], TN, preferred_element_type=F32)
        go.start()

    for cp in ins[:2]:
        cp.wait()
    loop(0, n1, lambda i: add(p1, b1, o1, 0, nk, duk, i))
    for cp in ins[2:]:
        cp.wait()
    loop(0, n2, lambda i: add(p2, b2, o2, n1, hk, dk, i))
    if rest:
        add(p2, b2, o2, n1, hk, dk, n2, f % tw)
    pltpu.make_async_copy(b1, o1, out_sem).wait()
    pltpu.make_async_copy(b2, o2, out_sem).wait()


def finish_weights(p1, p2, nk, dk, hk, duk):
    any_ = pl.BlockSpec(memory_space=pl.ANY)
    V, S = pltpu.VMEM, pltpu.SemaphoreType.DMA
    arrays = (p1, p2, nk, dk, hk, duk)
    return pl.pallas_call(
        weights_kernel,
        out_shape=(jax.ShapeDtypeStruct(p1.shape, F32), jax.ShapeDtypeStruct(p2.shape, F32)),
        in_specs=[any_] * 6,
        out_specs=[any_] * 2,
        scratch_shapes=[*[V(a.shape, a.dtype) for a in arrays], S((32,)), S, S((4,))],
        compiler_params=pltpu.CompilerParams(vmem_limit_bytes=60 << 20),
        cost_estimate=pl.CostEstimate(flops=8000 * p1.size, bytes_accessed=20 * p1.size, transcendentals=0),
        name="finish_weights",
    )(*arrays)


def table_kernel(tall, key_ref, first_ref, dx_in, far_own, far_across, far_partner, far_both, out_hbm, dxb, dxf, ring, dx_sem, t_sem):
    count, _ = dxb.shape
    t = count // 16
    shift = count.bit_length() - 1
    steps = out_hbm.shape[0] // tall
    z, r = lax.axis_index("data"), lax.axis_index("tensor")
    y, c = lax.div(r, 2), lax.rem(r, 2)
    late = lax.div(z, 2)

    def near(k):
        at = pl.ds(pl.multiple_of(late * (4 * t) + k * (2 * t), t), 2 * t)
        return at, pltpu.make_async_copy(dx_in.at[at], dxb.at[at], dx_sem.at[k])

    def far(cc, yy):
        return pl.multiple_of((1 - late) * (12 * t) + cc * (2 * t) + yy * t, t)

    def second(cc, yy):
        return pl.multiple_of((2 - late) * (4 * t) + cc * (2 * t) + yy * t + t // 2, t // 2)

    loop(0, 6, lambda k: near(k)[1].start())
    fars = ((far_own, c, y), (far_across, c, 1 - y), (far_partner, 1 - c, y), (far_both, 1 - c, 1 - y))

    def widen_from(src, begin, to, rows):
        def widen(i):
            dxf[pl.ds(to + i, 16), :] = src[pl.ds(begin + i, 16), :].astype(F32)

        rows_loop(rows, widen)

    for src, cc, yy in fars:
        widen_from(src, 0, far(cc, yy), t)

    def widen_piece(at, cp):
        cp.wait()

        def widen(i):
            rows = pl.ds(pl.multiple_of(at.start + i, 16), 16)
            dxf[rows, :] = dxb[rows, :].astype(F32)

        rows_loop(at.size, widen)

    loop(0, 6, lambda k: widen_piece(*near(k)))
    for src, cc, yy in fars:
        widen_from(src, t, second(cc, yy), t // 2)

    def tile_out(i):
        slot = lax.rem(i, RING)
        return pltpu.make_async_copy(ring.at[slot], out_hbm.at[pl.ds(pl.multiple_of(i * tall, 8), tall)], t_sem.at[slot])

    def tile(i):
        slot = lax.rem(i, RING)
        here = ring.at[slot]
        pl.when(i >= RING)(lambda: tile_out(i - RING).wait())
        here[...] = jnp.zeros_like(here)

        def add(j, key):
            ahead = key_ref[jnp.minimum(j + 1, count - 1)]
            to = pl.ds(jnp.right_shift(key, shift) - i * tall, 1)
            here[to, :] += dxf[pl.ds(key & (count - 1), 1), :]
            return ahead

        low = first_ref[i]
        lax.fori_loop(low, first_ref[i + 1], add, key_ref[jnp.minimum(low, count - 1)])
        tile_out(i).start()

    loop(0, steps, tile)
    loop(steps - RING, steps, lambda i: tile_out(i).wait())


def table_grad(ordered, first, dx_all, fars, shard_rows, tall):
    count, m = dx_all.shape
    any_ = pl.BlockSpec(memory_space=pl.ANY)
    V, S = pltpu.VMEM, pltpu.SemaphoreType.DMA
    return pl.pallas_call(
        functools.partial(table_kernel, tall),
        out_shape=jax.ShapeDtypeStruct((shard_rows, m), F32),
        grid_spec=pltpu.PrefetchScalarGridSpec(
            num_scalar_prefetch=2,
            grid=(1,),
            in_specs=[any_, *[pl.BlockSpec(memory_space=pltpu.VMEM)] * 4],
            out_specs=any_,
            scratch_shapes=[
                V((count, m), BF16), V((count, m), F32), V((RING, tall, m), F32), S((6,)), S((RING,)),
            ],
        ),
        compiler_params=pltpu.CompilerParams(vmem_limit_bytes=44 << 20),
        cost_estimate=pl.CostEstimate(flops=16000 * shard_rows * m // 10, bytes_accessed=4 * shard_rows * m, transcendentals=0),
        name="table_grad",
    )(ordered, first, dx_all, *fars)


def solution(mesh):
    tok_spec = P(("pod", "data", "tensor"), None)

    over_y, over_core = [(0, 2), (1, 3), (2, 0), (3, 1)], [(0, 1), (1, 0), (2, 3), (3, 2)]

    def per_device(token_ids, embed_table, norm_gain, w_in, w_out, d_out):
        shard_rows = embed_table.shape[0]
        tall = next(k for k in (160, 8) if shard_rows % k == 0)
        ids = token_ids.reshape(-1, LANES)
        masked = look_up(ids, embed_table)
        gain = norm_gain.reshape(-1, LANES)
        base, ysum, ordered, first, dx_all, far, *weights = run_group(
            ids, masked, w_in, w_out, gain, d_out, shard_rows, tall
        )
        far_x = lax.ppermute(far, "tensor", over_y)
        far_p = lax.ppermute(far, "tensor", over_core)
        other = lax.ppermute(ysum, "tensor", over_y)
        grad_w_in, grad_w_out = finish_weights(*weights)
        far_b = lax.ppermute(far_x, "tensor", over_core)
        fars = (far, far_x, far_p, far_b)
        grad_table = table_grad(ordered.reshape(-1), first.reshape(-1), dx_all, fars, shard_rows, tall)
        return (base + other).astype(BF16), grad_table, grad_w_in, grad_w_out

    return jax.shard_map(
        per_device,
        mesh=mesh,
        in_specs=(P(("pod", "data")), P("tensor", None), P(None), P(None, "tensor"), P("tensor", None), tok_spec),
        out_specs=(tok_spec, P(("pod", "tensor"), None), P("pod", "tensor"), P(("pod", "tensor"), None)),
        check_vma=False,
    )
```
